32 devices in a mesh: groups: 2 (over x), head: 8 (over z, y), batch: 2 (over core).
Axes of the slice: x: 2, y: 2, z: 4, core: 2. Of those that a mesh axis runs over, the one named last changes fastest.
Arguments:
- latent_rows: bfloat16 [4096, 576], P(('groups', 'batch', 'head')), parts along dimension 0, may hold values from -6 to 6
- pre_queries: bfloat16 [4096, 128, 192], P(('groups', 'batch'), 'head'), parts along dimension 0, may hold values from -270 to 270
- pre_lengths: int32 [4, 4], P('groups'), parts along dimension 0, may hold values from 1 to 512, 1024 in all within a row
- owner_map: int32 [4, 4], P('groups'), parts along dimension 0, may hold values from 0 to 31, as said below
- context_cache: bfloat16 [64, 4096, 576], P(('groups', 'batch', 'head')), parts along dimension 0, may hold values from -6 to 6
- context_lengths: int32 [64], P(('groups', 'batch', 'head')), parts along dimension 0, may hold values from 1 to 4096, 65536 in all
- new_latent: bfloat16 [4, 32, 576], P('groups', ('batch', 'head')), parts along dimension 0, may hold values from -6 to 6
- dec_queries: bfloat16 [4, 32, 128, 192], P('groups', 'batch', 'head'), parts along dimension 0, may hold values from -270 to 270
- key_weight: bfloat16 [512, 16384], P(None, 'head'), may hold values from -0.25 to 0.25
- value_weight: bfloat16 [512, 16384], P(None, 'head'), may hold values from -0.25 to 0.25
Outputs:
- prefill_out: bfloat16 [4096, 16384], P(('groups', 'batch'), 'head'), parts along dimension 0
- decode_out: bfloat16 [4, 32, 16384], P('groups', 'batch', 'head'), parts along dimension 0
The draws below stay inside these ranges and needn't reach their ends.
There are 2 independent parts, one for each index of `groups`. The reference program is written for one: setup_inputs(seed, part) draws one part's arguments, and reference() takes and returns one part's arrays. A program takes and returns all parts, laid end to end along the dimension named above; an argument that names none is the same for every part. Nothing has to cross between parts.
Inputs may be any that keep to these rules, and one draw needn't show every extreme that they name: `owner_map`: the entries are distinct decode requests.
All inputs are finite; a program needn't handle non-finite values. No bound on the sum of `context_lengths` on one device may be relied on, other than what follows from the above.
Results may differ from the reference program's by a relative error of at most 0.0061.
Values may be sent and summed in bfloat16 or wider, within the bound.
A program may use at most 192 MiB of HBM per device.

```python
import math
import jax
import jax.numpy as jnp
import numpy as np
from jax import lax

H = 128
HD = 128
ROPE = 64
LAT = 512
KV = 576
PRE = 1024
SEGS = 4
PMOST = 512
CTX = 4096
STEPS = 2
SPANS = 2
REQS = 32


def clipped_normal(key, salt, shape):
    return jnp.clip(jax.random.normal(jax.random.fold_in(key, salt), shape, jnp.float32), -6.0, 6.0)


def draw_latent_rows(key, part):
    latent = clipped_normal(key, 11, (SPANS * PRE, LAT))
    rope_part = clipped_normal(key, 12, (SPANS * PRE, ROPE))
    return jnp.concatenate([latent, rope_part], axis=1).astype(jnp.bfloat16)


def draw_pre_queries(key, part):
    drawn_part = clipped_normal(key, 13, (SPANS * PRE, H, HD))
    rope_part = clipped_normal(key, 14, (SPANS * PRE, H, ROPE))
    return jnp.concatenate([drawn_part, rope_part], axis=2).astype(jnp.bfloat16)


def draw_new_latent(key, part):
    latent = clipped_normal(key, 21, (STEPS, REQS, LAT))
    rope_part = clipped_normal(key, 22, (STEPS, REQS, ROPE))
    return jnp.concatenate([latent, rope_part], axis=2).astype(jnp.bfloat16)


def draw_dec_queries(key, part):
    drawn_part = clipped_normal(key, 23, (STEPS, REQS, H, HD))
    rope_part = clipped_normal(key, 24, (STEPS, REQS, H, ROPE))
    return jnp.concatenate([drawn_part, rope_part], axis=3).astype(jnp.bfloat16)


def draw_owner_map(key, part):
    middle = jax.random.permutation(jax.random.fold_in(key, 31), REQS - 2) + 1
    picked = jnp.concatenate([middle[:SPANS * SEGS - 2], jnp.array([0, REQS - 1], jnp.int32)]).astype(jnp.int32)
    order = jax.random.permutation(jax.random.fold_in(key, 32), SPANS * SEGS)
    return picked[order].reshape(SPANS, SEGS).astype(jnp.int32)


def level_of(rng, extent, split, smallest, top_value):
    level = 1.0
    for axis_at, parts in split:
        steps = jax.random.uniform(jax.random.fold_in(jax.random.fold_in(rng, 6), axis_at), (parts,), jnp.float32, smallest / len(split), top_value / len(split))
        level = level * jnp.repeat(jnp.exp(steps), extent[axis_at] // parts).reshape((-1,) + (1,) * (len(extent) - 1 - axis_at))
    return level


def split_up(number_of, total, limit, slope):
    weights = [(1 << 20) // math.isqrt(standing ** slope) + 1 for standing in range(2, number_of + 1)]
    rest, given = total - limit - (number_of - 1), [1] * (number_of - 1)
    while rest > 0:
        movable = [i for i in range(number_of - 1) if given[i] < limit]
        mass, budget = sum([weights[i] for i in movable]), rest
        for i in movable:
            more = min(limit - given[i], max(1, budget * weights[i] // mass), rest)
            given[i] = given[i] + more
            rest = rest - more
    return np.array([limit] + given)


def uneven(stream_key, count, total, reach, skew):
    if count == 2:
        one = jax.random.randint(stream_key, (), max(1, total - reach), min(reach, total - 1) + 1)
        return jnp.stack([one, total - one])
    lengths = jnp.asarray(split_up(count, total, reach, skew), jnp.int32)
    pairs = (count - 1) // 2
    giver, taker = lengths[1:1 + 2 * pairs:2], lengths[2:2 + 2 * pairs:2]
    room = jnp.minimum(giver - 1, reach - taker)
    passed = jax.random.randint(jax.random.fold_in(stream_key, 1), (pairs,), 0, 1 << 20) % (room + 1)
    lengths = lengths.at[1:1 + 2 * pairs:2].set(giver - passed).at[2:2 + 2 * pairs:2].set(taker + passed)
    return lengths[jax.random.permutation(jax.random.fold_in(stream_key, 2), count)]


def bell_draw(key, dims, deviation, most, split=(), kind=jnp.bfloat16):
    values = deviation * jax.random.normal(key, dims, jnp.float32)
    if split:
        values = values * level_of(key, dims, split, -0.22, 0.18)
    return jnp.clip(values, -most, most).astype(kind)


def setup_inputs(seed: int = 0, part: int = 0) -> dict:
    splits = jax.random.split(jax.random.key(seed), 11)
    part_keys = jax.random.split(jax.random.fold_in(splits[10], part), 11)
    latent_rows = draw_latent_rows(jax.random.fold_in(jax.random.fold_in(splits[10], part), 71), part)
    pre_queries = draw_pre_queries(jax.random.fold_in(jax.random.fold_in(splits[10], part), 71), part)
    pre_lengths = jax.vmap(lambda own: uneven(own, SEGS, PRE, PMOST, 1))(jax.random.split(part_keys[2], SPANS)).reshape((SPANS, SEGS)).astype(jnp.int32)
    owner_map = draw_owner_map(jax.random.fold_in(jax.random.fold_in(splits[10], part), 71), part)
    context_cache = bell_draw(part_keys[4], (REQS, CTX, KV), 1.0, 6.0, ((0, 16),))
    context_lengths = uneven(part_keys[5], REQS, REQS * CTX // 2, CTX, 2).astype(jnp.int32)
    new_latent = draw_new_latent(jax.random.fold_in(jax.random.fold_in(splits[10], part), 71), part)
    dec_queries = draw_dec_queries(jax.random.fold_in(jax.random.fold_in(splits[10], part), 71), part)
    key_weight = bell_draw(splits[8], (LAT, H * HD), LAT ** -0.5, 0.25, ((1, 8),))
    value_weight = bell_draw(splits[9], (LAT, H * HD), LAT ** -0.5, 0.25, ((1, 8),))
    return dict(latent_rows=latent_rows, pre_queries=pre_queries, pre_lengths=pre_lengths, owner_map=owner_map, context_cache=context_cache, context_lengths=context_lengths, new_latent=new_latent, dec_queries=dec_queries, key_weight=key_weight, value_weight=value_weight)


NEGATIVE = -1e+30

def request_table(pre_lengths, owner_map, span_len):
    seg_ends = jnp.cumsum(pre_lengths, axis=1)
    span_base = jnp.arange(pre_lengths.shape[0], dtype=jnp.int32)[:, None] * span_len
    seg_starts = seg_ends - pre_lengths + span_base
    return (owner_map.reshape(-1), seg_starts.reshape(-1), pre_lengths.reshape(-1))

def span_attention(span_rows, span_queries, span_lengths, key_weight, value_weight):
    score_scale = 1.0 / math.sqrt(HD + ROPE)
    seg_ends = jnp.cumsum(span_lengths)
    places = jnp.arange(PRE, dtype=jnp.int32)
    segment = lax.optimization_barrier(jnp.sum((places[:, None] >= seg_ends[None, :]).astype(jnp.int32), axis=1))
    allowed = (segment[:, None] == segment[None, :]) & (places[None, :] <= places[:, None])
    latent = span_rows[:, :LAT]
    rope_keys = span_rows[:, LAT:]

    def one_head(head_index):
        column = head_index * HD
        key_cols = lax.dynamic_slice_in_dim(key_weight, column, HD, 1)
        value_cols = lax.dynamic_slice_in_dim(value_weight, column, HD, 1)
        keys_nope = jnp.dot(latent, key_cols, preferred_element_type=jnp.float32).astype(jnp.bfloat16)
        values = jnp.dot(latent, value_cols, preferred_element_type=jnp.float32).astype(jnp.bfloat16)
        key_rows = jnp.concatenate([keys_nope, rope_keys], axis=1)
        queries = lax.dynamic_index_in_dim(span_queries, head_index, 1, keepdims=False)
        scores = jnp.dot(queries, key_rows.T, preferred_element_type=jnp.float32) * score_scale
        masked = jnp.where(allowed, scores, NEGATIVE)
        peak_score = lax.optimization_barrier(jnp.max(masked, axis=1, keepdims=True))
        weights = jnp.exp(masked - peak_score)
        weight_sum = lax.optimization_barrier(jnp.sum(weights, axis=1, keepdims=True))
        mixed_out = jnp.dot(weights.astype(jnp.bfloat16), values, preferred_element_type=jnp.float32) / weight_sum
        return mixed_out.astype(jnp.bfloat16)
    per_head = lax.map(one_head, jnp.arange(H, dtype=jnp.int32))
    return jnp.transpose(per_head, (1, 0, 2)).reshape(PRE, H * HD)

def reference(latent_rows, pre_queries, pre_lengths, owner_map, context_cache, context_lengths, new_latent, dec_queries, key_weight, value_weight):
    pieces = []
    for span in range(SPANS):
        pieces.append(span_attention(latent_rows[span * PRE:(span + 1) * PRE], pre_queries[span * PRE:(span + 1) * PRE], pre_lengths[span], key_weight, value_weight))
    prefill_out = jnp.concatenate(pieces, axis=0)
    flat_owner, flat_start, flat_length = request_table(pre_lengths, owner_map, PRE)
    row_ids = jnp.arange(REQS, dtype=jnp.int32)
    matches = (flat_owner[None, :] == row_ids[:, None]).astype(jnp.int32)
    is_target = lax.optimization_barrier(jnp.sum(matches, axis=1)) > 0
    first_row = lax.optimization_barrier(jnp.sum(matches * flat_start[None, :], axis=1)).astype(jnp.int32)
    prompt_len = lax.optimization_barrier(jnp.sum(matches * flat_length[None, :], axis=1))
    effective = jnp.where(is_target, prompt_len, context_lengths).astype(jnp.int32)
    padded = jnp.concatenate([latent_rows, jnp.zeros((PRE, KV), latent_rows.dtype)], axis=0)
    key_heads = key_weight.reshape(LAT, H, HD)
    value_heads = value_weight.reshape(LAT, H, HD)
    absorbed = jnp.einsum('srhd,lhd->srhl', dec_queries[..., :HD].astype(jnp.float32), key_heads.astype(jnp.float32)).astype(jnp.bfloat16)
    query_all = jnp.concatenate([absorbed, dec_queries[..., HD:]], axis=3)
    score_scale = 1.0 / math.sqrt(HD + ROPE)

    def one_row(entry):
        row_query, cache_rows, fresh_rows, row_length, row_target, row_first = entry
        replaced = lax.dynamic_slice_in_dim(padded, row_first, PRE, 0)
        front_rows = jnp.where(row_target, replaced, cache_rows[:PRE])
        key_rows = jnp.concatenate([front_rows, cache_rows[PRE:], fresh_rows], axis=0)
        flat_query = row_query.reshape(STEPS * H, KV)
        scores = jnp.dot(flat_query, key_rows.T, preferred_element_type=jnp.float32) * score_scale
        places = jnp.arange(CTX + STEPS, dtype=jnp.int32)
        step_of = jnp.arange(STEPS * H, dtype=jnp.int32) // H
        allowed = jnp.where(places[None, :] < CTX, places[None, :] < row_length, places[None, :] - CTX <= step_of[:, None])
        masked = jnp.where(allowed, scores, NEGATIVE)
        peak_score = lax.optimization_barrier(jnp.max(masked, axis=1, keepdims=True))
        weights = jnp.exp(masked - peak_score)
        weight_sum = lax.optimization_barrier(jnp.sum(weights, axis=1, keepdims=True))
        mixed_out = jnp.dot(weights.astype(jnp.bfloat16), key_rows[:, :LAT], preferred_element_type=jnp.float32) / weight_sum
        return mixed_out.astype(jnp.bfloat16).reshape(STEPS, H, LAT)
    latent_out = lax.map(one_row, (jnp.transpose(query_all, (1, 0, 2, 3)), context_cache, jnp.transpose(new_latent, (1, 0, 2)), effective, is_target, first_row))
    decode_out = jnp.einsum('rshl,lhd->srhd', latent_out.astype(jnp.float32), value_heads.astype(jnp.float32)).astype(jnp.bfloat16)
    return (prefill_out, decode_out.reshape(STEPS, REQS, H * HD))
```

```python
import functools
import math

import jax
import jax.numpy as jnp
from jax import lax
from jax.experimental import pallas as pl
from jax.experimental.pallas import tpu as pltpu
from jax.sharding import PartitionSpec as P

BLK = 512


NEGATIVE = -1e30


def from_partner(value, axis, distance):
    mask = 2**distance
    pairs = [(source, source ^ mask) for source in range(lax.axis_size(axis))]
    return lax.ppermute(value, axis, pairs)


def request_table(pre_lengths, owner_map, span_len):
    seg_ends = jnp.cumsum(pre_lengths, axis=1)
    span_base = jnp.arange(pre_lengths.shape[0], dtype=jnp.int32)[:, None] * span_len
    seg_starts = seg_ends - pre_lengths + span_base
    return (owner_map.reshape(-1), seg_starts.reshape(-1), pre_lengths.reshape(-1))


def prefill_heads(own_span, queries, span_lengths, key_weight, value_weight):
    span_len, head_count, query_width = queries.shape
    head_size = key_weight.shape[1] // head_count
    lat_width = key_weight.shape[0]
    score_scale = 1.0 / math.sqrt(query_width)
    latent = own_span[:, :lat_width]
    rope_keys = own_span[:, lat_width:]
    keys_nope = (
        jnp.dot(latent, key_weight, preferred_element_type=jnp.float32)
        .astype(jnp.bfloat16)
        .reshape(span_len, head_count, head_size)
    )
    values = (
        jnp.dot(latent, value_weight, preferred_element_type=jnp.float32)
        .astype(jnp.bfloat16)
        .reshape(span_len, head_count, head_size)
    )
    scores = jnp.einsum(
        "qhd,khd->hqk", queries[:, :, :head_size], keys_nope, preferred_element_type=jnp.float32
    )
    scores = scores + jnp.einsum(
        "qhr,kr->hqk", queries[:, :, head_size:], rope_keys, preferred_element_type=jnp.float32
    )
    scores = scores * score_scale
    seg_ends = jnp.cumsum(span_lengths)
    places = jnp.arange(span_len, dtype=jnp.int32)
    segment = jnp.sum((places[:, None] >= seg_ends[None, :]).astype(jnp.int32), axis=1)
    allowed = (segment[:, None] == segment[None, :]) & (places[None, :] <= places[:, None])
    masked = jnp.where(allowed[None], scores, NEGATIVE)
    peak_score = jnp.max(masked, axis=2, keepdims=True)
    weights = jnp.exp(masked - peak_score)
    weight_sum = jnp.sum(weights, axis=2)
    mixed_out = jnp.einsum(
        "hqk,khd->qhd", weights.astype(jnp.bfloat16), values, preferred_element_type=jnp.float32
    )
    mixed_out = mixed_out / jnp.transpose(weight_sum)[:, :, None]
    return mixed_out.astype(jnp.bfloat16).reshape(span_len, head_count * head_size)


def plain_on_device(
    latent_rows,
    pre_queries,
    pre_lengths,
    owner_map,
    context_cache,
    context_lengths,
    new_latent,
    dec_queries,
    key_weight,
    value_weight,
):
    head_rank = lax.axis_index("head")
    batch_rank = lax.axis_index("batch")
    span_len = pre_queries.shape[0]
    kv_width = latent_rows.shape[1]
    own_span = lax.all_gather(latent_rows, "head", axis=0, tiled=True)
    other_span = from_partner(own_span, "batch", 0)
    first_span = jnp.where(batch_rank == 0, own_span, other_span)
    second_span = jnp.where(batch_rank == 0, other_span, own_span)
    all_spans = jnp.concatenate([first_span, second_span], axis=0)
    span_lengths = lax.dynamic_index_in_dim(pre_lengths, batch_rank, 0, keepdims=False)
    prefill_out = prefill_heads(own_span, pre_queries, span_lengths, key_weight, value_weight)
    step_total, rows_local, head_count, query_width = dec_queries.shape
    lat_width = key_weight.shape[0]
    head_size = key_weight.shape[1] // head_count
    owned_rows = context_cache.shape[0]
    score_scale = 1.0 / math.sqrt(query_width)
    key_heads = key_weight.reshape(lat_width, head_count, head_size)
    value_heads = value_weight.reshape(lat_width, head_count, head_size)
    absorbed = jnp.einsum(
        "srhd,lhd->srhl",
        dec_queries[..., :head_size],
        key_heads,
        preferred_element_type=jnp.float32,
    ).astype(jnp.bfloat16)
    query_all = jnp.concatenate([absorbed, dec_queries[..., head_size:]], axis=3)
    flat_owner, flat_start, flat_length = request_table(pre_lengths, owner_map, span_len)
    row_ids = (
        batch_rank * rows_local + head_rank * owned_rows + jnp.arange(owned_rows, dtype=jnp.int32)
    )
    matches = (flat_owner[None, :] == row_ids[:, None]).astype(jnp.int32)
    is_target = jnp.sum(matches, axis=1) > 0
    first_row = jnp.sum(matches * flat_start[None, :], axis=1)
    prompt_len = jnp.sum(matches * flat_length[None, :], axis=1)
    effective = jnp.where(is_target, prompt_len, context_lengths)
    padded = jnp.concatenate([all_spans, jnp.zeros((span_len, kv_width), all_spans.dtype)], axis=0)
    replaced = jax.vmap(lambda offset: lax.dynamic_slice_in_dim(padded, offset, span_len, 0))(
        first_row
    )
    front_rows = jnp.where(is_target[:, None, None], replaced, context_cache[:, :span_len])
    front_blocks = span_len // BLK
    needed = (jnp.max(effective) + BLK - 1) // BLK
    fresh_latent = new_latent[..., :lat_width]
    owned_query = lax.all_to_all(query_all, "head", split_axis=1, concat_axis=2, tiled=True)
    fresh_scores = (
        jnp.einsum("srhk,jrk->srhj", owned_query, new_latent, preferred_element_type=jnp.float32)
        * score_scale
    )
    visible = (
        jnp.arange(new_latent.shape[0], dtype=jnp.int32)[None, :]
        <= jnp.arange(step_total, dtype=jnp.int32)[:, None]
    )
    fresh_scores = jnp.where(visible[:, None, None, :], fresh_scores, NEGATIVE)
    peak_score = jnp.max(fresh_scores, axis=3)
    weights = jnp.exp(fresh_scores - peak_score[..., None])
    weight_sum = jnp.sum(weights, axis=3)
    running = jnp.einsum(
        "srhj,jrl->srhl",
        weights.astype(jnp.bfloat16),
        fresh_latent,
        preferred_element_type=jnp.float32,
    )

    def advance(block_index, state_tuple, source):
        old_peak, old_sum, old_running = state_tuple
        key_block = lax.dynamic_slice_in_dim(source, block_index * BLK, BLK, 1)
        scores = (
            jnp.einsum("srhk,rtk->srht", owned_query, key_block, preferred_element_type=jnp.float32)
            * score_scale
        )
        places = block_index * BLK + jnp.arange(BLK, dtype=jnp.int32)
        in_context = places[None, :] < effective[:, None]
        scores = jnp.where(in_context[None, :, None, :], scores, NEGATIVE)
        new_peak = jnp.maximum(old_peak, jnp.max(scores, axis=3))
        factor = jnp.exp(old_peak - new_peak)
        block_weights = jnp.exp(scores - new_peak[..., None])
        new_sum = old_sum * factor + jnp.sum(block_weights, axis=3)
        new_running = old_running * factor[..., None] + jnp.einsum(
            "srht,rtl->srhl",
            block_weights.astype(jnp.bfloat16),
            key_block[..., :lat_width],
            preferred_element_type=jnp.float32,
        )
        return (new_peak, new_sum, new_running)

    state_tuple = lax.fori_loop(
        0,
        jnp.minimum(needed, front_blocks),
        lambda block_index, state_now: advance(block_index, state_now, front_rows),
        (peak_score, weight_sum, running),
    )
    state_tuple = lax.fori_loop(
        front_blocks,
        jnp.maximum(needed, front_blocks),
        lambda block_index, state_now: advance(block_index, state_now, context_cache),
        state_tuple,
    )
    latent_out = (state_tuple[2] / state_tuple[1][..., None]).astype(jnp.bfloat16)
    returned = lax.all_to_all(latent_out, "head", split_axis=2, concat_axis=1, tiled=True)
    projected = jnp.einsum(
        "srhl,lhd->srhd", returned, value_heads, preferred_element_type=jnp.float32
    ).astype(jnp.bfloat16)
    decode_out = projected.reshape(query_all.shape[0], rows_local, head_count * head_size)
    return (prefill_out, decode_out)


def trans_dot(left, right):
    return lax.dot_general(
        left, right, (((1,), (1,)), ((), ())), preferred_element_type=jnp.float32
    )


MESH = pl.DeviceIdType.MESH


def place_of(rank, ranks):
    odd = rank % 2
    return (1 - odd) * (rank // 2) + odd * (ranks - 1 - rank // 2)


def rank_at(place, ranks):
    late = place // (ranks // 2)
    return (1 - late) * (2 * place) + late * (2 * (ranks - 1 - place) + 1)


def start_marks(ends, keys, vals, hot, tri, rows_ref, lat):
    pair, span_len, _ = keys.shape
    segs = len(ends)
    marks = keys.shape[2] - 128 - (rows_ref.shape[1] - lat)
    where = lax.broadcasted_iota(jnp.int32, (span_len, marks), 0)
    lane = lax.broadcasted_iota(jnp.int32, (span_len, marks), 1)
    place = lax.broadcasted_iota(jnp.int32, (marks, span_len), 1)
    line = lax.broadcasted_iota(jnp.int32, (marks, span_len), 0)
    mine = jnp.zeros((span_len, marks), jnp.int32)
    seen = jnp.zeros((marks, span_len), jnp.int32)
    for k in range(segs - 1):
        mine = mine + (where >= ends[k]).astype(jnp.int32)
        seen = seen + (place >= ends[k]).astype(jnp.int32)
    mark = jnp.where((lane < segs) & (lane != mine), NEGATIVE, 0.0).astype(jnp.bfloat16)
    hot[...] = jnp.where(line == seen, 1.0, 0.0).astype(jnp.bfloat16)
    for p in range(pair):
        keys[p, :, 128 : keys.shape[2] - marks] = rows_ref[:, lat:]
        keys[p, :, keys.shape[2] - marks :] = mark
        vals[p, 128:, :] = jnp.ones((vals.shape[1] - 128, span_len), jnp.bfloat16)
    size = tri.shape[0]
    key_at = lax.broadcasted_iota(jnp.int32, (size, size), 0)
    query_at = lax.broadcasted_iota(jnp.int32, (size, size), 1)
    tri[...] = jnp.where(key_at <= query_at, 0.0, NEGATIVE)


def attend_pair(g, kw, vw, qs, spans_ref, rows_ref, keys, vals, hot, tri, part_ref, lat, look, scale):
    pair, span_len, _ = keys.shape
    qb = tri.shape[0]
    wide = pair * 128
    columns = pl.ds(pl.multiple_of(g * wide, wide), wide)
    made = jnp.dot(rows_ref[:, :lat], kw[:, columns], preferred_element_type=jnp.float32)
    made = made.astype(jnp.bfloat16)
    for p in range(pair):
        keys[p, :, :128] = made[:, p * 128 : (p + 1) * 128]
    turned = jnp.transpose(vw[:, columns])
    for c in range(span_len // 256):
        latents = jnp.concatenate(
            [spans_ref[2 * c, :lat, :], spans_ref[2 * c + 1, :lat, :]], axis=1
        )
        value = jnp.dot(turned, latents, preferred_element_type=jnp.float32).astype(jnp.bfloat16)
        for p in range(pair):
            vals[p, :128, c * 256 : (c + 1) * 256] = value[p * 128 : (p + 1) * 128]
    for i in range(span_len // qb):
        lo, hi = max(i - look, 0) * qb, (i + 1) * qb
        for p in range(pair):
            query = jnp.concatenate(
                [qs[g * pair + p, :, i * qb : hi], hot[:, i * qb : hi]], axis=0
            )
            s = jnp.dot(keys[p, lo:hi, :], query, preferred_element_type=jnp.float32)
            last = s[hi - lo - qb :] + tri[...]
            s = last if hi - lo == qb else jnp.concatenate([s[: hi - lo - qb], last], axis=0)
            m = jnp.max(s, axis=0, keepdims=True)
            w = jnp.exp2((s - m) * scale).astype(jnp.bfloat16)
            o = jnp.dot(vals[p, :, lo:hi], w, preferred_element_type=jnp.float32)
            o = o[:128] * (1.0 / o[128:129])
            part_ref[i * qb : hi, pl.ds(pl.multiple_of(g * wide + p * 128, 128), 128)] = (
                jnp.transpose(o.astype(jnp.bfloat16))
            )


def absorb_into(dq, kw, sent, flat, wide, heads, lat):
    rows = dq.shape[0]
    ranks, owned, block, _ = sent.shape
    steps = block // heads
    local = ranks * owned
    flat[...] = dq[:, :128].astype(jnp.float32)
    for h in range(heads):
        mine = flat[pl.ds(h, rows // heads, stride=heads), :].astype(jnp.bfloat16)
        res = trans_dot(mine, kw[:, h * 128 : (h + 1) * 128])
        for s in range(steps):
            for c in range(lat // 128):
                wide[c, pl.ds(s * heads + h, local, stride=block), :] = res[
                    s * local : (s + 1) * local, c * 128 : (c + 1) * 128
                ]
    for p in range(ranks):
        for r in range(owned):
            at = p * owned + r
            for c in range(lat // 128):
                sent[p, r, :, c * 128 : (c + 1) * 128] = wide[
                    c, at * block : (at + 1) * block
                ].astype(jnp.bfloat16)
            for s in range(steps):
                start = (s * local + at) * heads
                sent[p, r, s * heads : (s + 1) * heads, lat:] = dq[start : start + heads, 128:]


def span_ends(lens_ref, batch_rank):
    ends = []
    total = 0
    for k in range(lens_ref.shape[1]):
        total = total + lens_ref[batch_rank, k]
        ends.append(total)
    return ends


def gather_kernel(
    lens_ref, shard_hbm, dq_hbm, kw_hbm, vw_hbm, q_hbm,
    spans_ref, rows_ref, got_ref, part_ref,
    kw, vw, qs, dq, flat, wide, sent, keys, vals, hot, tri,
    load_sems, ring_send, ring_recv, swap_sems, give_sems, take_sems,
    *, lat, ranks, heads, look, scale
):
    me = lax.axis_index("head")
    batch_rank = lax.axis_index("batch")
    place = place_of(me, ranks)
    right = rank_at((place + 1) % ranks, ranks)
    left = rank_at((place + ranks - 1) % ranks, ranks)
    some = qs.shape[0]
    loads = [
        pltpu.make_async_copy(dq_hbm, dq, load_sems.at[0]),
        pltpu.make_async_copy(kw_hbm, kw, load_sems.at[1]),
        pltpu.make_async_copy(shard_hbm, spans_ref.at[me], load_sems.at[2]),
        pltpu.make_async_copy(vw_hbm.at[:, : some * 128], vw, load_sems.at[3]),
        pltpu.make_async_copy(q_hbm.at[:some], qs, load_sems.at[4]),
    ]
    barrier = pltpu.get_barrier_semaphore()
    for k in range(1, ranks):
        pl.semaphore_signal(
            barrier, inc=1, device_id={"head": (me + k) % ranks}, device_id_type=MESH
        )
    pl.semaphore_signal(
        barrier, inc=1, device_id={"batch": 1 - batch_rank}, device_id_type=MESH
    )
    for load in loads:
        load.start()
    pl.semaphore_wait(barrier, ranks)

    half = shard_hbm.shape[0] // 2
    most = ranks // 2

    def hop(way, part, t):
        back = t - 1 if way == 0 else ranks - t + 1
        origin = rank_at((place + ranks - back) % ranks, ranks)
        rows = pl.ds(part * half, half)
        source = shard_hbm.at[rows] if t == 1 else spans_ref.at[origin, rows]
        return pltpu.make_async_remote_copy(
            src_ref=source,
            dst_ref=spans_ref.at[origin, rows],
            send_sem=ring_send.at[way, part, t - 1],
            recv_sem=ring_recv.at[way, part, t - 1],
            device_id={"head": right if way == 0 else left},
            device_id_type=MESH,
        )

    def hops(way, part):
        return most if way == part else most - 1

    streams = [(0, 0), (1, 1), (0, 1), (1, 0)]
    for way, part in streams:
        hop(way, part, 1).start()
    loads[0].wait()
    loads[1].wait()
    absorb_into(dq, kw, sent, flat, wide, heads, lat)

    own = shard_hbm.shape[1]

    def turn(origin):
        rows_ref[pl.ds(pl.multiple_of(origin * own, own), own), :] = jnp.transpose(
            spans_ref[origin]
        )

    loads[2].wait()
    turn(me)
    for t in range(1, most + 1):
        for way, part in streams:
            if t <= hops(way, part):
                hop(way, part, t).wait_recv()
                if t < hops(way, part):
                    hop(way, part, t + 1).start()
        turn(rank_at((place + ranks - t) % ranks, ranks))
        if t < most:
            turn(rank_at((place + t) % ranks, ranks))

    gives = []
    for k in range(1, ranks):
        peer = (me + k) % ranks
        gives.append(
            pltpu.make_async_remote_copy(
                src_ref=sent.at[peer],
                dst_ref=got_ref.at[me],
                send_sem=give_sems.at[k - 1],
                recv_sem=take_sems.at[k - 1],
                device_id={"head": peer},
                device_id_type=MESH,
            )
        )
    for give in gives:
        give.start()
    keep = pltpu.make_async_copy(sent.at[me], got_ref.at[me], load_sems.at[5])
    keep.start()
    swap = pltpu.make_async_remote_copy(
        src_ref=spans_ref.at[:ranks],
        dst_ref=spans_ref.at[ranks:],
        send_sem=swap_sems.at[0],
        recv_sem=swap_sems.at[1],
        device_id={"batch": 1 - batch_rank},
        device_id_type=MESH,
    )
    swap.start()
    loads[3].wait()
    loads[4].wait()
    start_marks(span_ends(lens_ref, batch_rank), keys, vals, hot, tri, rows_ref, lat)

    def step(g, carry):
        attend_pair(
            g, kw, vw, qs, spans_ref, rows_ref, keys, vals, hot, tri, part_ref, lat, look, scale
        )
        return carry

    lax.fori_loop(0, some // keys.shape[0], step, 0)
    for way, part in streams:
        for t in range(1, hops(way, part) + 1):
            hop(way, part, t).wait_send()
    for give in gives:
        give.wait()
    keep.wait()
    swap.wait()


HBM_SPEC = pl.BlockSpec(memory_space=pltpu.HBM)
VMEM_SPEC = pl.BlockSpec(memory_space=pltpu.VMEM)
SMEM_SPEC = pl.BlockSpec(memory_space=pltpu.SMEM)


def attend_scratch(span_len, kv, lat, qb):
    pair = 2
    marks = 128 - (kv - lat)
    return [
        pltpu.VMEM((pair, span_len, 256), jnp.bfloat16),
        pltpu.VMEM((pair, 128 + 16, span_len), jnp.bfloat16),
        pltpu.VMEM((marks, span_len), jnp.bfloat16),
        pltpu.VMEM((qb, qb), jnp.float32),
    ]


def gather_pallas(lens, shard, flat_queries, key_weight, value_weight, turned, owned, ranks, first, qb):
    heads, width, span_len = turned.shape
    kv, own = shard.shape
    lat = key_weight.shape[0]
    rows = flat_queries.shape[0]
    block = rows // (ranks * owned)
    look = min(-(-(span_len // 2) // qb), span_len // qb - 1)
    bf16 = jnp.bfloat16
    return pl.pallas_call(
        functools.partial(
            gather_kernel,
            lat=lat,
            ranks=ranks,
            heads=heads,
            look=look,
            scale=math.log2(math.e) / math.sqrt(width),
        ),
        out_shape=(
            jax.ShapeDtypeStruct((2 * ranks, kv, own), bf16),
            jax.ShapeDtypeStruct((span_len, kv), bf16),
            jax.ShapeDtypeStruct((ranks, owned, block, kv), bf16),
            jax.ShapeDtypeStruct((span_len, first * 128), bf16),
        ),
        in_specs=[SMEM_SPEC] + [HBM_SPEC] * 5,
        out_specs=(VMEM_SPEC,) * 4,
        scratch_shapes=[
            pltpu.VMEM(key_weight.shape, bf16),
            pltpu.VMEM((lat, first * 128), bf16),
            pltpu.VMEM((first, width, span_len), bf16),
            pltpu.VMEM((rows, width), bf16),
            pltpu.VMEM((rows, 128), jnp.float32),
            pltpu.VMEM((lat // 128, rows, 128), jnp.float32),
            pltpu.VMEM((ranks, owned, block, kv), bf16),
            *attend_scratch(span_len, kv, lat, qb),
            pltpu.SemaphoreType.DMA((6,)),
            pltpu.SemaphoreType.DMA((2, 2, ranks // 2)),
            pltpu.SemaphoreType.DMA((2, 2, ranks // 2)),
            pltpu.SemaphoreType.DMA((2,)),
            pltpu.SemaphoreType.DMA((ranks - 1,)),
            pltpu.SemaphoreType.DMA((ranks - 1,)),
        ],
        compiler_params=pltpu.CompilerParams(
            collective_id=0, has_side_effects=True, vmem_limit_bytes=40 << 20
        ),
        cost_estimate=pl.CostEstimate(
            flops=12 * 10**9, bytes_accessed=12 << 20, transcendentals=6 << 20
        ),
    )(lens, shard, flat_queries, key_weight, value_weight, turned)


def decode_kernel(
    lens_ref, owner_ref, ctx_ref, q_ref, new_ref, spans_ref, part_ref, cache_ref,
    out_ref, whole_ref,
    bufs, sems, whole_sem, m_ref, l_ref, acc_ref,
    *, lat, heads, steps, blk, depth, scale, rows_local, span_len
):
    ranks, owned, block, kv = q_ref.shape
    rows = ranks * block
    batch_rank = lax.axis_index("batch")
    me = lax.axis_index("head")
    shown = pltpu.make_async_copy(
        part_ref, whole_ref.at[:, : part_ref.shape[1]], whole_sem.at[0]
    )
    shown.start()
    facts = []
    for r in range(owned):
        row = batch_rank * rows_local + me * owned + r
        target = jnp.int32(0)
        first = jnp.int32(0)
        length = jnp.int32(0)
        for c in range(lens_ref.shape[0]):
            start = jnp.int32(c * span_len)
            for k in range(lens_ref.shape[1]):
                hit = (owner_ref[c, k] == row).astype(jnp.int32)
                target = target + hit
                first = first + hit * start
                length = length + hit * lens_ref[c, k]
                start = start + lens_ref[c, k]
        first = lax.rem(first + batch_rank * span_len, 2 * span_len) * target
        length = jnp.where(target > 0, length, ctx_ref[r])
        facts.append((target, first, length))

    def copy_of(r, t):
        slot = lax.rem(t, depth)
        target, start, _ = facts[r]
        at = pl.multiple_of(start // blk * blk + t * blk, blk)

        @pl.when(target > 0)
        def _():
            own = spans_ref.shape[2]
            for c in range(blk // own):
                pltpu.make_async_copy(
                    spans_ref.at[at // own + c],
                    bufs.at[r, slot, :, c * own : (c + 1) * own],
                    sems.at[r, slot],
                ).start()

        @pl.when(target == 0)
        def _():
            pltpu.make_async_copy(
                cache_ref.at[r, :, pl.ds(at, blk)], bufs.at[r, slot], sems.at[r, slot]
            ).start()

    counts = []
    for r in range(owned):
        _, start, length = facts[r]
        counts.append((start + length + blk - 1) // blk - start // blk)
    for r in range(owned):
        for t in range(depth - 1):
            pl.when(t < counts[r])(functools.partial(copy_of, r, jnp.int32(t)))
    newest = new_ref[...].astype(jnp.float32)
    for r in range(owned):
        _, start, length = facts[r]
        base = start // blk * blk
        q = q_ref[:, r].reshape(rows, kv)
        fresh = jnp.concatenate(
            [newest[s, r : r + 1] for s in range(steps)]
            + [jnp.zeros((128 - steps, kv), jnp.float32)],
            axis=0,
        ).astype(jnp.bfloat16)
        s = trans_dot(q, fresh)
        row_step = (lax.broadcasted_iota(jnp.int32, s.shape, 0) // heads) % steps
        col = lax.broadcasted_iota(jnp.int32, s.shape, 1)
        s = jnp.where(col <= row_step, s, NEGATIVE)
        m = jnp.max(s, axis=1, keepdims=True)
        w = jnp.exp2((s - m) * scale)
        l_ref[...] = jnp.broadcast_to(jnp.sum(w, axis=1, keepdims=True), l_ref.shape)
        m_ref[...] = jnp.broadcast_to(m, m_ref.shape)
        acc_ref[...] = jnp.dot(
            w.astype(jnp.bfloat16), fresh[:, :lat], preferred_element_type=jnp.float32
        )

        def step(t, carry):
            slot = lax.rem(t, depth)
            pl.when(t + depth - 1 < counts[r])(lambda: copy_of(r, t + depth - 1))
            pltpu.make_async_copy(
                cache_ref.at[r, :, pl.ds(0, blk)], bufs.at[r, slot], sems.at[r, slot]
            ).wait()
            keys = bufs[r, slot]
            s = jnp.dot(q, keys, preferred_element_type=jnp.float32)
            place = base + t * blk + lax.broadcasted_iota(jnp.int32, (1, blk), 1)
            hide = jnp.where((place >= start) & (place < start + length), 0.0, NEGATIVE)
            s = s + hide
            old = m_ref[:, :1]
            new = jnp.maximum(old, jnp.max(s, axis=1, keepdims=True))
            alpha = jnp.exp2((old - new) * scale)
            w = jnp.exp2((s - new) * scale)
            l_new = l_ref[:, :1] * alpha + jnp.sum(w, axis=1, keepdims=True)
            l_ref[...] = jnp.broadcast_to(l_new, l_ref.shape)
            m_ref[...] = jnp.broadcast_to(new, m_ref.shape)
            acc_ref[...] = acc_ref[...] * alpha + trans_dot(w.astype(jnp.bfloat16), keys[:lat])
            return carry

        lax.fori_loop(0, counts[r], step, 0)
        done = (acc_ref[...] / l_ref[:, :1]).astype(out_ref.dtype)
        for p in range(ranks):
            out_ref[p, r] = done[p * block : (p + 1) * block]
    shown.wait()


def decode_pallas(lens, owner, ctx, query, newest, spans, part, cache, lat, heads, all_columns, width, rows_local, blk=512, depth=4):
    ranks, owned, block, kv = query.shape
    rows = ranks * block
    steps = block // heads
    span_len = part.shape[0]
    return pl.pallas_call(
        functools.partial(
            decode_kernel,
            lat=lat,
            heads=heads,
            steps=steps,
            blk=blk,
            depth=depth,
            scale=math.log2(math.e) / math.sqrt(width),
            rows_local=rows_local,
            span_len=span_len,
        ),
        out_shape=(
            jax.ShapeDtypeStruct((ranks, owned, block, lat), jnp.bfloat16),
            jax.ShapeDtypeStruct((span_len, all_columns), jnp.bfloat16),
        ),
        in_specs=[SMEM_SPEC] * 3
        + [VMEM_SPEC, VMEM_SPEC, pl.BlockSpec(memory_space=pl.ANY), VMEM_SPEC, HBM_SPEC],
        out_specs=(VMEM_SPEC, HBM_SPEC),
        scratch_shapes=[
            pltpu.VMEM((owned, depth, kv, blk), jnp.bfloat16),
            pltpu.SemaphoreType.DMA((owned, depth)),
            pltpu.SemaphoreType.DMA((1,)),
            pltpu.VMEM((rows, 128), jnp.float32),
            pltpu.VMEM((rows, 128), jnp.float32),
            pltpu.VMEM((rows, lat), jnp.float32),
        ],
        compiler_params=pltpu.CompilerParams(vmem_limit_bytes=40 << 20),
        cost_estimate=pl.CostEstimate(
            flops=5 * 10**9, bytes_accessed=10 << 20, transcendentals=2 << 20
        ),
    )(lens, owner, ctx, query, newest, spans, part, cache)


def return_kernel(
    lens_ref, rows_ref, spans_ref, lo_ref, kw_hbm, vw_hbm, q_hbm,
    back_ref, part_ref,
    kw, vw, qs, keys, vals, hot, tri, load_sems, give_sems, take_sems,
    *, lat, ranks, look, scale, turn_at
):
    me = lax.axis_index("head")
    batch_rank = lax.axis_index("batch")
    some = qs.shape[0]
    skip = q_hbm.shape[0] - some
    barrier = pltpu.get_barrier_semaphore()
    for k in range(1, ranks):
        pl.semaphore_signal(
            barrier, inc=1, device_id={"head": (me + k) % ranks}, device_id_type=MESH
        )
    loads = [
        pltpu.make_async_copy(kw_hbm.at[:, skip * 128 :], kw, load_sems.at[0]),
        pltpu.make_async_copy(vw_hbm.at[:, skip * 128 :], vw, load_sems.at[1]),
        pltpu.make_async_copy(q_hbm.at[skip:], qs, load_sems.at[2]),
    ]
    for load in loads:
        load.start()
    start_marks(span_ends(lens_ref, batch_rank), keys, vals, hot, tri, rows_ref, lat)
    for load in loads:
        load.wait()
    gives = []
    for k in range(1, ranks):
        peer = (me + k) % ranks
        gives.append(
            pltpu.make_async_remote_copy(
                src_ref=lo_ref.at[peer],
                dst_ref=back_ref.at[me],
                send_sem=give_sems.at[k - 1],
                recv_sem=take_sems.at[k - 1],
                device_id={"head": peer},
                device_id_type=MESH,
            )
        )
    keep = pltpu.make_async_copy(lo_ref.at[me], back_ref.at[me], load_sems.at[3])
    keep.start()

    def step(g, carry):
        @pl.when(g == turn_at)
        def _():
            pl.semaphore_wait(barrier, ranks - 1)
            for give in gives:
                give.start()

        attend_pair(
            g, kw, vw, qs, spans_ref, rows_ref, keys, vals, hot, tri, part_ref, lat, look, scale
        )
        return carry

    lax.fori_loop(0, some // keys.shape[0], step, 0)
    for give in gives:
        give.wait()
    keep.wait()


def return_pallas(lens, rows, spans, latent_out, key_weight, value_weight, turned, rest, qb, turn_at):
    heads, width, span_len = turned.shape
    ranks = latent_out.shape[0]
    lat = key_weight.shape[0]
    kv = rows.shape[1]
    look = min(-(-(span_len // 2) // qb), span_len // qb - 1)
    bf16 = jnp.bfloat16
    return pl.pallas_call(
        functools.partial(
            return_kernel,
            lat=lat,
            ranks=ranks,
            look=look,
            scale=math.log2(math.e) / math.sqrt(width),
            turn_at=turn_at,
        ),
        out_shape=(
            jax.ShapeDtypeStruct(latent_out.shape, bf16),
            jax.ShapeDtypeStruct((span_len, rest * 128), bf16),
        ),
        in_specs=[SMEM_SPEC] + [VMEM_SPEC] * 3 + [HBM_SPEC] * 3,
        out_specs=(VMEM_SPEC,) * 2,
        scratch_shapes=[
            pltpu.VMEM((lat, rest * 128), bf16),
            pltpu.VMEM((lat, rest * 128), bf16),
            pltpu.VMEM((rest, width, span_len), bf16),
            *attend_scratch(span_len, kv, lat, qb),
            pltpu.SemaphoreType.DMA((4,)),
            pltpu.SemaphoreType.DMA((ranks - 1,)),
            pltpu.SemaphoreType.DMA((ranks - 1,)),
        ],
        compiler_params=pltpu.CompilerParams(
            collective_id=1, has_side_effects=True, vmem_limit_bytes=40 << 20
        ),
        cost_estimate=pl.CostEstimate(
            flops=12 * 10**9, bytes_accessed=12 << 20, transcendentals=6 << 20
        ),
    )(lens, rows, spans, latent_out, key_weight, value_weight, turned)


def project_kernel(back_ref, vw_ref, part_ref, half_ref, out_ref, whole_ref, wide, sems, *, heads, lat):
    ranks, owned, block, _ = back_ref.shape
    steps = block // heads
    local = ranks * owned
    columns = part_ref.shape[1]
    shown = pltpu.make_async_copy(
        part_ref, whole_ref.at[:, whole_ref.shape[1] - columns :], sems.at[0]
    )
    shown.start()
    for p in range(ranks):
        for r in range(owned):
            at = (p * owned + r) * block
            for c in range(lat // 128):
                wide[c, at : at + block] = back_ref[p, r, :, c * 128 : (c + 1) * 128].astype(
                    jnp.float32
                )
    for h in range(heads):
        mine = jnp.concatenate(
            [
                jnp.concatenate(
                    [
                        wide[c, pl.ds(s * heads + h, local, stride=block), :]
                        for c in range(lat // 128)
                    ],
                    axis=1,
                )
                for s in range(steps)
            ],
            axis=0,
        ).astype(jnp.bfloat16)
        out_ref[:, h * 128 : (h + 1) * 128] = jnp.dot(
            mine, vw_ref[:, h * 128 : (h + 1) * 128], preferred_element_type=jnp.float32
        ).astype(jnp.bfloat16)
    shown.wait()


def project_pallas(back, value_weight, part, whole, heads):
    ranks, owned, block, lat = back.shape
    rows = ranks * owned * block
    return pl.pallas_call(
        functools.partial(project_kernel, heads=heads, lat=lat),
        out_shape=(
            jax.ShapeDtypeStruct((rows // heads, heads * 128), jnp.bfloat16),
            jax.ShapeDtypeStruct(whole.shape, whole.dtype),
        ),
        in_specs=[VMEM_SPEC, VMEM_SPEC, VMEM_SPEC, HBM_SPEC],
        out_specs=(VMEM_SPEC, HBM_SPEC),
        scratch_shapes=[
            pltpu.VMEM((lat // 128, rows, 128), jnp.float32),
            pltpu.SemaphoreType.DMA((1,)),
        ],
        input_output_aliases={3: 1},
        compiler_params=pltpu.CompilerParams(vmem_limit_bytes=24 << 20),
    )(back, value_weight, part, whole)


def on_device(
    latent_rows,
    pre_queries,
    pre_lengths,
    owner_map,
    context_cache,
    context_lengths,
    new_latent,
    dec_queries,
    key_weight,
    value_weight,
):
    steps, rows_local, heads, width = dec_queries.shape
    ranks = lax.axis_size("head")
    if heads % 16 or latent_rows.shape[0] % 128 or ranks % 2:
        return plain_on_device(
            latent_rows,
            pre_queries,
            pre_lengths,
            owner_map,
            context_cache,
            context_lengths,
            new_latent,
            dec_queries,
            key_weight,
            value_weight,
        )
    lat = key_weight.shape[0]
    owned = context_cache.shape[0]
    first = heads // 2
    qb = 256
    turned = jnp.transpose(pre_queries, (1, 2, 0))
    spans, rows, query, part = gather_pallas(
        pre_lengths,
        jnp.transpose(latent_rows),
        dec_queries.reshape(-1, width),
        key_weight,
        value_weight,
        turned,
        owned,
        ranks,
        first,
        qb,
    )
    latent_out, whole = decode_pallas(
        pre_lengths,
        owner_map,
        context_lengths,
        query,
        new_latent,
        spans,
        part,
        jnp.transpose(context_cache, (0, 2, 1)),
        lat,
        heads,
        heads * 128,
        width,
        rows_local,
    )
    back, rest = return_pallas(
        pre_lengths, rows, spans, latent_out, key_weight, value_weight, turned, heads - first, qb, 1
    )
    decode_out, prefill_out = project_pallas(back, value_weight, rest, whole, heads)
    return (prefill_out, decode_out.reshape(steps, rows_local, heads * 128))


def solution(mesh):
    placed = (
        P(("groups", "batch", "head"), None),
        P(("groups", "batch"), "head", None),
        P("groups", None),
        P("groups", None),
        P(("groups", "batch", "head"), None, None),
        P(("groups", "batch", "head")),
        P("groups", ("batch", "head"), None),
        P("groups", "batch", "head", None),
        P(None, "head"),
        P(None, "head"),
    )
    return jax.shard_map(
        on_device,
        mesh=mesh,
        in_specs=placed,
        out_specs=(P(("groups", "batch"), "head"), P("groups", "batch", "head")),
        check_vma=False,
    )
```

```python
import functools
import math

import jax
import jax.numpy as jnp
from jax import lax
from jax.experimental import pallas as pl
from jax.experimental.pallas import tpu as pltpu
from jax.sharding import PartitionSpec as P

BLK = 512


NEGATIVE = -1e30


def from_partner(value, axis, distance):
    mask = 2**distance
    pairs = [(source, source ^ mask) for source in range(lax.axis_size(axis))]
    return lax.ppermute(value, axis, pairs)


def request_table(pre_lengths, owner_map, span_len):
    seg_ends = jnp.cumsum(pre_lengths, axis=1)
    span_base = jnp.arange(pre_lengths.shape[0], dtype=jnp.int32)[:, None] * span_len
    seg_starts = seg_ends - pre_lengths + span_base
    return (owner_map.reshape(-1), seg_starts.reshape(-1), pre_lengths.reshape(-1))


def prefill_heads(own_span, queries, span_lengths, key_weight, value_weight):
    span_len, head_count, query_width = queries.shape
    head_size = key_weight.shape[1] // head_count
    lat_width = key_weight.shape[0]
    score_scale = 1.0 / math.sqrt(query_width)
    latent = own_span[:, :lat_width]
    rope_keys = own_span[:, lat_width:]
    keys_nope = (
        jnp.dot(latent, key_weight, preferred_element_type=jnp.float32)
        .astype(jnp.bfloat16)
        .reshape(span_len, head_count, head_size)
    )
    values = (
        jnp.dot(latent, value_weight, preferred_element_type=jnp.float32)
        .astype(jnp.bfloat16)
        .reshape(span_len, head_count, head_size)
    )
    scores = jnp.einsum(
        "qhd,khd->hqk", queries[:, :, :head_size], keys_nope, preferred_element_type=jnp.float32
    )
    scores = scores + jnp.einsum(
        "qhr,kr->hqk", queries[:, :, head_size:], rope_keys, preferred_element_type=jnp.float32
    )
    scores = scores * score_scale
    seg_ends = jnp.cumsum(span_lengths)
    places = jnp.arange(span_len, dtype=jnp.int32)
    segment = jnp.sum((places[:, None] >= seg_ends[None, :]).astype(jnp.int32), axis=1)
    allowed = (segment[:, None] == segment[None, :]) & (places[None, :] <= places[:, None])
    masked = jnp.where(allowed[None], scores, NEGATIVE)
    peak_score = jnp.max(masked, axis=2, keepdims=True)
    weights = jnp.exp(masked - peak_score)
    weight_sum = jnp.sum(weights, axis=2)
    mixed_out = jnp.einsum(
        "hqk,khd->qhd", weights.astype(jnp.bfloat16), values, preferred_element_type=jnp.float32
    )
    mixed_out = mixed_out / jnp.transpose(weight_sum)[:, :, None]
    return mixed_out.astype(jnp.bfloat16).reshape(span_len, head_count * head_size)


def plain_on_device(
    latent_rows,
    pre_queries,
    pre_lengths,
    owner_map,
    context_cache,
    context_lengths,
    new_latent,
    dec_queries,
    key_weight,
    value_weight,
):
    head_rank = lax.axis_index("head")
    batch_rank = lax.axis_index("batch")
    span_len = pre_queries.shape[0]
    kv_width = latent_rows.shape[1]
    own_span = lax.all_gather(latent_rows, "head", axis=0, tiled=True)
    other_span = from_partner(own_span, "batch", 0)
    first_span = jnp.where(batch_rank == 0, own_span, other_span)
    second_span = jnp.where(batch_rank == 0, other_span, own_span)
    all_spans = jnp.concatenate([first_span, second_span], axis=0)
    span_lengths = lax.dynamic_index_in_dim(pre_lengths, batch_rank, 0, keepdims=False)
    prefill_out = prefill_heads(own_span, pre_queries, span_lengths, key_weight, value_weight)
    step_total, rows_local, head_count, query_width = dec_queries.shape
    lat_width = key_weight.shape[0]
    head_size = key_weight.shape[1] // head_count
    owned_rows = context_cache.shape[0]
    score_scale = 1.0 / math.sqrt(query_width)
    key_heads = key_weight.reshape(lat_width, head_count, head_size)
    value_heads = value_weight.reshape(lat_width, head_count, head_size)
    absorbed = jnp.einsum(
        "srhd,lhd->srhl",
        dec_queries[..., :head_size],
        key_heads,
        preferred_element_type=jnp.float32,
    ).astype(jnp.bfloat16)
    query_all = jnp.concatenate([absorbed, dec_queries[..., head_size:]], axis=3)
    flat_owner, flat_start, flat_length = request_table(pre_lengths, owner_map, span_len)
    row_ids = (
        batch_rank * rows_local + head_rank * owned_rows + jnp.arange(owned_rows, dtype=jnp.int32)
    )
    matches = (flat_owner[None, :] == row_ids[:, None]).astype(jnp.int32)
    is_target = jnp.sum(matches, axis=1) > 0
    first_row = jnp.sum(matches * flat_start[None, :], axis=1)
    prompt_len = jnp.sum(matches * flat_length[None, :], axis=1)
    effective = jnp.where(is_target, prompt_len, context_lengths)
    padded = jnp.concatenate([all_spans, jnp.zeros((span_len, kv_width), all_spans.dtype)], axis=0)
    replaced = jax.vmap(lambda offset: lax.dynamic_slice_in_dim(padded, offset, span_len, 0))(
        first_row
    )
    front_rows = jnp.where(is_target[:, None, None], replaced, context_cache[:, :span_len])
    front_blocks = span_len // BLK
    needed = (jnp.max(effective) + BLK - 1) // BLK
    fresh_latent = new_latent[..., :lat_width]
    owned_query = lax.all_to_all(query_all, "head", split_axis=1, concat_axis=2, tiled=True)
    fresh_scores = (
        jnp.einsum("srhk,jrk->srhj", owned_query, new_latent, preferred_element_type=jnp.float32)
        * score_scale
    )
    visible = (
        jnp.arange(new_latent.shape[0], dtype=jnp.int32)[None, :]
        <= jnp.arange(step_total, dtype=jnp.int32)[:, None]
    )
    fresh_scores = jnp.where(visible[:, None, None, :], fresh_scores, NEGATIVE)
    peak_score = jnp.max(fresh_scores, axis=3)
    weights = jnp.exp(fresh_scores - peak_score[..., None])
    weight_sum = jnp.sum(weights, axis=3)
    running = jnp.einsum(
        "srhj,jrl->srhl",
        weights.astype(jnp.bfloat16),
        fresh_latent,
        preferred_element_type=jnp.float32,
    )

    def advance(block_index, state_tuple, source):
        old_peak, old_sum, old_running = state_tuple
        key_block = lax.dynamic_slice_in_dim(source, block_index * BLK, BLK, 1)
        scores = (
            jnp.einsum("srhk,rtk->srht", owned_query, key_block, preferred_element_type=jnp.float32)
            * score_scale
        )
        places = block_index * BLK + jnp.arange(BLK, dtype=jnp.int32)
        in_context = places[None, :] < effective[:, None]
        scores = jnp.where(in_context[None, :, None, :], scores, NEGATIVE)
        new_peak = jnp.maximum(old_peak, jnp.max(scores, axis=3))
        factor = jnp.exp(old_peak - new_peak)
        block_weights = jnp.exp(scores - new_peak[..., None])
        new_sum = old_sum * factor + jnp.sum(block_weights, axis=3)
        new_running = old_running * factor[..., None] + jnp.einsum(
            "srht,rtl->srhl",
            block_weights.astype(jnp.bfloat16),
            key_block[..., :lat_width],
            preferred_element_type=jnp.float32,
        )
        return (new_peak, new_sum, new_running)

    state_tuple = lax.fori_loop(
        0,
        jnp.minimum(needed, front_blocks),
        lambda block_index, state_now: advance(block_index, state_now, front_rows),
        (peak_score, weight_sum, running),
    )
    state_tuple = lax.fori_loop(
        front_blocks,
        jnp.maximum(needed, front_blocks),
        lambda block_index, state_now: advance(block_index, state_now, context_cache),
        state_tuple,
    )
    latent_out = (state_tuple[2] / state_tuple[1][..., None]).astype(jnp.bfloat16)
    returned = lax.all_to_all(latent_out, "head", split_axis=2, concat_axis=1, tiled=True)
    projected = jnp.einsum(
        "srhl,lhd->srhd", returned, value_heads, preferred_element_type=jnp.float32
    ).astype(jnp.bfloat16)
    decode_out = projected.reshape(query_all.shape[0], rows_local, head_count * head_size)
    return (prefill_out, decode_out)


def trans_dot(left, right):
    return lax.dot_general(
        left, right, (((1,), (1,)), ((), ())), preferred_element_type=jnp.float32
    )


MESH = pl.DeviceIdType.MESH


def place_of(rank, ranks):
    odd = rank % 2
    return (1 - odd) * (rank // 2) + odd * (ranks - 1 - rank // 2)


def rank_at(place, ranks):
    late = place // (ranks // 2)
    return (1 - late) * (2 * place) + late * (2 * (ranks - 1 - place) + 1)


def start_marks(ends, both_keys, both_vals, hot, tri, rows_ref, lat):
    pair, span_len, full = both_keys[0].shape
    segs = len(ends)
    marks = full - 128 - (rows_ref.shape[1] - lat)
    where = lax.broadcasted_iota(jnp.int32, (span_len, marks), 0)
    lane = lax.broadcasted_iota(jnp.int32, (span_len, marks), 1)
    place = lax.broadcasted_iota(jnp.int32, (marks, span_len), 1)
    line = lax.broadcasted_iota(jnp.int32, (marks, span_len), 0)
    mine = jnp.zeros((span_len, marks), jnp.int32)
    seen = jnp.zeros((marks, span_len), jnp.int32)
    for k in range(segs - 1):
        mine = mine + (where >= ends[k]).astype(jnp.int32)
        seen = seen + (place >= ends[k]).astype(jnp.int32)
    mark = jnp.where((lane < segs) & (lane != mine), NEGATIVE, 0.0).astype(jnp.bfloat16)
    hot[...] = jnp.where(line == seen, 1.0, 0.0).astype(jnp.bfloat16)
    for keys, vals in zip(both_keys, both_vals):
        for p in range(pair):
            keys[p, :, 128 : full - marks] = rows_ref[:, lat:]
            keys[p, :, full - marks :] = mark
            vals[p, 128:, :] = jnp.ones((vals.shape[1] - 128, span_len), jnp.bfloat16)
    size = tri.shape[0]
    key_at = lax.broadcasted_iota(jnp.int32, (size, size), 0)
    query_at = lax.broadcasted_iota(jnp.int32, (size, size), 1)
    tri[...] = jnp.where(key_at <= query_at, 0.0, NEGATIVE)


def value_piece(c, turned, spans_ref, vals, lat):
    latents = jnp.concatenate([spans_ref[2 * c, :lat, :], spans_ref[2 * c + 1, :lat, :]], axis=1)
    value = jnp.dot(turned[...], latents, preferred_element_type=jnp.float32).astype(jnp.bfloat16)
    for p in range(vals.shape[0]):
        vals[p, :128, c * 256 : (c + 1) * 256] = value[p * 128 : (p + 1) * 128]


def key_piece(rows, columns, kw, rows_ref, keys, lat):
    made = jnp.dot(rows_ref[rows, :lat], kw[:, columns], preferred_element_type=jnp.float32)
    made = made.astype(jnp.bfloat16)
    for p in range(keys.shape[0]):
        keys[p, rows, :128] = made[:, p * 128 : (p + 1) * 128]


def projections(g, kw, vw, spans_ref, rows_ref, turned, keys, vals, lat):
    pair, span_len, _ = keys.shape
    wide = pair * 128
    columns = pl.ds(pl.multiple_of(g * wide, wide), wide)

    def turn():
        turned[...] = jnp.transpose(vw[:, columns])

    half = span_len // 2
    pieces = [turn]
    for k in range(2):
        rows = slice(k * half, (k + 1) * half)
        pieces.append(functools.partial(key_piece, rows, columns, kw, rows_ref, keys, lat))
    for c in range(span_len // 256):
        pieces.append(functools.partial(value_piece, c, turned, spans_ref, vals, lat))
    return pieces


def attention(g, qs, keys, vals, hot, tri, part_ref, scores, weights, look, scale, others):
    pair, span_len, _ = keys.shape
    qb = tri.shape[0]
    blocks = span_len // qb
    order = [(0, 0)] + [(i, p) for i in range(1, blocks) for p in range(pair)]
    order += [(0, p) for p in range(1, pair)]
    count = len(order)
    lengths = [min(i, look) + 1 for i, _ in order]
    peaks = [None] * count
    tops = [None] * count
    sums = [None] * count

    def score(n, c):
        i, p = order[n]
        at = (i - lengths[n] + 1 + c) * qb
        query = jnp.concatenate(
            [qs[g * pair + p, :, i * qb : (i + 1) * qb], hot[:, i * qb : (i + 1) * qb]], axis=0
        )
        s = jnp.dot(keys[p, at : at + qb, :], query, preferred_element_type=jnp.float32)
        if c == lengths[n] - 1:
            s = s + tri[...]
        scores[n % 2][c * qb : (c + 1) * qb, :] = s
        top = jnp.max(s.reshape(qb // 8, 8, qb), axis=0)
        peaks[n] = top if peaks[n] is None else jnp.maximum(peaks[n], top)

    def soften(n, c):
        if c == 0:
            tops[n] = jnp.max(peaks[n], axis=0, keepdims=True)
        s = scores[n % 2][c * qb : (c + 1) * qb, :]
        w = jnp.exp2((s - tops[n]) * scale)
        weights[n % 2][c * qb : (c + 1) * qb, :] = w.astype(jnp.bfloat16)

    def mix(n, c):
        i, p = order[n]
        at = (i - lengths[n] + 1 + c) * qb
        o = jnp.dot(
            vals[p, :, at : at + qb],
            weights[n % 2][c * qb : (c + 1) * qb, :],
            preferred_element_type=jnp.float32,
        )
        sums[n] = o if sums[n] is None else sums[n] + o
        if c == lengths[n] - 1:
            o = sums[n]
            o = o[:128] * (1.0 / o[128:129])
            columns = pl.ds(pl.multiple_of((g * pair + p) * 128, 128), 128)
            part_ref[i * qb : (i + 1) * qb, columns] = jnp.transpose(o.astype(jnp.bfloat16))

    todo_score = [(n, c) for n in range(count) for c in range(lengths[n])]
    todo_soft = list(todo_score)
    todo_mix = list(todo_score)
    total = len(todo_score)
    scored = [0] * count
    softened = [0] * count
    mixed = [0] * count
    others = list(others)
    every = total / max(len(others), 1)
    done = 0
    step = 0
    while todo_mix:
        was = list(softened)
        if todo_score:
            n, c = todo_score[0]
            if n < 2 or softened[n - 2] == lengths[n - 2]:
                score(n, c)
                scored[n] += 1
                todo_score.pop(0)
        if todo_soft:
            n, c = todo_soft[0]
            free = n < 2 or mixed[n - 2] == lengths[n - 2]
            if scored[n] == lengths[n] and free and not (todo_score and todo_score[0][0] <= n):
                soften(n, c)
                softened[n] += 1
                todo_soft.pop(0)
        n, c = todo_mix[0]
        if c < was[n]:
            mix(n, c)
            mixed[n] += 1
            todo_mix.pop(0)
        step += 1
        while done < len(others) and done * every <= step - 1:
            others[done]()
            done += 1
    while done < len(others):
        others[done]()
        done += 1


def attend_all(turns, tools, shared, before):
    kw, vw, qs, spans_ref, rows_ref, part_ref, lat, look, scale = shared
    keys, vals, hot, tri, turned, scores, weights = tools
    for piece in projections(0, kw, vw, spans_ref, rows_ref, turned[0], keys[0], vals[0], lat):
        piece()

    def step(j, carry):
        before(j)
        for side in range(2):
            g = 2 * j + side
            following = jnp.minimum(g + 1, 2 * turns - 1)
            others = projections(
                following, kw, vw, spans_ref, rows_ref,
                turned[1 - side], keys[1 - side], vals[1 - side], lat,
            )
            attention(
                g, qs, keys[side], vals[side], hot, tri, part_ref,
                scores, weights, look, scale, others,
            )
        return carry

    lax.fori_loop(0, turns, step, 0)


def absorb_into(dq, kw, sent, flat, wide, heads, lat):
    rows = dq.shape[0]
    ranks, owned, block, _ = sent.shape
    steps = block // heads
    local = ranks * owned
    flat[...] = dq[:, :128].astype(jnp.float32)
    for h in range(heads):
        mine = flat[pl.ds(h, rows // heads, stride=heads), :].astype(jnp.bfloat16)
        res = trans_dot(mine, kw[:, h * 128 : (h + 1) * 128])
        for s in range(steps):
            for c in range(lat // 128):
                wide[c, pl.ds(s * heads + h, local, stride=block), :] = res[
                    s * local : (s + 1) * local, c * 128 : (c + 1) * 128
                ]
    for p in range(ranks):
        for r in range(owned):
            at = p * owned + r
            for c in range(lat // 128):
                sent[p, r, :, c * 128 : (c + 1) * 128] = wide[
                    c, at * block : (at + 1) * block
                ].astype(jnp.bfloat16)
            for s in range(steps):
                start = (s * local + at) * heads
                sent[p, r, s * heads : (s + 1) * heads, lat:] = dq[start : start + heads, 128:]


def span_ends(lens_ref, batch_rank):
    ends = []
    total = 0
    for k in range(lens_ref.shape[1]):
        total = total + lens_ref[batch_rank, k]
        ends.append(total)
    return ends


def gather_kernel(
    lens_ref, shard_hbm, dq_hbm, kw_hbm, vw_hbm, q_hbm,
    spans_ref, rows_ref, got_ref, part_ref,
    kw, vw, qs, dq, flat, wide, sent, tools,
    load_sems, ring_send, ring_recv, swap_sems, give_sems, take_sems,
    *, lat, ranks, heads, look, scale
):
    me = lax.axis_index("head")
    batch_rank = lax.axis_index("batch")
    place = place_of(me, ranks)
    right = rank_at((place + 1) % ranks, ranks)
    left = rank_at((place + ranks - 1) % ranks, ranks)
    some = qs.shape[0]
    loads = [
        pltpu.make_async_copy(dq_hbm, dq, load_sems.at[0]),
        pltpu.make_async_copy(kw_hbm, kw, load_sems.at[1]),
        pltpu.make_async_copy(shard_hbm, spans_ref.at[me], load_sems.at[2]),
        pltpu.make_async_copy(vw_hbm.at[:, : some * 128], vw, load_sems.at[3]),
        pltpu.make_async_copy(q_hbm.at[:some], qs, load_sems.at[4]),
    ]
    barrier = pltpu.get_barrier_semaphore()
    for k in range(1, ranks):
        pl.semaphore_signal(
            barrier, inc=1, device_id={"head": (me + k) % ranks}, device_id_type=MESH
        )
    pl.semaphore_signal(
        barrier, inc=1, device_id={"batch": 1 - batch_rank}, device_id_type=MESH
    )
    for load in loads:
        load.start()
    pl.semaphore_wait(barrier, ranks)

    half = shard_hbm.shape[0] // 2
    most = ranks // 2

    def hop(way, part, t):
        back = t - 1 if way == 0 else ranks - t + 1
        origin = rank_at((place + ranks - back) % ranks, ranks)
        rows = pl.ds(part * half, half)
        source = shard_hbm.at[rows] if t == 1 else spans_ref.at[origin, rows]
        return pltpu.make_async_remote_copy(
            src_ref=source,
            dst_ref=spans_ref.at[origin, rows],
            send_sem=ring_send.at[way, part, t - 1],
            recv_sem=ring_recv.at[way, part, t - 1],
            device_id={"head": right if way == 0 else left},
            device_id_type=MESH,
        )

    def hops(way, part):
        return most if way == part else most - 1

    streams = [(0, 0), (1, 1), (0, 1), (1, 0)]
    for way, part in streams:
        hop(way, part, 1).start()
    loads[0].wait()
    loads[1].wait()
    absorb_into(dq, kw, sent, flat, wide, heads, lat)

    own = shard_hbm.shape[1]

    def turn(origin):
        rows_ref[pl.ds(pl.multiple_of(origin * own, own), own), :] = jnp.transpose(
            spans_ref[origin]
        )

    loads[2].wait()
    turn(me)
    for t in range(1, most + 1):
        for way, part in streams:
            if t <= hops(way, part):
                hop(way, part, t).wait_recv()
                if t < hops(way, part):
                    hop(way, part, t + 1).start()
        turn(rank_at((place + ranks - t) % ranks, ranks))
        if t < most:
            turn(rank_at((place + t) % ranks, ranks))

    gives = []
    for k in range(1, ranks):
        peer = (me + k) % ranks
        gives.append(
            pltpu.make_async_remote_copy(
                src_ref=sent.at[peer],
                dst_ref=got_ref.at[me],
                send_sem=give_sems.at[k - 1],
                recv_sem=take_sems.at[k - 1],
                device_id={"head": peer},
                device_id_type=MESH,
            )
        )
    for give in gives:
        give.start()
    keep = pltpu.make_async_copy(sent.at[me], got_ref.at[me], load_sems.at[5])
    keep.start()
    swap = pltpu.make_async_remote_copy(
        src_ref=spans_ref.at[:ranks],
        dst_ref=spans_ref.at[ranks:],
        send_sem=swap_sems.at[0],
        recv_sem=swap_sems.at[1],
        device_id={"batch": 1 - batch_rank},
        device_id_type=MESH,
    )
    swap.start()
    loads[3].wait()
    loads[4].wait()
    keys, vals, hot, tri = tools[:4]
    start_marks(span_ends(lens_ref, batch_rank), keys, vals, hot, tri, rows_ref, lat)

    shared = (kw, vw, qs, spans_ref, rows_ref, part_ref, lat, look, scale)
    attend_all(some // 4, tools, shared, lambda j: None)
    for way, part in streams:
        for t in range(1, hops(way, part) + 1):
            hop(way, part, t).wait_send()
    for give in gives:
        give.wait()
    keep.wait()
    swap.wait()


HBM_SPEC = pl.BlockSpec(memory_space=pltpu.HBM)
VMEM_SPEC = pl.BlockSpec(memory_space=pltpu.VMEM)
SMEM_SPEC = pl.BlockSpec(memory_space=pltpu.SMEM)


def attend_scratch(span_len, kv, lat, qb, look):
    pair = 2
    marks = 128 - (kv - lat)
    bf16 = jnp.bfloat16
    twice = lambda shape, dtype: [pltpu.VMEM(shape, dtype)] * 2
    return [
        twice((pair, span_len, 256), bf16),
        twice((pair, 128 + 16, span_len), bf16),
        pltpu.VMEM((marks, span_len), bf16),
        pltpu.VMEM((qb, qb), jnp.float32),
        twice((pair * 128, lat), bf16),
        twice(((look + 1) * qb, qb), jnp.float32),
        twice(((look + 1) * qb, qb), bf16),
    ]


def gather_pallas(lens, shard, flat_queries, key_weight, value_weight, turned, owned, ranks, first, qb):
    heads, width, span_len = turned.shape
    kv, own = shard.shape
    lat = key_weight.shape[0]
    rows = flat_queries.shape[0]
    block = rows // (ranks * owned)
    look = min(-(-(span_len // 2) // qb), span_len // qb - 1)
    bf16 = jnp.bfloat16
    return pl.pallas_call(
        functools.partial(
            gather_kernel,
            lat=lat,
            ranks=ranks,
            heads=heads,
            look=look,
            scale=math.log2(math.e) / math.sqrt(width),
        ),
        out_shape=(
            jax.ShapeDtypeStruct((2 * ranks, kv, own), bf16),
            jax.ShapeDtypeStruct((span_len, kv), bf16),
            jax.ShapeDtypeStruct((ranks, owned, block, kv), bf16),
            jax.ShapeDtypeStruct((span_len, first * 128), bf16),
        ),
        in_specs=[SMEM_SPEC] + [HBM_SPEC] * 5,
        out_specs=(VMEM_SPEC,) * 4,
        scratch_shapes=[
            pltpu.VMEM(key_weight.shape, bf16),
            pltpu.VMEM((lat, first * 128), bf16),
            pltpu.VMEM((first, width, span_len), bf16),
            pltpu.VMEM((rows, width), bf16),
            pltpu.VMEM((rows, 128), jnp.float32),
            pltpu.VMEM((lat // 128, rows, 128), jnp.float32),
            pltpu.VMEM((ranks, owned, block, kv), bf16),
            attend_scratch(span_len, kv, lat, qb, look),
            pltpu.SemaphoreType.DMA((6,)),
            pltpu.SemaphoreType.DMA((2, 2, ranks // 2)),
            pltpu.SemaphoreType.DMA((2, 2, ranks // 2)),
            pltpu.SemaphoreType.DMA((2,)),
            pltpu.SemaphoreType.DMA((ranks - 1,)),
            pltpu.SemaphoreType.DMA((ranks - 1,)),
        ],
        compiler_params=pltpu.CompilerParams(
            collective_id=0, has_side_effects=True, vmem_limit_bytes=40 << 20
        ),
        cost_estimate=pl.CostEstimate(
            flops=12 * 10**9, bytes_accessed=12 << 20, transcendentals=6 << 20
        ),
    )(lens, shard, flat_queries, key_weight, value_weight, turned)


def decode_kernel(
    lens_ref, owner_ref, ctx_ref, q_ref, new_ref, spans_ref, part_ref, cache_ref,
    out_ref, whole_ref,
    bufs, sems, whole_sem, m_ref, l_ref, acc_ref,
    *, lat, heads, steps, blk, depth, scale, rows_local, span_len
):
    ranks, owned, block, kv = q_ref.shape
    rows = ranks * block
    batch_rank = lax.axis_index("batch")
    me = lax.axis_index("head")
    shown = pltpu.make_async_copy(
        part_ref, whole_ref.at[:, : part_ref.shape[1]], whole_sem.at[0]
    )
    shown.start()
    facts = []
    for r in range(owned):
        row = batch_rank * rows_local + me * owned + r
        target = jnp.int32(0)
        first = jnp.int32(0)
        length = jnp.int32(0)
        for c in range(lens_ref.shape[0]):
            start = jnp.int32(c * span_len)
            for k in range(lens_ref.shape[1]):
                hit = (owner_ref[c, k] == row).astype(jnp.int32)
                target = target + hit
                first = first + hit * start
                length = length + hit * lens_ref[c, k]
                start = start + lens_ref[c, k]
        first = lax.rem(first + batch_rank * span_len, 2 * span_len) * target
        length = jnp.where(target > 0, length, ctx_ref[r])
        facts.append((target, first, length))

    def copy_of(r, t):
        slot = lax.rem(t, depth)
        target, start, _ = facts[r]
        at = pl.multiple_of(start // blk * blk + t * blk, blk)

        @pl.when(target > 0)
        def _():
            own = spans_ref.shape[2]
            for c in range(blk // own):
                pltpu.make_async_copy(
                    spans_ref.at[at // own + c],
                    bufs.at[r, slot, :, c * own : (c + 1) * own],
                    sems.at[r, slot],
                ).start()

        @pl.when(target == 0)
        def _():
            pltpu.make_async_copy(
                cache_ref.at[r, :, pl.ds(at, blk)], bufs.at[r, slot], sems.at[r, slot]
            ).start()

    counts = []
    for r in range(owned):
        _, start, length = facts[r]
        counts.append((start + length + blk - 1) // blk - start // blk)
    for r in range(owned):
        for t in range(depth - 1):
            pl.when(t < counts[r])(functools.partial(copy_of, r, jnp.int32(t)))
    newest = new_ref[...].astype(jnp.float32)
    for r in range(owned):
        _, start, length = facts[r]
        base = start // blk * blk
        q = q_ref[:, r].reshape(rows, kv)
        fresh = jnp.concatenate(
            [newest[s, r : r + 1] for s in range(steps)]
            + [jnp.zeros((128 - steps, kv), jnp.float32)],
            axis=0,
        ).astype(jnp.bfloat16)
        s = trans_dot(q, fresh)
        row_step = (lax.broadcasted_iota(jnp.int32, s.shape, 0) // heads) % steps
        col = lax.broadcasted_iota(jnp.int32, s.shape, 1)
        s = jnp.where(col <= row_step, s, NEGATIVE)
        m = jnp.max(s, axis=1, keepdims=True)
        w = jnp.exp2((s - m) * scale)
        l_ref[...] = jnp.broadcast_to(jnp.sum(w, axis=1, keepdims=True), l_ref.shape)
        m_ref[...] = jnp.broadcast_to(m, m_ref.shape)
        acc_ref[...] = jnp.dot(
            w.astype(jnp.bfloat16), fresh[:, :lat], preferred_element_type=jnp.float32
        )

        def step(t, carry):
            slot = lax.rem(t, depth)
            pl.when(t + depth - 1 < counts[r])(lambda: copy_of(r, t + depth - 1))
            pltpu.make_async_copy(
                cache_ref.at[r, :, pl.ds(0, blk)], bufs.at[r, slot], sems.at[r, slot]
            ).wait()
            keys = bufs[r, slot]
            s = jnp.dot(q, keys, preferred_element_type=jnp.float32)
            place = base + t * blk + lax.broadcasted_iota(jnp.int32, (1, blk), 1)
            hide = jnp.where((place >= start) & (place < start + length), 0.0, NEGATIVE)
            s = s + hide
            old = m_ref[:, :1]
            new = jnp.maximum(old, jnp.max(s, axis=1, keepdims=True))
            alpha = jnp.exp2((old - new) * scale)
            w = jnp.exp2((s - new) * scale)
            l_new = l_ref[:, :1] * alpha + jnp.sum(w, axis=1, keepdims=True)
            l_ref[...] = jnp.broadcast_to(l_new, l_ref.shape)
            m_ref[...] = jnp.broadcast_to(new, m_ref.shape)
            acc_ref[...] = acc_ref[...] * alpha + trans_dot(w.astype(jnp.bfloat16), keys[:lat])
            return carry

        lax.fori_loop(0, counts[r], step, 0)
        done = (acc_ref[...] / l_ref[:, :1]).astype(out_ref.dtype)
        for p in range(ranks):
            out_ref[p, r] = done[p * block : (p + 1) * block]
    shown.wait()


def decode_pallas(lens, owner, ctx, query, newest, spans, part, cache, lat, heads, all_columns, width, rows_local, blk=512, depth=4):
    ranks, owned, block, kv = query.shape
    rows = ranks * block
    steps = block // heads
    span_len = part.shape[0]
    return pl.pallas_call(
        functools.partial(
            decode_kernel,
            lat=lat,
            heads=heads,
            steps=steps,
            blk=blk,
            depth=depth,
            scale=math.log2(math.e) / math.sqrt(width),
            rows_local=rows_local,
            span_len=span_len,
        ),
        out_shape=(
            jax.ShapeDtypeStruct((ranks, owned, block, lat), jnp.bfloat16),
            jax.ShapeDtypeStruct((span_len, all_columns), jnp.bfloat16),
        ),
        in_specs=[SMEM_SPEC] * 3
        + [VMEM_SPEC, VMEM_SPEC, pl.BlockSpec(memory_space=pl.ANY), VMEM_SPEC, HBM_SPEC],
        out_specs=(VMEM_SPEC, HBM_SPEC),
        scratch_shapes=[
            pltpu.VMEM((owned, depth, kv, blk), jnp.bfloat16),
            pltpu.SemaphoreType.DMA((owned, depth)),
            pltpu.SemaphoreType.DMA((1,)),
            pltpu.VMEM((rows, 128), jnp.float32),
            pltpu.VMEM((rows, 128), jnp.float32),
            pltpu.VMEM((rows, lat), jnp.float32),
        ],
        compiler_params=pltpu.CompilerParams(vmem_limit_bytes=40 << 20),
        cost_estimate=pl.CostEstimate(
            flops=5 * 10**9, bytes_accessed=10 << 20, transcendentals=2 << 20
        ),
    )(lens, owner, ctx, query, newest, spans, part, cache)


def return_kernel(
    lens_ref, rows_ref, spans_ref, lo_ref, kw_hbm, vw_hbm, q_hbm,
    back_ref, part_ref,
    kw, vw, qs, tools, load_sems, give_sems, take_sems,
    *, lat, ranks, look, scale, turn_at
):
    me = lax.axis_index("head")
    batch_rank = lax.axis_index("batch")
    some = qs.shape[0]
    skip = q_hbm.shape[0] - some
    barrier = pltpu.get_barrier_semaphore()
    for k in range(1, ranks):
        pl.semaphore_signal(
            barrier, inc=1, device_id={"head": (me + k) % ranks}, device_id_type=MESH
        )
    loads = [
        pltpu.make_async_copy(kw_hbm.at[:, skip * 128 :], kw, load_sems.at[0]),
        pltpu.make_async_copy(vw_hbm.at[:, skip * 128 :], vw, load_sems.at[1]),
        pltpu.make_async_copy(q_hbm.at[skip:], qs, load_sems.at[2]),
    ]
    for load in loads:
        load.start()
    keys, vals, hot, tri = tools[:4]
    start_marks(span_ends(lens_ref, batch_rank), keys, vals, hot, tri, rows_ref, lat)
    for load in loads:
        load.wait()
    gives = []
    for k in range(1, ranks):
        peer = (me + k) % ranks
        gives.append(
            pltpu.make_async_remote_copy(
                src_ref=lo_ref.at[peer],
                dst_ref=back_ref.at[me],
                send_sem=give_sems.at[k - 1],
                recv_sem=take_sems.at[k - 1],
                device_id={"head": peer},
                device_id_type=MESH,
            )
        )
    keep = pltpu.make_async_copy(lo_ref.at[me], back_ref.at[me], load_sems.at[3])
    keep.start()

    def before(j):
        @pl.when(j == turn_at)
        def _():
            pl.semaphore_wait(barrier, ranks - 1)
            for give in gives:
                give.start()

    shared = (kw, vw, qs, spans_ref, rows_ref, part_ref, lat, look, scale)
    attend_all(some // 4, tools, shared, before)
    for give in gives:
        give.wait()
    keep.wait()


def return_pallas(lens, rows, spans, latent_out, key_weight, value_weight, turned, rest, qb, turn_at):
    heads, width, span_len = turned.shape
    ranks = latent_out.shape[0]
    lat = key_weight.shape[0]
    kv = rows.shape[1]
    look = min(-(-(span_len // 2) // qb), span_len // qb - 1)
    bf16 = jnp.bfloat16
    return pl.pallas_call(
        functools.partial(
            return_kernel,
            lat=lat,
            ranks=ranks,
            look=look,
            scale=math.log2(math.e) / math.sqrt(width),
            turn_at=turn_at,
        ),
        out_shape=(
            jax.ShapeDtypeStruct(latent_out.shape, bf16),
            jax.ShapeDtypeStruct((span_len, rest * 128), bf16),
        ),
        in_specs=[SMEM_SPEC] + [VMEM_SPEC] * 3 + [HBM_SPEC] * 3,
        out_specs=(VMEM_SPEC,) * 2,
        scratch_shapes=[
            pltpu.VMEM((lat, rest * 128), bf16),
            pltpu.VMEM((lat, rest * 128), bf16),
            pltpu.VMEM((rest, width, span_len), bf16),
            attend_scratch(span_len, kv, lat, qb, look),
            pltpu.SemaphoreType.DMA((4,)),
            pltpu.SemaphoreType.DMA((ranks - 1,)),
            pltpu.SemaphoreType.DMA((ranks - 1,)),
        ],
        compiler_params=pltpu.CompilerParams(
            collective_id=1, has_side_effects=True, vmem_limit_bytes=40 << 20
        ),
        cost_estimate=pl.CostEstimate(
            flops=12 * 10**9, bytes_accessed=12 << 20, transcendentals=6 << 20
        ),
    )(lens, rows, spans, latent_out, key_weight, value_weight, turned)


def project_kernel(back_ref, vw_ref, part_ref, half_ref, out_ref, whole_ref, wide, sems, *, heads, lat):
    ranks, owned, block, _ = back_ref.shape
    steps = block // heads
    local = ranks * owned
    columns = part_ref.shape[1]
    shown = pltpu.make_async_copy(
        part_ref, whole_ref.at[:, whole_ref.shape[1] - columns :], sems.at[0]
    )
    shown.start()
    for p in range(ranks):
        for r in range(owned):
            at = (p * owned + r) * block
            for c in range(lat // 128):
                wide[c, at : at + block] = back_ref[p, r, :, c * 128 : (c + 1) * 128].astype(
                    jnp.float32
                )
    for h in range(heads):
        mine = jnp.concatenate(
            [
                jnp.concatenate(
                    [
                        wide[c, pl.ds(s * heads + h, local, stride=block), :]
                        for c in range(lat // 128)
                    ],
                    axis=1,
                )
                for s in range(steps)
            ],
            axis=0,
        ).astype(jnp.bfloat16)
        out_ref[:, h * 128 : (h + 1) * 128] = jnp.dot(
            mine, vw_ref[:, h * 128 : (h + 1) * 128], preferred_element_type=jnp.float32
        ).astype(jnp.bfloat16)
    shown.wait()


def project_pallas(back, value_weight, part, whole, heads):
    ranks, owned, block, lat = back.shape
    rows = ranks * owned * block
    return pl.pallas_call(
        functools.partial(project_kernel, heads=heads, lat=lat),
        out_shape=(
            jax.ShapeDtypeStruct((rows // heads, heads * 128), jnp.bfloat16),
            jax.ShapeDtypeStruct(whole.shape, whole.dtype),
        ),
        in_specs=[VMEM_SPEC, VMEM_SPEC, VMEM_SPEC, HBM_SPEC],
        out_specs=(VMEM_SPEC, HBM_SPEC),
        scratch_shapes=[
            pltpu.VMEM((lat // 128, rows, 128), jnp.float32),
            pltpu.SemaphoreType.DMA((1,)),
        ],
        input_output_aliases={3: 1},
        compiler_params=pltpu.CompilerParams(vmem_limit_bytes=24 << 20),
    )(back, value_weight, part, whole)


def on_device(
    latent_rows,
    pre_queries,
    pre_lengths,
    owner_map,
    context_cache,
    context_lengths,
    new_latent,
    dec_queries,
    key_weight,
    value_weight,
):
    steps, rows_local, heads, width = dec_queries.shape
    ranks = lax.axis_size("head")
    if heads % 16 or latent_rows.shape[0] % 128 or ranks % 2:
        return plain_on_device(
            latent_rows,
            pre_queries,
            pre_lengths,
            owner_map,
            context_cache,
            context_lengths,
            new_latent,
            dec_queries,
            key_weight,
            value_weight,
        )
    lat = key_weight.shape[0]
    owned = context_cache.shape[0]
    first = heads // 2
    qb = 256
    stay = lambda x: pltpu.with_memory_space_constraint(x, pltpu.HBM)
    turned = stay(jnp.transpose(pre_queries, (1, 2, 0)))
    kw_stay, vw_stay = stay(key_weight), stay(value_weight)
    spans, rows, query, part = gather_pallas(
        pre_lengths,
        stay(jnp.transpose(latent_rows)),
        stay(dec_queries.reshape(-1, width)),
        kw_stay,
        vw_stay,
        turned,
        owned,
        ranks,
        first,
        qb,
    )
    latent_out, whole = decode_pallas(
        pre_lengths,
        owner_map,
        context_lengths,
        query,
        new_latent,
        spans,
        part,
        stay(jnp.transpose(context_cache, (0, 2, 1))),
        lat,
        heads,
        heads * 128,
        width,
        rows_local,
    )
    back, rest = return_pallas(
        pre_lengths, rows, spans, latent_out, kw_stay, vw_stay, turned, heads - first, qb, 0
    )
    decode_out, prefill_out = project_pallas(back, value_weight, rest, whole, heads)
    return (prefill_out, decode_out.reshape(steps, rows_local, heads * 128))


def solution(mesh):
    placed = (
        P(("groups", "batch", "head"), None),
        P(("groups", "batch"), "head", None),
        P("groups", None),
        P("groups", None),
        P(("groups", "batch", "head"), None, None),
        P(("groups", "batch", "head")),
        P("groups", ("batch", "head"), None),
        P("groups", "batch", "head", None),
        P(None, "head"),
        P(None, "head"),
    )
    return jax.shard_map(
        on_device,
        mesh=mesh,
        in_specs=placed,
        out_specs=(P(("groups", "batch"), "head"), P("groups", "batch", "head")),
        check_vma=False,
    )
```

```python
import functools
import math

import jax
import jax.numpy as jnp
from jax import lax
from jax.experimental import pallas as pl
from jax.experimental.pallas import tpu as pltpu
from jax.sharding import PartitionSpec as P

BLK = 512


NEGATIVE = -1e30


def from_partner(value, axis, distance):
    mask = 2**distance
    pairs = [(source, source ^ mask) for source in range(lax.axis_size(axis))]
    return lax.ppermute(value, axis, pairs)


def request_table(pre_lengths, owner_map, span_len):
    seg_ends = jnp.cumsum(pre_lengths, axis=1)
    span_base = jnp.arange(pre_lengths.shape[0], dtype=jnp.int32)[:, None] * span_len
    seg_starts = seg_ends - pre_lengths + span_base
    return (owner_map.reshape(-1), seg_starts.reshape(-1), pre_lengths.reshape(-1))


def prefill_heads(own_span, queries, span_lengths, key_weight, value_weight):
    span_len, head_count, query_width = queries.shape
    head_size = key_weight.shape[1] // head_count
    lat_width = key_weight.shape[0]
    score_scale = 1.0 / math.sqrt(query_width)
    latent = own_span[:, :lat_width]
    rope_keys = own_span[:, lat_width:]
    keys_nope = (
        jnp.dot(latent, key_weight, preferred_element_type=jnp.float32)
        .astype(jnp.bfloat16)
        .reshape(span_len, head_count, head_size)
    )
    values = (
        jnp.dot(latent, value_weight, preferred_element_type=jnp.float32)
        .astype(jnp.bfloat16)
        .reshape(span_len, head_count, head_size)
    )
    scores = jnp.einsum(
        "qhd,khd->hqk", queries[:, :, :head_size], keys_nope, preferred_element_type=jnp.float32
    )
    scores = scores + jnp.einsum(
        "qhr,kr->hqk", queries[:, :, head_size:], rope_keys, preferred_element_type=jnp.float32
    )
    scores = scores * score_scale
    seg_ends = jnp.cumsum(span_lengths)
    places = jnp.arange(span_len, dtype=jnp.int32)
    segment = jnp.sum((places[:, None] >= seg_ends[None, :]).astype(jnp.int32), axis=1)
    allowed = (segment[:, None] == segment[None, :]) & (places[None, :] <= places[:, None])
    masked = jnp.where(allowed[None], scores, NEGATIVE)
    peak_score = jnp.max(masked, axis=2, keepdims=True)
    weights = jnp.exp(masked - peak_score)
    weight_sum = jnp.sum(weights, axis=2)
    mixed_out = jnp.einsum(
        "hqk,khd->qhd", weights.astype(jnp.bfloat16), values, preferred_element_type=jnp.float32
    )
    mixed_out = mixed_out / jnp.transpose(weight_sum)[:, :, None]
    return mixed_out.astype(jnp.bfloat16).reshape(span_len, head_count * head_size)


def plain_on_device(
    latent_rows,
    pre_queries,
    pre_lengths,
    owner_map,
    context_cache,
    context_lengths,
    new_latent,
    dec_queries,
    key_weight,
    value_weight,
):
    head_rank = lax.axis_index("head")
    batch_rank = lax.axis_index("batch")
    span_len = pre_queries.shape[0]
    kv_width = latent_rows.shape[1]
    own_span = lax.all_gather(latent_rows, "head", axis=0, tiled=True)
    other_span = from_partner(own_span, "batch", 0)
    first_span = jnp.where(batch_rank == 0, own_span, other_span)
    second_span = jnp.where(batch_rank == 0, other_span, own_span)
    all_spans = jnp.concatenate([first_span, second_span], axis=0)
    span_lengths = lax.dynamic_index_in_dim(pre_lengths, batch_rank, 0, keepdims=False)
    prefill_out = prefill_heads(own_span, pre_queries, span_lengths, key_weight, value_weight)
    step_total, rows_local, head_count, query_width = dec_queries.shape
    lat_width = key_weight.shape[0]
    head_size = key_weight.shape[1] // head_count
    owned_rows = context_cache.shape[0]
    score_scale = 1.0 / math.sqrt(query_width)
    key_heads = key_weight.reshape(lat_width, head_count, head_size)
    value_heads = value_weight.reshape(lat_width, head_count, head_size)
    absorbed = jnp.einsum(
        "srhd,lhd->srhl",
        dec_queries[..., :head_size],
        key_heads,
        preferred_element_type=jnp.float32,
    ).astype(jnp.bfloat16)
    query_all = jnp.concatenate([absorbed, dec_queries[..., head_size:]], axis=3)
    flat_owner, flat_start, flat_length = request_table(pre_lengths, owner_map, span_len)
    row_ids = (
        batch_rank * rows_local + head_rank * owned_rows + jnp.arange(owned_rows, dtype=jnp.int32)
    )
    matches = (flat_owner[None, :] == row_ids[:, None]).astype(jnp.int32)
    is_target = jnp.sum(matches, axis=1) > 0
    first_row = jnp.sum(matches * flat_start[None, :], axis=1)
    prompt_len = jnp.sum(matches * flat_length[None, :], axis=1)
    effective = jnp.where(is_target, prompt_len, context_lengths)
    padded = jnp.concatenate([all_spans, jnp.zeros((span_len, kv_width), all_spans.dtype)], axis=0)
    replaced = jax.vmap(lambda offset: lax.dynamic_slice_in_dim(padded, offset, span_len, 0))(
        first_row
    )
    front_rows = jnp.where(is_target[:, None, None], replaced, context_cache[:, :span_len])
    front_blocks = span_len // BLK
    needed = (jnp.max(effective) + BLK - 1) // BLK
    fresh_latent = new_latent[..., :lat_width]
    owned_query = lax.all_to_all(query_all, "head", split_axis=1, concat_axis=2, tiled=True)
    fresh_scores = (
        jnp.einsum("srhk,jrk->srhj", owned_query, new_latent, preferred_element_type=jnp.float32)
        * score_scale
    )
    visible = (
        jnp.arange(new_latent.shape[0], dtype=jnp.int32)[None, :]
        <= jnp.arange(step_total, dtype=jnp.int32)[:, None]
    )
    fresh_scores = jnp.where(visible[:, None, None, :], fresh_scores, NEGATIVE)
    peak_score = jnp.max(fresh_scores, axis=3)
    weights = jnp.exp(fresh_scores - peak_score[..., None])
    weight_sum = jnp.sum(weights, axis=3)
    running = jnp.einsum(
        "srhj,jrl->srhl",
        weights.astype(jnp.bfloat16),
        fresh_latent,
        preferred_element_type=jnp.float32,
    )

    def advance(block_index, state_tuple, source):
        old_peak, old_sum, old_running = state_tuple
        key_block = lax.dynamic_slice_in_dim(source, block_index * BLK, BLK, 1)
        scores = (
            jnp.einsum("srhk,rtk->srht", owned_query, key_block, preferred_element_type=jnp.float32)
            * score_scale
        )
        places = block_index * BLK + jnp.arange(BLK, dtype=jnp.int32)
        in_context = places[None, :] < effective[:, None]
        scores = jnp.where(in_context[None, :, None, :], scores, NEGATIVE)
        new_peak = jnp.maximum(old_peak, jnp.max(scores, axis=3))
        factor = jnp.exp(old_peak - new_peak)
        block_weights = jnp.exp(scores - new_peak[..., None])
        new_sum = old_sum * factor + jnp.sum(block_weights, axis=3)
        new_running = old_running * factor[..., None] + jnp.einsum(
            "srht,rtl->srhl",
            block_weights.astype(jnp.bfloat16),
            key_block[..., :lat_width],
            preferred_element_type=jnp.float32,
        )
        return (new_peak, new_sum, new_running)

    state_tuple = lax.fori_loop(
        0,
        jnp.minimum(needed, front_blocks),
        lambda block_index, state_now: advance(block_index, state_now, front_rows),
        (peak_score, weight_sum, running),
    )
    state_tuple = lax.fori_loop(
        front_blocks,
        jnp.maximum(needed, front_blocks),
        lambda block_index, state_now: advance(block_index, state_now, context_cache),
        state_tuple,
    )
    latent_out = (state_tuple[2] / state_tuple[1][..., None]).astype(jnp.bfloat16)
    returned = lax.all_to_all(latent_out, "head", split_axis=2, concat_axis=1, tiled=True)
    projected = jnp.einsum(
        "srhl,lhd->srhd", returned, value_heads, preferred_element_type=jnp.float32
    ).astype(jnp.bfloat16)
    decode_out = projected.reshape(query_all.shape[0], rows_local, head_count * head_size)
    return (prefill_out, decode_out)


def trans_dot(left, right):
    return lax.dot_general(
        left, right, (((1,), (1,)), ((), ())), preferred_element_type=jnp.float32
    )


MESH = pl.DeviceIdType.MESH


def place_of(rank, ranks):
    odd = rank % 2
    return (1 - odd) * (rank // 2) + odd * (ranks - 1 - rank // 2)


def rank_at(place, ranks):
    late = place // (ranks // 2)
    return (1 - late) * (2 * place) + late * (2 * (ranks - 1 - place) + 1)


def start_marks(ends, both_keys, both_vals, hot, tri, rows_ref, lat):
    pair, span_len, full = both_keys[0].shape
    segs = len(ends)
    marks = full - 128 - (rows_ref.shape[1] - lat)
    where = lax.broadcasted_iota(jnp.int32, (span_len, marks), 0)
    lane = lax.broadcasted_iota(jnp.int32, (span_len, marks), 1)
    place = lax.broadcasted_iota(jnp.int32, (marks, span_len), 1)
    line = lax.broadcasted_iota(jnp.int32, (marks, span_len), 0)
    mine = jnp.zeros((span_len, marks), jnp.int32)
    seen = jnp.zeros((marks, span_len), jnp.int32)
    for k in range(segs - 1):
        mine = mine + (where >= ends[k]).astype(jnp.int32)
        seen = seen + (place >= ends[k]).astype(jnp.int32)
    mark = jnp.where((lane < segs) & (lane != mine), NEGATIVE, 0.0).astype(jnp.bfloat16)
    hot[...] = jnp.where(line == seen, 1.0, 0.0).astype(jnp.bfloat16)
    for keys, vals in zip(both_keys, both_vals):
        for p in range(pair):
            keys[p, :, 128 : full - marks] = rows_ref[:, lat:]
            keys[p, :, full - marks :] = mark
            vals[p, 128:, :] = jnp.ones((vals.shape[1] - 128, span_len), jnp.bfloat16)
    size = tri.shape[0]
    key_at = lax.broadcasted_iota(jnp.int32, (size, size), 0)
    query_at = lax.broadcasted_iota(jnp.int32, (size, size), 1)
    tri[...] = jnp.where(key_at <= query_at, 0.0, NEGATIVE)


def value_piece(c, turned, spans_ref, vals, lat):
    latents = jnp.concatenate([spans_ref[2 * c, :lat, :], spans_ref[2 * c + 1, :lat, :]], axis=1)
    value = jnp.dot(turned[...], latents, preferred_element_type=jnp.float32).astype(jnp.bfloat16)
    for p in range(vals.shape[0]):
        vals[p, :128, c * 256 : (c + 1) * 256] = value[p * 128 : (p + 1) * 128]


def key_piece(rows, columns, kw, rows_ref, keys, lat):
    made = jnp.dot(rows_ref[rows, :lat], kw[:, columns], preferred_element_type=jnp.float32)
    made = made.astype(jnp.bfloat16)
    for p in range(keys.shape[0]):
        keys[p, rows, :128] = made[:, p * 128 : (p + 1) * 128]


def projections(g, kw, vw, spans_ref, rows_ref, turned, keys, vals, lat):
    pair, span_len, _ = keys.shape
    wide = pair * 128
    columns = pl.ds(pl.multiple_of(g * wide, wide), wide)

    def turn():
        turned[...] = jnp.transpose(vw[:, columns])

    half = span_len // 2
    pieces = [turn]
    for k in range(2):
        rows = slice(k * half, (k + 1) * half)
        pieces.append(functools.partial(key_piece, rows, columns, kw, rows_ref, keys, lat))
    for c in range(span_len // 256):
        pieces.append(functools.partial(value_piece, c, turned, spans_ref, vals, lat))
    return pieces


def attention(g, qs, keys, vals, hot, tri, part_ref, scores, weights, look, scale, others):
    pair, span_len, _ = keys.shape
    qb = tri.shape[0]
    blocks = span_len // qb
    order = [(0, 0)] + [(i, p) for i in range(1, blocks) for p in range(pair)]
    order += [(0, p) for p in range(1, pair)]
    count = len(order)
    lengths = [min(i, look) + 1 for i, _ in order]
    peaks = [None] * count
    tops = [None] * count
    sums = [None] * count

    def score(n, c):
        i, p = order[n]
        at = (i - lengths[n] + 1 + c) * qb
        query = jnp.concatenate(
            [qs[g * pair + p, :, i * qb : (i + 1) * qb], hot[:, i * qb : (i + 1) * qb]], axis=0
        )
        s = jnp.dot(keys[p, at : at + qb, :], query, preferred_element_type=jnp.float32)
        if c == lengths[n] - 1:
            s = s + tri[...]
        scores[n % 2][c * qb : (c + 1) * qb, :] = s
        top = jnp.max(s.reshape(qb // 8, 8, qb), axis=0)
        peaks[n] = top if peaks[n] is None else jnp.maximum(peaks[n], top)

    def soften(n, c):
        if c == 0:
            tops[n] = jnp.max(peaks[n], axis=0, keepdims=True)
        s = scores[n % 2][c * qb : (c + 1) * qb, :]
        w = jnp.exp2((s - tops[n]) * scale)
        weights[n % 2][c * qb : (c + 1) * qb, :] = w.astype(jnp.bfloat16)

    def mix(n, c):
        i, p = order[n]
        at = (i - lengths[n] + 1 + c) * qb
        o = jnp.dot(
            vals[p, :, at : at + qb],
            weights[n % 2][c * qb : (c + 1) * qb, :],
            preferred_element_type=jnp.float32,
        )
        sums[n] = o if sums[n] is None else sums[n] + o
        if c == lengths[n] - 1:
            o = sums[n]
            o = o[:128] * (1.0 / o[128:129])
            columns = pl.ds(pl.multiple_of((g * pair + p) * 128, 128), 128)
            part_ref[i * qb : (i + 1) * qb, columns] = jnp.transpose(o.astype(jnp.bfloat16))

    todo_score = [(n, c) for n in range(count) for c in range(lengths[n])]
    todo_soft = list(todo_score)
    todo_mix = list(todo_score)
    total = len(todo_score)
    scored = [0] * count
    softened = [0] * count
    mixed = [0] * count
    others = list(others)
    every = total / max(len(others), 1)
    done = 0
    step = 0
    while todo_mix:
        was = list(softened)
        if todo_score:
            n, c = todo_score[0]
            if n < 2 or softened[n - 2] == lengths[n - 2]:
                score(n, c)
                scored[n] += 1
                todo_score.pop(0)
        if todo_soft:
            n, c = todo_soft[0]
            free = n < 2 or mixed[n - 2] == lengths[n - 2]
            if scored[n] == lengths[n] and free and not (todo_score and todo_score[0][0] <= n):
                soften(n, c)
                softened[n] += 1
                todo_soft.pop(0)
        n, c = todo_mix[0]
        if c < was[n]:
            mix(n, c)
            mixed[n] += 1
            todo_mix.pop(0)
        step += 1
        while done < len(others) and done * every <= step - 1:
            others[done]()
            done += 1
    while done < len(others):
        others[done]()
        done += 1


def attend_all(turns, tools, shared, before):
    kw, vw, qs, spans_ref, rows_ref, part_ref, lat, look, scale = shared
    keys, vals, hot, tri, turned, scores, weights = tools
    for piece in projections(0, kw, vw, spans_ref, rows_ref, turned[0], keys[0], vals[0], lat):
        piece()

    def step(j, carry):
        before(j)
        for side in range(2):
            g = 2 * j + side
            following = jnp.minimum(g + 1, 2 * turns - 1)
            others = projections(
                following, kw, vw, spans_ref, rows_ref,
                turned[1 - side], keys[1 - side], vals[1 - side], lat,
            )
            attention(
                g, qs, keys[side], vals[side], hot, tri, part_ref,
                scores, weights, look, scale, others,
            )
        return carry

    lax.fori_loop(0, turns, step, 0)


def absorb_into(dq, kw, sent, flat, wide, heads, lat):
    rows = dq.shape[0]
    ranks, owned, block, _ = sent.shape
    steps = block // heads
    local = ranks * owned
    flat[...] = dq[:, :128].astype(jnp.float32)
    for h in range(heads):
        mine = flat[pl.ds(h, rows // heads, stride=heads), :].astype(jnp.bfloat16)
        res = trans_dot(mine, kw[:, h * 128 : (h + 1) * 128])
        for s in range(steps):
            for c in range(lat // 128):
                wide[c, pl.ds(s * heads + h, local, stride=block), :] = res[
                    s * local : (s + 1) * local, c * 128 : (c + 1) * 128
                ]
    for p in range(ranks):
        for r in range(owned):
            at = p * owned + r
            for c in range(lat // 128):
                sent[p, r, :, c * 128 : (c + 1) * 128] = wide[
                    c, at * block : (at + 1) * block
                ].astype(jnp.bfloat16)
            for s in range(steps):
                start = (s * local + at) * heads
                sent[p, r, s * heads : (s + 1) * heads, lat:] = dq[start : start + heads, 128:]


def span_ends(lens_ref, batch_rank):
    ends = []
    total = 0
    for k in range(lens_ref.shape[1]):
        total = total + lens_ref[batch_rank, k]
        ends.append(total)
    return ends


def gather_kernel(
    lens_ref, shard_hbm, dq_hbm, kw_hbm, vw_hbm, q_hbm,
    spans_ref, rows_ref, got_ref, part_ref,
    kw, vw, qs, dq, flat, wide, sent, tools,
    load_sems, ring_send, ring_recv, swap_sems, give_sems, take_sems,
    *, lat, ranks, heads, look, scale
):
    me = lax.axis_index("head")
    batch_rank = lax.axis_index("batch")
    place = place_of(me, ranks)
    right = rank_at((place + 1) % ranks, ranks)
    left = rank_at((place + ranks - 1) % ranks, ranks)
    some = qs.shape[0]
    loads = [
        pltpu.make_async_copy(dq_hbm, dq, load_sems.at[0]),
        pltpu.make_async_copy(kw_hbm, kw, load_sems.at[1]),
        pltpu.make_async_copy(shard_hbm, spans_ref.at[me], load_sems.at[2]),
        pltpu.make_async_copy(vw_hbm.at[:, : some * 128], vw, load_sems.at[3]),
        pltpu.make_async_copy(q_hbm.at[:some], qs, load_sems.at[4]),
    ]
    barrier = pltpu.get_barrier_semaphore()
    for k in range(1, ranks):
        pl.semaphore_signal(
            barrier, inc=1, device_id={"head": (me + k) % ranks}, device_id_type=MESH
        )
    pl.semaphore_signal(
        barrier, inc=1, device_id={"batch": 1 - batch_rank}, device_id_type=MESH
    )
    for load in loads:
        load.start()
    pl.semaphore_wait(barrier, ranks)

    half = shard_hbm.shape[0] // 2
    most = ranks // 2

    def hop(way, part, t):
        back = t - 1 if way == 0 else ranks - t + 1
        origin = rank_at((place + ranks - back) % ranks, ranks)
        rows = pl.ds(part * half, half)
        source = shard_hbm.at[rows] if t == 1 else spans_ref.at[origin, rows]
        return pltpu.make_async_remote_copy(
            src_ref=source,
            dst_ref=spans_ref.at[origin, rows],
            send_sem=ring_send.at[way, part, t - 1],
            recv_sem=ring_recv.at[way, part, t - 1],
            device_id={"head": right if way == 0 else left},
            device_id_type=MESH,
        )

    def hops(way, part):
        return most if way == part else most - 1

    streams = [(0, 0), (1, 1), (0, 1), (1, 0)]
    for way, part in streams:
        hop(way, part, 1).start()
    loads[0].wait()
    loads[1].wait()
    absorb_into(dq, kw, sent, flat, wide, heads, lat)

    own = shard_hbm.shape[1]

    def turn(origin):
        rows_ref[pl.ds(pl.multiple_of(origin * own, own), own), :] = jnp.transpose(
            spans_ref[origin]
        )

    loads[2].wait()
    turn(me)
    for t in range(1, most + 1):
        for way, part in streams:
            if t <= hops(way, part):
                hop(way, part, t).wait_recv()
                if t < hops(way, part):
                    hop(way, part, t + 1).start()
        turn(rank_at((place + ranks - t) % ranks, ranks))
        if t < most:
            turn(rank_at((place + t) % ranks, ranks))

    gives = []
    for k in range(1, ranks):
        peer = (me + k) % ranks
        gives.append(
            pltpu.make_async_remote_copy(
                src_ref=sent.at[peer],
                dst_ref=got_ref.at[me],
                send_sem=give_sems.at[k - 1],
                recv_sem=take_sems.at[k - 1],
                device_id={"head": peer},
                device_id_type=MESH,
            )
        )
    for give in gives:
        give.start()
    keep = pltpu.make_async_copy(sent.at[me], got_ref.at[me], load_sems.at[5])
    keep.start()
    swap = pltpu.make_async_remote_copy(
        src_ref=spans_ref.at[:ranks],
        dst_ref=spans_ref.at[ranks:],
        send_sem=swap_sems.at[0],
        recv_sem=swap_sems.at[1],
        device_id={"batch": 1 - batch_rank},
        device_id_type=MESH,
    )
    swap.start()
    loads[3].wait()
    loads[4].wait()
    keys, vals, hot, tri = tools[:4]
    start_marks(span_ends(lens_ref, batch_rank), keys, vals, hot, tri, rows_ref, lat)

    shared = (kw, vw, qs, spans_ref, rows_ref, part_ref, lat, look, scale)
    attend_all(some // 4, tools, shared, lambda j: None)
    for way, part in streams:
        for t in range(1, hops(way, part) + 1):
            hop(way, part, t).wait_send()
    for give in gives:
        give.wait()
    keep.wait()
    swap.wait()


HBM_SPEC = pl.BlockSpec(memory_space=pltpu.HBM)
VMEM_SPEC = pl.BlockSpec(memory_space=pltpu.VMEM)
SMEM_SPEC = pl.BlockSpec(memory_space=pltpu.SMEM)


def attend_scratch(span_len, kv, lat, qb, look):
    pair = 2
    marks = 128 - (kv - lat)
    bf16 = jnp.bfloat16
    twice = lambda shape, dtype: [pltpu.VMEM(shape, dtype)] * 2
    return [
        twice((pair, span_len, 256), bf16),
        twice((pair, 128 + 16, span_len), bf16),
        pltpu.VMEM((marks, span_len), bf16),
        pltpu.VMEM((qb, qb), jnp.float32),
        twice((pair * 128, lat), bf16),
        twice(((look + 1) * qb, qb), jnp.float32),
        twice(((look + 1) * qb, qb), bf16),
    ]


def gather_pallas(lens, shard, flat_queries, key_weight, value_weight, turned, owned, ranks, first, qb):
    heads, width, span_len = turned.shape
    kv, own = shard.shape
    lat = key_weight.shape[0]
    rows = flat_queries.shape[0]
    block = rows // (ranks * owned)
    look = min(-(-(span_len // 2) // qb), span_len // qb - 1)
    bf16 = jnp.bfloat16
    return pl.pallas_call(
        functools.partial(
            gather_kernel,
            lat=lat,
            ranks=ranks,
            heads=heads,
            look=look,
            scale=math.log2(math.e) / math.sqrt(width),
        ),
        out_shape=(
            jax.ShapeDtypeStruct((2 * ranks, kv, own), bf16),
            jax.ShapeDtypeStruct((span_len, kv), bf16),
            jax.ShapeDtypeStruct((ranks, owned, block, kv), bf16),
            jax.ShapeDtypeStruct((span_len, first * 128), bf16),
        ),
        in_specs=[SMEM_SPEC] + [HBM_SPEC] * 5,
        out_specs=(VMEM_SPEC,) * 4,
        scratch_shapes=[
            pltpu.VMEM(key_weight.shape, bf16),
            pltpu.VMEM((lat, first * 128), bf16),
            pltpu.VMEM((first, width, span_len), bf16),
            pltpu.VMEM((rows, width), bf16),
            pltpu.VMEM((rows, 128), jnp.float32),
            pltpu.VMEM((lat // 128, rows, 128), jnp.float32),
            pltpu.VMEM((ranks, owned, block, kv), bf16),
            attend_scratch(span_len, kv, lat, qb, look),
            pltpu.SemaphoreType.DMA((6,)),
            pltpu.SemaphoreType.DMA((2, 2, ranks // 2)),
            pltpu.SemaphoreType.DMA((2, 2, ranks // 2)),
            pltpu.SemaphoreType.DMA((2,)),
            pltpu.SemaphoreType.DMA((ranks - 1,)),
            pltpu.SemaphoreType.DMA((ranks - 1,)),
        ],
        compiler_params=pltpu.CompilerParams(
            collective_id=0, has_side_effects=True, vmem_limit_bytes=40 << 20
        ),
        cost_estimate=pl.CostEstimate(
            flops=12 * 10**9, bytes_accessed=12 << 20, transcendentals=6 << 20
        ),
    )(lens, shard, flat_queries, key_weight, value_weight, turned)


def decode_kernel(
    lens_ref, owner_ref, ctx_ref, q_ref, new_ref, spans_ref, part_ref, cache_ref,
    out_ref, whole_ref,
    bufs, sems, whole_sem, tools,
    *, lat, heads, steps, blk, depth, scale, rows_local, span_len
):
    ranks, owned, block, kv = q_ref.shape
    rows = ranks * block
    batch_rank = lax.axis_index("batch")
    me = lax.axis_index("head")
    shown = pltpu.make_async_copy(
        part_ref, whole_ref.at[:, : part_ref.shape[1]], whole_sem.at[0]
    )
    shown.start()
    facts = []
    for r in range(owned):
        row = batch_rank * rows_local + me * owned + r
        target = jnp.int32(0)
        first = jnp.int32(0)
        length = jnp.int32(0)
        for c in range(lens_ref.shape[0]):
            start = jnp.int32(c * span_len)
            for k in range(lens_ref.shape[1]):
                hit = (owner_ref[c, k] == row).astype(jnp.int32)
                target = target + hit
                first = first + hit * start
                length = length + hit * lens_ref[c, k]
                start = start + lens_ref[c, k]
        first = lax.rem(first + batch_rank * span_len, 2 * span_len) * target
        length = jnp.where(target > 0, length, ctx_ref[r])
        facts.append((target, first, length))

    counts = []
    for r in range(owned):
        _, start, length = facts[r]
        counts.append((start + length + blk - 1) // blk - start // blk)
    turns = [(count + 1) // 2 for count in counts]

    def copy_of(r, t):
        slot = lax.rem(t, depth)
        target, start, _ = facts[r]
        at = pl.multiple_of((start // blk + jnp.minimum(t, counts[r] - 1)) * blk, blk)

        @pl.when(target > 0)
        def _():
            own = spans_ref.shape[2]
            for c in range(blk // own):
                pltpu.make_async_copy(
                    spans_ref.at[at // own + c],
                    bufs.at[r, slot, :, c * own : (c + 1) * own],
                    sems.at[r, slot],
                ).start()

        @pl.when(target == 0)
        def _():
            pltpu.make_async_copy(
                cache_ref.at[r, :, pl.ds(at, blk)], bufs.at[r, slot], sems.at[r, slot]
            ).start()

    for r in range(owned):
        for t in range(3):
            copy_of(r, jnp.int32(t))
    newest = new_ref[...].astype(jnp.float32)
    full = tools[0][3].shape[1]
    tail = lax.broadcasted_iota(jnp.int32, (rows, full - kv), 1)
    lanes = lax.broadcasted_iota(jnp.int32, (rows, 128), 1)
    piece = 256

    def request(r, tools):
        peak_ref, sum_ref, acc_ref, asked, scores, tops, weights, fades = tools
        _, start, length = facts[r]
        base = start // blk * blk
        q = q_ref[:, r].reshape(rows, kv)
        asked[:, :kv] = q
        asked[:, kv:] = jnp.where(tail == 0, 1.0, 0.0).astype(jnp.bfloat16)
        fresh = jnp.concatenate(
            [newest[s, r : r + 1] for s in range(steps)]
            + [jnp.zeros((128 - steps, kv), jnp.float32)],
            axis=0,
        ).astype(jnp.bfloat16)

        def take(t):
            slot = lax.rem(t, depth)
            pltpu.make_async_copy(
                cache_ref.at[r, :, pl.ds(0, blk)], bufs.at[r, slot], sems.at[r, slot]
            ).wait()

        def score(t, side, c):
            slot = lax.rem(t, depth)
            place = base + t * blk + c * piece + lax.broadcasted_iota(jnp.int32, (16, piece), 1)
            hide = jnp.where((place >= start) & (place < start + length), 0.0, NEGATIVE)
            hide = hide.astype(jnp.bfloat16)
            keys = jnp.concatenate(
                [bufs[r, slot, :, c * piece : (c + 1) * piece]] + [hide] * ((full - kv) // 16),
                axis=0,
            )
            s = jnp.dot(asked[...], keys, preferred_element_type=jnp.float32)
            scores[side][:, c * piece : (c + 1) * piece] = s
            top = jnp.maximum(s[:, :128], s[:, 128:])
            if c > 0:
                top = jnp.maximum(top, tops[side][...])
            tops[side][...] = top

        def settle(side):
            old = peak_ref[...]
            new = jnp.maximum(old, jnp.max(tops[side][...], axis=1, keepdims=True))
            fade = jnp.exp2((old - new) * scale)
            fades[side][...] = fade
            peak_ref[...] = new
            sum_ref[...] = sum_ref[...] * fade

        def soften(side, c):
            at = slice(c * piece, (c + 1) * piece)
            new = peak_ref[...]
            s = scores[side][:, at]
            left = jnp.exp2((s[:, :128] - new) * scale)
            right = jnp.exp2((s[:, 128:] - new) * scale)
            sum_ref[...] = sum_ref[...] + (left + right)
            weights[side][:, at] = jnp.concatenate([left, right], axis=1).astype(jnp.bfloat16)

        def mix(t, side, c):
            slot = lax.rem(jnp.maximum(t, 0), depth)
            at = slice(c * piece, (c + 1) * piece)
            made = trans_dot(weights[side][...], bufs[r, slot, at, :])
            fade = fades[side][...]
            for k in range(piece // 128):
                columns = slice(c * piece + k * 128, c * piece + (k + 1) * 128)
                acc_ref[:, columns] = (
                    acc_ref[:, columns] * fade + made[:, k * 128 : (k + 1) * 128]
                )

        def begin():
            s = trans_dot(q, fresh)
            row_step = (lax.broadcasted_iota(jnp.int32, s.shape, 0) // heads) % steps
            s = jnp.where(lanes <= row_step, s, NEGATIVE)
            m = jnp.max(s, axis=1, keepdims=True)
            w = jnp.exp2((s - m) * scale)
            sum_ref[...] = w
            peak_ref[...] = jnp.broadcast_to(m, peak_ref.shape)
            acc_ref[...] = jnp.dot(
                w.astype(jnp.bfloat16), fresh[:, :lat], preferred_element_type=jnp.float32
            )
            weights[1][...] = jnp.zeros(weights[1].shape, jnp.bfloat16)
            fades[1][...] = jnp.ones(fades[1].shape, jnp.float32)

        def lead(c):
            score(jnp.int32(0), 0, c)

        def turn(j, carry):
            for k in (3, 4):
                pl.when(2 * j + k <= 2 * turns[r])(functools.partial(copy_of, r, 2 * j + k))
            take(2 * j + 1)
            take(2 * j + 2)
            for side in range(2):
                t = 2 * j + side
                settle(side)
                for c in range(blk // piece):
                    score(t + 1, 1 - side, c)
                    soften(side, c)
                    mix(t - 1, 1 - side, c)
            return carry

        def last(c):
            mix(2 * turns[r] - 1, 1, c)

        def finish():
            total = jnp.sum(sum_ref[...], axis=1, keepdims=True)
            done = (acc_ref[...] * (1.0 / total)).astype(out_ref.dtype)
            for p in range(ranks):
                out_ref[p, r] = done[p * block : (p + 1) * block]

        return take, begin, lead, turn, last, finish

    asks = [request(r, tools[r]) for r in range(owned)]
    for ask in asks:
        ask[1]()
    for ask in asks:
        ask[0](jnp.int32(0))
    for c in range(blk // piece):
        for ask in asks:
            ask[2](c)
    for r in range(owned):
        lax.fori_loop(0, turns[r], asks[r][3], 0)
    for c in range(lat // piece):
        for ask in asks:
            ask[4](c)
    for ask in asks:
        ask[5]()
    shown.wait()


def decode_pallas(lens, owner, ctx, query, newest, spans, part, cache, lat, heads, all_columns, width, rows_local, blk=512, depth=6):
    ranks, owned, block, kv = query.shape
    rows = ranks * block
    steps = block // heads
    span_len = part.shape[0]
    return pl.pallas_call(
        functools.partial(
            decode_kernel,
            lat=lat,
            heads=heads,
            steps=steps,
            blk=blk,
            depth=depth,
            scale=math.log2(math.e) / math.sqrt(width),
            rows_local=rows_local,
            span_len=span_len,
        ),
        out_shape=(
            jax.ShapeDtypeStruct((ranks, owned, block, lat), jnp.bfloat16),
            jax.ShapeDtypeStruct((span_len, all_columns), jnp.bfloat16),
        ),
        in_specs=[SMEM_SPEC] * 3
        + [VMEM_SPEC, VMEM_SPEC, pl.BlockSpec(memory_space=pl.ANY), VMEM_SPEC, HBM_SPEC],
        out_specs=(VMEM_SPEC, HBM_SPEC),
        scratch_shapes=[
            pltpu.VMEM((owned, depth, kv, blk), jnp.bfloat16),
            pltpu.SemaphoreType.DMA((owned, depth)),
            pltpu.SemaphoreType.DMA((1,)),
            [
                [
                    pltpu.VMEM((rows, 128), jnp.float32),
                    pltpu.VMEM((rows, 128), jnp.float32),
                    pltpu.VMEM((rows, lat), jnp.float32),
                    pltpu.VMEM((rows, -(-(kv + 16) // 128) * 128), jnp.bfloat16),
                    [pltpu.VMEM((rows, blk), jnp.float32)] * 2,
                    [pltpu.VMEM((rows, 128), jnp.float32)] * 2,
                    [pltpu.VMEM((rows, blk), jnp.bfloat16)] * 2,
                    [pltpu.VMEM((rows, 128), jnp.float32)] * 2,
                ]
            ]
            * owned,
        ],
        compiler_params=pltpu.CompilerParams(vmem_limit_bytes=40 << 20),
        cost_estimate=pl.CostEstimate(
            flops=5 * 10**9, bytes_accessed=10 << 20, transcendentals=2 << 20
        ),
    )(lens, owner, ctx, query, newest, spans, part, cache)


def return_kernel(
    lens_ref, rows_ref, spans_ref, lo_ref, kw_hbm, vw_hbm, q_hbm,
    back_ref, part_ref,
    kw, vw, qs, tools, load_sems, give_sems, take_sems,
    *, lat, ranks, look, scale, turn_at
):
    me = lax.axis_index("head")
    batch_rank = lax.axis_index("batch")
    some = qs.shape[0]
    skip = q_hbm.shape[0] - some
    barrier = pltpu.get_barrier_semaphore()
    for k in range(1, ranks):
        pl.semaphore_signal(
            barrier, inc=1, device_id={"head": (me + k) % ranks}, device_id_type=MESH
        )
    loads = [
        pltpu.make_async_copy(kw_hbm.at[:, skip * 128 :], kw, load_sems.at[0]),
        pltpu.make_async_copy(vw_hbm.at[:, skip * 128 :], vw, load_sems.at[1]),
        pltpu.make_async_copy(q_hbm.at[skip:], qs, load_sems.at[2]),
    ]
    for load in loads:
        load.start()
    keys, vals, hot, tri = tools[:4]
    start_marks(span_ends(lens_ref, batch_rank), keys, vals, hot, tri, rows_ref, lat)
    for load in loads:
        load.wait()
    gives = []
    for k in range(1, ranks):
        peer = (me + k) % ranks
        gives.append(
            pltpu.make_async_remote_copy(
                src_ref=lo_ref.at[peer],
                dst_ref=back_ref.at[me],
                send_sem=give_sems.at[k - 1],
                recv_sem=take_sems.at[k - 1],
                device_id={"head": peer},
                device_id_type=MESH,
            )
        )
    keep = pltpu.make_async_copy(lo_ref.at[me], back_ref.at[me], load_sems.at[3])
    keep.start()

    def before(j):
        @pl.when(j == turn_at)
        def _():
            pl.semaphore_wait(barrier, ranks - 1)
            for give in gives:
                give.start()

    shared = (kw, vw, qs, spans_ref, rows_ref, part_ref, lat, look, scale)
    attend_all(some // 4, tools, shared, before)
    for give in gives:
        give.wait()
    keep.wait()


def return_pallas(lens, rows, spans, latent_out, key_weight, value_weight, turned, rest, qb, turn_at):
    heads, width, span_len = turned.shape
    ranks = latent_out.shape[0]
    lat = key_weight.shape[0]
    kv = rows.shape[1]
    look = min(-(-(span_len // 2) // qb), span_len // qb - 1)
    bf16 = jnp.bfloat16
    return pl.pallas_call(
        functools.partial(
            return_kernel,
            lat=lat,
            ranks=ranks,
            look=look,
            scale=math.log2(math.e) / math.sqrt(width),
            turn_at=turn_at,
        ),
        out_shape=(
            jax.ShapeDtypeStruct(latent_out.shape, bf16),
            jax.ShapeDtypeStruct((span_len, rest * 128), bf16),
        ),
        in_specs=[SMEM_SPEC] + [VMEM_SPEC] * 3 + [HBM_SPEC] * 3,
        out_specs=(VMEM_SPEC,) * 2,
        scratch_shapes=[
            pltpu.VMEM((lat, rest * 128), bf16),
            pltpu.VMEM((lat, rest * 128), bf16),
            pltpu.VMEM((rest, width, span_len), bf16),
            attend_scratch(span_len, kv, lat, qb, look),
            pltpu.SemaphoreType.DMA((4,)),
            pltpu.SemaphoreType.DMA((ranks - 1,)),
            pltpu.SemaphoreType.DMA((ranks - 1,)),
        ],
        compiler_params=pltpu.CompilerParams(
            collective_id=1, has_side_effects=True, vmem_limit_bytes=40 << 20
        ),
        cost_estimate=pl.CostEstimate(
            flops=12 * 10**9, bytes_accessed=12 << 20, transcendentals=6 << 20
        ),
    )(lens, rows, spans, latent_out, key_weight, value_weight, turned)


def project_kernel(back_ref, vw_ref, part_ref, half_ref, out_ref, whole_ref, wide, sems, *, heads, lat):
    ranks, owned, block, _ = back_ref.shape
    steps = block // heads
    local = ranks * owned
    columns = part_ref.shape[1]
    shown = pltpu.make_async_copy(
        part_ref, whole_ref.at[:, whole_ref.shape[1] - columns :], sems.at[0]
    )
    shown.start()
    for p in range(ranks):
        for r in range(owned):
            at = (p * owned + r) * block
            for c in range(lat // 128):
                wide[c, at : at + block] = back_ref[p, r, :, c * 128 : (c + 1) * 128].astype(
                    jnp.float32
                )
    for h in range(heads):
        mine = jnp.concatenate(
            [
                jnp.concatenate(
                    [
                        wide[c, pl.ds(s * heads + h, local, stride=block), :]
                        for c in range(lat // 128)
                    ],
                    axis=1,
                )
                for s in range(steps)
            ],
            axis=0,
        ).astype(jnp.bfloat16)
        out_ref[:, h * 128 : (h + 1) * 128] = jnp.dot(
            mine, vw_ref[:, h * 128 : (h + 1) * 128], preferred_element_type=jnp.float32
        ).astype(jnp.bfloat16)
    shown.wait()


def project_pallas(back, value_weight, part, whole, heads):
    ranks, owned, block, lat = back.shape
    rows = ranks * owned * block
    return pl.pallas_call(
        functools.partial(project_kernel, heads=heads, lat=lat),
        out_shape=(
            jax.ShapeDtypeStruct((rows // heads, heads * 128), jnp.bfloat16),
            jax.ShapeDtypeStruct(whole.shape, whole.dtype),
        ),
        in_specs=[VMEM_SPEC, VMEM_SPEC, VMEM_SPEC, HBM_SPEC],
        out_specs=(VMEM_SPEC, HBM_SPEC),
        scratch_shapes=[
            pltpu.VMEM((lat // 128, rows, 128), jnp.float32),
            pltpu.SemaphoreType.DMA((1,)),
        ],
        input_output_aliases={3: 1},
        compiler_params=pltpu.CompilerParams(vmem_limit_bytes=24 << 20),
    )(back, value_weight, part, whole)


def on_device(
    latent_rows,
    pre_queries,
    pre_lengths,
    owner_map,
    context_cache,
    context_lengths,
    new_latent,
    dec_queries,
    key_weight,
    value_weight,
):
    steps, rows_local, heads, width = dec_queries.shape
    ranks = lax.axis_size("head")
    if heads % 16 or latent_rows.shape[0] % 128 or ranks % 2:
        return plain_on_device(
            latent_rows,
            pre_queries,
            pre_lengths,
            owner_map,
            context_cache,
            context_lengths,
            new_latent,
            dec_queries,
            key_weight,
            value_weight,
        )
    lat = key_weight.shape[0]
    owned = context_cache.shape[0]
    first = heads // 2
    qb = 256
    stay = lambda x: pltpu.with_memory_space_constraint(x, pltpu.HBM)
    turned = stay(jnp.transpose(pre_queries, (1, 2, 0)))
    kw_stay, vw_stay = stay(key_weight), stay(value_weight)
    spans, rows, query, part = gather_pallas(
        pre_lengths,
        stay(jnp.transpose(latent_rows)),
        stay(dec_queries.reshape(-1, width)),
        kw_stay,
        vw_stay,
        turned,
        owned,
        ranks,
        first,
        qb,
    )
    latent_out, whole = decode_pallas(
        pre_lengths,
        owner_map,
        context_lengths,
        query,
        new_latent,
        spans,
        part,
        stay(jnp.transpose(context_cache, (0, 2, 1))),
        lat,
        heads,
        heads * 128,
        width,
        rows_local,
    )
    back, rest = return_pallas(
        pre_lengths, rows, spans, latent_out, kw_stay, vw_stay, turned, heads - first, qb, 0
    )
    decode_out, prefill_out = project_pallas(back, value_weight, rest, whole, heads)
    return (prefill_out, decode_out.reshape(steps, rows_local, heads * 128))


def solution(mesh):
    placed = (
        P(("groups", "batch", "head"), None),
        P(("groups", "batch"), "head", None),
        P("groups", None),
        P("groups", None),
        P(("groups", "batch", "head"), None, None),
        P(("groups", "batch", "head")),
        P("groups", ("batch", "head"), None),
        P("groups", "batch", "head", None),
        P(None, "head"),
        P(None, "head"),
    )
    return jax.shard_map(
        on_device,
        mesh=mesh,
        in_specs=placed,
        out_specs=(P(("groups", "batch"), "head"), P("groups", "batch", "head")),
        check_vma=False,
    )
```

```python
import functools
import math

import jax
import jax.numpy as jnp
from jax import lax
from jax.experimental import pallas as pl
from jax.experimental.pallas import tpu as pltpu
from jax.sharding import PartitionSpec as P

BLK = 512


NEGATIVE = -1e30


def from_partner(value, axis, distance):
    mask = 2**distance
    pairs = [(source, source ^ mask) for source in range(lax.axis_size(axis))]
    return lax.ppermute(value, axis, pairs)


def request_table(pre_lengths, owner_map, span_len):
    seg_ends = jnp.cumsum(pre_lengths, axis=1)
    span_base = jnp.arange(pre_lengths.shape[0], dtype=jnp.int32)[:, None] * span_len
    seg_starts = seg_ends - pre_lengths + span_base
    return (owner_map.reshape(-1), seg_starts.reshape(-1), pre_lengths.reshape(-1))


def prefill_heads(own_span, queries, span_lengths, key_weight, value_weight):
    span_len, head_count, query_width = queries.shape
    head_size = key_weight.shape[1] // head_count
    lat_width = key_weight.shape[0]
    score_scale = 1.0 / math.sqrt(query_width)
    latent = own_span[:, :lat_width]
    rope_keys = own_span[:, lat_width:]
    keys_nope = (
        jnp.dot(latent, key_weight, preferred_element_type=jnp.float32)
        .astype(jnp.bfloat16)
        .reshape(span_len, head_count, head_size)
    )
    values = (
        jnp.dot(latent, value_weight, preferred_element_type=jnp.float32)
        .astype(jnp.bfloat16)
        .reshape(span_len, head_count, head_size)
    )
    scores = jnp.einsum(
        "qhd,khd->hqk", queries[:, :, :head_size], keys_nope, preferred_element_type=jnp.float32
    )
    scores = scores + jnp.einsum(
        "qhr,kr->hqk", queries[:, :, head_size:], rope_keys, preferred_element_type=jnp.float32
    )
    scores = scores * score_scale
    seg_ends = jnp.cumsum(span_lengths)
    places = jnp.arange(span_len, dtype=jnp.int32)
    segment = jnp.sum((places[:, None] >= seg_ends[None, :]).astype(jnp.int32), axis=1)
    allowed = (segment[:, None] == segment[None, :]) & (places[None, :] <= places[:, None])
    masked = jnp.where(allowed[None], scores, NEGATIVE)
    peak_score = jnp.max(masked, axis=2, keepdims=True)
    weights = jnp.exp(masked - peak_score)
    weight_sum = jnp.sum(weights, axis=2)
    mixed_out = jnp.einsum(
        "hqk,khd->qhd", weights.astype(jnp.bfloat16), values, preferred_element_type=jnp.float32
    )
    mixed_out = mixed_out / jnp.transpose(weight_sum)[:, :, None]
    return mixed_out.astype(jnp.bfloat16).reshape(span_len, head_count * head_size)


def plain_on_device(
    latent_rows,
    pre_queries,
    pre_lengths,
    owner_map,
    context_cache,
    context_lengths,
    new_latent,
    dec_queries,
    key_weight,
    value_weight,
):
    head_rank = lax.axis_index("head")
    batch_rank = lax.axis_index("batch")
    span_len = pre_queries.shape[0]
    kv_width = latent_rows.shape[1]
    own_span = lax.all_gather(latent_rows, "head", axis=0, tiled=True)
    other_span = from_partner(own_span, "batch", 0)
    first_span = jnp.where(batch_rank == 0, own_span, other_span)
    second_span = jnp.where(batch_rank == 0, other_span, own_span)
    all_spans = jnp.concatenate([first_span, second_span], axis=0)
    span_lengths = lax.dynamic_index_in_dim(pre_lengths, batch_rank, 0, keepdims=False)
    prefill_out = prefill_heads(own_span, pre_queries, span_lengths, key_weight, value_weight)
    step_total, rows_local, head_count, query_width = dec_queries.shape
    lat_width = key_weight.shape[0]
    head_size = key_weight.shape[1] // head_count
    owned_rows = context_cache.shape[0]
    score_scale = 1.0 / math.sqrt(query_width)
    key_heads = key_weight.reshape(lat_width, head_count, head_size)
    value_heads = value_weight.reshape(lat_width, head_count, head_size)
    absorbed = jnp.einsum(
        "srhd,lhd->srhl",
        dec_queries[..., :head_size],
        key_heads,
        preferred_element_type=jnp.float32,
    ).astype(jnp.bfloat16)
    query_all = jnp.concatenate([absorbed, dec_queries[..., head_size:]], axis=3)
    flat_owner, flat_start, flat_length = request_table(pre_lengths, owner_map, span_len)
    row_ids = (
        batch_rank * rows_local + head_rank * owned_rows + jnp.arange(owned_rows, dtype=jnp.int32)
    )
    matches = (flat_owner[None, :] == row_ids[:, None]).astype(jnp.int32)
    is_target = jnp.sum(matches, axis=1) > 0
    first_row = jnp.sum(matches * flat_start[None, :], axis=1)
    prompt_len = jnp.sum(matches * flat_length[None, :], axis=1)
    effective = jnp.where(is_target, prompt_len, context_lengths)
    padded = jnp.concatenate([all_spans, jnp.zeros((span_len, kv_width), all_spans.dtype)], axis=0)
    replaced = jax.vmap(lambda offset: lax.dynamic_slice_in_dim(padded, offset, span_len, 0))(
        first_row
    )
    front_rows = jnp.where(is_target[:, None, None], replaced, context_cache[:, :span_len])
    front_blocks = span_len // BLK
    needed = (jnp.max(effective) + BLK - 1) // BLK
    fresh_latent = new_latent[..., :lat_width]
    owned_query = lax.all_to_all(query_all, "head", split_axis=1, concat_axis=2, tiled=True)
    fresh_scores = (
        jnp.einsum("srhk,jrk->srhj", owned_query, new_latent, preferred_element_type=jnp.float32)
        * score_scale
    )
    visible = (
        jnp.arange(new_latent.shape[0], dtype=jnp.int32)[None, :]
        <= jnp.arange(step_total, dtype=jnp.int32)[:, None]
    )
    fresh_scores = jnp.where(visible[:, None, None, :], fresh_scores, NEGATIVE)
    peak_score = jnp.max(fresh_scores, axis=3)
    weights = jnp.exp(fresh_scores - peak_score[..., None])
    weight_sum = jnp.sum(weights, axis=3)
    running = jnp.einsum(
        "srhj,jrl->srhl",
        weights.astype(jnp.bfloat16),
        fresh_latent,
        preferred_element_type=jnp.float32,
    )

    def advance(block_index, state_tuple, source):
        old_peak, old_sum, old_running = state_tuple
        key_block = lax.dynamic_slice_in_dim(source, block_index * BLK, BLK, 1)
        scores = (
            jnp.einsum("srhk,rtk->srht", owned_query, key_block, preferred_element_type=jnp.float32)
            * score_scale
        )
        places = block_index * BLK + jnp.arange(BLK, dtype=jnp.int32)
        in_context = places[None, :] < effective[:, None]
        scores = jnp.where(in_context[None, :, None, :], scores, NEGATIVE)
        new_peak = jnp.maximum(old_peak, jnp.max(scores, axis=3))
        factor = jnp.exp(old_peak - new_peak)
        block_weights = jnp.exp(scores - new_peak[..., None])
        new_sum = old_sum * factor + jnp.sum(block_weights, axis=3)
        new_running = old_running * factor[..., None] + jnp.einsum(
            "srht,rtl->srhl",
            block_weights.astype(jnp.bfloat16),
            key_block[..., :lat_width],
            preferred_element_type=jnp.float32,
        )
        return (new_peak, new_sum, new_running)

    state_tuple = lax.fori_loop(
        0,
        jnp.minimum(needed, front_blocks),
        lambda block_index, state_now: advance(block_index, state_now, front_rows),
        (peak_score, weight_sum, running),
    )
    state_tuple = lax.fori_loop(
        front_blocks,
        jnp.maximum(needed, front_blocks),
        lambda block_index, state_now: advance(block_index, state_now, context_cache),
        state_tuple,
    )
    latent_out = (state_tuple[2] / state_tuple[1][..., None]).astype(jnp.bfloat16)
    returned = lax.all_to_all(latent_out, "head", split_axis=2, concat_axis=1, tiled=True)
    projected = jnp.einsum(
        "srhl,lhd->srhd", returned, value_heads, preferred_element_type=jnp.float32
    ).astype(jnp.bfloat16)
    decode_out = projected.reshape(query_all.shape[0], rows_local, head_count * head_size)
    return (prefill_out, decode_out)


def trans_dot(left, right):
    return lax.dot_general(
        left, right, (((1,), (1,)), ((), ())), preferred_element_type=jnp.float32
    )


MESH = pl.DeviceIdType.MESH


def place_of(rank, ranks):
    odd = rank % 2
    return (1 - odd) * (rank // 2) + odd * (ranks - 1 - rank // 2)


def rank_at(place, ranks):
    late = place // (ranks // 2)
    return (1 - late) * (2 * place) + late * (2 * (ranks - 1 - place) + 1)


def start_marks(ends, tail, vals_of, hot, tri):
    span_len, full = tail.shape
    marks = hot.shape[0]
    segs = len(ends)
    where = lax.broadcasted_iota(jnp.int32, (span_len, marks), 0)
    lane = lax.broadcasted_iota(jnp.int32, (span_len, marks), 1)
    place = lax.broadcasted_iota(jnp.int32, (marks, span_len), 1)
    line = lax.broadcasted_iota(jnp.int32, (marks, span_len), 0)
    mine = jnp.zeros((span_len, marks), jnp.int32)
    seen = jnp.zeros((marks, span_len), jnp.int32)
    for k in range(segs - 1):
        mine = mine + (where >= ends[k]).astype(jnp.int32)
        seen = seen + (place >= ends[k]).astype(jnp.int32)
    mark = jnp.where((lane < segs) & (lane != mine), NEGATIVE, 0.0).astype(jnp.bfloat16)
    hot[...] = jnp.where(line == seen, 1.0, 0.0).astype(jnp.bfloat16)
    tail[:, full - marks :] = mark
    for vals in vals_of:
        for h in range(vals.shape[0]):
            vals[h, 128:, :] = jnp.ones((vals.shape[1] - 128, span_len), jnp.bfloat16)
    size = tri.shape[0]
    key_at = lax.broadcasted_iota(jnp.int32, (size, size), 0)
    query_at = lax.broadcasted_iota(jnp.int32, (size, size), 1)
    tri[...] = jnp.where(key_at <= query_at, 0.0, NEGATIVE)


def project_shard(origin, spans_ref, kw, vw, keys_of, vals_of, tail, lat, heads):
    own = spans_ref.shape[2]
    rows = jnp.transpose(spans_ref[origin])
    at = pl.ds(pl.multiple_of(origin * own, own), own)
    tail[at, : rows.shape[1] - lat] = rows[:, lat:]
    latent = rows[:, :lat]
    pair = 2
    first = keys_of[0].shape[0]
    for g in range(heads // pair):
        columns = slice(g * pair * 128, (g + 1) * pair * 128)
        key = jnp.dot(latent, kw[:, columns], preferred_element_type=jnp.float32)
        value = jnp.dot(latent, vw[:, columns], preferred_element_type=jnp.float32)
        key = key.astype(jnp.bfloat16)
        value = jnp.transpose(value.astype(jnp.bfloat16))
        for p in range(pair):
            h = g * pair + p
            side, index = (0, h) if h < first else (1, h - first)
            keys_of[side][index, at, :] = key[:, p * 128 : (p + 1) * 128]
            vals_of[side][index, :128, at] = value[p * 128 : (p + 1) * 128]


def attention(g, pair, qs, keys, tail, vals, hot, tri, part_ref, scores, weights, look, scale):
    span_len = tail.shape[0]
    qb = tri.shape[0]
    blocks = span_len // qb
    order = [(0, p) for p in range(pair // 2)]
    order += [(i, p) for i in range(1, blocks) for p in range(pair)]
    order += [(0, p) for p in range(pair // 2, pair)]
    count = len(order)
    lengths = [min(i, look) + 1 for i, _ in order]
    peaks = [None] * count
    tops = [None] * count
    sums = [None] * count

    def score(n, c):
        i, p = order[n]
        if c > 0:
            return
        at = (i - lengths[n] + 1) * qb
        size = lengths[n] * qb
        query = jnp.concatenate(
            [qs[g * pair + p, :, i * qb : (i + 1) * qb], hot[:, i * qb : (i + 1) * qb]], axis=0
        )
        key = jnp.concatenate(
            [keys[g * pair + p, at : at + size, :], tail[at : at + size, :]], axis=1
        )
        s = jnp.dot(key, query, preferred_element_type=jnp.float32)
        if size > qb:
            scores[n % 4][: size - qb, :] = s[: size - qb]
            peaks[n] = jnp.max(s[: size - qb].reshape((size - qb) // 8, 8, qb), axis=0)
        last = s[size - qb :] + tri[...]
        scores[n % 4][size - qb : size, :] = last
        top = jnp.max(last.reshape(qb // 8, 8, qb), axis=0)
        peaks[n] = top if peaks[n] is None else jnp.maximum(peaks[n], top)

    def soften(n, c):
        if c == 0:
            tops[n] = jnp.max(peaks[n], axis=0, keepdims=True)
        for k in range(0, qb, 32):
            at = slice(c * qb + k, c * qb + k + 32)
            w = jnp.exp2((scores[n % 4][at, :] - tops[n]) * scale)
            weights[n % 4][at, :] = w.astype(jnp.bfloat16)

    def mix(n, c):
        i, p = order[n]
        at = (i - lengths[n] + 1) * qb
        if c == 0:
            o = jnp.dot(
                vals[g * pair + p, :, at : at + lengths[n] * qb],
                weights[n % 4][: lengths[n] * qb, :],
                preferred_element_type=jnp.float32,
            )
            o = o[:128] * (1.0 / o[128:129])
            columns = pl.ds(pl.multiple_of((g * pair + p) * 128, 128), 128)
            part_ref[i * qb : (i + 1) * qb, columns] = jnp.transpose(o.astype(jnp.bfloat16))

    todo_score = [(n, c) for n in range(count) for c in range(lengths[n])]
    todo_soft = list(todo_score)
    todo_mix = list(todo_score)
    scored = [0] * count
    softened = [0] * count
    mixed = [0] * count
    while todo_mix:
        was = list(softened)
        if todo_score:
            n, c = todo_score[0]
            if n < 4 or softened[n - 4] == lengths[n - 4]:
                score(n, c)
                scored[n] += 1
                todo_score.pop(0)
        if todo_soft:
            n, c = todo_soft[0]
            free = n < 4 or mixed[n - 4] == lengths[n - 4]
            if scored[n] == lengths[n] and free and not (todo_score and todo_score[0][0] <= n + 2):
                soften(n, c)
                softened[n] += 1
                todo_soft.pop(0)
        n, c = todo_mix[0]
        if was[n] == lengths[n]:
            mix(n, c)
            mixed[n] += 1
            todo_mix.pop(0)


def attend_all(pair, qs, keys, tail, vals, hot, tri, part_ref, buffers, look, scale):
    scores, weights = buffers

    def step(g, carry):
        attention(
            g, pair, qs, keys, tail, vals, hot, tri, part_ref, scores, weights, look, scale
        )
        return carry

    lax.fori_loop(0, qs.shape[0] // pair, step, 0)


def absorb_into(dq, kw, sent, flat, wide, heads, lat):
    rows = dq.shape[0]
    ranks, owned, block, _ = sent.shape
    steps = block // heads
    local = ranks * owned
    flat[...] = dq[:, :128].astype(jnp.float32)
    for h in range(heads):
        mine = flat[pl.ds(h, rows // heads, stride=heads), :].astype(jnp.bfloat16)
        res = trans_dot(mine, kw[:, h * 128 : (h + 1) * 128])
        for s in range(steps):
            for c in range(lat // 128):
                wide[c, pl.ds(s * heads + h, local, stride=block), :] = res[
                    s * local : (s + 1) * local, c * 128 : (c + 1) * 128
                ]
    for p in range(ranks):
        for r in range(owned):
            at = p * owned + r
            for c in range(lat // 128):
                sent[p, r, :, c * 128 : (c + 1) * 128] = wide[
                    c, at * block : (at + 1) * block
                ].astype(jnp.bfloat16)
            for s in range(steps):
                start = (s * local + at) * heads
                sent[p, r, s * heads : (s + 1) * heads, lat:] = dq[start : start + heads, 128:]


def span_ends(lens_ref, batch_rank):
    ends = []
    total = 0
    for k in range(lens_ref.shape[1]):
        total = total + lens_ref[batch_rank, k]
        ends.append(total)
    return ends


def gather_kernel(
    lens_ref, shard_hbm, dq_hbm, kw_hbm, vw_hbm, q_hbm,
    spans_ref, got_ref, part_ref, tail, hot, tri, keys_b, vals_b,
    kw, vw, qs, dq, flat, wide, sent, keys_a, vals_a, buffers,
    load_sems, ring_send, ring_recv, swap_sems, give_sems, take_sems,
    *, lat, ranks, heads, look, scale, pair
):
    me = lax.axis_index("head")
    batch_rank = lax.axis_index("batch")
    place = place_of(me, ranks)
    right = rank_at((place + 1) % ranks, ranks)
    left = rank_at((place + ranks - 1) % ranks, ranks)
    some = qs.shape[0]
    loads = [
        pltpu.make_async_copy(dq_hbm, dq, load_sems.at[0]),
        pltpu.make_async_copy(kw_hbm, kw, load_sems.at[1]),
        pltpu.make_async_copy(shard_hbm, spans_ref.at[me], load_sems.at[2]),
        pltpu.make_async_copy(vw_hbm, vw, load_sems.at[3]),
        pltpu.make_async_copy(q_hbm.at[:some], qs, load_sems.at[4]),
    ]
    barrier = pltpu.get_barrier_semaphore()
    for k in range(1, ranks):
        pl.semaphore_signal(
            barrier, inc=1, device_id={"head": (me + k) % ranks}, device_id_type=MESH
        )
    pl.semaphore_signal(
        barrier, inc=1, device_id={"batch": 1 - batch_rank}, device_id_type=MESH
    )
    for load in loads:
        load.start()
    start_marks(span_ends(lens_ref, batch_rank), tail, (vals_a, vals_b), hot, tri)
    pl.semaphore_wait(barrier, ranks)

    half = shard_hbm.shape[0] // 2
    most = ranks // 2

    def hop(way, part, t):
        back = t - 1 if way == 0 else ranks - t + 1
        origin = rank_at((place + ranks - back) % ranks, ranks)
        rows = pl.ds(part * half, half)
        return pltpu.make_async_remote_copy(
            src_ref=spans_ref.at[origin, rows],
            dst_ref=spans_ref.at[origin, rows],
            send_sem=ring_send.at[way, part, t - 1],
            recv_sem=ring_recv.at[way, part, t - 1],
            device_id={"head": right if way == 0 else left},
            device_id_type=MESH,
        )

    def hops(way, part):
        return most if way == part else most - 1

    streams = [(0, 0), (1, 1), (0, 1), (1, 0)]
    loads[2].wait()
    for way, part in streams:
        hop(way, part, 1).start()
    loads[0].wait()
    loads[1].wait()
    absorb_into(dq, kw, sent, flat, wide, heads, lat)
    loads[3].wait()

    def project(origin):
        project_shard(
            origin, spans_ref, kw, vw, (keys_a, keys_b), (vals_a, vals_b), tail, lat, heads
        )

    def arrive(t, carry):
        for way, part in streams:
            if hops(way, part) == most:
                hop(way, part, t).wait_recv()
                pl.when(t < most)(lambda: hop(way, part, t + 1).start())
            else:

                @pl.when(t < most)
                def _():
                    hop(way, part, t).wait_recv()
                    pl.when(t < most - 1)(lambda: hop(way, part, t + 1).start())

        def one(side, carry):
            project(rank_at((place + side * t + (1 - side) * (ranks - t)) % ranks, ranks))
            return carry

        lax.fori_loop(0, 2 - t // most, one, 0)
        return carry

    project(me)
    lax.fori_loop(1, most + 1, arrive, 0)

    gives = []
    for k in range(1, ranks):
        peer = (me + k) % ranks
        gives.append(
            pltpu.make_async_remote_copy(
                src_ref=sent.at[peer],
                dst_ref=got_ref.at[me],
                send_sem=give_sems.at[k - 1],
                recv_sem=take_sems.at[k - 1],
                device_id={"head": peer},
                device_id_type=MESH,
            )
        )
    for give in gives:
        give.start()
    keep = pltpu.make_async_copy(sent.at[me], got_ref.at[me], load_sems.at[5])
    keep.start()
    swap = pltpu.make_async_remote_copy(
        src_ref=spans_ref.at[:ranks],
        dst_ref=spans_ref.at[ranks:],
        send_sem=swap_sems.at[0],
        recv_sem=swap_sems.at[1],
        device_id={"batch": 1 - batch_rank},
        device_id_type=MESH,
    )
    swap.start()
    loads[4].wait()
    attend_all(pair, qs, keys_a, tail, vals_a, hot, tri, part_ref, buffers, look, scale)
    for way, part in streams:
        for t in range(1, hops(way, part) + 1):
            hop(way, part, t).wait_send()
    for give in gives:
        give.wait()
    keep.wait()
    swap.wait()


HBM_SPEC = pl.BlockSpec(memory_space=pltpu.HBM)
VMEM_SPEC = pl.BlockSpec(memory_space=pltpu.VMEM)
SMEM_SPEC = pl.BlockSpec(memory_space=pltpu.SMEM)


def attend_scratch(qb, look):
    deep = (look + 1) * qb
    return [
        [pltpu.VMEM((deep, qb), jnp.float32)] * 4,
        [pltpu.VMEM((deep, qb), jnp.bfloat16)] * 4,
    ]


def gather_pallas(lens, shard, flat_queries, key_weight, value_weight, turned, owned, ranks, first, qb, pair):
    heads, width, span_len = turned.shape
    kv, own = shard.shape
    lat = key_weight.shape[0]
    rows = flat_queries.shape[0]
    block = rows // (ranks * owned)
    look = min(-(-(span_len // 2) // qb), span_len // qb - 1)
    rest = heads - first
    marks = 128 - (kv - lat)
    bf16 = jnp.bfloat16
    return pl.pallas_call(
        functools.partial(
            gather_kernel,
            lat=lat,
            ranks=ranks,
            heads=heads,
            look=look,
            scale=math.log2(math.e) / math.sqrt(width),
            pair=pair,
        ),
        out_shape=(
            jax.ShapeDtypeStruct((2 * ranks, kv, own), bf16),
            jax.ShapeDtypeStruct((ranks, owned, block, kv), bf16),
            jax.ShapeDtypeStruct((span_len, first * 128), bf16),
            jax.ShapeDtypeStruct((span_len, 128), bf16),
            jax.ShapeDtypeStruct((marks, span_len), bf16),
            jax.ShapeDtypeStruct((qb, qb), jnp.float32),
            jax.ShapeDtypeStruct((rest, span_len, 128), bf16),
            jax.ShapeDtypeStruct((rest, 144, span_len), bf16),
        ),
        in_specs=[SMEM_SPEC] + [HBM_SPEC] * 5,
        out_specs=(VMEM_SPEC,) * 8,
        scratch_shapes=[
            pltpu.VMEM(key_weight.shape, bf16),
            pltpu.VMEM(value_weight.shape, bf16),
            pltpu.VMEM((first, width, span_len), bf16),
            pltpu.VMEM((rows, width), bf16),
            pltpu.VMEM((rows, 128), jnp.float32),
            pltpu.VMEM((lat // 128, rows, 128), jnp.float32),
            pltpu.VMEM((ranks, owned, block, kv), bf16),
            pltpu.VMEM((first, span_len, 128), bf16),
            pltpu.VMEM((first, 144, span_len), bf16),
            attend_scratch(qb, look),
            pltpu.SemaphoreType.DMA((6,)),
            pltpu.SemaphoreType.DMA((2, 2, ranks // 2)),
            pltpu.SemaphoreType.DMA((2, 2, ranks // 2)),
            pltpu.SemaphoreType.DMA((2,)),
            pltpu.SemaphoreType.DMA((ranks - 1,)),
            pltpu.SemaphoreType.DMA((ranks - 1,)),
        ],
        compiler_params=pltpu.CompilerParams(
            collective_id=0, has_side_effects=True, vmem_limit_bytes=36 << 20
        ),
        cost_estimate=pl.CostEstimate(
            flops=12 * 10**9, bytes_accessed=12 << 20, transcendentals=6 << 20
        ),
    )(lens, shard, flat_queries, key_weight, value_weight, turned)


def decode_kernel(
    lens_ref, owner_ref, ctx_ref, q_ref, new_ref, spans_ref, part_ref, cache_ref,
    out_ref, whole_ref,
    bufs, sems, whole_sem, tools,
    *, lat, heads, steps, blk, depth, scale, rows_local, span_len
):
    ranks, owned, block, kv = q_ref.shape
    rows = ranks * block
    batch_rank = lax.axis_index("batch")
    me = lax.axis_index("head")
    shown = pltpu.make_async_copy(
        part_ref, whole_ref.at[:, : part_ref.shape[1]], whole_sem.at[0]
    )
    shown.start()
    facts = []
    for r in range(owned):
        row = batch_rank * rows_local + me * owned + r
        target = jnp.int32(0)
        first = jnp.int32(0)
        length = jnp.int32(0)
        for c in range(lens_ref.shape[0]):
            start = jnp.int32(c * span_len)
            for k in range(lens_ref.shape[1]):
                hit = (owner_ref[c, k] == row).astype(jnp.int32)
                target = target + hit
                first = first + hit * start
                length = length + hit * lens_ref[c, k]
                start = start + lens_ref[c, k]
        first = lax.rem(first + batch_rank * span_len, 2 * span_len) * target
        length = jnp.where(target > 0, length, ctx_ref[r])
        facts.append((target, first, length))

    counts = []
    for r in range(owned):
        _, start, length = facts[r]
        counts.append((start + length + blk - 1) // blk - start // blk)
    turns = [(count + 1) // 2 for count in counts]

    def copy_of(r, t):
        slot = lax.rem(t, depth)
        target, start, _ = facts[r]
        at = pl.multiple_of((start // blk + jnp.minimum(t, counts[r] - 1)) * blk, blk)

        @pl.when(target > 0)
        def _():
            own = spans_ref.shape[2]
            for c in range(blk // own):
                pltpu.make_async_copy(
                    spans_ref.at[at // own + c],
                    bufs.at[r, slot, :, c * own : (c + 1) * own],
                    sems.at[r, slot],
                ).start()

        @pl.when(target == 0)
        def _():
            pltpu.make_async_copy(
                cache_ref.at[r, :, pl.ds(at, blk)], bufs.at[r, slot], sems.at[r, slot]
            ).start()

    for r in range(owned):
        for t in range(3):
            copy_of(r, jnp.int32(t))
    newest = new_ref[...].astype(jnp.float32)
    full = tools[0][3].shape[1]
    tail = lax.broadcasted_iota(jnp.int32, (rows, full - kv), 1)
    lanes = lax.broadcasted_iota(jnp.int32, (rows, 128), 1)
    piece = 256

    def request(r, tools):
        peak_ref, sum_ref, acc_ref, asked, scores, tops, weights, fades = tools
        _, start, length = facts[r]
        base = start // blk * blk
        q = q_ref[:, r].reshape(rows, kv)
        asked[:, :kv] = q
        asked[:, kv:] = jnp.where(tail == 0, 1.0, 0.0).astype(jnp.bfloat16)
        fresh = jnp.concatenate(
            [newest[s, r : r + 1] for s in range(steps)]
            + [jnp.zeros((128 - steps, kv), jnp.float32)],
            axis=0,
        ).astype(jnp.bfloat16)

        def take(t):
            slot = lax.rem(t, depth)
            pltpu.make_async_copy(
                cache_ref.at[r, :, pl.ds(0, blk)], bufs.at[r, slot], sems.at[r, slot]
            ).wait()

        def score(t, side, c):
            slot = lax.rem(t, depth)
            place = base + t * blk + c * piece + lax.broadcasted_iota(jnp.int32, (16, piece), 1)
            hide = jnp.where((place >= start) & (place < start + length), 0.0, NEGATIVE)
            hide = hide.astype(jnp.bfloat16)
            keys = jnp.concatenate(
                [bufs[r, slot, :, c * piece : (c + 1) * piece]] + [hide] * ((full - kv) // 16),
                axis=0,
            )
            s = jnp.dot(asked[...], keys, preferred_element_type=jnp.float32)
            scores[side][:, c * piece : (c + 1) * piece] = s
            top = jnp.maximum(s[:, :128], s[:, 128:])
            if c > 0:
                top = jnp.maximum(top, tops[side][...])
            tops[side][...] = top

        def settle(side):
            old = peak_ref[...]
            new = jnp.maximum(old, jnp.max(tops[side][...], axis=1, keepdims=True))
            fade = jnp.exp2((old - new) * scale)
            fades[side][...] = fade
            peak_ref[...] = new
            sum_ref[...] = sum_ref[...] * fade

        def soften(side, c):
            at = slice(c * piece, (c + 1) * piece)
            new = peak_ref[...]
            s = scores[side][:, at]
            left = jnp.exp2((s[:, :128] - new) * scale)
            right = jnp.exp2((s[:, 128:] - new) * scale)
            sum_ref[...] = sum_ref[...] + (left + right)
            weights[side][:, at] = jnp.concatenate([left, right], axis=1).astype(jnp.bfloat16)

        def mix(t, side, c):
            slot = lax.rem(jnp.maximum(t, 0), depth)
            at = slice(c * piece, (c + 1) * piece)
            made = trans_dot(weights[side][...], bufs[r, slot, at, :])
            fade = fades[side][...]
            for k in range(piece // 128):
                columns = slice(c * piece + k * 128, c * piece + (k + 1) * 128)
                acc_ref[:, columns] = (
                    acc_ref[:, columns] * fade + made[:, k * 128 : (k + 1) * 128]
                )

        def begin():
            s = trans_dot(q, fresh)
            row_step = (lax.broadcasted_iota(jnp.int32, s.shape, 0) // heads) % steps
            s = jnp.where(lanes <= row_step, s, NEGATIVE)
            m = jnp.max(s, axis=1, keepdims=True)
            w = jnp.exp2((s - m) * scale)
            sum_ref[...] = w
            peak_ref[...] = jnp.broadcast_to(m, peak_ref.shape)
            acc_ref[...] = jnp.dot(
                w.astype(jnp.bfloat16), fresh[:, :lat], preferred_element_type=jnp.float32
            )
            weights[1][...] = jnp.zeros(weights[1].shape, jnp.bfloat16)
            fades[1][...] = jnp.ones(fades[1].shape, jnp.float32)

        def lead(c):
            score(jnp.int32(0), 0, c)

        def turn(j, carry):
            for k in (3, 4):
                pl.when(2 * j + k <= 2 * turns[r])(functools.partial(copy_of, r, 2 * j + k))
            take(2 * j + 1)
            take(2 * j + 2)
            for side in range(2):
                t = 2 * j + side
                settle(side)
                for c in range(blk // piece):
                    score(t + 1, 1 - side, c)
                    soften(side, c)
                    mix(t - 1, 1 - side, c)
            return carry

        def last(c):
            mix(2 * turns[r] - 1, 1, c)

        def finish():
            total = jnp.sum(sum_ref[...], axis=1, keepdims=True)
            done = (acc_ref[...] * (1.0 / total)).astype(out_ref.dtype)
            for p in range(ranks):
                out_ref[p, r] = done[p * block : (p + 1) * block]

        return take, begin, lead, turn, last, finish

    asks = [request(r, tools[r]) for r in range(owned)]
    for ask in asks:
        ask[1]()
    for ask in asks:
        ask[0](jnp.int32(0))
    for c in range(blk // piece):
        for ask in asks:
            ask[2](c)
    for r in range(owned):
        lax.fori_loop(0, turns[r], asks[r][3], 0)
    for c in range(lat // piece):
        for ask in asks:
            ask[4](c)
    for ask in asks:
        ask[5]()
    shown.wait()


def decode_pallas(lens, owner, ctx, query, newest, spans, part, cache, lat, heads, all_columns, width, rows_local, blk=512, depth=6):
    ranks, owned, block, kv = query.shape
    rows = ranks * block
    steps = block // heads
    span_len = part.shape[0]
    return pl.pallas_call(
        functools.partial(
            decode_kernel,
            lat=lat,
            heads=heads,
            steps=steps,
            blk=blk,
            depth=depth,
            scale=math.log2(math.e) / math.sqrt(width),
            rows_local=rows_local,
            span_len=span_len,
        ),
        out_shape=(
            jax.ShapeDtypeStruct((ranks, owned, block, lat), jnp.bfloat16),
            jax.ShapeDtypeStruct((span_len, all_columns), jnp.bfloat16),
        ),
        in_specs=[SMEM_SPEC] * 3
        + [VMEM_SPEC, VMEM_SPEC, pl.BlockSpec(memory_space=pl.ANY), VMEM_SPEC, HBM_SPEC],
        out_specs=(VMEM_SPEC, HBM_SPEC),
        scratch_shapes=[
            pltpu.VMEM((owned, depth, kv, blk), jnp.bfloat16),
            pltpu.SemaphoreType.DMA((owned, depth)),
            pltpu.SemaphoreType.DMA((1,)),
            [
                [
                    pltpu.VMEM((rows, 128), jnp.float32),
                    pltpu.VMEM((rows, 128), jnp.float32),
                    pltpu.VMEM((rows, lat), jnp.float32),
                    pltpu.VMEM((rows, -(-(kv + 16) // 128) * 128), jnp.bfloat16),
                    [pltpu.VMEM((rows, blk), jnp.float32)] * 2,
                    [pltpu.VMEM((rows, 128), jnp.float32)] * 2,
                    [pltpu.VMEM((rows, blk), jnp.bfloat16)] * 2,
                    [pltpu.VMEM((rows, 128), jnp.float32)] * 2,
                ]
            ]
            * owned,
        ],
        compiler_params=pltpu.CompilerParams(vmem_limit_bytes=24 << 20),
        cost_estimate=pl.CostEstimate(
            flops=5 * 10**9, bytes_accessed=10 << 20, transcendentals=2 << 20
        ),
    )(lens, owner, ctx, query, newest, spans, part, cache)


def return_kernel(
    tail, hot, tri, keys, vals, lo_ref, q_hbm,
    back_ref, part_ref,
    qs, buffers, load_sems, give_sems, take_sems,
    *, ranks, look, scale, pair
):
    me = lax.axis_index("head")
    some = qs.shape[0]
    skip = q_hbm.shape[0] - some
    barrier = pltpu.get_barrier_semaphore()
    for k in range(1, ranks):
        pl.semaphore_signal(
            barrier, inc=1, device_id={"head": (me + k) % ranks}, device_id_type=MESH
        )
    load = pltpu.make_async_copy(q_hbm.at[skip:], qs, load_sems.at[0])
    load.start()
    gives = []
    for k in range(1, ranks):
        peer = (me + k) % ranks
        gives.append(
            pltpu.make_async_remote_copy(
                src_ref=lo_ref.at[peer],
                dst_ref=back_ref.at[me],
                send_sem=give_sems.at[k - 1],
                recv_sem=take_sems.at[k - 1],
                device_id={"head": peer},
                device_id_type=MESH,
            )
        )
    keep = pltpu.make_async_copy(lo_ref.at[me], back_ref.at[me], load_sems.at[1])
    keep.start()
    pl.semaphore_wait(barrier, ranks - 1)
    for give in gives:
        give.start()
    load.wait()
    attend_all(pair, qs, keys, tail, vals, hot, tri, part_ref, buffers, look, scale)
    for give in gives:
        give.wait()
    keep.wait()


def return_pallas(tail, hot, tri, keys, vals, latent_out, turned, pair):
    heads, width, span_len = turned.shape
    ranks = latent_out.shape[0]
    rest = keys.shape[0]
    qb = tri.shape[0]
    look = min(-(-(span_len // 2) // qb), span_len // qb - 1)
    bf16 = jnp.bfloat16
    return pl.pallas_call(
        functools.partial(
            return_kernel,
            ranks=ranks,
            look=look,
            scale=math.log2(math.e) / math.sqrt(width),
            pair=pair,
        ),
        out_shape=(
            jax.ShapeDtypeStruct(latent_out.shape, bf16),
            jax.ShapeDtypeStruct((span_len, rest * 128), bf16),
        ),
        in_specs=[VMEM_SPEC] * 6 + [HBM_SPEC],
        out_specs=(VMEM_SPEC,) * 2,
        scratch_shapes=[
            pltpu.VMEM((rest, width, span_len), bf16),
            attend_scratch(qb, look),
            pltpu.SemaphoreType.DMA((2,)),
            pltpu.SemaphoreType.DMA((ranks - 1,)),
            pltpu.SemaphoreType.DMA((ranks - 1,)),
        ],
        compiler_params=pltpu.CompilerParams(
            collective_id=1, has_side_effects=True, vmem_limit_bytes=20 << 20
        ),
        cost_estimate=pl.CostEstimate(
            flops=12 * 10**9, bytes_accessed=12 << 20, transcendentals=6 << 20
        ),
    )(tail, hot, tri, keys, vals, latent_out, turned)


def project_kernel(back_ref, vw_ref, part_ref, half_ref, out_ref, whole_ref, wide, sems, *, heads, lat):
    ranks, owned, block, _ = back_ref.shape
    steps = block // heads
    local = ranks * owned
    columns = part_ref.shape[1]
    shown = pltpu.make_async_copy(
        part_ref, whole_ref.at[:, whole_ref.shape[1] - columns :], sems.at[0]
    )
    shown.start()
    for p in range(ranks):
        for r in range(owned):
            at = (p * owned + r) * block
            for c in range(lat // 128):
                wide[c, at : at + block] = back_ref[p, r, :, c * 128 : (c + 1) * 128].astype(
                    jnp.float32
                )
    for h in range(heads):
        mine = jnp.concatenate(
            [
                jnp.concatenate(
                    [
                        wide[c, pl.ds(s * heads + h, local, stride=block), :]
                        for c in range(lat // 128)
                    ],
                    axis=1,
                )
                for s in range(steps)
            ],
            axis=0,
        ).astype(jnp.bfloat16)
        out_ref[:, h * 128 : (h + 1) * 128] = jnp.dot(
            mine, vw_ref[:, h * 128 : (h + 1) * 128], preferred_element_type=jnp.float32
        ).astype(jnp.bfloat16)
    shown.wait()


def project_pallas(back, value_weight, part, whole, heads):
    ranks, owned, block, lat = back.shape
    rows = ranks * owned * block
    return pl.pallas_call(
        functools.partial(project_kernel, heads=heads, lat=lat),
        out_shape=(
            jax.ShapeDtypeStruct((rows // heads, heads * 128), jnp.bfloat16),
            jax.ShapeDtypeStruct(whole.shape, whole.dtype),
        ),
        in_specs=[VMEM_SPEC, VMEM_SPEC, VMEM_SPEC, HBM_SPEC],
        out_specs=(VMEM_SPEC, HBM_SPEC),
        scratch_shapes=[
            pltpu.VMEM((lat // 128, rows, 128), jnp.float32),
            pltpu.SemaphoreType.DMA((1,)),
        ],
        input_output_aliases={3: 1},
        compiler_params=pltpu.CompilerParams(vmem_limit_bytes=24 << 20),
    )(back, value_weight, part, whole)


def on_device(
    latent_rows,
    pre_queries,
    pre_lengths,
    owner_map,
    context_cache,
    context_lengths,
    new_latent,
    dec_queries,
    key_weight,
    value_weight,
):
    steps, rows_local, heads, width = dec_queries.shape
    ranks = lax.axis_size("head")
    if heads % 16 or latent_rows.shape[0] % 128 or ranks % 2:
        return plain_on_device(
            latent_rows,
            pre_queries,
            pre_lengths,
            owner_map,
            context_cache,
            context_lengths,
            new_latent,
            dec_queries,
            key_weight,
            value_weight,
        )
    lat = key_weight.shape[0]
    owned = context_cache.shape[0]
    pair = 4
    first = heads * 3 // 4
    qb = 256
    stay = lambda x: pltpu.with_memory_space_constraint(x, pltpu.HBM)
    turned = stay(jnp.transpose(pre_queries, (1, 2, 0)))
    kw_stay, vw_stay = stay(key_weight), stay(value_weight)
    spans, query, part, tail, hot, tri, keys, vals = gather_pallas(
        pre_lengths,
        stay(jnp.transpose(latent_rows)),
        stay(dec_queries.reshape(-1, width)),
        kw_stay,
        vw_stay,
        turned,
        owned,
        ranks,
        first,
        qb,
        pair,
    )
    latent_out, whole = decode_pallas(
        pre_lengths,
        owner_map,
        context_lengths,
        query,
        new_latent,
        spans,
        part,
        stay(jnp.transpose(context_cache, (0, 2, 1))),
        lat,
        heads,
        heads * 128,
        width,
        rows_local,
    )
    back, rest = return_pallas(tail, hot, tri, keys, vals, latent_out, turned, pair)
    decode_out, prefill_out = project_pallas(back, value_weight, rest, whole, heads)
    return (prefill_out, decode_out.reshape(steps, rows_local, heads * 128))


def solution(mesh):
    placed = (
        P(("groups", "batch", "head"), None),
        P(("groups", "batch"), "head", None),
        P("groups", None),
        P("groups", None),
        P(("groups", "batch", "head"), None, None),
        P(("groups", "batch", "head")),
        P("groups", ("batch", "head"), None),
        P("groups", "batch", "head", None),
        P(None, "head"),
        P(None, "head"),
    )
    return jax.shard_map(
        on_device,
        mesh=mesh,
        in_specs=placed,
        out_specs=(P(("groups", "batch"), "head"), P("groups", "batch", "head")),
        check_vma=False,
    )
```

```python
import functools
import math

import jax
import jax.numpy as jnp
from jax import lax
from jax.experimental import pallas as pl
from jax.experimental.pallas import tpu as pltpu
from jax.sharding import PartitionSpec as P

BLK = 512


NEGATIVE = -1e30


def from_partner(value, axis, distance):
    mask = 2**distance
    pairs = [(source, source ^ mask) for source in range(lax.axis_size(axis))]
    return lax.ppermute(value, axis, pairs)


def request_table(pre_lengths, owner_map, span_len):
    seg_ends = jnp.cumsum(pre_lengths, axis=1)
    span_base = jnp.arange(pre_lengths.shape[0], dtype=jnp.int32)[:, None] * span_len
    seg_starts = seg_ends - pre_lengths + span_base
    return (owner_map.reshape(-1), seg_starts.reshape(-1), pre_lengths.reshape(-1))


def prefill_heads(own_span, queries, span_lengths, key_weight, value_weight):
    span_len, head_count, query_width = queries.shape
    head_size = key_weight.shape[1] // head_count
    lat_width = key_weight.shape[0]
    score_scale = 1.0 / math.sqrt(query_width)
    latent = own_span[:, :lat_width]
    rope_keys = own_span[:, lat_width:]
    keys_nope = (
        jnp.dot(latent, key_weight, preferred_element_type=jnp.float32)
        .astype(jnp.bfloat16)
        .reshape(span_len, head_count, head_size)
    )
    values = (
        jnp.dot(latent, value_weight, preferred_element_type=jnp.float32)
        .astype(jnp.bfloat16)
        .reshape(span_len, head_count, head_size)
    )
    scores = jnp.einsum(
        "qhd,khd->hqk", queries[:, :, :head_size], keys_nope, preferred_element_type=jnp.float32
    )
    scores = scores + jnp.einsum(
        "qhr,kr->hqk", queries[:, :, head_size:], rope_keys, preferred_element_type=jnp.float32
    )
    scores = scores * score_scale
    seg_ends = jnp.cumsum(span_lengths)
    places = jnp.arange(span_len, dtype=jnp.int32)
    segment = jnp.sum((places[:, None] >= seg_ends[None, :]).astype(jnp.int32), axis=1)
    allowed = (segment[:, None] == segment[None, :]) & (places[None, :] <= places[:, None])
    masked = jnp.where(allowed[None], scores, NEGATIVE)
    peak_score = jnp.max(masked, axis=2, keepdims=True)
    weights = jnp.exp(masked - peak_score)
    weight_sum = jnp.sum(weights, axis=2)
    mixed_out = jnp.einsum(
        "hqk,khd->qhd", weights.astype(jnp.bfloat16), values, preferred_element_type=jnp.float32
    )
    mixed_out = mixed_out / jnp.transpose(weight_sum)[:, :, None]
    return mixed_out.astype(jnp.bfloat16).reshape(span_len, head_count * head_size)


def plain_on_device(
    latent_rows,
    pre_queries,
    pre_lengths,
    owner_map,
    context_cache,
    context_lengths,
    new_latent,
    dec_queries,
    key_weight,
    value_weight,
):
    head_rank = lax.axis_index("head")
    batch_rank = lax.axis_index("batch")
    span_len = pre_queries.shape[0]
    kv_width = latent_rows.shape[1]
    own_span = lax.all_gather(latent_rows, "head", axis=0, tiled=True)
    other_span = from_partner(own_span, "batch", 0)
    first_span = jnp.where(batch_rank == 0, own_span, other_span)
    second_span = jnp.where(batch_rank == 0, other_span, own_span)
    all_spans = jnp.concatenate([first_span, second_span], axis=0)
    span_lengths = lax.dynamic_index_in_dim(pre_lengths, batch_rank, 0, keepdims=False)
    prefill_out = prefill_heads(own_span, pre_queries, span_lengths, key_weight, value_weight)
    step_total, rows_local, head_count, query_width = dec_queries.shape
    lat_width = key_weight.shape[0]
    head_size = key_weight.shape[1] // head_count
    owned_rows = context_cache.shape[0]
    score_scale = 1.0 / math.sqrt(query_width)
    key_heads = key_weight.reshape(lat_width, head_count, head_size)
    value_heads = value_weight.reshape(lat_width, head_count, head_size)
    absorbed = jnp.einsum(
        "srhd,lhd->srhl",
        dec_queries[..., :head_size],
        key_heads,
        preferred_element_type=jnp.float32,
    ).astype(jnp.bfloat16)
    query_all = jnp.concatenate([absorbed, dec_queries[..., head_size:]], axis=3)
    flat_owner, flat_start, flat_length = request_table(pre_lengths, owner_map, span_len)
    row_ids = (
        batch_rank * rows_local + head_rank * owned_rows + jnp.arange(owned_rows, dtype=jnp.int32)
    )
    matches = (flat_owner[None, :] == row_ids[:, None]).astype(jnp.int32)
    is_target = jnp.sum(matches, axis=1) > 0
    first_row = jnp.sum(matches * flat_start[None, :], axis=1)
    prompt_len = jnp.sum(matches * flat_length[None, :], axis=1)
    effective = jnp.where(is_target, prompt_len, context_lengths)
    padded = jnp.concatenate([all_spans, jnp.zeros((span_len, kv_width), all_spans.dtype)], axis=0)
    replaced = jax.vmap(lambda offset: lax.dynamic_slice_in_dim(padded, offset, span_len, 0))(
        first_row
    )
    front_rows = jnp.where(is_target[:, None, None], replaced, context_cache[:, :span_len])
    front_blocks = span_len // BLK
    needed = (jnp.max(effective) + BLK - 1) // BLK
    fresh_latent = new_latent[..., :lat_width]
    owned_query = lax.all_to_all(query_all, "head", split_axis=1, concat_axis=2, tiled=True)
    fresh_scores = (
        jnp.einsum("srhk,jrk->srhj", owned_query, new_latent, preferred_element_type=jnp.float32)
        * score_scale
    )
    visible = (
        jnp.arange(new_latent.shape[0], dtype=jnp.int32)[None, :]
        <= jnp.arange(step_total, dtype=jnp.int32)[:, None]
    )
    fresh_scores = jnp.where(visible[:, None, None, :], fresh_scores, NEGATIVE)
    peak_score = jnp.max(fresh_scores, axis=3)
    weights = jnp.exp(fresh_scores - peak_score[..., None])
    weight_sum = jnp.sum(weights, axis=3)
    running = jnp.einsum(
        "srhj,jrl->srhl",
        weights.astype(jnp.bfloat16),
        fresh_latent,
        preferred_element_type=jnp.float32,
    )

    def advance(block_index, state_tuple, source):
        old_peak, old_sum, old_running = state_tuple
        key_block = lax.dynamic_slice_in_dim(source, block_index * BLK, BLK, 1)
        scores = (
            jnp.einsum("srhk,rtk->srht", owned_query, key_block, preferred_element_type=jnp.float32)
            * score_scale
        )
        places = block_index * BLK + jnp.arange(BLK, dtype=jnp.int32)
        in_context = places[None, :] < effective[:, None]
        scores = jnp.where(in_context[None, :, None, :], scores, NEGATIVE)
        new_peak = jnp.maximum(old_peak, jnp.max(scores, axis=3))
        factor = jnp.exp(old_peak - new_peak)
        block_weights = jnp.exp(scores - new_peak[..., None])
        new_sum = old_sum * factor + jnp.sum(block_weights, axis=3)
        new_running = old_running * factor[..., None] + jnp.einsum(
            "srht,rtl->srhl",
            block_weights.astype(jnp.bfloat16),
            key_block[..., :lat_width],
            preferred_element_type=jnp.float32,
        )
        return (new_peak, new_sum, new_running)

    state_tuple = lax.fori_loop(
        0,
        jnp.minimum(needed, front_blocks),
        lambda block_index, state_now: advance(block_index, state_now, front_rows),
        (peak_score, weight_sum, running),
    )
    state_tuple = lax.fori_loop(
        front_blocks,
        jnp.maximum(needed, front_blocks),
        lambda block_index, state_now: advance(block_index, state_now, context_cache),
        state_tuple,
    )
    latent_out = (state_tuple[2] / state_tuple[1][..., None]).astype(jnp.bfloat16)
    returned = lax.all_to_all(latent_out, "head", split_axis=2, concat_axis=1, tiled=True)
    projected = jnp.einsum(
        "srhl,lhd->srhd", returned, value_heads, preferred_element_type=jnp.float32
    ).astype(jnp.bfloat16)
    decode_out = projected.reshape(query_all.shape[0], rows_local, head_count * head_size)
    return (prefill_out, decode_out)


def trans_dot(left, right):
    return lax.dot_general(
        left, right, (((1,), (1,)), ((), ())), preferred_element_type=jnp.float32
    )


MESH = pl.DeviceIdType.MESH


def place_of(rank, ranks):
    odd = rank % 2
    return (1 - odd) * (rank // 2) + odd * (ranks - 1 - rank // 2)


def rank_at(place, ranks):
    late = place // (ranks // 2)
    return (1 - late) * (2 * place) + late * (2 * (ranks - 1 - place) + 1)


def start_marks(ends, tail, vals, hot, tri):
    span_len, full = tail.shape
    marks = hot.shape[0]
    segs = len(ends)
    where = lax.broadcasted_iota(jnp.int32, (span_len, marks), 0)
    lane = lax.broadcasted_iota(jnp.int32, (span_len, marks), 1)
    place = lax.broadcasted_iota(jnp.int32, (marks, span_len), 1)
    line = lax.broadcasted_iota(jnp.int32, (marks, span_len), 0)
    mine = jnp.zeros((span_len, marks), jnp.int32)
    seen = jnp.zeros((marks, span_len), jnp.int32)
    for k in range(segs - 1):
        mine = mine + (where >= ends[k]).astype(jnp.int32)
        seen = seen + (place >= ends[k]).astype(jnp.int32)
    mark = jnp.where((lane < segs) & (lane != mine), NEGATIVE, 0.0).astype(jnp.bfloat16)
    hot[...] = jnp.where(line == seen, 1.0, 0.0).astype(jnp.bfloat16)
    tail[:, full - marks :] = mark
    for h in range(vals.shape[0]):
        vals[h, 128:, :] = jnp.ones((vals.shape[1] - 128, span_len), jnp.bfloat16)
    size = tri.shape[0]
    key_at = lax.broadcasted_iota(jnp.int32, (size, size), 0)
    query_at = lax.broadcasted_iota(jnp.int32, (size, size), 1)
    tri[...] = jnp.where(key_at <= query_at, 0.0, NEGATIVE)


def project_shard(origin, spans_ref, kw, vw, keys, vals, tail, lat, heads):
    own = spans_ref.shape[2]
    rows = jnp.transpose(spans_ref[origin])
    at = pl.ds(pl.multiple_of(origin * own, own), own)
    tail[at, : rows.shape[1] - lat] = rows[:, lat:]
    latent = rows[:, :lat]
    pair = 2
    for g in range(heads // pair):
        columns = slice(g * pair * 128, (g + 1) * pair * 128)
        key = jnp.dot(latent, kw[:, columns], preferred_element_type=jnp.float32)
        value = jnp.dot(latent, vw[:, columns], preferred_element_type=jnp.float32)
        key = key.astype(jnp.bfloat16)
        value = jnp.transpose(value.astype(jnp.bfloat16))
        for p in range(pair):
            h = g * pair + p
            keys[h, at, :] = key[:, p * 128 : (p + 1) * 128]
            vals[h, :128, at] = value[p * 128 : (p + 1) * 128]


def attention(g, pair, qs, keys, tail, vals, hot, tri, part_ref, scores, weights, look, scale):
    span_len = tail.shape[0]
    qb = tri.shape[0]
    blocks = span_len // qb
    order = [(0, p) for p in range(pair // 2)]
    order += [(i, p) for i in range(1, blocks) for p in range(pair)]
    order += [(0, p) for p in range(pair // 2, pair)]
    count = len(order)
    lengths = [min(i, look) + 1 for i, _ in order]
    peaks = [None] * count
    tops = [None] * count
    sums = [None] * count

    def score(n, c):
        i, p = order[n]
        if c > 0:
            return
        at = (i - lengths[n] + 1) * qb
        size = lengths[n] * qb
        query = jnp.concatenate(
            [qs[g * pair + p, :, i * qb : (i + 1) * qb], hot[:, i * qb : (i + 1) * qb]], axis=0
        )
        key = jnp.concatenate(
            [keys[g * pair + p, at : at + size, :], tail[at : at + size, :]], axis=1
        )
        s = jnp.dot(key, query, preferred_element_type=jnp.float32)
        if size > qb:
            scores[n % 4][: size - qb, :] = s[: size - qb]
            peaks[n] = jnp.max(s[: size - qb].reshape((size - qb) // 8, 8, qb), axis=0)
        last = s[size - qb :] + tri[...]
        scores[n % 4][size - qb : size, :] = last
        top = jnp.max(last.reshape(qb // 8, 8, qb), axis=0)
        peaks[n] = top if peaks[n] is None else jnp.maximum(peaks[n], top)

    def soften(n, c):
        if c == 0:
            tops[n] = jnp.max(peaks[n], axis=0, keepdims=True)
        for k in range(0, qb, 32):
            at = slice(c * qb + k, c * qb + k + 32)
            w = jnp.exp2((scores[n % 4][at, :] - tops[n]) * scale)
            weights[n % 4][at, :] = w.astype(jnp.bfloat16)

    def mix(n, c):
        i, p = order[n]
        at = (i - lengths[n] + 1) * qb
        if c == 0:
            o = jnp.dot(
                vals[g * pair + p, :, at : at + lengths[n] * qb],
                weights[n % 4][: lengths[n] * qb, :],
                preferred_element_type=jnp.float32,
            )
            o = o[:128] * (1.0 / o[128:129])
            columns = pl.ds(pl.multiple_of((g * pair + p) * 128, 128), 128)
            part_ref[i * qb : (i + 1) * qb, columns] = jnp.transpose(o.astype(jnp.bfloat16))

    todo_score = [(n, c) for n in range(count) for c in range(lengths[n])]
    todo_soft = list(todo_score)
    todo_mix = list(todo_score)
    scored = [0] * count
    softened = [0] * count
    mixed = [0] * count
    while todo_mix:
        was = list(softened)
        if todo_score:
            n, c = todo_score[0]
            if n < 4 or softened[n - 4] == lengths[n - 4]:
                score(n, c)
                scored[n] += 1
                todo_score.pop(0)
        if todo_soft:
            n, c = todo_soft[0]
            free = n < 4 or mixed[n - 4] == lengths[n - 4]
            if scored[n] == lengths[n] and free and not (todo_score and todo_score[0][0] <= n + 2):
                soften(n, c)
                softened[n] += 1
                todo_soft.pop(0)
        n, c = todo_mix[0]
        if was[n] == lengths[n]:
            mix(n, c)
            mixed[n] += 1
            todo_mix.pop(0)


def attend_groups(low, high, pair, qs, keys, tail, vals, hot, tri, part_ref, buffers, look, scale):
    scores, weights = buffers

    def step(g, carry):
        attention(
            g, pair, qs, keys, tail, vals, hot, tri, part_ref, scores, weights, look, scale
        )
        return carry

    lax.fori_loop(low, high, step, 0)


def absorb_into(dq, kw, sent, flat, wide, heads, lat):
    rows = dq.shape[0]
    ranks, owned, block, _ = sent.shape
    steps = block // heads
    local = ranks * owned
    flat[...] = dq[:, :128].astype(jnp.float32)
    for h in range(heads):
        mine = flat[pl.ds(h, rows // heads, stride=heads), :].astype(jnp.bfloat16)
        res = trans_dot(mine, kw[:, h * 128 : (h + 1) * 128])
        for s in range(steps):
            for c in range(lat // 128):
                wide[c, pl.ds(s * heads + h, local, stride=block), :] = res[
                    s * local : (s + 1) * local, c * 128 : (c + 1) * 128
                ]
    for p in range(ranks):
        for r in range(owned):
            at = p * owned + r
            for c in range(lat // 128):
                sent[p, r, :, c * 128 : (c + 1) * 128] = wide[
                    c, at * block : (at + 1) * block
                ].astype(jnp.bfloat16)
            for s in range(steps):
                start = (s * local + at) * heads
                sent[p, r, s * heads : (s + 1) * heads, lat:] = dq[start : start + heads, 128:]


def span_ends(lens_ref, batch_rank):
    ends = []
    total = 0
    for k in range(lens_ref.shape[1]):
        total = total + lens_ref[batch_rank, k]
        ends.append(total)
    return ends


def request_facts(lens_ref, owner_ref, ctx_ref, r, row, batch_rank, span_len):
    target = jnp.int32(0)
    first = jnp.int32(0)
    length = jnp.int32(0)
    spans = lens_ref.shape[0]
    for c in range(spans):
        start = jnp.int32(((c + spans) % spans) * span_len)
        for k in range(lens_ref.shape[1]):
            hit = (owner_ref[c, k] == row).astype(jnp.int32)
            target = target + hit
            first = first + hit * start
            length = length + hit * lens_ref[c, k]
            start = start + lens_ref[c, k]
    first = ((first + batch_rank * span_len) % (2 * span_len)) * target
    return first, length, ctx_ref[r] * (1 - target)


def decode_request(r, facts, got, new_ref, spans_ref, cache, lo, tools, *, lat, heads, steps, scale, blk):
    peak_ref, sum_ref, acc_ref, asked, scores, tops, weights, fades = tools
    ranks, _, block, kv = got.shape
    rows = ranks * block
    first, length, held = facts
    own = spans_ref.shape[2]
    full = asked.shape[1]
    piece = 256
    blocks = cache.shape[2] // blk
    spread = (full - kv) // 16
    tail = lax.broadcasted_iota(jnp.int32, (rows, full - kv), 1)
    lanes = lax.broadcasted_iota(jnp.int32, (rows, 128), 1)
    columns = lax.broadcasted_iota(jnp.int32, (16, piece), 1)

    def hidden(keep):
        return [jnp.where(keep, 0.0, NEGATIVE).astype(jnp.bfloat16)] * spread

    def begin():
        asked[:, :kv] = got[:, r].reshape(rows, kv)
        asked[:, kv:] = jnp.where(tail == 0, 1.0, 0.0).astype(jnp.bfloat16)
        newest = new_ref[...].astype(jnp.float32)
        fresh = jnp.concatenate(
            [newest[s, r : r + 1] for s in range(steps)]
            + [jnp.zeros((128 - steps, kv), jnp.float32)],
            axis=0,
        ).astype(jnp.bfloat16)
        s = trans_dot(asked[:, :kv], fresh)
        row_step = (lax.broadcasted_iota(jnp.int32, s.shape, 0) // heads) % steps
        s = jnp.where(lanes <= row_step, s, NEGATIVE)
        most = -(-(cache_front(spans_ref) + own - 1) // piece)
        base = jnp.minimum(first // own, spans_ref.shape[0] - most * (piece // own))
        top = s
        for c in range(most):
            at = base + c * (piece // own)
            shards = jnp.concatenate([spans_ref[at + i] for i in range(piece // own)], axis=1)
            place = at * own + columns
            keys = jnp.concatenate(
                [shards] + hidden((place >= first) & (place < first + length)), axis=0
            )
            part = jnp.dot(asked[...], keys, preferred_element_type=jnp.float32)
            scores[c // 2][:, (c % 2) * piece : (c % 2 + 1) * piece] = part
            top = jnp.maximum(top, jnp.maximum(part[:, :128], part[:, 128:]))
        m = jnp.max(top, axis=1, keepdims=True)
        peak_ref[...] = jnp.broadcast_to(m, peak_ref.shape)
        w = jnp.exp2((s - m) * scale)
        total = w
        acc = jnp.dot(w.astype(jnp.bfloat16), fresh[:, :lat], preferred_element_type=jnp.float32)
        for c in range(most):
            at = base + c * (piece // own)
            shards = jnp.concatenate(
                [spans_ref[at + i, :lat] for i in range(piece // own)], axis=1
            )
            w = jnp.exp2((scores[c // 2][:, (c % 2) * piece : (c % 2 + 1) * piece] - m) * scale)
            total = total + (w[:, :128] + w[:, 128:])
            acc = acc + trans_dot(w.astype(jnp.bfloat16), shards)
        sum_ref[...] = total
        acc_ref[...] = acc
        weights[1][...] = jnp.zeros(weights[1].shape, jnp.bfloat16)
        fades[1][...] = jnp.ones(fades[1].shape, jnp.float32)

    def score(t, side, c):
        at = pl.multiple_of(t * blk + c * piece, piece)
        keys = jnp.concatenate(
            [cache[r, :, pl.ds(at, piece)]] + hidden(at + columns < held), axis=0
        )
        s = jnp.dot(asked[...], keys, preferred_element_type=jnp.float32)
        scores[side][:, c * piece : (c + 1) * piece] = s
        top = jnp.maximum(s[:, :128], s[:, 128:])
        if c > 0:
            top = jnp.maximum(top, tops[side][...])
        tops[side][...] = top

    def settle(side):
        old = peak_ref[...]
        new = jnp.maximum(old, jnp.max(tops[side][...], axis=1, keepdims=True))
        fade = jnp.exp2((old - new) * scale)
        fades[side][...] = fade
        peak_ref[...] = new
        sum_ref[...] = sum_ref[...] * fade

    def soften(side, c):
        at = slice(c * piece, (c + 1) * piece)
        new = peak_ref[...]
        s = scores[side][:, at]
        left = jnp.exp2((s[:, :128] - new) * scale)
        right = jnp.exp2((s[:, 128:] - new) * scale)
        sum_ref[...] = sum_ref[...] + (left + right)
        weights[side][:, at] = jnp.concatenate([left, right], axis=1).astype(jnp.bfloat16)

    def mix(t, side, c):
        at = pl.multiple_of(jnp.maximum(t, 0) * blk, blk)
        some = slice(c * piece, (c + 1) * piece)
        made = trans_dot(weights[side][...], cache[r, some, pl.ds(at, blk)])
        fade = fades[side][...]
        for k in range(piece // 128):
            here = slice(c * piece + k * 128, c * piece + (k + 1) * 128)
            acc_ref[:, here] = acc_ref[:, here] * fade + made[:, k * 128 : (k + 1) * 128]

    def turn(j, carry):
        for side in range(2):
            t = 2 * j + side
            settle(side)
            for c in range(blk // piece):
                score(jnp.minimum(t + 1, blocks - 1), 1 - side, c)
                soften(side, c)
                mix(t - 1, 1 - side, c)
        return carry

    begin()
    for c in range(blk // piece):
        score(jnp.int32(0), 0, c)
    lax.fori_loop(0, blocks // 2, turn, 0)
    for c in range(lat // piece):
        mix(jnp.int32(blocks - 1), 1, c)
    total = jnp.sum(sum_ref[...], axis=1, keepdims=True)
    done = (acc_ref[...] * (1.0 / total)).astype(lo.dtype)
    for p in range(ranks):
        lo[p, r] = done[p * block : (p + 1) * block]


def cache_front(spans_ref):
    return spans_ref.shape[0] * spans_ref.shape[2] // 4


def serve_kernel(
    lens_ref, owner_ref, ctx_ref, new_ref, shard_hbm, dq_hbm, kw_hbm, vw_hbm, q_hbm, cache_hbm,
    back, part_ref,
    spans_ref, got, tail, hot, tri, kw, vw, qs, dq, flat, wide, sent, keys, vals, buffers, cache,
    lo, tools,
    load_sems, cache_sems, ring_send, ring_recv, swap_sems,
    give_sems, take_sems, back_send, back_recv,
    *, lat, ranks, heads, look, scale, pair, before, blk
):
    me = lax.axis_index("head")
    batch_rank = lax.axis_index("batch")
    place = place_of(me, ranks)
    right = rank_at((place + 1) % ranks, ranks)
    left = rank_at((place + ranks - 1) % ranks, ranks)
    owned = cache.shape[0]
    span_len = tail.shape[0]
    steps = sent.shape[2] // heads
    loads = [
        pltpu.make_async_copy(shard_hbm, spans_ref.at[me], load_sems.at[0]),
        pltpu.make_async_copy(dq_hbm, dq, load_sems.at[1]),
        pltpu.make_async_copy(kw_hbm, kw, load_sems.at[2]),
        pltpu.make_async_copy(vw_hbm, vw, load_sems.at[3]),
        pltpu.make_async_copy(q_hbm, qs, load_sems.at[4]),
    ] + [
        pltpu.make_async_copy(cache_hbm.at[r], cache.at[r], cache_sems.at[r])
        for r in range(owned)
    ]
    barrier = pltpu.get_barrier_semaphore()
    for k in range(1, ranks):
        pl.semaphore_signal(
            barrier, inc=1, device_id={"head": (me + k) % ranks}, device_id_type=MESH
        )
    pl.semaphore_signal(
        barrier, inc=1, device_id={"batch": 1 - batch_rank}, device_id_type=MESH
    )
    for load in loads:
        load.start()
    start_marks(span_ends(lens_ref, batch_rank), tail, vals, hot, tri)
    pl.semaphore_wait(barrier, ranks)

    half = shard_hbm.shape[0] // 2
    most = ranks // 2

    def hop(way, part, t):
        back_by = t - 1 if way == 0 else ranks - t + 1
        origin = rank_at((place + ranks - back_by) % ranks, ranks)
        rows = pl.ds(part * half, half)
        return pltpu.make_async_remote_copy(
            src_ref=spans_ref.at[origin, rows],
            dst_ref=spans_ref.at[origin, rows],
            send_sem=ring_send.at[way, part, t - 1],
            recv_sem=ring_recv.at[way, part, t - 1],
            device_id={"head": right if way == 0 else left},
            device_id_type=MESH,
        )

    def hops(way, part):
        return most if way == part else most - 1

    streams = [(0, 0), (1, 1), (0, 1), (1, 0)]
    loads[0].wait()
    for way, part in streams:
        hop(way, part, 1).start()
    loads[1].wait()
    loads[2].wait()
    absorb_into(dq, kw, sent, flat, wide, heads, lat)
    loads[3].wait()

    def project(origin):
        project_shard(origin, spans_ref, kw, vw, keys, vals, tail, lat, heads)

    def arrive(t, carry):
        for way, part in streams:
            if hops(way, part) == most:
                hop(way, part, t).wait_recv()
                pl.when(t < most)(lambda: hop(way, part, t + 1).start())
            else:

                @pl.when(t < most)
                def _():
                    hop(way, part, t).wait_recv()
                    pl.when(t < most - 1)(lambda: hop(way, part, t + 1).start())

        def one(side, carry):
            project(rank_at((place + side * t + (1 - side) * (ranks - t)) % ranks, ranks))
            return carry

        lax.fori_loop(0, 2 - t // most, one, 0)
        return carry

    project(me)
    lax.fori_loop(1, most + 1, arrive, 0)

    def exchange(source, target, r, send_sems, recv_sems):
        return [
            pltpu.make_async_remote_copy(
                src_ref=source.at[(me + k) % ranks, r],
                dst_ref=target.at[me, r],
                send_sem=send_sems.at[r, k - 1],
                recv_sem=recv_sems.at[r, k - 1],
                device_id={"head": (me + k) % ranks},
                device_id_type=MESH,
            )
            for k in range(1, ranks)
        ]

    gives = [exchange(sent, got, r, give_sems, take_sems) for r in range(owned)]
    backs = [exchange(lo, back, r, back_send, back_recv) for r in range(owned)]
    swap = pltpu.make_async_remote_copy(
        src_ref=spans_ref.at[:ranks],
        dst_ref=spans_ref.at[ranks:],
        send_sem=swap_sems.at[0],
        recv_sem=swap_sems.at[1],
        device_id={"batch": 1 - batch_rank},
        device_id_type=MESH,
    )
    for copies in gives:
        for copy in copies:
            copy.start()
    swap.start()
    keep = pltpu.make_async_copy(sent.at[me], got.at[me], load_sems.at[5])
    keep.start()
    loads[4].wait()

    def attend(low, high):
        attend_groups(
            low, high, pair, qs, keys, tail, vals, hot, tri, part_ref, buffers, look, scale
        )

    groups = heads // pair
    attend(0, before)
    keep.wait()
    swap.wait()
    for r in range(owned):
        for copy in gives[r]:
            copy.wait()
        loads[5 + r].wait()
        row = batch_rank * (ranks * owned) + me * owned + r
        facts = request_facts(lens_ref, owner_ref, ctx_ref, r, row, batch_rank, span_len)
        decode_request(
            r, facts, got, new_ref, spans_ref, cache, lo, tools[r],
            lat=lat, heads=heads, steps=steps, scale=scale, blk=blk,
        )
        for copy in backs[r]:
            copy.start()
    stay = pltpu.make_async_copy(lo.at[me], back.at[me], load_sems.at[6])
    stay.start()
    attend(before, groups)
    for way, part in streams:
        for t in range(1, hops(way, part) + 1):
            hop(way, part, t).wait_send()
    for copies in backs:
        for copy in copies:
            copy.wait()
    stay.wait()


HBM_SPEC = pl.BlockSpec(memory_space=pltpu.HBM)
VMEM_SPEC = pl.BlockSpec(memory_space=pltpu.VMEM)
SMEM_SPEC = pl.BlockSpec(memory_space=pltpu.SMEM)


def serve_pallas(lens, owner, ctx, newest, shard, flat_queries, key_weight, value_weight, turned, cache, ranks, qb=256, pair=4, before=2, blk=512, ahead=4):
    heads, width, span_len = turned.shape
    kv, own = shard.shape
    lat = key_weight.shape[0]
    rows = flat_queries.shape[0]
    owned = cache.shape[0]
    block = rows // (ranks * owned)
    look = min(-(-(span_len // 2) // qb), span_len // qb - 1)
    marks = 128 - (kv - lat)
    deep = (look + 1) * qb
    asks = ranks * block
    bf16, f32 = jnp.bfloat16, jnp.float32
    vmem, dma = pltpu.VMEM, pltpu.SemaphoreType.DMA
    return pl.pallas_call(
        functools.partial(
            serve_kernel,
            lat=lat,
            ranks=ranks,
            heads=heads,
            look=look,
            scale=math.log2(math.e) / math.sqrt(width),
            pair=pair,
            before=before,
            blk=blk,
        ),
        out_shape=(
            jax.ShapeDtypeStruct((ranks, owned, block, lat), bf16),
            jax.ShapeDtypeStruct((span_len, heads * 128), bf16),
        ),
        in_specs=[SMEM_SPEC] * 3 + [VMEM_SPEC] + [HBM_SPEC] * 6,
        out_specs=(VMEM_SPEC,) * 2,
        scratch_shapes=[
            vmem((2 * ranks, kv, own), bf16),
            vmem((ranks, owned, block, kv), bf16),
            vmem((span_len, 128), bf16),
            vmem((marks, span_len), bf16),
            vmem((qb, qb), f32),
            vmem(key_weight.shape, bf16),
            vmem(value_weight.shape, bf16),
            vmem((heads, width, span_len), bf16),
            vmem((rows, width), bf16),
            vmem((rows, 128), f32),
            vmem((lat // 128, rows, 128), f32),
            vmem((ranks, owned, block, kv), bf16),
            vmem((heads, span_len, 128), bf16),
            vmem((heads, 144, span_len), bf16),
            [[vmem((deep, qb), f32)] * ahead, [vmem((deep, qb), bf16)] * ahead],
            vmem(cache.shape, bf16),
            vmem((ranks, owned, block, lat), bf16),
            [
                [
                    vmem((asks, 128), f32),
                    vmem((asks, 128), f32),
                    vmem((asks, lat), f32),
                    vmem((asks, -(-(kv + 16) // 128) * 128), bf16),
                    [vmem((asks, blk), f32)] * 2,
                    [vmem((asks, 128), f32)] * 2,
                    [vmem((asks, blk), bf16)] * 2,
                    [vmem((asks, 128), f32)] * 2,
                ]
            ]
            * owned,
            dma((7,)),
            dma((owned,)),
            dma((2, 2, ranks // 2)),
            dma((2, 2, ranks // 2)),
            dma((2,)),
            dma((owned, ranks - 1)),
            dma((owned, ranks - 1)),
            dma((owned, ranks - 1)),
            dma((owned, ranks - 1)),
        ],
        compiler_params=pltpu.CompilerParams(
            collective_id=0, has_side_effects=True, vmem_limit_bytes=54 << 20
        ),
        cost_estimate=pl.CostEstimate(
            flops=30 * 10**9, bytes_accessed=24 << 20, transcendentals=14 << 20
        ),
    )(lens, owner, ctx, newest, shard, flat_queries, key_weight, value_weight, turned, cache)


def project_kernel(back_ref, vw_ref, part_ref, out_ref, whole_ref, wide, sems, *, heads, lat):
    ranks, owned, block, _ = back_ref.shape
    steps = block // heads
    local = ranks * owned
    shown = pltpu.make_async_copy(part_ref, whole_ref, sems.at[0])
    shown.start()
    for p in range(ranks):
        for r in range(owned):
            at = (p * owned + r) * block
            for c in range(lat // 128):
                wide[c, at : at + block] = back_ref[p, r, :, c * 128 : (c + 1) * 128].astype(
                    jnp.float32
                )
    for h in range(heads):
        mine = jnp.concatenate(
            [
                jnp.concatenate(
                    [
                        wide[c, pl.ds(s * heads + h, local, stride=block), :]
                        for c in range(lat // 128)
                    ],
                    axis=1,
                )
                for s in range(steps)
            ],
            axis=0,
        ).astype(jnp.bfloat16)
        out_ref[:, h * 128 : (h + 1) * 128] = jnp.dot(
            mine, vw_ref[:, h * 128 : (h + 1) * 128], preferred_element_type=jnp.float32
        ).astype(jnp.bfloat16)
    shown.wait()


def project_pallas(back, value_weight, part, heads):
    ranks, owned, block, lat = back.shape
    rows = ranks * owned * block
    return pl.pallas_call(
        functools.partial(project_kernel, heads=heads, lat=lat),
        out_shape=(
            jax.ShapeDtypeStruct((rows // heads, heads * 128), jnp.bfloat16),
            jax.ShapeDtypeStruct(part.shape, part.dtype),
        ),
        in_specs=[VMEM_SPEC, VMEM_SPEC, VMEM_SPEC],
        out_specs=(VMEM_SPEC, HBM_SPEC),
        scratch_shapes=[
            pltpu.VMEM((lat // 128, rows, 128), jnp.float32),
            pltpu.SemaphoreType.DMA((1,)),
        ],
        compiler_params=pltpu.CompilerParams(vmem_limit_bytes=8 << 20),
    )(back, value_weight, part)


def on_device(
    latent_rows,
    pre_queries,
    pre_lengths,
    owner_map,
    context_cache,
    context_lengths,
    new_latent,
    dec_queries,
    key_weight,
    value_weight,
):
    steps, rows_local, heads, width = dec_queries.shape
    ranks = lax.axis_size("head")
    if heads % 16 or latent_rows.shape[0] % 128 or ranks % 2:
        return plain_on_device(
            latent_rows,
            pre_queries,
            pre_lengths,
            owner_map,
            context_cache,
            context_lengths,
            new_latent,
            dec_queries,
            key_weight,
            value_weight,
        )
    stay = lambda x: pltpu.with_memory_space_constraint(x, pltpu.HBM)
    back, part = serve_pallas(
        pre_lengths,
        owner_map,
        context_lengths,
        new_latent,
        stay(jnp.transpose(latent_rows)),
        stay(dec_queries.reshape(-1, width)),
        stay(key_weight),
        stay(value_weight),
        stay(jnp.transpose(pre_queries, (1, 2, 0))),
        stay(jnp.transpose(context_cache, (0, 2, 1))),
        ranks,
    )
    decode_out, prefill_out = project_pallas(back, value_weight, part, heads)
    return (prefill_out, decode_out.reshape(steps, rows_local, heads * 128))


def solution(mesh):
    placed = (
        P(("groups", "batch", "head"), None),
        P(("groups", "batch"), "head", None),
        P("groups", None),
        P("groups", None),
        P(("groups", "batch", "head"), None, None),
        P(("groups", "batch", "head")),
        P("groups", ("batch", "head"), None),
        P("groups", "batch", "head", None),
        P(None, "head"),
        P(None, "head"),
    )
    return jax.shard_map(
        on_device,
        mesh=mesh,
        in_specs=placed,
        out_specs=(P(("groups", "batch"), "head"), P("groups", "batch", "head")),
        check_vma=False,
    )
```

```python
import functools
import math

import jax
import jax.numpy as jnp
from jax import lax
from jax.experimental import pallas as pl
from jax.experimental.pallas import tpu as pltpu
from jax.sharding import PartitionSpec as P

BLK = 512


NEGATIVE = -1e30


def from_partner(value, axis, distance):
    mask = 2**distance
    pairs = [(source, source ^ mask) for source in range(lax.axis_size(axis))]
    return lax.ppermute(value, axis, pairs)


def request_table(pre_lengths, owner_map, span_len):
    seg_ends = jnp.cumsum(pre_lengths, axis=1)
    span_base = jnp.arange(pre_lengths.shape[0], dtype=jnp.int32)[:, None] * span_len
    seg_starts = seg_ends - pre_lengths + span_base
    return (owner_map.reshape(-1), seg_starts.reshape(-1), pre_lengths.reshape(-1))


def prefill_heads(own_span, queries, span_lengths, key_weight, value_weight):
    span_len, head_count, query_width = queries.shape
    head_size = key_weight.shape[1] // head_count
    lat_width = key_weight.shape[0]
    score_scale = 1.0 / math.sqrt(query_width)
    latent = own_span[:, :lat_width]
    rope_keys = own_span[:, lat_width:]
    keys_nope = (
        jnp.dot(latent, key_weight, preferred_element_type=jnp.float32)
        .astype(jnp.bfloat16)
        .reshape(span_len, head_count, head_size)
    )
    values = (
        jnp.dot(latent, value_weight, preferred_element_type=jnp.float32)
        .astype(jnp.bfloat16)
        .reshape(span_len, head_count, head_size)
    )
    scores = jnp.einsum(
        "qhd,khd->hqk", queries[:, :, :head_size], keys_nope, preferred_element_type=jnp.float32
    )
    scores = scores + jnp.einsum(
        "qhr,kr->hqk", queries[:, :, head_size:], rope_keys, preferred_element_type=jnp.float32
    )
    scores = scores * score_scale
    seg_ends = jnp.cumsum(span_lengths)
    places = jnp.arange(span_len, dtype=jnp.int32)
    segment = jnp.sum((places[:, None] >= seg_ends[None, :]).astype(jnp.int32), axis=1)
    allowed = (segment[:, None] == segment[None, :]) & (places[None, :] <= places[:, None])
    masked = jnp.where(allowed[None], scores, NEGATIVE)
    peak_score = jnp.max(masked, axis=2, keepdims=True)
    weights = jnp.exp(masked - peak_score)
    weight_sum = jnp.sum(weights, axis=2)
    mixed_out = jnp.einsum(
        "hqk,khd->qhd", weights.astype(jnp.bfloat16), values, preferred_element_type=jnp.float32
    )
    mixed_out = mixed_out / jnp.transpose(weight_sum)[:, :, None]
    return mixed_out.astype(jnp.bfloat16).reshape(span_len, head_count * head_size)


def plain_on_device(
    latent_rows,
    pre_queries,
    pre_lengths,
    owner_map,
    context_cache,
    context_lengths,
    new_latent,
    dec_queries,
    key_weight,
    value_weight,
):
    head_rank = lax.axis_index("head")
    batch_rank = lax.axis_index("batch")
    span_len = pre_queries.shape[0]
    kv_width = latent_rows.shape[1]
    own_span = lax.all_gather(latent_rows, "head", axis=0, tiled=True)
    other_span = from_partner(own_span, "batch", 0)
    first_span = jnp.where(batch_rank == 0, own_span, other_span)
    second_span = jnp.where(batch_rank == 0, other_span, own_span)
    all_spans = jnp.concatenate([first_span, second_span], axis=0)
    span_lengths = lax.dynamic_index_in_dim(pre_lengths, batch_rank, 0, keepdims=False)
    prefill_out = prefill_heads(own_span, pre_queries, span_lengths, key_weight, value_weight)
    step_total, rows_local, head_count, query_width = dec_queries.shape
    lat_width = key_weight.shape[0]
    head_size = key_weight.shape[1] // head_count
    owned_rows = context_cache.shape[0]
    score_scale = 1.0 / math.sqrt(query_width)
    key_heads = key_weight.reshape(lat_width, head_count, head_size)
    value_heads = value_weight.reshape(lat_width, head_count, head_size)
    absorbed = jnp.einsum(
        "srhd,lhd->srhl",
        dec_queries[..., :head_size],
        key_heads,
        preferred_element_type=jnp.float32,
    ).astype(jnp.bfloat16)
    query_all = jnp.concatenate([absorbed, dec_queries[..., head_size:]], axis=3)
    flat_owner, flat_start, flat_length = request_table(pre_lengths, owner_map, span_len)
    row_ids = (
        batch_rank * rows_local + head_rank * owned_rows + jnp.arange(owned_rows, dtype=jnp.int32)
    )
    matches = (flat_owner[None, :] == row_ids[:, None]).astype(jnp.int32)
    is_target = jnp.sum(matches, axis=1) > 0
    first_row = jnp.sum(matches * flat_start[None, :], axis=1)
    prompt_len = jnp.sum(matches * flat_length[None, :], axis=1)
    effective = jnp.where(is_target, prompt_len, context_lengths)
    padded = jnp.concatenate([all_spans, jnp.zeros((span_len, kv_width), all_spans.dtype)], axis=0)
    replaced = jax.vmap(lambda offset: lax.dynamic_slice_in_dim(padded, offset, span_len, 0))(
        first_row
    )
    front_rows = jnp.where(is_target[:, None, None], replaced, context_cache[:, :span_len])
    front_blocks = span_len // BLK
    needed = (jnp.max(effective) + BLK - 1) // BLK
    fresh_latent = new_latent[..., :lat_width]
    owned_query = lax.all_to_all(query_all, "head", split_axis=1, concat_axis=2, tiled=True)
    fresh_scores = (
        jnp.einsum("srhk,jrk->srhj", owned_query, new_latent, preferred_element_type=jnp.float32)
        * score_scale
    )
    visible = (
        jnp.arange(new_latent.shape[0], dtype=jnp.int32)[None, :]
        <= jnp.arange(step_total, dtype=jnp.int32)[:, None]
    )
    fresh_scores = jnp.where(visible[:, None, None, :], fresh_scores, NEGATIVE)
    peak_score = jnp.max(fresh_scores, axis=3)
    weights = jnp.exp(fresh_scores - peak_score[..., None])
    weight_sum = jnp.sum(weights, axis=3)
    running = jnp.einsum(
        "srhj,jrl->srhl",
        weights.astype(jnp.bfloat16),
        fresh_latent,
        preferred_element_type=jnp.float32,
    )

    def advance(block_index, state_tuple, source):
        old_peak, old_sum, old_running = state_tuple
        key_block = lax.dynamic_slice_in_dim(source, block_index * BLK, BLK, 1)
        scores = (
            jnp.einsum("srhk,rtk->srht", owned_query, key_block, preferred_element_type=jnp.float32)
            * score_scale
        )
        places = block_index * BLK + jnp.arange(BLK, dtype=jnp.int32)
        in_context = places[None, :] < effective[:, None]
        scores = jnp.where(in_context[None, :, None, :], scores, NEGATIVE)
        new_peak = jnp.maximum(old_peak, jnp.max(scores, axis=3))
        factor = jnp.exp(old_peak - new_peak)
        block_weights = jnp.exp(scores - new_peak[..., None])
        new_sum = old_sum * factor + jnp.sum(block_weights, axis=3)
        new_running = old_running * factor[..., None] + jnp.einsum(
            "srht,rtl->srhl",
            block_weights.astype(jnp.bfloat16),
            key_block[..., :lat_width],
            preferred_element_type=jnp.float32,
        )
        return (new_peak, new_sum, new_running)

    state_tuple = lax.fori_loop(
        0,
        jnp.minimum(needed, front_blocks),
        lambda block_index, state_now: advance(block_index, state_now, front_rows),
        (peak_score, weight_sum, running),
    )
    state_tuple = lax.fori_loop(
        front_blocks,
        jnp.maximum(needed, front_blocks),
        lambda block_index, state_now: advance(block_index, state_now, context_cache),
        state_tuple,
    )
    latent_out = (state_tuple[2] / state_tuple[1][..., None]).astype(jnp.bfloat16)
    returned = lax.all_to_all(latent_out, "head", split_axis=2, concat_axis=1, tiled=True)
    projected = jnp.einsum(
        "srhl,lhd->srhd", returned, value_heads, preferred_element_type=jnp.float32
    ).astype(jnp.bfloat16)
    decode_out = projected.reshape(query_all.shape[0], rows_local, head_count * head_size)
    return (prefill_out, decode_out)


def trans_dot(left, right):
    return lax.dot_general(
        left, right, (((1,), (1,)), ((), ())), preferred_element_type=jnp.float32
    )


MESH = pl.DeviceIdType.MESH


def place_of(rank, ranks):
    odd = rank % 2
    return (1 - odd) * (rank // 2) + odd * (ranks - 1 - rank // 2)


def rank_at(place, ranks):
    late = place // (ranks // 2)
    return (1 - late) * (2 * place) + late * (2 * (ranks - 1 - place) + 1)


def start_marks(ends, tail, vals, hot, tri):
    span_len, full = tail.shape
    marks = hot.shape[0]
    segs = len(ends)
    where = lax.broadcasted_iota(jnp.int32, (span_len, marks), 0)
    lane = lax.broadcasted_iota(jnp.int32, (span_len, marks), 1)
    place = lax.broadcasted_iota(jnp.int32, (marks, span_len), 1)
    line = lax.broadcasted_iota(jnp.int32, (marks, span_len), 0)
    mine = jnp.zeros((span_len, marks), jnp.int32)
    seen = jnp.zeros((marks, span_len), jnp.int32)
    for k in range(segs - 1):
        mine = mine + (where >= ends[k]).astype(jnp.int32)
        seen = seen + (place >= ends[k]).astype(jnp.int32)
    mark = jnp.where((lane < segs) & (lane != mine), NEGATIVE, 0.0).astype(jnp.bfloat16)
    hot[...] = jnp.where(line == seen, 1.0, 0.0).astype(jnp.bfloat16)
    tail[:, full - marks :] = mark
    for h in range(vals.shape[0]):
        vals[h, 128:, :] = jnp.ones((vals.shape[1] - 128, span_len), jnp.bfloat16)
    size = tri.shape[0]
    key_at = lax.broadcasted_iota(jnp.int32, (size, size), 0)
    query_at = lax.broadcasted_iota(jnp.int32, (size, size), 1)
    tri[...] = jnp.where(key_at <= query_at, 0.0, NEGATIVE)


def project_shard(origin, spans_ref, kw, vw, keys, vals, tail, lat, heads):
    own = spans_ref.shape[2]
    rows = jnp.transpose(spans_ref[origin])
    at = pl.ds(pl.multiple_of(origin * own, own), own)
    tail[at, : rows.shape[1] - lat] = rows[:, lat:]
    latent = rows[:, :lat]
    pair = 2
    for g in range(heads // pair):
        columns = slice(g * pair * 128, (g + 1) * pair * 128)
        key = jnp.dot(latent, kw[:, columns], preferred_element_type=jnp.float32)
        value = jnp.dot(latent, vw[:, columns], preferred_element_type=jnp.float32)
        key = key.astype(jnp.bfloat16)
        value = jnp.transpose(value.astype(jnp.bfloat16))
        for p in range(pair):
            h = g * pair + p
            keys[h, at, :] = key[:, p * 128 : (p + 1) * 128]
            vals[h, :128, at] = value[p * 128 : (p + 1) * 128]


def attention(g, pair, qs, keys, tail, vals, hot, tri, part_ref, scores, weights, look, scale):
    span_len = tail.shape[0]
    qb = tri.shape[0]
    blocks = span_len // qb
    order = [(0, p) for p in range(pair // 2)]
    order += [(i, p) for i in range(1, blocks) for p in range(pair)]
    order += [(0, p) for p in range(pair // 2, pair)]
    count = len(order)
    lengths = [min(i, look) + 1 for i, _ in order]
    peaks = [None] * count
    tops = [None] * count
    sums = [None] * count

    def score(n, c):
        i, p = order[n]
        if c > 0:
            return
        at = (i - lengths[n] + 1) * qb
        size = lengths[n] * qb
        query = jnp.concatenate(
            [qs[g * pair + p, :, i * qb : (i + 1) * qb], hot[:, i * qb : (i + 1) * qb]], axis=0
        )
        key = jnp.concatenate(
            [keys[g * pair + p, at : at + size, :], tail[at : at + size, :]], axis=1
        )
        s = jnp.dot(key, query, preferred_element_type=jnp.float32)
        if size > qb:
            scores[n % 4][: size - qb, :] = s[: size - qb]
            peaks[n] = jnp.max(s[: size - qb].reshape((size - qb) // 8, 8, qb), axis=0)
        last = s[size - qb :] + tri[...]
        scores[n % 4][size - qb : size, :] = last
        top = jnp.max(last.reshape(qb // 8, 8, qb), axis=0)
        peaks[n] = top if peaks[n] is None else jnp.maximum(peaks[n], top)

    def soften(n, c):
        if c == 0:
            tops[n] = jnp.max(peaks[n], axis=0, keepdims=True)
        for k in range(0, qb, 32):
            at = slice(c * qb + k, c * qb + k + 32)
            w = jnp.exp2((scores[n % 4][at, :] - tops[n]) * scale)
            weights[n % 4][at, :] = w.astype(jnp.bfloat16)

    def mix(n, c):
        i, p = order[n]
        at = (i - lengths[n] + 1) * qb
        if c == 0:
            o = jnp.dot(
                vals[g * pair + p, :, at : at + lengths[n] * qb],
                weights[n % 4][: lengths[n] * qb, :],
                preferred_element_type=jnp.float32,
            )
            o = o[:128] * (1.0 / o[128:129])
            columns = pl.ds(pl.multiple_of((g * pair + p) * 128, 128), 128)
            part_ref[i * qb : (i + 1) * qb, columns] = jnp.transpose(o.astype(jnp.bfloat16))

    todo_score = [(n, c) for n in range(count) for c in range(lengths[n])]
    todo_soft = list(todo_score)
    todo_mix = list(todo_score)
    scored = [0] * count
    softened = [0] * count
    mixed = [0] * count
    while todo_mix:
        was = list(softened)
        if todo_score:
            n, c = todo_score[0]
            if n < 4 or softened[n - 4] == lengths[n - 4]:
                score(n, c)
                scored[n] += 1
                todo_score.pop(0)
        if todo_soft:
            n, c = todo_soft[0]
            free = n < 4 or mixed[n - 4] == lengths[n - 4]
            if scored[n] == lengths[n] and free and not (todo_score and todo_score[0][0] <= n + 2):
                soften(n, c)
                softened[n] += 1
                todo_soft.pop(0)
        n, c = todo_mix[0]
        if was[n] == lengths[n]:
            mix(n, c)
            mixed[n] += 1
            todo_mix.pop(0)


def attend_groups(low, high, pair, qs, keys, tail, vals, hot, tri, part_ref, buffers, look, scale):
    scores, weights = buffers

    def step(g, carry):
        attention(
            g, pair, qs, keys, tail, vals, hot, tri, part_ref, scores, weights, look, scale
        )
        return carry

    lax.fori_loop(low, high, step, 0)


def absorb_into(dq, kw, sent, flat, wide, heads, lat):
    rows = dq.shape[0]
    ranks, owned, block, _ = sent.shape
    steps = block // heads
    local = ranks * owned
    flat[...] = dq[:, :128].astype(jnp.float32)
    for h in range(heads):
        mine = flat[pl.ds(h, rows // heads, stride=heads), :].astype(jnp.bfloat16)
        res = trans_dot(mine, kw[:, h * 128 : (h + 1) * 128])
        for s in range(steps):
            for c in range(lat // 128):
                wide[c, pl.ds(s * heads + h, local, stride=block), :] = res[
                    s * local : (s + 1) * local, c * 128 : (c + 1) * 128
                ]
    for p in range(ranks):
        for r in range(owned):
            at = p * owned + r
            for c in range(lat // 128):
                sent[p, r, :, c * 128 : (c + 1) * 128] = wide[
                    c, at * block : (at + 1) * block
                ].astype(jnp.bfloat16)
            for s in range(steps):
                start = (s * local + at) * heads
                sent[p, r, s * heads : (s + 1) * heads, lat:] = dq[start : start + heads, 128:]


def span_ends(lens_ref, batch_rank):
    ends = []
    total = 0
    for k in range(lens_ref.shape[1]):
        total = total + lens_ref[batch_rank, k]
        ends.append(total)
    return ends


def request_facts(lens_ref, owner_ref, ctx_ref, r, row, batch_rank, span_len):
    target = jnp.int32(0)
    first = jnp.int32(0)
    length = jnp.int32(0)
    spans = lens_ref.shape[0]
    for c in range(spans):
        start = jnp.int32(((c + spans) % spans) * span_len)
        for k in range(lens_ref.shape[1]):
            hit = (owner_ref[c, k] == row).astype(jnp.int32)
            target = target + hit
            first = first + hit * start
            length = length + hit * lens_ref[c, k]
            start = start + lens_ref[c, k]
    first = ((first + batch_rank * span_len) % (2 * span_len)) * target
    return first, length, ctx_ref[r] * (1 - target)


def decode_request(r, facts, got, new_ref, spans_ref, cache, lo, tools, *, lat, heads, steps, scale, blk):
    peak_ref, sum_ref, acc_ref, asked, scores, tops, weights, fades = tools
    ranks, _, block, kv = got.shape
    rows = ranks * block
    first, length, held = facts
    own = spans_ref.shape[2]
    full = asked.shape[1]
    piece = 256
    blocks = cache.shape[2] // blk
    spread = (full - kv) // 16
    tail = lax.broadcasted_iota(jnp.int32, (rows, full - kv), 1)
    lanes = lax.broadcasted_iota(jnp.int32, (rows, 128), 1)
    columns = lax.broadcasted_iota(jnp.int32, (16, piece), 1)

    def hidden(keep):
        return [jnp.where(keep, 0.0, NEGATIVE).astype(jnp.bfloat16)] * spread

    def begin():
        asked[:, :kv] = got[:, r].reshape(rows, kv)
        asked[:, kv:] = jnp.where(tail == 0, 1.0, 0.0).astype(jnp.bfloat16)
        newest = new_ref[...].astype(jnp.float32)
        fresh = jnp.concatenate(
            [newest[s, r : r + 1] for s in range(steps)]
            + [jnp.zeros((128 - steps, kv), jnp.float32)],
            axis=0,
        ).astype(jnp.bfloat16)
        s = trans_dot(asked[:, :kv], fresh)
        row_step = (lax.broadcasted_iota(jnp.int32, s.shape, 0) // heads) % steps
        s = jnp.where(lanes <= row_step, s, NEGATIVE)
        most = -(-(cache_front(spans_ref) + own - 1) // piece)
        base = jnp.minimum(first // own, spans_ref.shape[0] - most * (piece // own))
        top = s
        for c in range(most):
            at = base + c * (piece // own)
            shards = jnp.concatenate([spans_ref[at + i] for i in range(piece // own)], axis=1)
            place = at * own + columns
            keys = jnp.concatenate(
                [shards] + hidden((place >= first) & (place < first + length)), axis=0
            )
            part = jnp.dot(asked[...], keys, preferred_element_type=jnp.float32)
            scores[c // 2][:, (c % 2) * piece : (c % 2 + 1) * piece] = part
            top = jnp.maximum(top, jnp.maximum(part[:, :128], part[:, 128:]))
        m = jnp.max(top, axis=1, keepdims=True)
        peak_ref[...] = jnp.broadcast_to(m, peak_ref.shape)
        w = jnp.exp2((s - m) * scale)
        total = w
        acc = jnp.dot(w.astype(jnp.bfloat16), fresh[:, :lat], preferred_element_type=jnp.float32)
        for c in range(most):
            at = base + c * (piece // own)
            shards = jnp.concatenate(
                [spans_ref[at + i, :lat] for i in range(piece // own)], axis=1
            )
            w = jnp.exp2((scores[c // 2][:, (c % 2) * piece : (c % 2 + 1) * piece] - m) * scale)
            total = total + (w[:, :128] + w[:, 128:])
            acc = acc + trans_dot(w.astype(jnp.bfloat16), shards)
        sum_ref[...] = total
        acc_ref[...] = acc
        weights[1][...] = jnp.zeros(weights[1].shape, jnp.bfloat16)
        fades[1][...] = jnp.ones(fades[1].shape, jnp.float32)

    def score(t, side, c):
        at = pl.multiple_of(t * blk + c * piece, piece)
        keys = jnp.concatenate(
            [cache[r, :, pl.ds(at, piece)]] + hidden(at + columns < held), axis=0
        )
        s = jnp.dot(asked[...], keys, preferred_element_type=jnp.float32)
        scores[side][:, c * piece : (c + 1) * piece] = s
        top = jnp.maximum(s[:, :128], s[:, 128:])
        if c > 0:
            top = jnp.maximum(top, tops[side][...])
        tops[side][...] = top

    def settle(side):
        old = peak_ref[...]
        new = jnp.maximum(old, jnp.max(tops[side][...], axis=1, keepdims=True))
        fade = jnp.exp2((old - new) * scale)
        fades[side][...] = fade
        peak_ref[...] = new
        sum_ref[...] = sum_ref[...] * fade

    def soften(side, c):
        at = slice(c * piece, (c + 1) * piece)
        new = peak_ref[...]
        s = scores[side][:, at]
        left = jnp.exp2((s[:, :128] - new) * scale)
        right = jnp.exp2((s[:, 128:] - new) * scale)
        sum_ref[...] = sum_ref[...] + (left + right)
        weights[side][:, at] = jnp.concatenate([left, right], axis=1).astype(jnp.bfloat16)

    def mix(t, side, c):
        at = pl.multiple_of(jnp.maximum(t, 0) * blk, blk)
        some = slice(c * piece, (c + 1) * piece)
        made = trans_dot(weights[side][...], cache[r, some, pl.ds(at, blk)])
        fade = fades[side][...]
        for k in range(piece // 128):
            here = slice(c * piece + k * 128, c * piece + (k + 1) * 128)
            acc_ref[:, here] = acc_ref[:, here] * fade + made[:, k * 128 : (k + 1) * 128]

    def turn(j, carry):
        for side in range(2):
            t = 2 * j + side
            settle(side)
            for c in range(blk // piece):
                score(jnp.minimum(t + 1, blocks - 1), 1 - side, c)
                soften(side, c)
                mix(t - 1, 1 - side, c)
        return carry

    begin()
    for c in range(blk // piece):
        score(jnp.int32(0), 0, c)
    lax.fori_loop(0, blocks // 2, turn, 0)
    for c in range(lat // piece):
        mix(jnp.int32(blocks - 1), 1, c)
    total = jnp.sum(sum_ref[...], axis=1, keepdims=True)
    done = (acc_ref[...] * (1.0 / total)).astype(lo.dtype)
    for p in range(ranks):
        lo[p, r] = done[p * block : (p + 1) * block]


def cache_front(spans_ref):
    return spans_ref.shape[0] * spans_ref.shape[2] // 4


def serve_kernel(
    lens_hbm, owner_hbm, ctx_hbm, new_hbm, shard_hbm, dq_hbm, kw_hbm, vw_hbm, q_hbm, cache_hbm,
    back, part_ref,
    spans_ref, got, tail, hot, tri, kw, vw, qs, dq, flat, wide, sent, keys, vals, buffers, cache,
    lo, tools, lens_ref, owner_ref, ctx_ref, new_ref,
    load_sems, cache_sems, small_sems, ring_send, ring_recv, swap_sems,
    give_sems, take_sems, back_send, back_recv,
    *, lat, ranks, heads, look, scale, pair, before, blk
):
    me = lax.axis_index("head")
    batch_rank = lax.axis_index("batch")
    place = place_of(me, ranks)
    right = rank_at((place + 1) % ranks, ranks)
    left = rank_at((place + ranks - 1) % ranks, ranks)
    owned = cache.shape[0]
    span_len = tail.shape[0]
    steps = sent.shape[2] // heads
    loads = [
        pltpu.make_async_copy(shard_hbm, spans_ref.at[me], load_sems.at[0]),
        pltpu.make_async_copy(dq_hbm, dq, load_sems.at[1]),
        pltpu.make_async_copy(kw_hbm, kw, load_sems.at[2]),
        pltpu.make_async_copy(vw_hbm, vw, load_sems.at[3]),
        pltpu.make_async_copy(q_hbm, qs, load_sems.at[4]),
    ] + [
        pltpu.make_async_copy(cache_hbm.at[r], cache.at[r], cache_sems.at[r])
        for r in range(owned)
    ]
    barrier = pltpu.get_barrier_semaphore()
    for k in range(1, ranks):
        pl.semaphore_signal(
            barrier, inc=1, device_id={"head": (me + k) % ranks}, device_id_type=MESH
        )
    pl.semaphore_signal(
        barrier, inc=1, device_id={"batch": 1 - batch_rank}, device_id_type=MESH
    )
    smalls = [
        pltpu.make_async_copy(lens_hbm, lens_ref, small_sems.at[0]),
        pltpu.make_async_copy(owner_hbm, owner_ref, small_sems.at[1]),
        pltpu.make_async_copy(ctx_hbm, ctx_ref, small_sems.at[2]),
        pltpu.make_async_copy(new_hbm, new_ref, small_sems.at[3]),
    ]
    for load in smalls + loads:
        load.start()
    for small in smalls:
        small.wait()
    start_marks(span_ends(lens_ref, batch_rank), tail, vals, hot, tri)
    pl.semaphore_wait(barrier, ranks)

    half = shard_hbm.shape[0] // 2
    most = ranks // 2

    def hop(way, part, t):
        back_by = t - 1 if way == 0 else ranks - t + 1
        origin = rank_at((place + ranks - back_by) % ranks, ranks)
        rows = pl.ds(part * half, half)
        return pltpu.make_async_remote_copy(
            src_ref=spans_ref.at[origin, rows],
            dst_ref=spans_ref.at[origin, rows],
            send_sem=ring_send.at[way, part, t - 1],
            recv_sem=ring_recv.at[way, part, t - 1],
            device_id={"head": right if way == 0 else left},
            device_id_type=MESH,
        )

    def hops(way, part):
        return most if way == part else most - 1

    streams = [(0, 0), (1, 1), (0, 1), (1, 0)]
    loads[0].wait()
    for way, part in streams:
        hop(way, part, 1).start()
    loads[1].wait()
    loads[2].wait()
    absorb_into(dq, kw, sent, flat, wide, heads, lat)
    loads[3].wait()

    def project(origin):
        project_shard(origin, spans_ref, kw, vw, keys, vals, tail, lat, heads)

    def arrive(t, carry):
        for way, part in streams:
            if hops(way, part) == most:
                hop(way, part, t).wait_recv()
                pl.when(t < most)(lambda: hop(way, part, t + 1).start())
            else:

                @pl.when(t < most)
                def _():
                    hop(way, part, t).wait_recv()
                    pl.when(t < most - 1)(lambda: hop(way, part, t + 1).start())

        def one(side, carry):
            project(rank_at((place + side * t + (1 - side) * (ranks - t)) % ranks, ranks))
            return carry

        lax.fori_loop(0, 2 - t // most, one, 0)
        return carry

    project(me)
    lax.fori_loop(1, most + 1, arrive, 0)

    def exchange(source, target, r, send_sems, recv_sems):
        return [
            pltpu.make_async_remote_copy(
                src_ref=source.at[(me + k) % ranks, r],
                dst_ref=target.at[me, r],
                send_sem=send_sems.at[r, k - 1],
                recv_sem=recv_sems.at[r, k - 1],
                device_id={"head": (me + k) % ranks},
                device_id_type=MESH,
            )
            for k in range(1, ranks)
        ]

    gives = [exchange(sent, got, r, give_sems, take_sems) for r in range(owned)]
    backs = [exchange(lo, back, r, back_send, back_recv) for r in range(owned)]
    swap = pltpu.make_async_remote_copy(
        src_ref=spans_ref.at[:ranks],
        dst_ref=spans_ref.at[ranks:],
        send_sem=swap_sems.at[0],
        recv_sem=swap_sems.at[1],
        device_id={"batch": 1 - batch_rank},
        device_id_type=MESH,
    )
    for copies in gives:
        for copy in copies:
            copy.start()
    swap.start()
    keep = pltpu.make_async_copy(sent.at[me], got.at[me], load_sems.at[5])
    keep.start()
    loads[4].wait()

    def attend(low, high):
        attend_groups(
            low, high, pair, qs, keys, tail, vals, hot, tri, part_ref, buffers, look, scale
        )

    groups = heads // pair
    attend(0, before)
    keep.wait()
    swap.wait()
    for r in range(owned):
        for copy in gives[r]:
            copy.wait()
        loads[5 + r].wait()
        row = batch_rank * (ranks * owned) + me * owned + r
        facts = request_facts(lens_ref, owner_ref, ctx_ref, r, row, batch_rank, span_len)
        decode_request(
            r, facts, got, new_ref, spans_ref, cache, lo, tools,
            lat=lat, heads=heads, steps=steps, scale=scale, blk=blk,
        )
        for copy in backs[r]:
            copy.start()
    stay = pltpu.make_async_copy(lo.at[me], back.at[me], load_sems.at[6])
    stay.start()
    attend(before, groups)
    for way, part in streams:
        for t in range(1, hops(way, part) + 1):
            hop(way, part, t).wait_send()
    for copies in backs:
        for copy in copies:
            copy.wait()
    stay.wait()


HBM_SPEC = pl.BlockSpec(memory_space=pltpu.HBM)
VMEM_SPEC = pl.BlockSpec(memory_space=pltpu.VMEM)
SMEM_SPEC = pl.BlockSpec(memory_space=pltpu.SMEM)


def serve_pallas(lens, owner, ctx, newest, shard, flat_queries, key_weight, value_weight, turned, cache, ranks, qb=256, pair=4, before=2, blk=512, ahead=4):
    heads, width, span_len = turned.shape
    kv, own = shard.shape
    lat = key_weight.shape[0]
    rows = flat_queries.shape[0]
    owned = cache.shape[0]
    block = rows // (ranks * owned)
    look = min(-(-(span_len // 2) // qb), span_len // qb - 1)
    marks = 128 - (kv - lat)
    deep = (look + 1) * qb
    asks = ranks * block
    bf16, f32 = jnp.bfloat16, jnp.float32
    vmem, dma = pltpu.VMEM, pltpu.SemaphoreType.DMA
    return pl.pallas_call(
        functools.partial(
            serve_kernel,
            lat=lat,
            ranks=ranks,
            heads=heads,
            look=look,
            scale=math.log2(math.e) / math.sqrt(width),
            pair=pair,
            before=before,
            blk=blk,
        ),
        out_shape=(
            jax.ShapeDtypeStruct((ranks, owned, block, lat), bf16),
            jax.ShapeDtypeStruct((span_len, heads * 128), bf16),
        ),
        in_specs=[HBM_SPEC] * 10,
        out_specs=(VMEM_SPEC,) * 2,
        scratch_shapes=[
            vmem((2 * ranks, kv, own), bf16),
            vmem((ranks, owned, block, kv), bf16),
            vmem((span_len, 128), bf16),
            vmem((marks, span_len), bf16),
            vmem((qb, qb), f32),
            vmem(key_weight.shape, bf16),
            vmem(value_weight.shape, bf16),
            vmem((heads, width, span_len), bf16),
            vmem((rows, width), bf16),
            vmem((rows, 128), f32),
            vmem((lat // 128, rows, 128), f32),
            vmem((ranks, owned, block, kv), bf16),
            vmem((heads, span_len, 128), bf16),
            vmem((heads, 144, span_len), bf16),
            [[vmem((deep, qb), f32)] * ahead, [vmem((deep, qb), bf16)] * ahead],
            vmem(cache.shape, bf16),
            vmem((ranks, owned, block, lat), bf16),
            [
                vmem((asks, 128), f32),
                vmem((asks, 128), f32),
                vmem((asks, lat), f32),
                vmem((asks, -(-(kv + 16) // 128) * 128), bf16),
                [vmem((asks, blk), f32)] * 2,
                [vmem((asks, 128), f32)] * 2,
                [vmem((asks, blk), bf16)] * 2,
                [vmem((asks, 128), f32)] * 2,
            ],
            pltpu.SMEM(lens.shape, lens.dtype),
            pltpu.SMEM(owner.shape, owner.dtype),
            pltpu.SMEM(ctx.shape, ctx.dtype),
            vmem(newest.shape, newest.dtype),
            dma((7,)),
            dma((owned,)),
            dma((4,)),
            dma((2, 2, ranks // 2)),
            dma((2, 2, ranks // 2)),
            dma((2,)),
            dma((owned, ranks - 1)),
            dma((owned, ranks - 1)),
            dma((owned, ranks - 1)),
            dma((owned, ranks - 1)),
        ],
        compiler_params=pltpu.CompilerParams(
            collective_id=0, has_side_effects=True, vmem_limit_bytes=46 << 20
        ),
        cost_estimate=pl.CostEstimate(
            flops=30 * 10**9, bytes_accessed=24 << 20, transcendentals=14 << 20
        ),
    )(lens, owner, ctx, newest, shard, flat_queries, key_weight, value_weight, turned, cache)


def project_kernel(back_ref, vw_ref, part_ref, out_ref, whole_ref, wide, sems, *, heads, lat):
    ranks, owned, block, _ = back_ref.shape
    steps = block // heads
    local = ranks * owned
    shown = pltpu.make_async_copy(part_ref, whole_ref, sems.at[0])
    shown.start()
    for p in range(ranks):
        for r in range(owned):
            at = (p * owned + r) * block
            for c in range(lat // 128):
                wide[c, at : at + block] = back_ref[p, r, :, c * 128 : (c + 1) * 128].astype(
                    jnp.float32
                )
    for h in range(heads):
        mine = jnp.concatenate(
            [
                jnp.concatenate(
                    [
                        wide[c, pl.ds(s * heads + h, local, stride=block), :]
                        for c in range(lat // 128)
                    ],
                    axis=1,
                )
                for s in range(steps)
            ],
            axis=0,
        ).astype(jnp.bfloat16)
        out_ref[:, h * 128 : (h + 1) * 128] = jnp.dot(
            mine, vw_ref[:, h * 128 : (h + 1) * 128], preferred_element_type=jnp.float32
        ).astype(jnp.bfloat16)
    shown.wait()


def project_pallas(back, value_weight, part, heads):
    ranks, owned, block, lat = back.shape
    rows = ranks * owned * block
    return pl.pallas_call(
        functools.partial(project_kernel, heads=heads, lat=lat),
        out_shape=(
            jax.ShapeDtypeStruct((rows // heads, heads * 128), jnp.bfloat16),
            jax.ShapeDtypeStruct(part.shape, part.dtype),
        ),
        in_specs=[VMEM_SPEC, VMEM_SPEC, VMEM_SPEC],
        out_specs=(VMEM_SPEC, HBM_SPEC),
        scratch_shapes=[
            pltpu.VMEM((lat // 128, rows, 128), jnp.float32),
            pltpu.SemaphoreType.DMA((1,)),
        ],
        compiler_params=pltpu.CompilerParams(vmem_limit_bytes=8 << 20),
    )(back, value_weight, part)


def on_device(
    latent_rows,
    pre_queries,
    pre_lengths,
    owner_map,
    context_cache,
    context_lengths,
    new_latent,
    dec_queries,
    key_weight,
    value_weight,
):
    steps, rows_local, heads, width = dec_queries.shape
    ranks = lax.axis_size("head")
    if heads % 16 or latent_rows.shape[0] % 128 or ranks % 2:
        return plain_on_device(
            latent_rows,
            pre_queries,
            pre_lengths,
            owner_map,
            context_cache,
            context_lengths,
            new_latent,
            dec_queries,
            key_weight,
            value_weight,
        )
    stay = lambda x: pltpu.with_memory_space_constraint(x, pltpu.HBM)
    back, part = serve_pallas(
        stay(pre_lengths),
        stay(owner_map),
        stay(context_lengths),
        stay(new_latent),
        stay(jnp.transpose(latent_rows)),
        stay(dec_queries.reshape(-1, width)),
        stay(key_weight),
        stay(value_weight),
        stay(jnp.transpose(pre_queries, (1, 2, 0))),
        stay(jnp.transpose(context_cache, (0, 2, 1))),
        ranks,
    )
    decode_out, prefill_out = project_pallas(back, value_weight, part, heads)
    return (prefill_out, decode_out.reshape(steps, rows_local, heads * 128))


def solution(mesh):
    placed = (
        P(("groups", "batch", "head"), None),
        P(("groups", "batch"), "head", None),
        P("groups", None),
        P("groups", None),
        P(("groups", "batch", "head"), None, None),
        P(("groups", "batch", "head")),
        P("groups", ("batch", "head"), None),
        P("groups", "batch", "head", None),
        P(None, "head"),
        P(None, "head"),
    )
    return jax.shard_map(
        on_device,
        mesh=mesh,
        in_specs=placed,
        out_specs=(P(("groups", "batch"), "head"), P("groups", "batch", "head")),
        check_vma=False,
    )
```

```python
import functools
import math

import jax
import jax.numpy as jnp
from jax import lax
from jax.experimental import pallas as pl
from jax.experimental.pallas import tpu as pltpu
from jax.sharding import PartitionSpec as P

BLK = 512


NEGATIVE = -1e30


def from_partner(value, axis, distance):
    mask = 2**distance
    pairs = [(source, source ^ mask) for source in range(lax.axis_size(axis))]
    return lax.ppermute(value, axis, pairs)


def request_table(pre_lengths, owner_map, span_len):
    seg_ends = jnp.cumsum(pre_lengths, axis=1)
    span_base = jnp.arange(pre_lengths.shape[0], dtype=jnp.int32)[:, None] * span_len
    seg_starts = seg_ends - pre_lengths + span_base
    return (owner_map.reshape(-1), seg_starts.reshape(-1), pre_lengths.reshape(-1))


def prefill_heads(own_span, queries, span_lengths, key_weight, value_weight):
    span_len, head_count, query_width = queries.shape
    head_size = key_weight.shape[1] // head_count
    lat_width = key_weight.shape[0]
    score_scale = 1.0 / math.sqrt(query_width)
    latent = own_span[:, :lat_width]
    rope_keys = own_span[:, lat_width:]
    keys_nope = (
        jnp.dot(latent, key_weight, preferred_element_type=jnp.float32)
        .astype(jnp.bfloat16)
        .reshape(span_len, head_count, head_size)
    )
    values = (
        jnp.dot(latent, value_weight, preferred_element_type=jnp.float32)
        .astype(jnp.bfloat16)
        .reshape(span_len, head_count, head_size)
    )
    scores = jnp.einsum(
        "qhd,khd->hqk", queries[:, :, :head_size], keys_nope, preferred_element_type=jnp.float32
    )
    scores = scores + jnp.einsum(
        "qhr,kr->hqk", queries[:, :, head_size:], rope_keys, preferred_element_type=jnp.float32
    )
    scores = scores * score_scale
    seg_ends = jnp.cumsum(span_lengths)
    places = jnp.arange(span_len, dtype=jnp.int32)
    segment = jnp.sum((places[:, None] >= seg_ends[None, :]).astype(jnp.int32), axis=1)
    allowed = (segment[:, None] == segment[None, :]) & (places[None, :] <= places[:, None])
    masked = jnp.where(allowed[None], scores, NEGATIVE)
    peak_score = jnp.max(masked, axis=2, keepdims=True)
    weights = jnp.exp(masked - peak_score)
    weight_sum = jnp.sum(weights, axis=2)
    mixed_out = jnp.einsum(
        "hqk,khd->qhd", weights.astype(jnp.bfloat16), values, preferred_element_type=jnp.float32
    )
    mixed_out = mixed_out / jnp.transpose(weight_sum)[:, :, None]
    return mixed_out.astype(jnp.bfloat16).reshape(span_len, head_count * head_size)


def plain_on_device(
    latent_rows,
    pre_queries,
    pre_lengths,
    owner_map,
    context_cache,
    context_lengths,
    new_latent,
    dec_queries,
    key_weight,
    value_weight,
):
    head_rank = lax.axis_index("head")
    batch_rank = lax.axis_index("batch")
    span_len = pre_queries.shape[0]
    kv_width = latent_rows.shape[1]
    own_span = lax.all_gather(latent_rows, "head", axis=0, tiled=True)
    other_span = from_partner(own_span, "batch", 0)
    first_span = jnp.where(batch_rank == 0, own_span, other_span)
    second_span = jnp.where(batch_rank == 0, other_span, own_span)
    all_spans = jnp.concatenate([first_span, second_span], axis=0)
    span_lengths = lax.dynamic_index_in_dim(pre_lengths, batch_rank, 0, keepdims=False)
    prefill_out = prefill_heads(own_span, pre_queries, span_lengths, key_weight, value_weight)
    step_total, rows_local, head_count, query_width = dec_queries.shape
    lat_width = key_weight.shape[0]
    head_size = key_weight.shape[1] // head_count
    owned_rows = context_cache.shape[0]
    score_scale = 1.0 / math.sqrt(query_width)
    key_heads = key_weight.reshape(lat_width, head_count, head_size)
    value_heads = value_weight.reshape(lat_width, head_count, head_size)
    absorbed = jnp.einsum(
        "srhd,lhd->srhl",
        dec_queries[..., :head_size],
        key_heads,
        preferred_element_type=jnp.float32,
    ).astype(jnp.bfloat16)
    query_all = jnp.concatenate([absorbed, dec_queries[..., head_size:]], axis=3)
    flat_owner, flat_start, flat_length = request_table(pre_lengths, owner_map, span_len)
    row_ids = (
        batch_rank * rows_local + head_rank * owned_rows + jnp.arange(owned_rows, dtype=jnp.int32)
    )
    matches = (flat_owner[None, :] == row_ids[:, None]).astype(jnp.int32)
    is_target = jnp.sum(matches, axis=1) > 0
    first_row = jnp.sum(matches * flat_start[None, :], axis=1)
    prompt_len = jnp.sum(matches * flat_length[None, :], axis=1)
    effective = jnp.where(is_target, prompt_len, context_lengths)
    padded = jnp.concatenate([all_spans, jnp.zeros((span_len, kv_width), all_spans.dtype)], axis=0)
    replaced = jax.vmap(lambda offset: lax.dynamic_slice_in_dim(padded, offset, span_len, 0))(
        first_row
    )
    front_rows = jnp.where(is_target[:, None, None], replaced, context_cache[:, :span_len])
    front_blocks = span_len // BLK
    needed = (jnp.max(effective) + BLK - 1) // BLK
    fresh_latent = new_latent[..., :lat_width]
    owned_query = lax.all_to_all(query_all, "head", split_axis=1, concat_axis=2, tiled=True)
    fresh_scores = (
        jnp.einsum("srhk,jrk->srhj", owned_query, new_latent, preferred_element_type=jnp.float32)
        * score_scale
    )
    visible = (
        jnp.arange(new_latent.shape[0], dtype=jnp.int32)[None, :]
        <= jnp.arange(step_total, dtype=jnp.int32)[:, None]
    )
    fresh_scores = jnp.where(visible[:, None, None, :], fresh_scores, NEGATIVE)
    peak_score = jnp.max(fresh_scores, axis=3)
    weights = jnp.exp(fresh_scores - peak_score[..., None])
    weight_sum = jnp.sum(weights, axis=3)
    running = jnp.einsum(
        "srhj,jrl->srhl",
        weights.astype(jnp.bfloat16),
        fresh_latent,
        preferred_element_type=jnp.float32,
    )

    def advance(block_index, state_tuple, source):
        old_peak, old_sum, old_running = state_tuple
        key_block = lax.dynamic_slice_in_dim(source, block_index * BLK, BLK, 1)
        scores = (
            jnp.einsum("srhk,rtk->srht", owned_query, key_block, preferred_element_type=jnp.float32)
            * score_scale
        )
        places = block_index * BLK + jnp.arange(BLK, dtype=jnp.int32)
        in_context = places[None, :] < effective[:, None]
        scores = jnp.where(in_context[None, :, None, :], scores, NEGATIVE)
        new_peak = jnp.maximum(old_peak, jnp.max(scores, axis=3))
        factor = jnp.exp(old_peak - new_peak)
        block_weights = jnp.exp(scores - new_peak[..., None])
        new_sum = old_sum * factor + jnp.sum(block_weights, axis=3)
        new_running = old_running * factor[..., None] + jnp.einsum(
            "srht,rtl->srhl",
            block_weights.astype(jnp.bfloat16),
            key_block[..., :lat_width],
            preferred_element_type=jnp.float32,
        )
        return (new_peak, new_sum, new_running)

    state_tuple = lax.fori_loop(
        0,
        jnp.minimum(needed, front_blocks),
        lambda block_index, state_now: advance(block_index, state_now, front_rows),
        (peak_score, weight_sum, running),
    )
    state_tuple = lax.fori_loop(
        front_blocks,
        jnp.maximum(needed, front_blocks),
        lambda block_index, state_now: advance(block_index, state_now, context_cache),
        state_tuple,
    )
    latent_out = (state_tuple[2] / state_tuple[1][..., None]).astype(jnp.bfloat16)
    returned = lax.all_to_all(latent_out, "head", split_axis=2, concat_axis=1, tiled=True)
    projected = jnp.einsum(
        "srhl,lhd->srhd", returned, value_heads, preferred_element_type=jnp.float32
    ).astype(jnp.bfloat16)
    decode_out = projected.reshape(query_all.shape[0], rows_local, head_count * head_size)
    return (prefill_out, decode_out)


def trans_dot(left, right):
    return lax.dot_general(
        left, right, (((1,), (1,)), ((), ())), preferred_element_type=jnp.float32
    )


MESH = pl.DeviceIdType.MESH


def place_of(rank, ranks):
    odd = rank % 2
    return (1 - odd) * (rank // 2) + odd * (ranks - 1 - rank // 2)


def rank_at(place, ranks):
    late = place // (ranks // 2)
    return (1 - late) * (2 * place) + late * (2 * (ranks - 1 - place) + 1)


def start_marks(ends, tail, vals, hot, tri):
    span_len, full = tail.shape
    marks = hot.shape[0]
    segs = len(ends)
    where = lax.broadcasted_iota(jnp.int32, (span_len, marks), 0)
    lane = lax.broadcasted_iota(jnp.int32, (span_len, marks), 1)
    place = lax.broadcasted_iota(jnp.int32, (marks, span_len), 1)
    line = lax.broadcasted_iota(jnp.int32, (marks, span_len), 0)
    mine = jnp.zeros((span_len, marks), jnp.int32)
    seen = jnp.zeros((marks, span_len), jnp.int32)
    for k in range(segs - 1):
        mine = mine + (where >= ends[k]).astype(jnp.int32)
        seen = seen + (place >= ends[k]).astype(jnp.int32)
    mark = jnp.where((lane < segs) & (lane != mine), NEGATIVE, 0.0).astype(jnp.bfloat16)
    hot[...] = jnp.where(line == seen, 1.0, 0.0).astype(jnp.bfloat16)
    tail[:, full - marks :] = mark
    for h in range(vals.shape[0]):
        vals[h, 128:, :] = jnp.ones((vals.shape[1] - 128, span_len), jnp.bfloat16)
    size = tri.shape[0]
    key_at = lax.broadcasted_iota(jnp.int32, (size, size), 0)
    query_at = lax.broadcasted_iota(jnp.int32, (size, size), 1)
    tri[...] = jnp.where(key_at <= query_at, 0.0, NEGATIVE)


def project_shard(origin, spans_ref, kw, vw, keys, vals, tail, lat, heads):
    own = spans_ref.shape[2]
    rows = jnp.transpose(spans_ref[origin])
    at = pl.ds(pl.multiple_of(origin * own, own), own)
    tail[at, : rows.shape[1] - lat] = rows[:, lat:]
    latent = rows[:, :lat]
    pair = 2
    for g in range(heads // pair):
        columns = slice(g * pair * 128, (g + 1) * pair * 128)
        key = jnp.dot(latent, kw[:, columns], preferred_element_type=jnp.float32)
        value = jnp.dot(latent, vw[:, columns], preferred_element_type=jnp.float32)
        key = key.astype(jnp.bfloat16)
        value = jnp.transpose(value.astype(jnp.bfloat16))
        for p in range(pair):
            h = g * pair + p
            keys[h, at, :] = key[:, p * 128 : (p + 1) * 128]
            vals[h, :128, at] = value[p * 128 : (p + 1) * 128]


def attention(g, pair, qs, keys, tail, vals, hot, tri, part_ref, scores, weights, look, scale):
    span_len = tail.shape[0]
    qb = tri.shape[0]
    blocks = span_len // qb
    order = [(0, p) for p in range(pair // 2)]
    order += [(i, p) for i in range(1, blocks) for p in range(pair)]
    order += [(0, p) for p in range(pair // 2, pair)]
    count = len(order)
    lengths = [min(i, look) + 1 for i, _ in order]
    peaks = [None] * count
    tops = [None] * count
    sums = [None] * count

    def score(n, c):
        i, p = order[n]
        if c > 0:
            return
        at = (i - lengths[n] + 1) * qb
        size = lengths[n] * qb
        query = jnp.concatenate(
            [qs[g * pair + p, :, i * qb : (i + 1) * qb], hot[:, i * qb : (i + 1) * qb]], axis=0
        )
        key = jnp.concatenate(
            [keys[g * pair + p, at : at + size, :], tail[at : at + size, :]], axis=1
        )
        s = jnp.dot(key, query, preferred_element_type=jnp.float32)
        if size > qb:
            scores[n % 4][: size - qb, :] = s[: size - qb]
            peaks[n] = jnp.max(s[: size - qb].reshape((size - qb) // 8, 8, qb), axis=0)
        last = s[size - qb :] + tri[...]
        scores[n % 4][size - qb : size, :] = last
        top = jnp.max(last.reshape(qb // 8, 8, qb), axis=0)
        peaks[n] = top if peaks[n] is None else jnp.maximum(peaks[n], top)

    def soften(n, c):
        if c == 0:
            tops[n] = jnp.max(peaks[n], axis=0, keepdims=True)
        for k in range(0, qb, 32):
            at = slice(c * qb + k, c * qb + k + 32)
            w = jnp.exp2((scores[n % 4][at, :] - tops[n]) * scale)
            weights[n % 4][at, :] = w.astype(jnp.bfloat16)

    def mix(n, c):
        i, p = order[n]
        at = (i - lengths[n] + 1) * qb
        if c == 0:
            o = jnp.dot(
                vals[g * pair + p, :, at : at + lengths[n] * qb],
                weights[n % 4][: lengths[n] * qb, :],
                preferred_element_type=jnp.float32,
            )
            o = o[:128] * (1.0 / o[128:129])
            columns = pl.ds(pl.multiple_of((g * pair + p) * 128, 128), 128)
            part_ref[i * qb : (i + 1) * qb, columns] = jnp.transpose(o.astype(jnp.bfloat16))

    todo_score = [(n, c) for n in range(count) for c in range(lengths[n])]
    todo_soft = list(todo_score)
    todo_mix = list(todo_score)
    scored = [0] * count
    softened = [0] * count
    mixed = [0] * count
    while todo_mix:
        was = list(softened)
        if todo_score:
            n, c = todo_score[0]
            if n < 4 or softened[n - 4] == lengths[n - 4]:
                score(n, c)
                scored[n] += 1
                todo_score.pop(0)
        if todo_soft:
            n, c = todo_soft[0]
            free = n < 4 or mixed[n - 4] == lengths[n - 4]
            if scored[n] == lengths[n] and free and not (todo_score and todo_score[0][0] <= n + 2):
                soften(n, c)
                softened[n] += 1
                todo_soft.pop(0)
        n, c = todo_mix[0]
        if was[n] == lengths[n]:
            mix(n, c)
            mixed[n] += 1
            todo_mix.pop(0)


def attend_groups(low, high, pair, qs, keys, tail, vals, hot, tri, part_ref, buffers, look, scale):
    scores, weights = buffers

    def step(g, carry):
        attention(
            g, pair, qs, keys, tail, vals, hot, tri, part_ref, scores, weights, look, scale
        )
        return carry

    lax.fori_loop(low, high, step, 0)


def absorb_into(dq, kw, sent, flat, wide, heads, lat):
    rows = dq.shape[0]
    ranks, owned, block, _ = sent.shape
    steps = block // heads
    local = ranks * owned
    flat[...] = dq[:, :128].astype(jnp.float32)
    for h in range(heads):
        mine = flat[pl.ds(h, rows // heads, stride=heads), :].astype(jnp.bfloat16)
        res = trans_dot(mine, kw[:, h * 128 : (h + 1) * 128])
        for s in range(steps):
            for c in range(lat // 128):
                wide[c, pl.ds(s * heads + h, local, stride=block), :] = res[
                    s * local : (s + 1) * local, c * 128 : (c + 1) * 128
                ]
    for p in range(ranks):
        for r in range(owned):
            at = p * owned + r
            for c in range(lat // 128):
                sent[p, r, :, c * 128 : (c + 1) * 128] = wide[
                    c, at * block : (at + 1) * block
                ].astype(jnp.bfloat16)
            for s in range(steps):
                start = (s * local + at) * heads
                sent[p, r, s * heads : (s + 1) * heads, lat:] = dq[start : start + heads, 128:]


def span_ends(lens_ref, batch_rank):
    ends = []
    total = 0
    for k in range(lens_ref.shape[1]):
        total = total + lens_ref[batch_rank, k]
        ends.append(total)
    return ends


def request_facts(lens_ref, owner_ref, ctx_ref, r, row, batch_rank, span_len):
    target = jnp.int32(0)
    first = jnp.int32(0)
    length = jnp.int32(0)
    spans = lens_ref.shape[0]
    for c in range(spans):
        start = jnp.int32(((c + spans) % spans) * span_len)
        for k in range(lens_ref.shape[1]):
            hit = (owner_ref[c, k] == row).astype(jnp.int32)
            target = target + hit
            first = first + hit * start
            length = length + hit * lens_ref[c, k]
            start = start + lens_ref[c, k]
    first = ((first + batch_rank * span_len) % (2 * span_len)) * target
    return first, length, ctx_ref[r] * (1 - target)


def decode_request(r, facts, got, new_ref, spans_ref, cache, lo, tools, *, lat, heads, steps, scale, blk):
    peak_ref, sum_ref, acc_ref, asked, scores, tops, weights, fades = tools
    ranks, _, block, kv = got.shape
    rows = ranks * block
    first, length, held = facts
    own = spans_ref.shape[2]
    full = asked.shape[1]
    piece = 256
    blocks = cache.shape[2] // blk
    spread = (full - kv) // 16
    tail = lax.broadcasted_iota(jnp.int32, (rows, full - kv), 1)
    columns = lax.broadcasted_iota(jnp.int32, (16, piece), 1)

    line = lax.broadcasted_iota(jnp.int32, (16, piece), 0)

    def hidden(keep):
        mask = jnp.where((line == 0) & jnp.logical_not(keep), NEGATIVE, 0.0)
        return [mask.astype(jnp.bfloat16)] * spread

    def begin():
        asked[:, :kv] = got[:, r].reshape(rows, kv)
        row_step = (lax.broadcasted_iota(jnp.int32, tail.shape, 0) // heads) % steps
        asked[:, kv:] = jnp.where((tail == 0) | (tail == row_step + 1), 1.0, 0.0).astype(
            jnp.bfloat16
        )
        newest = new_ref[...].astype(jnp.float32)
        fresh = jnp.concatenate(
            [newest[s, r : r + 1] for s in range(steps)]
            + [jnp.zeros((own - steps, kv), jnp.float32)],
            axis=0,
        ).astype(jnp.bfloat16)
        fresh = jnp.transpose(fresh)
        span_len = spans_ref.shape[0] * own // 2
        shards = -(-(span_len // 2 + own - 1) // own)
        base = jnp.minimum(first // own, spans_ref.shape[0] - shards)
        each = piece // own
        most = (shards + 1) // each

        def block(c):
            parts = []
            for i in range(c * each, (c + 1) * each):
                parts.append(spans_ref[base + i] if i < shards else fresh)
            return jnp.concatenate(parts, axis=1)

        top = None
        for c in range(most):
            place = (base + c * each) * own + columns
            keep = (place >= first) & (place < first + length)
            mask = jnp.where((line == 0) & jnp.logical_not(keep), NEGATIVE, 0.0)
            if c == most - 1:
                new_at = columns - (piece - own)
                late = (line == 0) & (new_at >= steps)
                late = late | ((line > 0) & (new_at > line - 1))
                mask = jnp.where(new_at >= 0, jnp.where(late, NEGATIVE, 0.0), mask)
            keys = jnp.concatenate([block(c)] + [mask.astype(jnp.bfloat16)] * spread, axis=0)
            part = jnp.dot(asked[...], keys, preferred_element_type=jnp.float32)
            scores[c // 2][:, (c % 2) * piece : (c % 2 + 1) * piece] = part
            best = jnp.maximum(part[:, :128], part[:, 128:])
            top = best if top is None else jnp.maximum(top, best)
        m = jnp.max(top, axis=1, keepdims=True)
        peak_ref[...] = jnp.broadcast_to(m, peak_ref.shape)
        total, acc = None, None
        for c in range(most):
            w = jnp.exp2((scores[c // 2][:, (c % 2) * piece : (c % 2 + 1) * piece] - m) * scale)
            both = w[:, :128] + w[:, 128:]
            made = trans_dot(w.astype(jnp.bfloat16), block(c)[:lat])
            total = both if total is None else total + both
            acc = made if acc is None else acc + made
        sum_ref[...] = total
        acc_ref[...] = acc
        weights[1][...] = jnp.zeros(weights[1].shape, jnp.bfloat16)
        fades[1][...] = jnp.ones(fades[1].shape, jnp.float32)

    def score(t, side, c):
        at = pl.multiple_of(t * blk + c * piece, piece)
        keys = jnp.concatenate(
            [cache[r, :, pl.ds(at, piece)]] + hidden(at + columns < held), axis=0
        )
        s = jnp.dot(asked[...], keys, preferred_element_type=jnp.float32)
        scores[side][:, c * piece : (c + 1) * piece] = s
        top = jnp.maximum(s[:, :128], s[:, 128:])
        if c > 0:
            top = jnp.maximum(top, tops[side][...])
        tops[side][...] = top

    def settle(side):
        old = peak_ref[...]
        new = jnp.maximum(old, jnp.max(tops[side][...], axis=1, keepdims=True))
        fade = jnp.exp2((old - new) * scale)
        fades[side][...] = fade
        peak_ref[...] = new
        sum_ref[...] = sum_ref[...] * fade

    def soften(side, c):
        at = slice(c * piece, (c + 1) * piece)
        new = peak_ref[...]
        s = scores[side][:, at]
        left = jnp.exp2((s[:, :128] - new) * scale)
        right = jnp.exp2((s[:, 128:] - new) * scale)
        sum_ref[...] = sum_ref[...] + (left + right)
        weights[side][:, at] = jnp.concatenate([left, right], axis=1).astype(jnp.bfloat16)

    def mix(t, side, c):
        at = pl.multiple_of(jnp.maximum(t, 0) * blk, blk)
        some = slice(c * piece, (c + 1) * piece)
        made = trans_dot(weights[side][...], cache[r, some, pl.ds(at, blk)])
        fade = fades[side][...]
        for k in range(piece // 128):
            here = slice(c * piece + k * 128, c * piece + (k + 1) * 128)
            acc_ref[:, here] = acc_ref[:, here] * fade + made[:, k * 128 : (k + 1) * 128]

    def turn(j, carry):
        for side in range(2):
            t = 2 * j + side
            settle(side)
            for c in range(blk // piece):
                if not (isinstance(t, int) and t + 1 == blocks):
                    score(t + 1, 1 - side, c)
                soften(side, c)
                mix(t - 1, 1 - side, c)
        return carry

    begin()
    for c in range(blk // piece):
        score(0, 0, c)
    lax.fori_loop(0, blocks // 2 - 1, turn, 0)
    turn(blocks // 2 - 1, 0)
    for c in range(lat // piece):
        mix(blocks - 1, 1, c)
    total = jnp.sum(sum_ref[...], axis=1, keepdims=True)
    done = (acc_ref[...] * (1.0 / total)).astype(lo.dtype)
    for p in range(ranks):
        lo[p, r] = done[p * block : (p + 1) * block]


def serve_kernel(
    lens_hbm, owner_hbm, ctx_hbm, new_hbm, shard_hbm, dq_hbm, kw_hbm, vw_hbm, q_hbm, cache_hbm,
    back, part_ref,
    spans_ref, got, tail, hot, tri, kw, vw, qs, dq, flat, wide, sent, keys, vals, buffers, cache,
    lo, tools, lens_ref, owner_ref, ctx_ref, new_ref,
    load_sems, cache_sems, small_sems, ring_send, ring_recv, swap_sems,
    give_sems, take_sems, back_send, back_recv,
    *, lat, ranks, heads, look, scale, pair, before, blk
):
    me = lax.axis_index("head")
    batch_rank = lax.axis_index("batch")
    place = place_of(me, ranks)
    right = rank_at((place + 1) % ranks, ranks)
    left = rank_at((place + ranks - 1) % ranks, ranks)
    owned = cache.shape[0]
    span_len = tail.shape[0]
    steps = sent.shape[2] // heads
    loads = [
        pltpu.make_async_copy(shard_hbm, spans_ref.at[me], load_sems.at[0]),
        pltpu.make_async_copy(dq_hbm, dq, load_sems.at[1]),
        pltpu.make_async_copy(kw_hbm, kw, load_sems.at[2]),
        pltpu.make_async_copy(vw_hbm, vw, load_sems.at[3]),
        pltpu.make_async_copy(q_hbm, qs, load_sems.at[4]),
    ] + [
        pltpu.make_async_copy(cache_hbm.at[r], cache.at[r], cache_sems.at[r])
        for r in range(owned)
    ]
    barrier = pltpu.get_barrier_semaphore()
    for k in range(1, ranks):
        pl.semaphore_signal(
            barrier, inc=1, device_id={"head": (me + k) % ranks}, device_id_type=MESH
        )
    pl.semaphore_signal(
        barrier, inc=1, device_id={"batch": 1 - batch_rank}, device_id_type=MESH
    )
    smalls = [
        pltpu.make_async_copy(lens_hbm, lens_ref, small_sems.at[0]),
        pltpu.make_async_copy(owner_hbm, owner_ref, small_sems.at[1]),
        pltpu.make_async_copy(ctx_hbm, ctx_ref, small_sems.at[2]),
        pltpu.make_async_copy(new_hbm, new_ref, small_sems.at[3]),
    ]
    for load in smalls + loads:
        load.start()
    for small in smalls:
        small.wait()
    start_marks(span_ends(lens_ref, batch_rank), tail, vals, hot, tri)
    pl.semaphore_wait(barrier, ranks)

    quarter = shard_hbm.shape[0] // 4
    most = ranks // 2

    def hop(way, part, t):
        back_by = t - 1 if way == 0 else ranks - t + 1
        origin = rank_at((place + ranks - back_by) % ranks, ranks)
        rows = pl.ds(part * quarter, quarter)
        return pltpu.make_async_remote_copy(
            src_ref=spans_ref.at[origin, rows],
            dst_ref=spans_ref.at[origin, rows],
            send_sem=ring_send.at[way, part, t - 1],
            recv_sem=ring_recv.at[way, part, t - 1],
            device_id={"head": right if way == 0 else left},
            device_id_type=MESH,
        )

    def hops(way, part):
        return most if way == part // 2 else most - 1

    streams = [(0, 0), (1, 2), (0, 1), (1, 3), (0, 2), (1, 0), (0, 3), (1, 1)]
    loads[0].wait()
    for way, part in streams:
        hop(way, part, 1).start()
    loads[1].wait()
    loads[2].wait()
    absorb_into(dq, kw, sent, flat, wide, heads, lat)
    loads[3].wait()

    def project(origin):
        project_shard(origin, spans_ref, kw, vw, keys, vals, tail, lat, heads)

    def arrive(t, carry):
        for way, part in streams:
            if hops(way, part) == most:
                hop(way, part, t).wait_recv()
                pl.when(t < most)(lambda: hop(way, part, t + 1).start())
            else:

                @pl.when(t < most)
                def _():
                    hop(way, part, t).wait_recv()
                    pl.when(t < most - 1)(lambda: hop(way, part, t + 1).start())

        def one(side, carry):
            project(rank_at((place + side * t + (1 - side) * (ranks - t)) % ranks, ranks))
            return carry

        lax.fori_loop(0, 2 - t // most, one, 0)
        return carry

    project(me)
    lax.fori_loop(1, most + 1, arrive, 0)

    def exchange(source, target, r, send_sems, recv_sems):
        return [
            pltpu.make_async_remote_copy(
                src_ref=source.at[(me + k) % ranks, r],
                dst_ref=target.at[me, r],
                send_sem=send_sems.at[r, k - 1],
                recv_sem=recv_sems.at[r, k - 1],
                device_id={"head": (me + k) % ranks},
                device_id_type=MESH,
            )
            for k in range(1, ranks)
        ]

    gives = [exchange(sent, got, r, give_sems, take_sems) for r in range(owned)]
    backs = [exchange(lo, back, r, back_send, back_recv) for r in range(owned)]
    swap = pltpu.make_async_remote_copy(
        src_ref=spans_ref.at[:ranks],
        dst_ref=spans_ref.at[ranks:],
        send_sem=swap_sems.at[0],
        recv_sem=swap_sems.at[1],
        device_id={"batch": 1 - batch_rank},
        device_id_type=MESH,
    )
    for copies in gives:
        for copy in copies:
            copy.start()
    swap.start()
    keep = pltpu.make_async_copy(sent.at[me], got.at[me], load_sems.at[5])
    keep.start()
    loads[4].wait()

    def attend(low, high):
        attend_groups(
            low, high, pair, qs, keys, tail, vals, hot, tri, part_ref, buffers, look, scale
        )

    groups = heads // pair
    attend(0, before)
    keep.wait()
    swap.wait()
    for r in range(owned):
        for copy in gives[r]:
            copy.wait()
        loads[5 + r].wait()
        row = batch_rank * (ranks * owned) + me * owned + r
        facts = request_facts(lens_ref, owner_ref, ctx_ref, r, row, batch_rank, span_len)
        decode_request(
            r, facts, got, new_ref, spans_ref, cache, lo, tools,
            lat=lat, heads=heads, steps=steps, scale=scale, blk=blk,
        )
        for copy in backs[r]:
            copy.start()
    stay = pltpu.make_async_copy(lo.at[me], back.at[me], load_sems.at[6])
    stay.start()
    attend(before, groups)
    for way, part in streams:
        for t in range(1, hops(way, part) + 1):
            hop(way, part, t).wait_send()
    for copies in backs:
        for copy in copies:
            copy.wait()
    stay.wait()


HBM_SPEC = pl.BlockSpec(memory_space=pltpu.HBM)
VMEM_SPEC = pl.BlockSpec(memory_space=pltpu.VMEM)
SMEM_SPEC = pl.BlockSpec(memory_space=pltpu.SMEM)


def serve_pallas(lens, owner, ctx, newest, shard, flat_queries, key_weight, value_weight, turned, cache, ranks, qb=256, pair=4, before=2, blk=512, ahead=4):
    heads, width, span_len = turned.shape
    kv, own = shard.shape
    lat = key_weight.shape[0]
    rows = flat_queries.shape[0]
    owned = cache.shape[0]
    block = rows // (ranks * owned)
    look = min(-(-(span_len // 2) // qb), span_len // qb - 1)
    marks = 128 - (kv - lat)
    deep = (look + 1) * qb
    asks = ranks * block
    bf16, f32 = jnp.bfloat16, jnp.float32
    vmem, dma = pltpu.VMEM, pltpu.SemaphoreType.DMA
    return pl.pallas_call(
        functools.partial(
            serve_kernel,
            lat=lat,
            ranks=ranks,
            heads=heads,
            look=look,
            scale=math.log2(math.e) / math.sqrt(width),
            pair=pair,
            before=before,
            blk=blk,
        ),
        out_shape=(
            jax.ShapeDtypeStruct((ranks, owned, block, lat), bf16),
            jax.ShapeDtypeStruct((span_len, heads * 128), bf16),
        ),
        in_specs=[HBM_SPEC] * 10,
        out_specs=(VMEM_SPEC,) * 2,
        scratch_shapes=[
            vmem((2 * ranks, kv, own), bf16),
            vmem((ranks, owned, block, kv), bf16),
            vmem((span_len, 128), bf16),
            vmem((marks, span_len), bf16),
            vmem((qb, qb), f32),
            vmem(key_weight.shape, bf16),
            vmem(value_weight.shape, bf16),
            vmem((heads, width, span_len), bf16),
            vmem((rows, width), bf16),
            vmem((rows, 128), f32),
            vmem((lat // 128, rows, 128), f32),
            vmem((ranks, owned, block, kv), bf16),
            vmem((heads, span_len, 128), bf16),
            vmem((heads, 144, span_len), bf16),
            [[vmem((deep, qb), f32)] * ahead, [vmem((deep, qb), bf16)] * ahead],
            vmem(cache.shape, bf16),
            vmem((ranks, owned, block, lat), bf16),
            [
                vmem((asks, 128), f32),
                vmem((asks, 128), f32),
                vmem((asks, lat), f32),
                vmem((asks, -(-(kv + 16) // 128) * 128), bf16),
                [vmem((asks, blk), f32)] * 2,
                [vmem((asks, 128), f32)] * 2,
                [vmem((asks, blk), bf16)] * 2,
                [vmem((asks, 128), f32)] * 2,
            ],
            pltpu.SMEM(lens.shape, lens.dtype),
            pltpu.SMEM(owner.shape, owner.dtype),
            pltpu.SMEM(ctx.shape, ctx.dtype),
            vmem(newest.shape, newest.dtype),
            dma((7,)),
            dma((owned,)),
            dma((4,)),
            dma((2, 4, ranks // 2)),
            dma((2, 4, ranks // 2)),
            dma((2,)),
            dma((owned, ranks - 1)),
            dma((owned, ranks - 1)),
            dma((owned, ranks - 1)),
            dma((owned, ranks - 1)),
        ],
        compiler_params=pltpu.CompilerParams(
            collective_id=0, has_side_effects=True, vmem_limit_bytes=46 << 20
        ),
        cost_estimate=pl.CostEstimate(
            flops=30 * 10**9, bytes_accessed=24 << 20, transcendentals=14 << 20
        ),
    )(lens, owner, ctx, newest, shard, flat_queries, key_weight, value_weight, turned, cache)


def project_kernel(back_ref, vw_ref, part_ref, out_ref, whole_ref, wide, sems, *, heads, lat):
    ranks, owned, block, _ = back_ref.shape
    steps = block // heads
    local = ranks * owned
    shown = pltpu.make_async_copy(part_ref, whole_ref, sems.at[0])
    shown.start()
    for p in range(ranks):
        for r in range(owned):
            at = (p * owned + r) * block
            for c in range(lat // 128):
                wide[c, at : at + block] = back_ref[p, r, :, c * 128 : (c + 1) * 128].astype(
                    jnp.float32
                )

    def some_heads(g, carry):
        for p in range(4):
            h = g * 4 + p
            mine = jnp.concatenate(
                [
                    jnp.concatenate(
                        [
                            wide[c, pl.ds(s * heads + h, local, stride=block), :]
                            for c in range(lat // 128)
                        ],
                        axis=1,
                    )
                    for s in range(steps)
                ],
                axis=0,
            ).astype(jnp.bfloat16)
            columns = pl.ds(pl.multiple_of(h * 128, 128), 128)
            out_ref[:, columns] = jnp.dot(
                mine, vw_ref[:, columns], preferred_element_type=jnp.float32
            ).astype(jnp.bfloat16)
        return carry

    lax.fori_loop(0, heads // 4, some_heads, 0)
    shown.wait()


def project_pallas(back, value_weight, part, heads):
    ranks, owned, block, lat = back.shape
    rows = ranks * owned * block
    return pl.pallas_call(
        functools.partial(project_kernel, heads=heads, lat=lat),
        out_shape=(
            jax.ShapeDtypeStruct((rows // heads, heads * 128), jnp.bfloat16),
            jax.ShapeDtypeStruct(part.shape, part.dtype),
        ),
        in_specs=[VMEM_SPEC, VMEM_SPEC, VMEM_SPEC],
        out_specs=(VMEM_SPEC, HBM_SPEC),
        scratch_shapes=[
            pltpu.VMEM((lat // 128, rows, 128), jnp.float32),
            pltpu.SemaphoreType.DMA((1,)),
        ],
        compiler_params=pltpu.CompilerParams(vmem_limit_bytes=8 << 20),
    )(back, value_weight, part)


def on_device(
    latent_rows,
    pre_queries,
    pre_lengths,
    owner_map,
    context_cache,
    context_lengths,
    new_latent,
    dec_queries,
    key_weight,
    value_weight,
):
    steps, rows_local, heads, width = dec_queries.shape
    ranks = lax.axis_size("head")
    if heads % 16 or latent_rows.shape[0] % 128 or ranks % 2:
        return plain_on_device(
            latent_rows,
            pre_queries,
            pre_lengths,
            owner_map,
            context_cache,
            context_lengths,
            new_latent,
            dec_queries,
            key_weight,
            value_weight,
        )
    stay = lambda x: pltpu.with_memory_space_constraint(x, pltpu.HBM)
    back, part = serve_pallas(
        stay(pre_lengths),
        stay(owner_map),
        stay(context_lengths),
        stay(new_latent),
        stay(jnp.transpose(latent_rows)),
        stay(dec_queries.reshape(-1, width)),
        stay(key_weight),
        stay(value_weight),
        stay(jnp.transpose(pre_queries, (1, 2, 0))),
        stay(jnp.transpose(context_cache, (0, 2, 1))),
        ranks,
    )
    decode_out, prefill_out = project_pallas(back, value_weight, part, heads)
    return (prefill_out, decode_out.reshape(steps, rows_local, heads * 128))


def solution(mesh):
    placed = (
        P(("groups", "batch", "head"), None),
        P(("groups", "batch"), "head", None),
        P("groups", None),
        P("groups", None),
        P(("groups", "batch", "head"), None, None),
        P(("groups", "batch", "head")),
        P("groups", ("batch", "head"), None),
        P("groups", "batch", "head", None),
        P(None, "head"),
        P(None, "head"),
    )
    return jax.shard_map(
        on_device,
        mesh=mesh,
        in_specs=placed,
        out_specs=(P(("groups", "batch"), "head"), P("groups", "batch", "head")),
        check_vma=False,
    )
```

```python
import functools
import math

import jax
import jax.numpy as jnp
from jax import lax
from jax.experimental import pallas as pl
from jax.experimental.pallas import tpu as pltpu
from jax.sharding import PartitionSpec as P

BLK = 512


NEGATIVE = -1e30


def from_partner(value, axis, distance):
    mask = 2**distance
    pairs = [(source, source ^ mask) for source in range(lax.axis_size(axis))]
    return lax.ppermute(value, axis, pairs)


def request_table(pre_lengths, owner_map, span_len):
    seg_ends = jnp.cumsum(pre_lengths, axis=1)
    span_base = jnp.arange(pre_lengths.shape[0], dtype=jnp.int32)[:, None] * span_len
    seg_starts = seg_ends - pre_lengths + span_base
    return (owner_map.reshape(-1), seg_starts.reshape(-1), pre_lengths.reshape(-1))


def prefill_heads(own_span, queries, span_lengths, key_weight, value_weight):
    span_len, head_count, query_width = queries.shape
    head_size = key_weight.shape[1] // head_count
    lat_width = key_weight.shape[0]
    score_scale = 1.0 / math.sqrt(query_width)
    latent = own_span[:, :lat_width]
    rope_keys = own_span[:, lat_width:]
    keys_nope = (
        jnp.dot(latent, key_weight, preferred_element_type=jnp.float32)
        .astype(jnp.bfloat16)
        .reshape(span_len, head_count, head_size)
    )
    values = (
        jnp.dot(latent, value_weight, preferred_element_type=jnp.float32)
        .astype(jnp.bfloat16)
        .reshape(span_len, head_count, head_size)
    )
    scores = jnp.einsum(
        "qhd,khd->hqk", queries[:, :, :head_size], keys_nope, preferred_element_type=jnp.float32
    )
    scores = scores + jnp.einsum(
        "qhr,kr->hqk", queries[:, :, head_size:], rope_keys, preferred_element_type=jnp.float32
    )
    scores = scores * score_scale
    seg_ends = jnp.cumsum(span_lengths)
    places = jnp.arange(span_len, dtype=jnp.int32)
    segment = jnp.sum((places[:, None] >= seg_ends[None, :]).astype(jnp.int32), axis=1)
    allowed = (segment[:, None] == segment[None, :]) & (places[None, :] <= places[:, None])
    masked = jnp.where(allowed[None], scores, NEGATIVE)
    peak_score = jnp.max(masked, axis=2, keepdims=True)
    weights = jnp.exp(masked - peak_score)
    weight_sum = jnp.sum(weights, axis=2)
    mixed_out = jnp.einsum(
        "hqk,khd->qhd", weights.astype(jnp.bfloat16), values, preferred_element_type=jnp.float32
    )
    mixed_out = mixed_out / jnp.transpose(weight_sum)[:, :, None]
    return mixed_out.astype(jnp.bfloat16).reshape(span_len, head_count * head_size)


def plain_on_device(
    latent_rows,
    pre_queries,
    pre_lengths,
    owner_map,
    context_cache,
    context_lengths,
    new_latent,
    dec_queries,
    key_weight,
    value_weight,
):
    head_rank = lax.axis_index("head")
    batch_rank = lax.axis_index("batch")
    span_len = pre_queries.shape[0]
    kv_width = latent_rows.shape[1]
    own_span = lax.all_gather(latent_rows, "head", axis=0, tiled=True)
    other_span = from_partner(own_span, "batch", 0)
    first_span = jnp.where(batch_rank == 0, own_span, other_span)
    second_span = jnp.where(batch_rank == 0, other_span, own_span)
    all_spans = jnp.concatenate([first_span, second_span], axis=0)
    span_lengths = lax.dynamic_index_in_dim(pre_lengths, batch_rank, 0, keepdims=False)
    prefill_out = prefill_heads(own_span, pre_queries, span_lengths, key_weight, value_weight)
    step_total, rows_local, head_count, query_width = dec_queries.shape
    lat_width = key_weight.shape[0]
    head_size = key_weight.shape[1] // head_count
    owned_rows = context_cache.shape[0]
    score_scale = 1.0 / math.sqrt(query_width)
    key_heads = key_weight.reshape(lat_width, head_count, head_size)
    value_heads = value_weight.reshape(lat_width, head_count, head_size)
    absorbed = jnp.einsum(
        "srhd,lhd->srhl",
        dec_queries[..., :head_size],
        key_heads,
        preferred_element_type=jnp.float32,
    ).astype(jnp.bfloat16)
    query_all = jnp.concatenate([absorbed, dec_queries[..., head_size:]], axis=3)
    flat_owner, flat_start, flat_length = request_table(pre_lengths, owner_map, span_len)
    row_ids = (
        batch_rank * rows_local + head_rank * owned_rows + jnp.arange(owned_rows, dtype=jnp.int32)
    )
    matches = (flat_owner[None, :] == row_ids[:, None]).astype(jnp.int32)
    is_target = jnp.sum(matches, axis=1) > 0
    first_row = jnp.sum(matches * flat_start[None, :], axis=1)
    prompt_len = jnp.sum(matches * flat_length[None, :], axis=1)
    effective = jnp.where(is_target, prompt_len, context_lengths)
    padded = jnp.concatenate([all_spans, jnp.zeros((span_len, kv_width), all_spans.dtype)], axis=0)
    replaced = jax.vmap(lambda offset: lax.dynamic_slice_in_dim(padded, offset, span_len, 0))(
        first_row
    )
    front_rows = jnp.where(is_target[:, None, None], replaced, context_cache[:, :span_len])
    front_blocks = span_len // BLK
    needed = (jnp.max(effective) + BLK - 1) // BLK
    fresh_latent = new_latent[..., :lat_width]
    owned_query = lax.all_to_all(query_all, "head", split_axis=1, concat_axis=2, tiled=True)
    fresh_scores = (
        jnp.einsum("srhk,jrk->srhj", owned_query, new_latent, preferred_element_type=jnp.float32)
        * score_scale
    )
    visible = (
        jnp.arange(new_latent.shape[0], dtype=jnp.int32)[None, :]
        <= jnp.arange(step_total, dtype=jnp.int32)[:, None]
    )
    fresh_scores = jnp.where(visible[:, None, None, :], fresh_scores, NEGATIVE)
    peak_score = jnp.max(fresh_scores, axis=3)
    weights = jnp.exp(fresh_scores - peak_score[..., None])
    weight_sum = jnp.sum(weights, axis=3)
    running = jnp.einsum(
        "srhj,jrl->srhl",
        weights.astype(jnp.bfloat16),
        fresh_latent,
        preferred_element_type=jnp.float32,
    )

    def advance(block_index, state_tuple, source):
        old_peak, old_sum, old_running = state_tuple
        key_block = lax.dynamic_slice_in_dim(source, block_index * BLK, BLK, 1)
        scores = (
            jnp.einsum("srhk,rtk->srht", owned_query, key_block, preferred_element_type=jnp.float32)
            * score_scale
        )
        places = block_index * BLK + jnp.arange(BLK, dtype=jnp.int32)
        in_context = places[None, :] < effective[:, None]
        scores = jnp.where(in_context[None, :, None, :], scores, NEGATIVE)
        new_peak = jnp.maximum(old_peak, jnp.max(scores, axis=3))
        factor = jnp.exp(old_peak - new_peak)
        block_weights = jnp.exp(scores - new_peak[..., None])
        new_sum = old_sum * factor + jnp.sum(block_weights, axis=3)
        new_running = old_running * factor[..., None] + jnp.einsum(
            "srht,rtl->srhl",
            block_weights.astype(jnp.bfloat16),
            key_block[..., :lat_width],
            preferred_element_type=jnp.float32,
        )
        return (new_peak, new_sum, new_running)

    state_tuple = lax.fori_loop(
        0,
        jnp.minimum(needed, front_blocks),
        lambda block_index, state_now: advance(block_index, state_now, front_rows),
        (peak_score, weight_sum, running),
    )
    state_tuple = lax.fori_loop(
        front_blocks,
        jnp.maximum(needed, front_blocks),
        lambda block_index, state_now: advance(block_index, state_now, context_cache),
        state_tuple,
    )
    latent_out = (state_tuple[2] / state_tuple[1][..., None]).astype(jnp.bfloat16)
    returned = lax.all_to_all(latent_out, "head", split_axis=2, concat_axis=1, tiled=True)
    projected = jnp.einsum(
        "srhl,lhd->srhd", returned, value_heads, preferred_element_type=jnp.float32
    ).astype(jnp.bfloat16)
    decode_out = projected.reshape(query_all.shape[0], rows_local, head_count * head_size)
    return (prefill_out, decode_out)


def trans_dot(left, right):
    return lax.dot_general(
        left, right, (((1,), (1,)), ((), ())), preferred_element_type=jnp.float32
    )


MESH = pl.DeviceIdType.MESH


def place_of(rank, ranks):
    odd = rank % 2
    return (1 - odd) * (rank // 2) + odd * (ranks - 1 - rank // 2)


def rank_at(place, ranks):
    late = place // (ranks // 2)
    return (1 - late) * (2 * place) + late * (2 * (ranks - 1 - place) + 1)


def start_marks(ends, tail, vals, hot, tri):
    span_len, full = tail.shape
    marks = hot.shape[0]
    segs = len(ends)
    where = lax.broadcasted_iota(jnp.int32, (span_len, marks), 0)
    lane = lax.broadcasted_iota(jnp.int32, (span_len, marks), 1)
    place = lax.broadcasted_iota(jnp.int32, (marks, span_len), 1)
    line = lax.broadcasted_iota(jnp.int32, (marks, span_len), 0)
    mine = jnp.zeros((span_len, marks), jnp.int32)
    seen = jnp.zeros((marks, span_len), jnp.int32)
    for k in range(segs - 1):
        mine = mine + (where >= ends[k]).astype(jnp.int32)
        seen = seen + (place >= ends[k]).astype(jnp.int32)
    mark = jnp.where((lane < segs) & (lane != mine), NEGATIVE, 0.0).astype(jnp.bfloat16)
    hot[...] = jnp.where(line == seen, 1.0, 0.0).astype(jnp.bfloat16)
    tail[:, full - marks :] = mark
    for h in range(vals.shape[0]):
        vals[h, 128:, :] = jnp.ones((vals.shape[1] - 128, span_len), jnp.bfloat16)
    size = tri.shape[0]
    key_at = lax.broadcasted_iota(jnp.int32, (size, size), 0)
    query_at = lax.broadcasted_iota(jnp.int32, (size, size), 1)
    tri[...] = jnp.where(key_at <= query_at, 0.0, NEGATIVE)


def project_piece(slot, origin, piece, pieces, spans_ref, held, kw, vw, keys, vals, tail, lat, heads):
    own = spans_ref.shape[2]
    at = pl.ds(pl.multiple_of(origin * own, own), own)
    if piece == 0:
        rows = jnp.transpose(spans_ref[origin])
        held[slot] = rows
        tail[at, : rows.shape[1] - lat] = rows[:, lat:]
    latent = held[slot, :, :lat]
    pair = 2
    each = heads // pair // pieces
    for g in range(piece * each, (piece + 1) * each):
        columns = slice(g * pair * 128, (g + 1) * pair * 128)
        key = jnp.dot(latent, kw[:, columns], preferred_element_type=jnp.float32)
        value = jnp.dot(latent, vw[:, columns], preferred_element_type=jnp.float32)
        key = key.astype(jnp.bfloat16)
        value = jnp.transpose(value.astype(jnp.bfloat16))
        for p in range(pair):
            h = g * pair + p
            keys[h, at, :] = key[:, p * 128 : (p + 1) * 128]
            vals[h, :128, at] = value[p * 128 : (p + 1) * 128]


def attention(g, pair, qs, keys, tail, vals, hot, tri, part_ref, scores, weights, look, scale):
    span_len = tail.shape[0]
    qb = tri.shape[0]
    blocks = span_len // qb
    order = [(0, p) for p in range(pair // 2)]
    order += [(i, p) for i in range(1, blocks) for p in range(pair)]
    order += [(0, p) for p in range(pair // 2, pair)]
    count = len(order)
    lengths = [min(i, look) + 1 for i, _ in order]
    peaks = [None] * count
    tops = [None] * count
    sums = [None] * count

    def score(n, c):
        i, p = order[n]
        if c > 0:
            return
        at = (i - lengths[n] + 1) * qb
        size = lengths[n] * qb
        query = jnp.concatenate(
            [qs[g * pair + p, :, i * qb : (i + 1) * qb], hot[:, i * qb : (i + 1) * qb]], axis=0
        )
        key = jnp.concatenate(
            [keys[g * pair + p, at : at + size, :], tail[at : at + size, :]], axis=1
        )
        s = jnp.dot(key, query, preferred_element_type=jnp.float32)
        if size > qb:
            scores[n % 4][: size - qb, :] = s[: size - qb]
            peaks[n] = jnp.max(s[: size - qb].reshape((size - qb) // 8, 8, qb), axis=0)
        last = s[size - qb :] + tri[...]
        scores[n % 4][size - qb : size, :] = last
        top = jnp.max(last.reshape(qb // 8, 8, qb), axis=0)
        peaks[n] = top if peaks[n] is None else jnp.maximum(peaks[n], top)

    def soften(n, c):
        if c == 0:
            tops[n] = jnp.max(peaks[n], axis=0, keepdims=True)
        for k in range(0, qb, 32):
            at = slice(c * qb + k, c * qb + k + 32)
            w = jnp.exp2((scores[n % 4][at, :] - tops[n]) * scale)
            weights[n % 4][at, :] = w.astype(jnp.bfloat16)

    def mix(n, c):
        i, p = order[n]
        at = (i - lengths[n] + 1) * qb
        if c == 0:
            o = jnp.dot(
                vals[g * pair + p, :, at : at + lengths[n] * qb],
                weights[n % 4][: lengths[n] * qb, :],
                preferred_element_type=jnp.float32,
            )
            o = o[:128] * (1.0 / o[128:129])
            columns = pl.ds(pl.multiple_of((g * pair + p) * 128, 128), 128)
            part_ref[i * qb : (i + 1) * qb, columns] = jnp.transpose(o.astype(jnp.bfloat16))

    todo_score = [(n, c) for n in range(count) for c in range(lengths[n])]
    todo_soft = list(todo_score)
    todo_mix = list(todo_score)
    scored = [0] * count
    softened = [0] * count
    mixed = [0] * count
    while todo_mix:
        was = list(softened)
        if todo_score:
            n, c = todo_score[0]
            if n < 4 or softened[n - 4] == lengths[n - 4]:
                score(n, c)
                scored[n] += 1
                todo_score.pop(0)
        if todo_soft:
            n, c = todo_soft[0]
            free = n < 4 or mixed[n - 4] == lengths[n - 4]
            if scored[n] == lengths[n] and free and not (todo_score and todo_score[0][0] <= n + 2):
                soften(n, c)
                softened[n] += 1
                todo_soft.pop(0)
        n, c = todo_mix[0]
        if was[n] == lengths[n]:
            mix(n, c)
            mixed[n] += 1
            todo_mix.pop(0)


def attend_groups(low, high, pair, qs, keys, tail, vals, hot, tri, part_ref, buffers, look, scale):
    scores, weights = buffers

    def step(g, carry):
        attention(
            g, pair, qs, keys, tail, vals, hot, tri, part_ref, scores, weights, look, scale
        )
        return carry

    lax.fori_loop(low, high, step, 0)


def absorb_heads(low, high, kw, sent, flat, wide, heads, lat):
    ranks, owned, block, _ = sent.shape
    steps = block // heads
    local = ranks * owned
    for h in range(low, high):
        mine = flat[pl.ds(h, steps * local, stride=heads), :].astype(jnp.bfloat16)
        res = trans_dot(mine, kw[:, h * 128 : (h + 1) * 128])
        for s in range(steps):
            for c in range(lat // 128):
                wide[c, pl.ds(s * heads + h, local, stride=block), :] = res[
                    s * local : (s + 1) * local, c * 128 : (c + 1) * 128
                ]


def absorb_finish(dq, sent, wide, heads, lat):
    ranks, owned, block, _ = sent.shape
    steps = block // heads
    local = ranks * owned
    for p in range(ranks):
        for r in range(owned):
            at = p * owned + r
            for c in range(lat // 128):
                sent[p, r, :, c * 128 : (c + 1) * 128] = wide[
                    c, at * block : (at + 1) * block
                ].astype(jnp.bfloat16)
            for s in range(steps):
                start = (s * local + at) * heads
                sent[p, r, s * heads : (s + 1) * heads, lat:] = dq[start : start + heads, 128:]


def span_ends(lens_ref, batch_rank):
    ends = []
    total = 0
    for k in range(lens_ref.shape[1]):
        total = total + lens_ref[batch_rank, k]
        ends.append(total)
    return ends


def request_facts(lens_ref, owner_ref, ctx_ref, r, row, batch_rank, span_len):
    target = jnp.int32(0)
    first = jnp.int32(0)
    length = jnp.int32(0)
    spans = lens_ref.shape[0]
    for c in range(spans):
        start = jnp.int32(((c + spans) % spans) * span_len)
        for k in range(lens_ref.shape[1]):
            hit = (owner_ref[c, k] == row).astype(jnp.int32)
            target = target + hit
            first = first + hit * start
            length = length + hit * lens_ref[c, k]
            start = start + lens_ref[c, k]
    first = ((first + batch_rank * span_len) % (2 * span_len)) * target
    return first, length, ctx_ref[r] * (1 - target)


def decode_request(r, facts, got, new_ref, spans_ref, cache, lo, tools, *, lat, heads, steps, scale, blk):
    peak_ref, sum_ref, acc_ref, asked, scores, tops, weights, fades = tools
    ranks, _, block, kv = got.shape
    rows = ranks * block
    first, length, held = facts
    own = spans_ref.shape[2]
    full = asked.shape[1]
    piece = 256
    blocks = cache.shape[2] // blk
    spread = (full - kv) // 16
    tail = lax.broadcasted_iota(jnp.int32, (rows, full - kv), 1)
    columns = lax.broadcasted_iota(jnp.int32, (16, piece), 1)

    line = lax.broadcasted_iota(jnp.int32, (16, piece), 0)

    def hidden(keep):
        mask = jnp.where((line == 0) & jnp.logical_not(keep), NEGATIVE, 0.0)
        return [mask.astype(jnp.bfloat16)] * spread

    def begin():
        asked[:, :kv] = got[:, r].reshape(rows, kv)
        row_step = (lax.broadcasted_iota(jnp.int32, tail.shape, 0) // heads) % steps
        asked[:, kv:] = jnp.where((tail == 0) | (tail == row_step + 1), 1.0, 0.0).astype(
            jnp.bfloat16
        )
        newest = new_ref[...].astype(jnp.float32)
        fresh = jnp.concatenate(
            [newest[s, r : r + 1] for s in range(steps)]
            + [jnp.zeros((own - steps, kv), jnp.float32)],
            axis=0,
        ).astype(jnp.bfloat16)
        fresh = jnp.transpose(fresh)
        span_len = spans_ref.shape[0] * own // 2
        shards = -(-(span_len // 2 + own - 1) // own)
        base = jnp.minimum(first // own, spans_ref.shape[0] - shards)
        each = piece // own
        most = (shards + 1) // each

        def block(c):
            parts = []
            for i in range(c * each, (c + 1) * each):
                parts.append(spans_ref[base + i] if i < shards else fresh)
            return jnp.concatenate(parts, axis=1)

        top = None
        for c in range(most):
            place = (base + c * each) * own + columns
            keep = (place >= first) & (place < first + length)
            mask = jnp.where((line == 0) & jnp.logical_not(keep), NEGATIVE, 0.0)
            if c == most - 1:
                new_at = columns - (piece - own)
                late = (line == 0) & (new_at >= steps)
                late = late | ((line > 0) & (new_at > line - 1))
                mask = jnp.where(new_at >= 0, jnp.where(late, NEGATIVE, 0.0), mask)
            keys = jnp.concatenate([block(c)] + [mask.astype(jnp.bfloat16)] * spread, axis=0)
            part = jnp.dot(asked[...], keys, preferred_element_type=jnp.float32)
            scores[c // 2][:, (c % 2) * piece : (c % 2 + 1) * piece] = part
            best = jnp.maximum(part[:, :128], part[:, 128:])
            top = best if top is None else jnp.maximum(top, best)
        m = jnp.max(top, axis=1, keepdims=True)
        peak_ref[...] = jnp.broadcast_to(m, peak_ref.shape)
        total, acc = None, None
        for c in range(most):
            w = jnp.exp2((scores[c // 2][:, (c % 2) * piece : (c % 2 + 1) * piece] - m) * scale)
            both = w[:, :128] + w[:, 128:]
            made = trans_dot(w.astype(jnp.bfloat16), block(c)[:lat])
            total = both if total is None else total + both
            acc = made if acc is None else acc + made
        sum_ref[...] = total
        acc_ref[...] = acc
        weights[1][...] = jnp.zeros(weights[1].shape, jnp.bfloat16)
        fades[1][...] = jnp.ones(fades[1].shape, jnp.float32)

    def score(t, side, c):
        at = pl.multiple_of(t * blk + c * piece, piece)
        keys = jnp.concatenate(
            [cache[r, :, pl.ds(at, piece)]] + hidden(at + columns < held), axis=0
        )
        s = jnp.dot(asked[...], keys, preferred_element_type=jnp.float32)
        scores[side][:, c * piece : (c + 1) * piece] = s
        top = jnp.maximum(s[:, :128], s[:, 128:])
        if c > 0:
            top = jnp.maximum(top, tops[side][...])
        tops[side][...] = top

    def settle(side):
        old = peak_ref[...]
        new = jnp.maximum(old, jnp.max(tops[side][...], axis=1, keepdims=True))
        fade = jnp.exp2((old - new) * scale)
        fades[side][...] = fade
        peak_ref[...] = new
        sum_ref[...] = sum_ref[...] * fade

    def soften(side, c):
        at = slice(c * piece, (c + 1) * piece)
        new = peak_ref[...]
        s = scores[side][:, at]
        left = jnp.exp2((s[:, :128] - new) * scale)
        right = jnp.exp2((s[:, 128:] - new) * scale)
        sum_ref[...] = sum_ref[...] + (left + right)
        weights[side][:, at] = jnp.concatenate([left, right], axis=1).astype(jnp.bfloat16)

    def mix(t, side, c):
        at = pl.multiple_of(jnp.maximum(t, 0) * blk, blk)
        some = slice(c * piece, (c + 1) * piece)
        made = trans_dot(weights[side][...], cache[r, some, pl.ds(at, blk)])
        fade = fades[side][...]
        for k in range(piece // 128):
            here = slice(c * piece + k * 128, c * piece + (k + 1) * 128)
            acc_ref[:, here] = acc_ref[:, here] * fade + made[:, k * 128 : (k + 1) * 128]

    def turn(j, carry):
        for side in range(2):
            t = 2 * j + side
            settle(side)
            for c in range(blk // piece):
                if not (isinstance(t, int) and t + 1 == blocks):
                    score(t + 1, 1 - side, c)
                soften(side, c)
                mix(t - 1, 1 - side, c)
        return carry

    begin()
    for c in range(blk // piece):
        score(0, 0, c)
    lax.fori_loop(0, blocks // 2 - 1, turn, 0)
    turn(blocks // 2 - 1, 0)
    for c in range(lat // piece):
        mix(blocks - 1, 1, c)
    total = jnp.sum(sum_ref[...], axis=1, keepdims=True)
    done = (acc_ref[...] * (1.0 / total)).astype(lo.dtype)
    for p in range(ranks):
        lo[p, r] = done[p * block : (p + 1) * block]


def serve_kernel(
    lens_hbm, owner_hbm, ctx_hbm, new_hbm, shard_hbm, dq_hbm, kw_hbm, vw_hbm, q_hbm, cache_hbm,
    back, part_ref,
    spans_ref, got, tail, hot, tri, kw, vw, qs, dq, flat, wide, sent, keys, vals, buffers, cache,
    lo, tools, held, lens_ref, owner_ref, ctx_ref, new_ref,
    load_sems, cache_sems, small_sems, ring_send, ring_recv, swap_sems,
    give_sems, take_sems, back_send, back_recv,
    *, lat, ranks, heads, look, scale, pair, before, blk
):
    me = lax.axis_index("head")
    batch_rank = lax.axis_index("batch")
    place = place_of(me, ranks)
    right = rank_at((place + 1) % ranks, ranks)
    left = rank_at((place + ranks - 1) % ranks, ranks)
    owned = cache.shape[0]
    span_len = tail.shape[0]
    steps = sent.shape[2] // heads
    loads = [
        pltpu.make_async_copy(shard_hbm, spans_ref.at[me], load_sems.at[0]),
        pltpu.make_async_copy(dq_hbm, dq, load_sems.at[1]),
        pltpu.make_async_copy(kw_hbm, kw, load_sems.at[2]),
        pltpu.make_async_copy(vw_hbm, vw, load_sems.at[3]),
        pltpu.make_async_copy(q_hbm, qs, load_sems.at[4]),
    ] + [
        pltpu.make_async_copy(cache_hbm.at[r], cache.at[r], cache_sems.at[r])
        for r in range(owned)
    ]
    barrier = pltpu.get_barrier_semaphore()
    for k in range(1, ranks):
        pl.semaphore_signal(
            barrier, inc=1, device_id={"head": (me + k) % ranks}, device_id_type=MESH
        )
    pl.semaphore_signal(
        barrier, inc=1, device_id={"batch": 1 - batch_rank}, device_id_type=MESH
    )
    smalls = [
        pltpu.make_async_copy(lens_hbm, lens_ref, small_sems.at[0]),
        pltpu.make_async_copy(owner_hbm, owner_ref, small_sems.at[1]),
        pltpu.make_async_copy(ctx_hbm, ctx_ref, small_sems.at[2]),
        pltpu.make_async_copy(new_hbm, new_ref, small_sems.at[3]),
    ]
    for load in smalls + loads:
        load.start()
    for small in smalls:
        small.wait()
    start_marks(span_ends(lens_ref, batch_rank), tail, vals, hot, tri)
    pl.semaphore_wait(barrier, ranks)

    quarter = shard_hbm.shape[0] // 4
    most = ranks // 2

    def hop(way, part, t):
        back_by = t - 1 if way == 0 else ranks - t + 1
        origin = rank_at((place + ranks - back_by) % ranks, ranks)
        rows = pl.ds(part * quarter, quarter)
        return pltpu.make_async_remote_copy(
            src_ref=spans_ref.at[origin, rows],
            dst_ref=spans_ref.at[origin, rows],
            send_sem=ring_send.at[way, part, t - 1],
            recv_sem=ring_recv.at[way, part, t - 1],
            device_id={"head": right if way == 0 else left},
            device_id_type=MESH,
        )

    def hops(way, part):
        return most if way == part // 2 else most - 1

    streams = [(0, 0), (1, 2), (0, 1), (1, 3), (0, 2), (1, 0), (0, 3), (1, 1)]
    loads[0].wait()
    for way, part in streams:
        hop(way, part, 1).start()
    loads[2].wait()
    loads[3].wait()
    pieces = 4

    def project(slot, origin, piece):
        project_piece(
            slot, origin, piece, pieces, spans_ref, held, kw, vw, keys, vals, tail, lat, heads
        )

    for piece in range(pieces):
        project(0, me, piece)
    loads[1].wait()
    flat[...] = dq[:, :128].astype(jnp.float32)
    each = heads // pieces
    for i, (way, part) in enumerate(streams):
        hop(way, part, 1).wait_recv()
        hop(way, part, 2).start()
        if i < pieces:
            absorb_heads(i * each, (i + 1) * each, kw, sent, flat, wide, heads, lat)
        if i == pieces:
            absorb_finish(dq, sent, wide, heads, lat)

    def arrive(t, carry):
        near = [rank_at((place + ranks - t + 1) % ranks, ranks), rank_at((place + t - 1) % ranks, ranks)]
        for i, (way, part) in enumerate(streams):
            if hops(way, part) == most:
                hop(way, part, t).wait_recv()
                pl.when(t < most)(lambda: hop(way, part, t + 1).start())
            else:

                @pl.when(t < most)
                def _():
                    hop(way, part, t).wait_recv()
                    pl.when(t < most - 1)(lambda: hop(way, part, t + 1).start())

            project(i % 2, near[i % 2], i // 2)
        return carry

    lax.fori_loop(2, most + 1, arrive, 0)
    for piece in range(pieces):
        project(0, rank_at((place + most) % ranks, ranks), piece)

    def exchange(source, target, r, send_sems, recv_sems):
        return [
            pltpu.make_async_remote_copy(
                src_ref=source.at[(me + k) % ranks, r],
                dst_ref=target.at[me, r],
                send_sem=send_sems.at[r, k - 1],
                recv_sem=recv_sems.at[r, k - 1],
                device_id={"head": (me + k) % ranks},
                device_id_type=MESH,
            )
            for k in range(1, ranks)
        ]

    gives = [exchange(sent, got, r, give_sems, take_sems) for r in range(owned)]
    backs = [exchange(lo, back, r, back_send, back_recv) for r in range(owned)]
    swap = pltpu.make_async_remote_copy(
        src_ref=spans_ref.at[:ranks],
        dst_ref=spans_ref.at[ranks:],
        send_sem=swap_sems.at[0],
        recv_sem=swap_sems.at[1],
        device_id={"batch": 1 - batch_rank},
        device_id_type=MESH,
    )
    for copies in gives:
        for copy in copies:
            copy.start()
    swap.start()
    keep = pltpu.make_async_copy(sent.at[me], got.at[me], load_sems.at[5])
    keep.start()
    loads[4].wait()

    def attend(low, high):
        attend_groups(
            low, high, pair, qs, keys, tail, vals, hot, tri, part_ref, buffers, look, scale
        )

    groups = heads // pair
    attend(0, before)
    keep.wait()
    swap.wait()
    for r in range(owned):
        for copy in gives[r]:
            copy.wait()
        loads[5 + r].wait()
        row = batch_rank * (ranks * owned) + me * owned + r
        facts = request_facts(lens_ref, owner_ref, ctx_ref, r, row, batch_rank, span_len)
        decode_request(
            r, facts, got, new_ref, spans_ref, cache, lo, tools,
            lat=lat, heads=heads, steps=steps, scale=scale, blk=blk,
        )
        for copy in backs[r]:
            copy.start()
    stay = pltpu.make_async_copy(lo.at[me], back.at[me], load_sems.at[6])
    stay.start()
    attend(before, groups)
    for way, part in streams:
        for t in range(1, hops(way, part) + 1):
            hop(way, part, t).wait_send()
    for copies in backs:
        for copy in copies:
            copy.wait()
    stay.wait()


HBM_SPEC = pl.BlockSpec(memory_space=pltpu.HBM)
VMEM_SPEC = pl.BlockSpec(memory_space=pltpu.VMEM)
SMEM_SPEC = pl.BlockSpec(memory_space=pltpu.SMEM)


def serve_pallas(lens, owner, ctx, newest, shard, flat_queries, key_weight, value_weight, turned, cache, ranks, qb=256, pair=4, before=2, blk=512, ahead=4):
    heads, width, span_len = turned.shape
    kv, own = shard.shape
    lat = key_weight.shape[0]
    rows = flat_queries.shape[0]
    owned = cache.shape[0]
    block = rows // (ranks * owned)
    look = min(-(-(span_len // 2) // qb), span_len // qb - 1)
    marks = 128 - (kv - lat)
    deep = (look + 1) * qb
    asks = ranks * block
    bf16, f32 = jnp.bfloat16, jnp.float32
    vmem, dma = pltpu.VMEM, pltpu.SemaphoreType.DMA
    return pl.pallas_call(
        functools.partial(
            serve_kernel,
            lat=lat,
            ranks=ranks,
            heads=heads,
            look=look,
            scale=math.log2(math.e) / math.sqrt(width),
            pair=pair,
            before=before,
            blk=blk,
        ),
        out_shape=(
            jax.ShapeDtypeStruct((ranks, owned, block, lat), bf16),
            jax.ShapeDtypeStruct((span_len, heads * 128), bf16),
        ),
        in_specs=[HBM_SPEC] * 10,
        out_specs=(VMEM_SPEC,) * 2,
        scratch_shapes=[
            vmem((2 * ranks, kv, own), bf16),
            vmem((ranks, owned, block, kv), bf16),
            vmem((span_len, 128), bf16),
            vmem((marks, span_len), bf16),
            vmem((qb, qb), f32),
            vmem(key_weight.shape, bf16),
            vmem(value_weight.shape, bf16),
            vmem((heads, width, span_len), bf16),
            vmem((rows, width), bf16),
            vmem((rows, 128), f32),
            vmem((lat // 128, rows, 128), f32),
            vmem((ranks, owned, block, kv), bf16),
            vmem((heads, span_len, 128), bf16),
            vmem((heads, 144, span_len), bf16),
            [[vmem((deep, qb), f32)] * ahead, [vmem((deep, qb), bf16)] * ahead],
            vmem(cache.shape, bf16),
            vmem((ranks, owned, block, lat), bf16),
            [
                vmem((asks, 128), f32),
                vmem((asks, 128), f32),
                vmem((asks, lat), f32),
                vmem((asks, -(-(kv + 16) // 128) * 128), bf16),
                [vmem((asks, blk), f32)] * 2,
                [vmem((asks, 128), f32)] * 2,
                [vmem((asks, blk), bf16)] * 2,
                [vmem((asks, 128), f32)] * 2,
            ],
            vmem((2, own, kv), bf16),
            pltpu.SMEM(lens.shape, lens.dtype),
            pltpu.SMEM(owner.shape, owner.dtype),
            pltpu.SMEM(ctx.shape, ctx.dtype),
            vmem(newest.shape, newest.dtype),
            dma((7,)),
            dma((owned,)),
            dma((4,)),
            dma((2, 4, ranks // 2)),
            dma((2, 4, ranks // 2)),
            dma((2,)),
            dma((owned, ranks - 1)),
            dma((owned, ranks - 1)),
            dma((owned, ranks - 1)),
            dma((owned, ranks - 1)),
        ],
        compiler_params=pltpu.CompilerParams(
            collective_id=0, has_side_effects=True, vmem_limit_bytes=46 << 20
        ),
        cost_estimate=pl.CostEstimate(
            flops=30 * 10**9, bytes_accessed=24 << 20, transcendentals=14 << 20
        ),
    )(lens, owner, ctx, newest, shard, flat_queries, key_weight, value_weight, turned, cache)


def project_kernel(back_ref, vw_ref, part_ref, out_ref, whole_ref, wide, sems, *, heads, lat):
    ranks, owned, block, _ = back_ref.shape
    steps = block // heads
    local = ranks * owned
    shown = pltpu.make_async_copy(part_ref, whole_ref, sems.at[0])
    shown.start()
    for p in range(ranks):
        for r in range(owned):
            at = (p * owned + r) * block
            for c in range(lat // 128):
                wide[c, at : at + block] = back_ref[p, r, :, c * 128 : (c + 1) * 128].astype(
                    jnp.float32
                )

    def some_heads(g, carry):
        for p in range(4):
            h = g * 4 + p
            mine = jnp.concatenate(
                [
                    jnp.concatenate(
                        [
                            wide[c, pl.ds(s * heads + h, local, stride=block), :]
                            for c in range(lat // 128)
                        ],
                        axis=1,
                    )
                    for s in range(steps)
                ],
                axis=0,
            ).astype(jnp.bfloat16)
            columns = pl.ds(pl.multiple_of(h * 128, 128), 128)
            out_ref[:, columns] = jnp.dot(
                mine, vw_ref[:, columns], preferred_element_type=jnp.float32
            ).astype(jnp.bfloat16)
        return carry

    lax.fori_loop(0, heads // 4, some_heads, 0)
    shown.wait()


def project_pallas(back, value_weight, part, heads):
    ranks, owned, block, lat = back.shape
    rows = ranks * owned * block
    return pl.pallas_call(
        functools.partial(project_kernel, heads=heads, lat=lat),
        out_shape=(
            jax.ShapeDtypeStruct((rows // heads, heads * 128), jnp.bfloat16),
            jax.ShapeDtypeStruct(part.shape, part.dtype),
        ),
        in_specs=[VMEM_SPEC, VMEM_SPEC, VMEM_SPEC],
        out_specs=(VMEM_SPEC, HBM_SPEC),
        scratch_shapes=[
            pltpu.VMEM((lat // 128, rows, 128), jnp.float32),
            pltpu.SemaphoreType.DMA((1,)),
        ],
        compiler_params=pltpu.CompilerParams(vmem_limit_bytes=8 << 20),
    )(back, value_weight, part)


def on_device(
    latent_rows,
    pre_queries,
    pre_lengths,
    owner_map,
    context_cache,
    context_lengths,
    new_latent,
    dec_queries,
    key_weight,
    value_weight,
):
    steps, rows_local, heads, width = dec_queries.shape
    ranks = lax.axis_size("head")
    if heads % 16 or latent_rows.shape[0] % 128 or ranks % 2 or ranks < 8:
        return plain_on_device(
            latent_rows,
            pre_queries,
            pre_lengths,
            owner_map,
            context_cache,
            context_lengths,
            new_latent,
            dec_queries,
            key_weight,
            value_weight,
        )
    stay = lambda x: pltpu.with_memory_space_constraint(x, pltpu.HBM)
    back, part = serve_pallas(
        stay(pre_lengths),
        stay(owner_map),
        stay(context_lengths),
        stay(new_latent),
        stay(jnp.transpose(latent_rows)),
        stay(dec_queries.reshape(-1, width)),
        stay(key_weight),
        stay(value_weight),
        stay(jnp.transpose(pre_queries, (1, 2, 0))),
        stay(jnp.transpose(context_cache, (0, 2, 1))),
        ranks,
    )
    decode_out, prefill_out = project_pallas(back, value_weight, part, heads)
    return (prefill_out, decode_out.reshape(steps, rows_local, heads * 128))


def solution(mesh):
    placed = (
        P(("groups", "batch", "head"), None),
        P(("groups", "batch"), "head", None),
        P("groups", None),
        P("groups", None),
        P(("groups", "batch", "head"), None, None),
        P(("groups", "batch", "head")),
        P("groups", ("batch", "head"), None),
        P("groups", "batch", "head", None),
        P(None, "head"),
        P(None, "head"),
    )
    return jax.shard_map(
        on_device,
        mesh=mesh,
        in_specs=placed,
        out_specs=(P(("groups", "batch"), "head"), P("groups", "batch", "head")),
        check_vma=False,
    )
```

```python
import functools
import math

import jax
import jax.numpy as jnp
from jax import lax
from jax.experimental import pallas as pl
from jax.experimental.pallas import tpu as pltpu
from jax.sharding import PartitionSpec as P

BLK = 512


NEGATIVE = -1e30


def from_partner(value, axis, distance):
    mask = 2**distance
    pairs = [(source, source ^ mask) for source in range(lax.axis_size(axis))]
    return lax.ppermute(value, axis, pairs)


def request_table(pre_lengths, owner_map, span_len):
    seg_ends = jnp.cumsum(pre_lengths, axis=1)
    span_base = jnp.arange(pre_lengths.shape[0], dtype=jnp.int32)[:, None] * span_len
    seg_starts = seg_ends - pre_lengths + span_base
    return (owner_map.reshape(-1), seg_starts.reshape(-1), pre_lengths.reshape(-1))


def prefill_heads(own_span, queries, span_lengths, key_weight, value_weight):
    span_len, head_count, query_width = queries.shape
    head_size = key_weight.shape[1] // head_count
    lat_width = key_weight.shape[0]
    score_scale = 1.0 / math.sqrt(query_width)
    latent = own_span[:, :lat_width]
    rope_keys = own_span[:, lat_width:]
    keys_nope = (
        jnp.dot(latent, key_weight, preferred_element_type=jnp.float32)
        .astype(jnp.bfloat16)
        .reshape(span_len, head_count, head_size)
    )
    values = (
        jnp.dot(latent, value_weight, preferred_element_type=jnp.float32)
        .astype(jnp.bfloat16)
        .reshape(span_len, head_count, head_size)
    )
    scores = jnp.einsum(
        "qhd,khd->hqk", queries[:, :, :head_size], keys_nope, preferred_element_type=jnp.float32
    )
    scores = scores + jnp.einsum(
        "qhr,kr->hqk", queries[:, :, head_size:], rope_keys, preferred_element_type=jnp.float32
    )
    scores = scores * score_scale
    seg_ends = jnp.cumsum(span_lengths)
    places = jnp.arange(span_len, dtype=jnp.int32)
    segment = jnp.sum((places[:, None] >= seg_ends[None, :]).astype(jnp.int32), axis=1)
    allowed = (segment[:, None] == segment[None, :]) & (places[None, :] <= places[:, None])
    masked = jnp.where(allowed[None], scores, NEGATIVE)
    peak_score = jnp.max(masked, axis=2, keepdims=True)
    weights = jnp.exp(masked - peak_score)
    weight_sum = jnp.sum(weights, axis=2)
    mixed_out = jnp.einsum(
        "hqk,khd->qhd", weights.astype(jnp.bfloat16), values, preferred_element_type=jnp.float32
    )
    mixed_out = mixed_out / jnp.transpose(weight_sum)[:, :, None]
    return mixed_out.astype(jnp.bfloat16).reshape(span_len, head_count * head_size)


def plain_on_device(
    latent_rows,
    pre_queries,
    pre_lengths,
    owner_map,
    context_cache,
    context_lengths,
    new_latent,
    dec_queries,
    key_weight,
    value_weight,
):
    head_rank = lax.axis_index("head")
    batch_rank = lax.axis_index("batch")
    span_len = pre_queries.shape[0]
    kv_width = latent_rows.shape[1]
    own_span = lax.all_gather(latent_rows, "head", axis=0, tiled=True)
    other_span = from_partner(own_span, "batch", 0)
    first_span = jnp.where(batch_rank == 0, own_span, other_span)
    second_span = jnp.where(batch_rank == 0, other_span, own_span)
    all_spans = jnp.concatenate([first_span, second_span], axis=0)
    span_lengths = lax.dynamic_index_in_dim(pre_lengths, batch_rank, 0, keepdims=False)
    prefill_out = prefill_heads(own_span, pre_queries, span_lengths, key_weight, value_weight)
    step_total, rows_local, head_count, query_width = dec_queries.shape
    lat_width = key_weight.shape[0]
    head_size = key_weight.shape[1] // head_count
    owned_rows = context_cache.shape[0]
    score_scale = 1.0 / math.sqrt(query_width)
    key_heads = key_weight.reshape(lat_width, head_count, head_size)
    value_heads = value_weight.reshape(lat_width, head_count, head_size)
    absorbed = jnp.einsum(
        "srhd,lhd->srhl",
        dec_queries[..., :head_size],
        key_heads,
        preferred_element_type=jnp.float32,
    ).astype(jnp.bfloat16)
    query_all = jnp.concatenate([absorbed, dec_queries[..., head_size:]], axis=3)
    flat_owner, flat_start, flat_length = request_table(pre_lengths, owner_map, span_len)
    row_ids = (
        batch_rank * rows_local + head_rank * owned_rows + jnp.arange(owned_rows, dtype=jnp.int32)
    )
    matches = (flat_owner[None, :] == row_ids[:, None]).astype(jnp.int32)
    is_target = jnp.sum(matches, axis=1) > 0
    first_row = jnp.sum(matches * flat_start[None, :], axis=1)
    prompt_len = jnp.sum(matches * flat_length[None, :], axis=1)
    effective = jnp.where(is_target, prompt_len, context_lengths)
    padded = jnp.concatenate([all_spans, jnp.zeros((span_len, kv_width), all_spans.dtype)], axis=0)
    replaced = jax.vmap(lambda offset: lax.dynamic_slice_in_dim(padded, offset, span_len, 0))(
        first_row
    )
    front_rows = jnp.where(is_target[:, None, None], replaced, context_cache[:, :span_len])
    front_blocks = span_len // BLK
    needed = (jnp.max(effective) + BLK - 1) // BLK
    fresh_latent = new_latent[..., :lat_width]
    owned_query = lax.all_to_all(query_all, "head", split_axis=1, concat_axis=2, tiled=True)
    fresh_scores = (
        jnp.einsum("srhk,jrk->srhj", owned_query, new_latent, preferred_element_type=jnp.float32)
        * score_scale
    )
    visible = (
        jnp.arange(new_latent.shape[0], dtype=jnp.int32)[None, :]
        <= jnp.arange(step_total, dtype=jnp.int32)[:, None]
    )
    fresh_scores = jnp.where(visible[:, None, None, :], fresh_scores, NEGATIVE)
    peak_score = jnp.max(fresh_scores, axis=3)
    weights = jnp.exp(fresh_scores - peak_score[..., None])
    weight_sum = jnp.sum(weights, axis=3)
    running = jnp.einsum(
        "srhj,jrl->srhl",
        weights.astype(jnp.bfloat16),
        fresh_latent,
        preferred_element_type=jnp.float32,
    )

    def advance(block_index, state_tuple, source):
        old_peak, old_sum, old_running = state_tuple
        key_block = lax.dynamic_slice_in_dim(source, block_index * BLK, BLK, 1)
        scores = (
            jnp.einsum("srhk,rtk->srht", owned_query, key_block, preferred_element_type=jnp.float32)
            * score_scale
        )
        places = block_index * BLK + jnp.arange(BLK, dtype=jnp.int32)
        in_context = places[None, :] < effective[:, None]
        scores = jnp.where(in_context[None, :, None, :], scores, NEGATIVE)
        new_peak = jnp.maximum(old_peak, jnp.max(scores, axis=3))
        factor = jnp.exp(old_peak - new_peak)
        block_weights = jnp.exp(scores - new_peak[..., None])
        new_sum = old_sum * factor + jnp.sum(block_weights, axis=3)
        new_running = old_running * factor[..., None] + jnp.einsum(
            "srht,rtl->srhl",
            block_weights.astype(jnp.bfloat16),
            key_block[..., :lat_width],
            preferred_element_type=jnp.float32,
        )
        return (new_peak, new_sum, new_running)

    state_tuple = lax.fori_loop(
        0,
        jnp.minimum(needed, front_blocks),
        lambda block_index, state_now: advance(block_index, state_now, front_rows),
        (peak_score, weight_sum, running),
    )
    state_tuple = lax.fori_loop(
        front_blocks,
        jnp.maximum(needed, front_blocks),
        lambda block_index, state_now: advance(block_index, state_now, context_cache),
        state_tuple,
    )
    latent_out = (state_tuple[2] / state_tuple[1][..., None]).astype(jnp.bfloat16)
    returned = lax.all_to_all(latent_out, "head", split_axis=2, concat_axis=1, tiled=True)
    projected = jnp.einsum(
        "srhl,lhd->srhd", returned, value_heads, preferred_element_type=jnp.float32
    ).astype(jnp.bfloat16)
    decode_out = projected.reshape(query_all.shape[0], rows_local, head_count * head_size)
    return (prefill_out, decode_out)


def trans_dot(left, right):
    return lax.dot_general(
        left, right, (((1,), (1,)), ((), ())), preferred_element_type=jnp.float32
    )


MESH = pl.DeviceIdType.MESH


def place_of(rank, ranks):
    odd = rank % 2
    return (1 - odd) * (rank // 2) + odd * (ranks - 1 - rank // 2)


def rank_at(place, ranks):
    late = place // (ranks // 2)
    return (1 - late) * (2 * place) + late * (2 * (ranks - 1 - place) + 1)


def start_marks(ends, tail, vals, hot, tri):
    span_len, full = tail.shape
    marks = hot.shape[0]
    segs = len(ends)
    where = lax.broadcasted_iota(jnp.int32, (span_len, marks), 0)
    lane = lax.broadcasted_iota(jnp.int32, (span_len, marks), 1)
    place = lax.broadcasted_iota(jnp.int32, (marks, span_len), 1)
    line = lax.broadcasted_iota(jnp.int32, (marks, span_len), 0)
    mine = jnp.zeros((span_len, marks), jnp.int32)
    seen = jnp.zeros((marks, span_len), jnp.int32)
    for k in range(segs - 1):
        mine = mine + (where >= ends[k]).astype(jnp.int32)
        seen = seen + (place >= ends[k]).astype(jnp.int32)
    mark = jnp.where((lane < segs) & (lane != mine), NEGATIVE, 0.0).astype(jnp.bfloat16)
    hot[...] = jnp.where(line == seen, 1.0, 0.0).astype(jnp.bfloat16)
    tail[:, full - marks :] = mark
    for h in range(vals.shape[0]):
        vals[h, 128:, :] = jnp.ones((vals.shape[1] - 128, span_len), jnp.bfloat16)
    size = tri.shape[0]
    key_at = lax.broadcasted_iota(jnp.int32, (size, size), 0)
    query_at = lax.broadcasted_iota(jnp.int32, (size, size), 1)
    tri[...] = jnp.where(key_at <= query_at, 0.0, NEGATIVE)


def project_shard(origin, spans_ref, kw, vw, keys, vals, tail, lat, heads):
    own = spans_ref.shape[2]
    rows = jnp.transpose(spans_ref[origin])
    at = pl.ds(pl.multiple_of(origin * own, own), own)
    tail[at, : rows.shape[1] - lat] = rows[:, lat:]
    latent = rows[:, :lat]
    pair = 2
    for g in range(heads // pair):
        columns = slice(g * pair * 128, (g + 1) * pair * 128)
        key = jnp.dot(latent, kw[:, columns], preferred_element_type=jnp.float32)
        value = jnp.dot(latent, vw[:, columns], preferred_element_type=jnp.float32)
        key = key.astype(jnp.bfloat16)
        value = jnp.transpose(value.astype(jnp.bfloat16))
        for p in range(pair):
            h = g * pair + p
            keys[h, at, :] = key[:, p * 128 : (p + 1) * 128]
            vals[h, :128, at] = value[p * 128 : (p + 1) * 128]


def attention(g, pair, qs, keys, tail, vals, hot, tri, part_ref, scores, weights, look, scale):
    span_len = tail.shape[0]
    qb = 2 * tri.shape[0]
    blocks = span_len // qb
    order = [(0, p) for p in range(pair // 2)]
    order += [(i, p) for i in range(1, blocks) for p in range(pair)]
    order += [(0, p) for p in range(pair // 2, pair)]
    count = len(order)
    lengths = [min(i, look) + 1 for i, _ in order]
    half = qb // 2
    skips = [half if length == look + 1 else 0 for length in lengths]
    peaks = [None] * count
    tops = [None] * count
    sums = [None] * count

    def score(n, c):
        i, p = order[n]
        if c > 0:
            return
        at = (i - lengths[n] + 1) * qb
        size = lengths[n] * qb
        query = jnp.concatenate(
            [qs[g * pair + p, :, i * qb : (i + 1) * qb], hot[:, i * qb : (i + 1) * qb]], axis=0
        )
        key = jnp.concatenate(
            [keys[g * pair + p, at : at + size, :], tail[at : at + size, :]], axis=1
        )
        s = jnp.dot(key, query, preferred_element_type=jnp.float32)
        left = [s[: size - qb, :half], s[size - qb : size - half, :half] + tri[...]]
        right = [s[skips[n] : size - half, half:], s[size - half :, half:] + tri[...]]
        row = 0
        for piece in left:
            if piece.shape[0]:
                scores[n % 4][row : row + piece.shape[0], :half] = piece
                row += piece.shape[0]
        row = skips[n]
        for piece in right:
            scores[n % 4][row : row + piece.shape[0], half:] = piece
            row += piece.shape[0]
        both = []
        for side in (left, right):
            best = None
            for piece in side:
                if piece.shape[0]:
                    top = jnp.max(piece.reshape(piece.shape[0] // 8, 8, half), axis=0)
                    best = top if best is None else jnp.maximum(best, top)
            both.append(best)
        peaks[n] = both

    def soften(n, c):
        if c == 0:
            tops[n] = [jnp.max(peak, axis=0, keepdims=True) for peak in peaks[n]]
        size = lengths[n] * qb
        for side in range(2):
            low, high = (0, size - half) if side == 0 else (skips[n], size)
            lanes = slice(side * half, (side + 1) * half)
            for k in range(c * qb, (c + 1) * qb, 64):
                at = slice(k, k + 64)
                if low <= k < high:
                    w = jnp.exp2((scores[n % 4][at, lanes] - tops[n][side]) * scale)
                    weights[n % 4][at, lanes] = w.astype(jnp.bfloat16)
                else:
                    weights[n % 4][at, lanes] = jnp.zeros((64, half), jnp.bfloat16)

    def mix(n, c):
        i, p = order[n]
        at = (i - lengths[n] + 1) * qb
        if c == 0:
            o = jnp.dot(
                vals[g * pair + p, :, at : at + lengths[n] * qb],
                weights[n % 4][: lengths[n] * qb, :],
                preferred_element_type=jnp.float32,
            )
            o = o[:128] * (1.0 / o[128:129])
            columns = pl.ds(pl.multiple_of((g * pair + p) * 128, 128), 128)
            part_ref[i * qb : (i + 1) * qb, columns] = jnp.transpose(o.astype(jnp.bfloat16))

    todo_score = [(n, c) for n in range(count) for c in range(lengths[n])]
    todo_soft = list(todo_score)
    todo_mix = list(todo_score)
    scored = [0] * count
    softened = [0] * count
    mixed = [0] * count
    while todo_mix:
        was = list(softened)
        if todo_score:
            n, c = todo_score[0]
            if n < 4 or softened[n - 4] == lengths[n - 4]:
                score(n, c)
                scored[n] += 1
                todo_score.pop(0)
        if todo_soft:
            n, c = todo_soft[0]
            free = n < 4 or mixed[n - 4] == lengths[n - 4]
            if scored[n] == lengths[n] and free and not (todo_score and todo_score[0][0] <= n + 2):
                soften(n, c)
                softened[n] += 1
                todo_soft.pop(0)
        n, c = todo_mix[0]
        if was[n] == lengths[n]:
            mix(n, c)
            mixed[n] += 1
            todo_mix.pop(0)


def attend_groups(low, high, pair, qs, keys, tail, vals, hot, tri, part_ref, buffers, look, scale):
    scores, weights = buffers

    def step(g, carry):
        attention(
            g, pair, qs, keys, tail, vals, hot, tri, part_ref, scores, weights, look, scale
        )
        return carry

    lax.fori_loop(low, high, step, 0)


def absorb_into(dq, kw, sent, flat, wide, heads, lat):
    rows = dq.shape[0]
    ranks, owned, block, _ = sent.shape
    steps = block // heads
    local = ranks * owned
    flat[...] = dq[:, :128].astype(jnp.float32)
    for h in range(heads):
        mine = flat[pl.ds(h, rows // heads, stride=heads), :].astype(jnp.bfloat16)
        res = trans_dot(mine, kw[:, h * 128 : (h + 1) * 128])
        for s in range(steps):
            for c in range(lat // 128):
                wide[c, pl.ds(s * heads + h, local, stride=block), :] = res[
                    s * local : (s + 1) * local, c * 128 : (c + 1) * 128
                ]
    for p in range(ranks):
        for r in range(owned):
            at = p * owned + r
            for c in range(lat // 128):
                sent[p, r, :, c * 128 : (c + 1) * 128] = wide[
                    c, at * block : (at + 1) * block
                ].astype(jnp.bfloat16)
            for s in range(steps):
                start = (s * local + at) * heads
                sent[p, r, s * heads : (s + 1) * heads, lat:] = dq[start : start + heads, 128:]


def span_ends(lens_ref, batch_rank):
    ends = []
    total = 0
    for k in range(lens_ref.shape[1]):
        total = total + lens_ref[batch_rank, k]
        ends.append(total)
    return ends


def request_facts(lens_ref, owner_ref, ctx_ref, r, row, batch_rank, span_len):
    target = jnp.int32(0)
    first = jnp.int32(0)
    length = jnp.int32(0)
    spans = lens_ref.shape[0]
    for c in range(spans):
        start = jnp.int32(((c + spans) % spans) * span_len)
        for k in range(lens_ref.shape[1]):
            hit = (owner_ref[c, k] == row).astype(jnp.int32)
            target = target + hit
            first = first + hit * start
            length = length + hit * lens_ref[c, k]
            start = start + lens_ref[c, k]
    first = ((first + batch_rank * span_len) % (2 * span_len)) * target
    return first, length, ctx_ref[r] * (1 - target)


def decode_request(r, facts, got, new_ref, spans_ref, cache, lo, tools, *, lat, heads, steps, scale, blk):
    peak_ref, sum_ref, acc_ref, asked, scores, tops, weights, fades = tools
    ranks, _, block, kv = got.shape
    rows = ranks * block
    first, length, held = facts
    own = spans_ref.shape[2]
    full = asked.shape[1]
    piece = 256
    blocks = cache.shape[2] // blk
    spread = (full - kv) // 16
    tail = lax.broadcasted_iota(jnp.int32, (rows, full - kv), 1)
    columns = lax.broadcasted_iota(jnp.int32, (16, piece), 1)

    line = lax.broadcasted_iota(jnp.int32, (16, piece), 0)

    def hidden(keep):
        mask = jnp.where((line == 0) & jnp.logical_not(keep), NEGATIVE, 0.0)
        return [mask.astype(jnp.bfloat16)] * spread

    def begin():
        asked[:, :kv] = got[:, r].reshape(rows, kv)
        row_step = (lax.broadcasted_iota(jnp.int32, tail.shape, 0) // heads) % steps
        asked[:, kv:] = jnp.where((tail == 0) | (tail == row_step + 1), 1.0, 0.0).astype(
            jnp.bfloat16
        )
        newest = new_ref[...].astype(jnp.float32)
        fresh = jnp.concatenate(
            [newest[s, r : r + 1] for s in range(steps)]
            + [jnp.zeros((own - steps, kv), jnp.float32)],
            axis=0,
        ).astype(jnp.bfloat16)
        fresh = jnp.transpose(fresh)
        span_len = spans_ref.shape[0] * own // 2
        shards = -(-(span_len // 2 + own - 1) // own)
        base = jnp.minimum(first // own, spans_ref.shape[0] - shards)
        each = piece // own
        most = (shards + 1) // each

        def block(c):
            parts = []
            for i in range(c * each, (c + 1) * each):
                parts.append(spans_ref[base + i] if i < shards else fresh)
            return jnp.concatenate(parts, axis=1)

        top = None
        for c in range(most):
            place = (base + c * each) * own + columns
            keep = (place >= first) & (place < first + length)
            mask = jnp.where((line == 0) & jnp.logical_not(keep), NEGATIVE, 0.0)
            if c == most - 1:
                new_at = columns - (piece - own)
                late = (line == 0) & (new_at >= steps)
                late = late | ((line > 0) & (new_at > line - 1))
                mask = jnp.where(new_at >= 0, jnp.where(late, NEGATIVE, 0.0), mask)
            keys = jnp.concatenate([block(c)] + [mask.astype(jnp.bfloat16)] * spread, axis=0)
            part = jnp.dot(asked[...], keys, preferred_element_type=jnp.float32)
            scores[c // 2][:, (c % 2) * piece : (c % 2 + 1) * piece] = part
            best = jnp.maximum(part[:, :128], part[:, 128:])
            top = best if top is None else jnp.maximum(top, best)
        m = jnp.max(top, axis=1, keepdims=True)
        peak_ref[...] = jnp.broadcast_to(m, peak_ref.shape)
        total, acc = None, None
        for c in range(most):
            w = jnp.exp2((scores[c // 2][:, (c % 2) * piece : (c % 2 + 1) * piece] - m) * scale)
            both = w[:, :128] + w[:, 128:]
            made = trans_dot(w.astype(jnp.bfloat16), block(c)[:lat])
            total = both if total is None else total + both
            acc = made if acc is None else acc + made
        sum_ref[...] = total
        acc_ref[...] = acc
        weights[1][...] = jnp.zeros(weights[1].shape, jnp.bfloat16)
        fades[1][...] = jnp.ones(fades[1].shape, jnp.float32)

    def score(t, side, c):
        at = pl.multiple_of(t * blk + c * piece, piece)
        keys = jnp.concatenate(
            [cache[r, :, pl.ds(at, piece)]] + hidden(at + columns < held), axis=0
        )
        s = jnp.dot(asked[...], keys, preferred_element_type=jnp.float32)
        scores[side][:, c * piece : (c + 1) * piece] = s
        top = jnp.maximum(s[:, :128], s[:, 128:])
        if c > 0:
            top = jnp.maximum(top, tops[side][...])
        tops[side][...] = top

    def settle(side):
        old = peak_ref[...]
        new = jnp.maximum(old, jnp.max(tops[side][...], axis=1, keepdims=True))
        fade = jnp.exp2((old - new) * scale)
        fades[side][...] = fade
        peak_ref[...] = new
        sum_ref[...] = sum_ref[...] * fade

    def soften(side, c):
        at = slice(c * piece, (c + 1) * piece)
        new = peak_ref[...]
        s = scores[side][:, at]
        left = jnp.exp2((s[:, :128] - new) * scale)
        right = jnp.exp2((s[:, 128:] - new) * scale)
        sum_ref[...] = sum_ref[...] + (left + right)
        weights[side][:, at] = jnp.concatenate([left, right], axis=1).astype(jnp.bfloat16)

    def mix(t, side, c):
        at = pl.multiple_of(jnp.maximum(t, 0) * blk, blk)
        some = slice(c * piece, (c + 1) * piece)
        made = trans_dot(weights[side][...], cache[r, some, pl.ds(at, blk)])
        fade = fades[side][...]
        for k in range(piece // 128):
            here = slice(c * piece + k * 128, c * piece + (k + 1) * 128)
            acc_ref[:, here] = acc_ref[:, here] * fade + made[:, k * 128 : (k + 1) * 128]

    def turn(j, carry):
        for side in range(2):
            t = 2 * j + side
            settle(side)
            for c in range(blk // piece):
                if not (isinstance(t, int) and t + 1 == blocks):
                    score(t + 1, 1 - side, c)
                soften(side, c)
                mix(t - 1, 1 - side, c)
        return carry

    begin()
    for c in range(blk // piece):
        score(0, 0, c)
    lax.fori_loop(0, blocks // 2 - 1, turn, 0)
    turn(blocks // 2 - 1, 0)
    for c in range(lat // piece):
        mix(blocks - 1, 1, c)
    total = jnp.sum(sum_ref[...], axis=1, keepdims=True)
    done = (acc_ref[...] * (1.0 / total)).astype(lo.dtype)
    for p in range(ranks):
        lo[p, r] = done[p * block : (p + 1) * block]


def serve_kernel(
    lens_hbm, owner_hbm, ctx_hbm, new_hbm, shard_hbm, dq_hbm, kw_hbm, vw_hbm, q_hbm, cache_hbm,
    back, part_ref,
    spans_ref, got, tail, hot, tri, kw, vw, qs, dq, flat, wide, sent, keys, vals, buffers, cache,
    lo, tools, lens_ref, owner_ref, ctx_ref, new_ref,
    load_sems, cache_sems, small_sems, ring_send, ring_recv, swap_sems,
    give_sems, take_sems, back_send, back_recv,
    *, lat, ranks, heads, look, scale, pair, before, blk
):
    me = lax.axis_index("head")
    batch_rank = lax.axis_index("batch")
    place = place_of(me, ranks)
    right = rank_at((place + 1) % ranks, ranks)
    left = rank_at((place + ranks - 1) % ranks, ranks)
    owned = cache.shape[0]
    span_len = tail.shape[0]
    steps = sent.shape[2] // heads
    loads = [
        pltpu.make_async_copy(shard_hbm, spans_ref.at[me], load_sems.at[0]),
        pltpu.make_async_copy(dq_hbm, dq, load_sems.at[1]),
        pltpu.make_async_copy(kw_hbm, kw, load_sems.at[2]),
        pltpu.make_async_copy(vw_hbm, vw, load_sems.at[3]),
        pltpu.make_async_copy(q_hbm, qs, load_sems.at[4]),
    ] + [
        pltpu.make_async_copy(cache_hbm.at[r], cache.at[r], cache_sems.at[r])
        for r in range(owned)
    ]
    barrier = pltpu.get_barrier_semaphore()
    for k in range(1, ranks):
        pl.semaphore_signal(
            barrier, inc=1, device_id={"head": (me + k) % ranks}, device_id_type=MESH
        )
    pl.semaphore_signal(
        barrier, inc=1, device_id={"batch": 1 - batch_rank}, device_id_type=MESH
    )
    smalls = [
        pltpu.make_async_copy(lens_hbm, lens_ref, small_sems.at[0]),
        pltpu.make_async_copy(owner_hbm, owner_ref, small_sems.at[1]),
        pltpu.make_async_copy(ctx_hbm, ctx_ref, small_sems.at[2]),
        pltpu.make_async_copy(new_hbm, new_ref, small_sems.at[3]),
    ]
    for load in smalls + loads:
        load.start()
    for small in smalls:
        small.wait()
    start_marks(span_ends(lens_ref, batch_rank), tail, vals, hot, tri)
    pl.semaphore_wait(barrier, ranks)

    quarter = shard_hbm.shape[0] // 4
    most = ranks // 2

    def hop(way, part, t):
        back_by = t - 1 if way == 0 else ranks - t + 1
        origin = rank_at((place + ranks - back_by) % ranks, ranks)
        rows = pl.ds(part * quarter, quarter)
        return pltpu.make_async_remote_copy(
            src_ref=spans_ref.at[origin, rows],
            dst_ref=spans_ref.at[origin, rows],
            send_sem=ring_send.at[way, part, t - 1],
            recv_sem=ring_recv.at[way, part, t - 1],
            device_id={"head": right if way == 0 else left},
            device_id_type=MESH,
        )

    def hops(way, part):
        return most if way == part // 2 else most - 1

    streams = [(0, 0), (1, 2), (0, 1), (1, 3), (0, 2), (1, 0), (0, 3), (1, 1)]
    loads[0].wait()
    for way, part in streams:
        hop(way, part, 1).start()
    loads[1].wait()
    loads[2].wait()
    absorb_into(dq, kw, sent, flat, wide, heads, lat)
    loads[3].wait()

    def project(origin):
        project_shard(origin, spans_ref, kw, vw, keys, vals, tail, lat, heads)

    def arrive(t, carry):
        for way, part in streams:
            if hops(way, part) == most:
                hop(way, part, t).wait_recv()
                pl.when(t < most)(lambda: hop(way, part, t + 1).start())
            else:

                @pl.when(t < most)
                def _():
                    hop(way, part, t).wait_recv()
                    pl.when(t < most - 1)(lambda: hop(way, part, t + 1).start())

        def one(side, carry):
            project(rank_at((place + side * t + (1 - side) * (ranks - t)) % ranks, ranks))
            return carry

        lax.fori_loop(0, 2 - t // most, one, 0)
        return carry

    project(me)
    lax.fori_loop(1, most + 1, arrive, 0)

    def exchange(source, target, r, send_sems, recv_sems):
        return [
            pltpu.make_async_remote_copy(
                src_ref=source.at[(me + k) % ranks, r],
                dst_ref=target.at[me, r],
                send_sem=send_sems.at[r, k - 1],
                recv_sem=recv_sems.at[r, k - 1],
                device_id={"head": (me + k) % ranks},
                device_id_type=MESH,
            )
            for k in range(1, ranks)
        ]

    gives = [exchange(sent, got, r, give_sems, take_sems) for r in range(owned)]
    backs = [exchange(lo, back, r, back_send, back_recv) for r in range(owned)]
    swap = pltpu.make_async_remote_copy(
        src_ref=spans_ref.at[:ranks],
        dst_ref=spans_ref.at[ranks:],
        send_sem=swap_sems.at[0],
        recv_sem=swap_sems.at[1],
        device_id={"batch": 1 - batch_rank},
        device_id_type=MESH,
    )
    for copies in gives:
        for copy in copies:
            copy.start()
    swap.start()
    keep = pltpu.make_async_copy(sent.at[me], got.at[me], load_sems.at[5])
    keep.start()
    loads[4].wait()

    def attend(low, high):
        attend_groups(
            low, high, pair, qs, keys, tail, vals, hot, tri, part_ref, buffers, look, scale
        )

    groups = heads // pair
    attend(0, before)
    keep.wait()
    swap.wait()
    for r in range(owned):
        for copy in gives[r]:
            copy.wait()
        loads[5 + r].wait()
        row = batch_rank * (ranks * owned) + me * owned + r
        facts = request_facts(lens_ref, owner_ref, ctx_ref, r, row, batch_rank, span_len)
        decode_request(
            r, facts, got, new_ref, spans_ref, cache, lo, tools,
            lat=lat, heads=heads, steps=steps, scale=scale, blk=blk,
        )
        for copy in backs[r]:
            copy.start()
    stay = pltpu.make_async_copy(lo.at[me], back.at[me], load_sems.at[6])
    stay.start()
    attend(before, groups)
    for way, part in streams:
        for t in range(1, hops(way, part) + 1):
            hop(way, part, t).wait_send()
    for copies in backs:
        for copy in copies:
            copy.wait()
    stay.wait()


HBM_SPEC = pl.BlockSpec(memory_space=pltpu.HBM)
VMEM_SPEC = pl.BlockSpec(memory_space=pltpu.VMEM)
SMEM_SPEC = pl.BlockSpec(memory_space=pltpu.SMEM)


def serve_pallas(lens, owner, ctx, newest, shard, flat_queries, key_weight, value_weight, turned, cache, ranks, qb=256, pair=4, before=2, blk=512, ahead=4):
    heads, width, span_len = turned.shape
    kv, own = shard.shape
    lat = key_weight.shape[0]
    rows = flat_queries.shape[0]
    owned = cache.shape[0]
    block = rows // (ranks * owned)
    look = min(-(-(span_len // 2) // qb), span_len // qb - 1)
    marks = 128 - (kv - lat)
    deep = (look + 1) * qb
    asks = ranks * block
    bf16, f32 = jnp.bfloat16, jnp.float32
    vmem, dma = pltpu.VMEM, pltpu.SemaphoreType.DMA
    return pl.pallas_call(
        functools.partial(
            serve_kernel,
            lat=lat,
            ranks=ranks,
            heads=heads,
            look=look,
            scale=math.log2(math.e) / math.sqrt(width),
            pair=pair,
            before=before,
            blk=blk,
        ),
        out_shape=(
            jax.ShapeDtypeStruct((ranks, owned, block, lat), bf16),
            jax.ShapeDtypeStruct((span_len, heads * 128), bf16),
        ),
        in_specs=[HBM_SPEC] * 10,
        out_specs=(VMEM_SPEC,) * 2,
        scratch_shapes=[
            vmem((2 * ranks, kv, own), bf16),
            vmem((ranks, owned, block, kv), bf16),
            vmem((span_len, 128), bf16),
            vmem((marks, span_len), bf16),
            vmem((qb // 2, qb // 2), f32),
            vmem(key_weight.shape, bf16),
            vmem(value_weight.shape, bf16),
            vmem((heads, width, span_len), bf16),
            vmem((rows, width), bf16),
            vmem((rows, 128), f32),
            vmem((lat // 128, rows, 128), f32),
            vmem((ranks, owned, block, kv), bf16),
            vmem((heads, span_len, 128), bf16),
            vmem((heads, 144, span_len), bf16),
            [[vmem((deep, qb), f32)] * ahead, [vmem((deep, qb), bf16)] * ahead],
            vmem(cache.shape, bf16),
            vmem((ranks, owned, block, lat), bf16),
            [
                vmem((asks, 128), f32),
                vmem((asks, 128), f32),
                vmem((asks, lat), f32),
                vmem((asks, -(-(kv + 16) // 128) * 128), bf16),
                [vmem((asks, blk), f32)] * 2,
                [vmem((asks, 128), f32)] * 2,
                [vmem((asks, blk), bf16)] * 2,
                [vmem((asks, 128), f32)] * 2,
            ],
            pltpu.SMEM(lens.shape, lens.dtype),
            pltpu.SMEM(owner.shape, owner.dtype),
            pltpu.SMEM(ctx.shape, ctx.dtype),
            vmem(newest.shape, newest.dtype),
            dma((7,)),
            dma((owned,)),
            dma((4,)),
            dma((2, 4, ranks // 2)),
            dma((2, 4, ranks // 2)),
            dma((2,)),
            dma((owned, ranks - 1)),
            dma((owned, ranks - 1)),
            dma((owned, ranks - 1)),
            dma((owned, ranks - 1)),
        ],
        compiler_params=pltpu.CompilerParams(
            collective_id=0, has_side_effects=True, vmem_limit_bytes=46 << 20
        ),
        cost_estimate=pl.CostEstimate(
            flops=30 * 10**9, bytes_accessed=24 << 20, transcendentals=14 << 20
        ),
    )(lens, owner, ctx, newest, shard, flat_queries, key_weight, value_weight, turned, cache)


def project_kernel(back_ref, vw_ref, part_ref, out_ref, whole_ref, wide, sems, *, heads, lat):
    ranks, owned, block, _ = back_ref.shape
    steps = block // heads
    local = ranks * owned
    shown = pltpu.make_async_copy(part_ref, whole_ref, sems.at[0])
    shown.start()
    for p in range(ranks):
        for r in range(owned):
            at = (p * owned + r) * block
            for c in range(lat // 128):
                wide[c, at : at + block] = back_ref[p, r, :, c * 128 : (c + 1) * 128].astype(
                    jnp.float32
                )

    def some_heads(g, carry):
        for p in range(4):
            h = g * 4 + p
            mine = jnp.concatenate(
                [
                    jnp.concatenate(
                        [
                            wide[c, pl.ds(s * heads + h, local, stride=block), :]
                            for c in range(lat // 128)
                        ],
                        axis=1,
                    )
                    for s in range(steps)
                ],
                axis=0,
            ).astype(jnp.bfloat16)
            columns = pl.ds(pl.multiple_of(h * 128, 128), 128)
            out_ref[:, columns] = jnp.dot(
                mine, vw_ref[:, columns], preferred_element_type=jnp.float32
            ).astype(jnp.bfloat16)
        return carry

    lax.fori_loop(0, heads // 4, some_heads, 0)
    shown.wait()


def project_pallas(back, value_weight, part, heads):
    ranks, owned, block, lat = back.shape
    rows = ranks * owned * block
    return pl.pallas_call(
        functools.partial(project_kernel, heads=heads, lat=lat),
        out_shape=(
            jax.ShapeDtypeStruct((rows // heads, heads * 128), jnp.bfloat16),
            jax.ShapeDtypeStruct(part.shape, part.dtype),
        ),
        in_specs=[VMEM_SPEC, VMEM_SPEC, VMEM_SPEC],
        out_specs=(VMEM_SPEC, HBM_SPEC),
        scratch_shapes=[
            pltpu.VMEM((lat // 128, rows, 128), jnp.float32),
            pltpu.SemaphoreType.DMA((1,)),
        ],
        compiler_params=pltpu.CompilerParams(vmem_limit_bytes=8 << 20),
    )(back, value_weight, part)


def on_device(
    latent_rows,
    pre_queries,
    pre_lengths,
    owner_map,
    context_cache,
    context_lengths,
    new_latent,
    dec_queries,
    key_weight,
    value_weight,
):
    steps, rows_local, heads, width = dec_queries.shape
    ranks = lax.axis_size("head")
    if heads % 16 or latent_rows.shape[0] % 128 or ranks % 2:
        return plain_on_device(
            latent_rows,
            pre_queries,
            pre_lengths,
            owner_map,
            context_cache,
            context_lengths,
            new_latent,
            dec_queries,
            key_weight,
            value_weight,
        )
    stay = lambda x: pltpu.with_memory_space_constraint(x, pltpu.HBM)
    back, part = serve_pallas(
        stay(pre_lengths),
        stay(owner_map),
        stay(context_lengths),
        stay(new_latent),
        stay(jnp.transpose(latent_rows)),
        stay(dec_queries.reshape(-1, width)),
        stay(key_weight),
        stay(value_weight),
        stay(jnp.transpose(pre_queries, (1, 2, 0))),
        stay(jnp.transpose(context_cache, (0, 2, 1))),
        ranks,
    )
    decode_out, prefill_out = project_pallas(back, value_weight, part, heads)
    return (prefill_out, decode_out.reshape(steps, rows_local, heads * 128))


def solution(mesh):
    placed = (
        P(("groups", "batch", "head"), None),
        P(("groups", "batch"), "head", None),
        P("groups", None),
        P("groups", None),
        P(("groups", "batch", "head"), None, None),
        P(("groups", "batch", "head")),
        P("groups", ("batch", "head"), None),
        P("groups", "batch", "head", None),
        P(None, "head"),
        P(None, "head"),
    )
    return jax.shard_map(
        on_device,
        mesh=mesh,
        in_specs=placed,
        out_specs=(P(("groups", "batch"), "head"), P("groups", "batch", "head")),
        check_vma=False,
    )
```

```python
import functools
import math

import jax
import jax.numpy as jnp
from jax import lax
from jax.experimental import pallas as pl
from jax.experimental.pallas import tpu as pltpu
from jax.sharding import PartitionSpec as P

BLK = 512


NEGATIVE = -1e30


def from_partner(value, axis, distance):
    mask = 2**distance
    pairs = [(source, source ^ mask) for source in range(lax.axis_size(axis))]
    return lax.ppermute(value, axis, pairs)


def request_table(pre_lengths, owner_map, span_len):
    seg_ends = jnp.cumsum(pre_lengths, axis=1)
    span_base = jnp.arange(pre_lengths.shape[0], dtype=jnp.int32)[:, None] * span_len
    seg_starts = seg_ends - pre_lengths + span_base
    return (owner_map.reshape(-1), seg_starts.reshape(-1), pre_lengths.reshape(-1))


def prefill_heads(own_span, queries, span_lengths, key_weight, value_weight):
    span_len, head_count, query_width = queries.shape
    head_size = key_weight.shape[1] // head_count
    lat_width = key_weight.shape[0]
    score_scale = 1.0 / math.sqrt(query_width)
    latent = own_span[:, :lat_width]
    rope_keys = own_span[:, lat_width:]
    keys_nope = (
        jnp.dot(latent, key_weight, preferred_element_type=jnp.float32)
        .astype(jnp.bfloat16)
        .reshape(span_len, head_count, head_size)
    )
    values = (
        jnp.dot(latent, value_weight, preferred_element_type=jnp.float32)
        .astype(jnp.bfloat16)
        .reshape(span_len, head_count, head_size)
    )
    scores = jnp.einsum(
        "qhd,khd->hqk", queries[:, :, :head_size], keys_nope, preferred_element_type=jnp.float32
    )
    scores = scores + jnp.einsum(
        "qhr,kr->hqk", queries[:, :, head_size:], rope_keys, preferred_element_type=jnp.float32
    )
    scores = scores * score_scale
    seg_ends = jnp.cumsum(span_lengths)
    places = jnp.arange(span_len, dtype=jnp.int32)
    segment = jnp.sum((places[:, None] >= seg_ends[None, :]).astype(jnp.int32), axis=1)
    allowed = (segment[:, None] == segment[None, :]) & (places[None, :] <= places[:, None])
    masked = jnp.where(allowed[None], scores, NEGATIVE)
    peak_score = jnp.max(masked, axis=2, keepdims=True)
    weights = jnp.exp(masked - peak_score)
    weight_sum = jnp.sum(weights, axis=2)
    mixed_out = jnp.einsum(
        "hqk,khd->qhd", weights.astype(jnp.bfloat16), values, preferred_element_type=jnp.float32
    )
    mixed_out = mixed_out / jnp.transpose(weight_sum)[:, :, None]
    return mixed_out.astype(jnp.bfloat16).reshape(span_len, head_count * head_size)


def plain_on_device(
    latent_rows,
    pre_queries,
    pre_lengths,
    owner_map,
    context_cache,
    context_lengths,
    new_latent,
    dec_queries,
    key_weight,
    value_weight,
):
    head_rank = lax.axis_index("head")
    batch_rank = lax.axis_index("batch")
    span_len = pre_queries.shape[0]
    kv_width = latent_rows.shape[1]
    own_span = lax.all_gather(latent_rows, "head", axis=0, tiled=True)
    other_span = from_partner(own_span, "batch", 0)
    first_span = jnp.where(batch_rank == 0, own_span, other_span)
    second_span = jnp.where(batch_rank == 0, other_span, own_span)
    all_spans = jnp.concatenate([first_span, second_span], axis=0)
    span_lengths = lax.dynamic_index_in_dim(pre_lengths, batch_rank, 0, keepdims=False)
    prefill_out = prefill_heads(own_span, pre_queries, span_lengths, key_weight, value_weight)
    step_total, rows_local, head_count, query_width = dec_queries.shape
    lat_width = key_weight.shape[0]
    head_size = key_weight.shape[1] // head_count
    owned_rows = context_cache.shape[0]
    score_scale = 1.0 / math.sqrt(query_width)
    key_heads = key_weight.reshape(lat_width, head_count, head_size)
    value_heads = value_weight.reshape(lat_width, head_count, head_size)
    absorbed = jnp.einsum(
        "srhd,lhd->srhl",
        dec_queries[..., :head_size],
        key_heads,
        preferred_element_type=jnp.float32,
    ).astype(jnp.bfloat16)
    query_all = jnp.concatenate([absorbed, dec_queries[..., head_size:]], axis=3)
    flat_owner, flat_start, flat_length = request_table(pre_lengths, owner_map, span_len)
    row_ids = (
        batch_rank * rows_local + head_rank * owned_rows + jnp.arange(owned_rows, dtype=jnp.int32)
    )
    matches = (flat_owner[None, :] == row_ids[:, None]).astype(jnp.int32)
    is_target = jnp.sum(matches, axis=1) > 0
    first_row = jnp.sum(matches * flat_start[None, :], axis=1)
    prompt_len = jnp.sum(matches * flat_length[None, :], axis=1)
    effective = jnp.where(is_target, prompt_len, context_lengths)
    padded = jnp.concatenate([all_spans, jnp.zeros((span_len, kv_width), all_spans.dtype)], axis=0)
    replaced = jax.vmap(lambda offset: lax.dynamic_slice_in_dim(padded, offset, span_len, 0))(
        first_row
    )
    front_rows = jnp.where(is_target[:, None, None], replaced, context_cache[:, :span_len])
    front_blocks = span_len // BLK
    needed = (jnp.max(effective) + BLK - 1) // BLK
    fresh_latent = new_latent[..., :lat_width]
    owned_query = lax.all_to_all(query_all, "head", split_axis=1, concat_axis=2, tiled=True)
    fresh_scores = (
        jnp.einsum("srhk,jrk->srhj", owned_query, new_latent, preferred_element_type=jnp.float32)
        * score_scale
    )
    visible = (
        jnp.arange(new_latent.shape[0], dtype=jnp.int32)[None, :]
        <= jnp.arange(step_total, dtype=jnp.int32)[:, None]
    )
    fresh_scores = jnp.where(visible[:, None, None, :], fresh_scores, NEGATIVE)
    peak_score = jnp.max(fresh_scores, axis=3)
    weights = jnp.exp(fresh_scores - peak_score[..., None])
    weight_sum = jnp.sum(weights, axis=3)
    running = jnp.einsum(
        "srhj,jrl->srhl",
        weights.astype(jnp.bfloat16),
        fresh_latent,
        preferred_element_type=jnp.float32,
    )

    def advance(block_index, state_tuple, source):
        old_peak, old_sum, old_running = state_tuple
        key_block = lax.dynamic_slice_in_dim(source, block_index * BLK, BLK, 1)
        scores = (
            jnp.einsum("srhk,rtk->srht", owned_query, key_block, preferred_element_type=jnp.float32)
            * score_scale
        )
        places = block_index * BLK + jnp.arange(BLK, dtype=jnp.int32)
        in_context = places[None, :] < effective[:, None]
        scores = jnp.where(in_context[None, :, None, :], scores, NEGATIVE)
        new_peak = jnp.maximum(old_peak, jnp.max(scores, axis=3))
        factor = jnp.exp(old_peak - new_peak)
        block_weights = jnp.exp(scores - new_peak[..., None])
        new_sum = old_sum * factor + jnp.sum(block_weights, axis=3)
        new_running = old_running * factor[..., None] + jnp.einsum(
            "srht,rtl->srhl",
            block_weights.astype(jnp.bfloat16),
            key_block[..., :lat_width],
            preferred_element_type=jnp.float32,
        )
        return (new_peak, new_sum, new_running)

    state_tuple = lax.fori_loop(
        0,
        jnp.minimum(needed, front_blocks),
        lambda block_index, state_now: advance(block_index, state_now, front_rows),
        (peak_score, weight_sum, running),
    )
    state_tuple = lax.fori_loop(
        front_blocks,
        jnp.maximum(needed, front_blocks),
        lambda block_index, state_now: advance(block_index, state_now, context_cache),
        state_tuple,
    )
    latent_out = (state_tuple[2] / state_tuple[1][..., None]).astype(jnp.bfloat16)
    returned = lax.all_to_all(latent_out, "head", split_axis=2, concat_axis=1, tiled=True)
    projected = jnp.einsum(
        "srhl,lhd->srhd", returned, value_heads, preferred_element_type=jnp.float32
    ).astype(jnp.bfloat16)
    decode_out = projected.reshape(query_all.shape[0], rows_local, head_count * head_size)
    return (prefill_out, decode_out)


def trans_dot(left, right):
    return lax.dot_general(
        left, right, (((1,), (1,)), ((), ())), preferred_element_type=jnp.float32
    )


MESH = pl.DeviceIdType.MESH


def place_of(rank, ranks):
    odd = rank % 2
    return (1 - odd) * (rank // 2) + odd * (ranks - 1 - rank // 2)


def rank_at(place, ranks):
    late = place // (ranks // 2)
    return (1 - late) * (2 * place) + late * (2 * (ranks - 1 - place) + 1)


def start_marks(ends, tail, vals, hot, tri):
    span_len, full = tail.shape
    marks = hot.shape[0]
    segs = len(ends)
    where = lax.broadcasted_iota(jnp.int32, (span_len, marks), 0)
    lane = lax.broadcasted_iota(jnp.int32, (span_len, marks), 1)
    place = lax.broadcasted_iota(jnp.int32, (marks, span_len), 1)
    line = lax.broadcasted_iota(jnp.int32, (marks, span_len), 0)
    mine = jnp.zeros((span_len, marks), jnp.int32)
    seen = jnp.zeros((marks, span_len), jnp.int32)
    for k in range(segs - 1):
        mine = mine + (where >= ends[k]).astype(jnp.int32)
        seen = seen + (place >= ends[k]).astype(jnp.int32)
    mark = jnp.where((lane < segs) & (lane != mine), NEGATIVE, 0.0).astype(jnp.bfloat16)
    hot[...] = jnp.where(line == seen, 1.0, 0.0).astype(jnp.bfloat16)
    tail[:, full - marks :] = mark
    for h in range(vals.shape[0]):
        vals[h, 128:, :] = jnp.ones((vals.shape[1] - 128, span_len), jnp.bfloat16)
    size = tri.shape[0]
    key_at = lax.broadcasted_iota(jnp.int32, (size, size), 0)
    query_at = lax.broadcasted_iota(jnp.int32, (size, size), 1)
    tri[...] = jnp.where(key_at <= query_at, 0.0, NEGATIVE)


def project_shard(origin, spans_ref, kw, vw, keys, vals, tail, lat, heads):
    own = spans_ref.shape[2]
    rows = jnp.transpose(spans_ref[origin])
    at = pl.ds(pl.multiple_of(origin * own, own), own)
    tail[at, : rows.shape[1] - lat] = rows[:, lat:]
    latent = rows[:, :lat]
    pair = 2
    for g in range(heads // pair):
        columns = slice(g * pair * 128, (g + 1) * pair * 128)
        key = jnp.dot(latent, kw[:, columns], preferred_element_type=jnp.float32)
        value = jnp.dot(latent, vw[:, columns], preferred_element_type=jnp.float32)
        key = key.astype(jnp.bfloat16)
        value = jnp.transpose(value.astype(jnp.bfloat16))
        for p in range(pair):
            h = g * pair + p
            keys[h, at, :] = key[:, p * 128 : (p + 1) * 128]
            vals[h, :128, at] = value[p * 128 : (p + 1) * 128]


def attention(g, pair, qs, keys, tail, vals, hot, tri, part_ref, scores, weights, look, scale):
    span_len = tail.shape[0]
    qb = 2 * tri.shape[0]
    blocks = span_len // qb
    order = [(0, p) for p in range(pair // 2)]
    order += [(i, p) for i in range(1, blocks) for p in range(pair)]
    order += [(0, p) for p in range(pair // 2, pair)]
    count = len(order)
    lengths = [min(i, look) + 1 for i, _ in order]
    half = qb // 2
    skips = [half if length == look + 1 else 0 for length in lengths]
    peaks = [None] * count
    tops = [None] * count
    sums = [None] * count

    def score(n, c):
        i, p = order[n]
        if c > 0:
            return
        at = (i - lengths[n] + 1) * qb
        size = lengths[n] * qb
        query = jnp.concatenate(
            [qs[g * pair + p, :, i * qb : (i + 1) * qb], hot[:, i * qb : (i + 1) * qb]], axis=0
        )
        key = jnp.concatenate(
            [keys[g * pair + p, at : at + size, :], tail[at : at + size, :]], axis=1
        )
        s = jnp.dot(key, query, preferred_element_type=jnp.float32)
        left = [s[: size - qb, :half], s[size - qb : size - half, :half] + tri[...]]
        right = [s[skips[n] : size - half, half:], s[size - half :, half:] + tri[...]]
        row = 0
        for piece in left:
            if piece.shape[0]:
                scores[n % 4][row : row + piece.shape[0], :half] = piece
                row += piece.shape[0]
        row = skips[n]
        for piece in right:
            scores[n % 4][row : row + piece.shape[0], half:] = piece
            row += piece.shape[0]
        both = []
        for side in (left, right):
            best = None
            for piece in side:
                if piece.shape[0]:
                    top = jnp.max(piece.reshape(piece.shape[0] // 8, 8, half), axis=0)
                    best = top if best is None else jnp.maximum(best, top)
            both.append(best)
        peaks[n] = both

    def soften(n, c):
        if c == 0:
            tops[n] = [jnp.max(peak, axis=0, keepdims=True) for peak in peaks[n]]
        size = lengths[n] * qb
        for side in range(2):
            low, high = (0, size - half) if side == 0 else (skips[n], size)
            lanes = slice(side * half, (side + 1) * half)
            for k in range(c * qb, (c + 1) * qb, 64):
                at = slice(k, k + 64)
                if low <= k < high:
                    w = jnp.exp2((scores[n % 4][at, lanes] - tops[n][side]) * scale)
                    weights[n % 4][at, lanes] = w.astype(jnp.bfloat16)
                else:
                    weights[n % 4][at, lanes] = jnp.zeros((64, half), jnp.bfloat16)

    def mix(n, c):
        i, p = order[n]
        at = (i - lengths[n] + 1) * qb
        if c == 0:
            o = jnp.dot(
                vals[g * pair + p, :, at : at + lengths[n] * qb],
                weights[n % 4][: lengths[n] * qb, :],
                preferred_element_type=jnp.float32,
            )
            o = o[:128] * (1.0 / o[128:129])
            columns = pl.ds(pl.multiple_of((g * pair + p) * 128, 128), 128)
            part_ref[i * qb : (i + 1) * qb, columns] = jnp.transpose(o.astype(jnp.bfloat16))

    todo_score = [(n, c) for n in range(count) for c in range(lengths[n])]
    todo_soft = list(todo_score)
    todo_mix = list(todo_score)
    scored = [0] * count
    softened = [0] * count
    mixed = [0] * count
    while todo_mix:
        was = list(softened)
        if todo_score:
            n, c = todo_score[0]
            if n < 4 or softened[n - 4] == lengths[n - 4]:
                score(n, c)
                scored[n] += 1
                todo_score.pop(0)
        if todo_soft:
            n, c = todo_soft[0]
            free = n < 4 or mixed[n - 4] == lengths[n - 4]
            if scored[n] == lengths[n] and free and not (todo_score and todo_score[0][0] <= n + 2):
                soften(n, c)
                softened[n] += 1
                todo_soft.pop(0)
        n, c = todo_mix[0]
        if was[n] == lengths[n]:
            mix(n, c)
            mixed[n] += 1
            todo_mix.pop(0)


def attend_groups(low, high, pair, qs, keys, tail, vals, hot, tri, part_ref, buffers, look, scale):
    scores, weights = buffers

    def step(g, carry):
        attention(
            g, pair, qs, keys, tail, vals, hot, tri, part_ref, scores, weights, look, scale
        )
        return carry

    lax.fori_loop(low, high, step, 0)


def absorb_into(dq, kw, sent, flat, wide, heads, lat):
    rows = dq.shape[0]
    ranks, owned, block, _ = sent.shape
    steps = block // heads
    local = ranks * owned
    flat[...] = dq[:, :128].astype(jnp.float32)
    for h in range(heads):
        mine = flat[pl.ds(h, rows // heads, stride=heads), :].astype(jnp.bfloat16)
        res = trans_dot(mine, kw[:, h * 128 : (h + 1) * 128])
        for s in range(steps):
            for c in range(lat // 128):
                wide[c, pl.ds(s * heads + h, local, stride=block), :] = res[
                    s * local : (s + 1) * local, c * 128 : (c + 1) * 128
                ]
    for p in range(ranks):
        for r in range(owned):
            at = p * owned + r
            for c in range(lat // 128):
                sent[p, r, :, c * 128 : (c + 1) * 128] = wide[
                    c, at * block : (at + 1) * block
                ].astype(jnp.bfloat16)
            for s in range(steps):
                start = (s * local + at) * heads
                sent[p, r, s * heads : (s + 1) * heads, lat:] = dq[start : start + heads, 128:]


def span_ends(lens_ref, batch_rank):
    ends = []
    total = 0
    for k in range(lens_ref.shape[1]):
        total = total + lens_ref[batch_rank, k]
        ends.append(total)
    return ends


def request_facts(lens_ref, owner_ref, ctx_ref, r, row, batch_rank, span_len):
    target = jnp.int32(0)
    first = jnp.int32(0)
    length = jnp.int32(0)
    spans = lens_ref.shape[0]
    for c in range(spans):
        start = jnp.int32(((c + spans) % spans) * span_len)
        for k in range(lens_ref.shape[1]):
            hit = (owner_ref[c, k] == row).astype(jnp.int32)
            target = target + hit
            first = first + hit * start
            length = length + hit * lens_ref[c, k]
            start = start + lens_ref[c, k]
    first = ((first + batch_rank * span_len) % (2 * span_len)) * target
    return first, length, ctx_ref[r] * (1 - target)


def decode_request(r, facts, got, new_ref, spans_ref, cache, lo, tools, *, lat, heads, steps, scale, blk):
    peak_ref, sum_ref, acc_ref, asked, scores, tops, weights, fades = tools
    ranks, _, block, kv = got.shape
    rows = ranks * block
    first, length, held = facts
    own = spans_ref.shape[2]
    full = asked.shape[1]
    piece = 256
    blocks = cache.shape[2] // blk
    spread = (full - kv) // 16
    tail = lax.broadcasted_iota(jnp.int32, (rows, full - kv), 1)
    columns = lax.broadcasted_iota(jnp.int32, (16, piece), 1)

    line = lax.broadcasted_iota(jnp.int32, (16, piece), 0)

    def hidden(keep):
        mask = jnp.where((line == 0) & jnp.logical_not(keep), NEGATIVE, 0.0)
        return [mask.astype(jnp.bfloat16)] * spread

    def begin():
        asked[:, :kv] = got[:, r].reshape(rows, kv)
        row_step = (lax.broadcasted_iota(jnp.int32, tail.shape, 0) // heads) % steps
        asked[:, kv:] = jnp.where((tail == 0) | (tail == row_step + 1), 1.0, 0.0).astype(
            jnp.bfloat16
        )
        newest = new_ref[...].astype(jnp.float32)
        fresh = jnp.concatenate(
            [newest[s, r : r + 1] for s in range(steps)]
            + [jnp.zeros((own - steps, kv), jnp.float32)],
            axis=0,
        ).astype(jnp.bfloat16)
        fresh = jnp.transpose(fresh)
        span_len = spans_ref.shape[0] * own // 2
        shards = -(-(span_len // 2 + own - 1) // own)
        base = jnp.minimum(first // own, spans_ref.shape[0] - shards)
        each = piece // own
        most = (shards + 1) // each

        def block(c):
            parts = []
            for i in range(c * each, (c + 1) * each):
                parts.append(spans_ref[base + i] if i < shards else fresh)
            return jnp.concatenate(parts, axis=1)

        top = None
        for c in range(most):
            place = (base + c * each) * own + columns
            keep = (place >= first) & (place < first + length)
            mask = jnp.where((line == 0) & jnp.logical_not(keep), NEGATIVE, 0.0)
            if c == most - 1:
                new_at = columns - (piece - own)
                late = (line == 0) & (new_at >= steps)
                late = late | ((line > 0) & (new_at > line - 1))
                mask = jnp.where(new_at >= 0, jnp.where(late, NEGATIVE, 0.0), mask)
            keys = jnp.concatenate([block(c)] + [mask.astype(jnp.bfloat16)] * spread, axis=0)
            part = jnp.dot(asked[...], keys, preferred_element_type=jnp.float32)
            scores[c // 2][:, (c % 2) * piece : (c % 2 + 1) * piece] = part
            best = jnp.maximum(part[:, :128], part[:, 128:])
            top = best if top is None else jnp.maximum(top, best)
        m = jnp.max(top, axis=1, keepdims=True)
        peak_ref[...] = jnp.broadcast_to(m, peak_ref.shape)
        total, acc = None, None
        for c in range(most):
            w = jnp.exp2((scores[c // 2][:, (c % 2) * piece : (c % 2 + 1) * piece] - m) * scale)
            both = w[:, :128] + w[:, 128:]
            made = trans_dot(w.astype(jnp.bfloat16), block(c)[:lat])
            total = both if total is None else total + both
            acc = made if acc is None else acc + made
        sum_ref[...] = total
        acc_ref[...] = acc
        weights[1][...] = jnp.zeros(weights[1].shape, jnp.bfloat16)
        fades[1][...] = jnp.ones(fades[1].shape, jnp.float32)

    def score(t, side, c):
        at = pl.multiple_of(t * blk + c * piece, piece)
        keys = jnp.concatenate(
            [cache[r, :, pl.ds(at, piece)]] + hidden(at + columns < held), axis=0
        )
        s = jnp.dot(asked[...], keys, preferred_element_type=jnp.float32)
        scores[side][:, c * piece : (c + 1) * piece] = s
        top = jnp.maximum(s[:, :128], s[:, 128:])
        if c > 0:
            top = jnp.maximum(top, tops[side][...])
        tops[side][...] = top

    def settle(side):
        old = peak_ref[...]
        new = jnp.maximum(old, jnp.max(tops[side][...], axis=1, keepdims=True))
        fade = jnp.exp2((old - new) * scale)
        fades[side][...] = fade
        peak_ref[...] = new
        sum_ref[...] = sum_ref[...] * fade

    def soften(side, c):
        at = slice(c * piece, (c + 1) * piece)
        new = peak_ref[...]
        s = scores[side][:, at]
        left = jnp.exp2((s[:, :128] - new) * scale)
        right = jnp.exp2((s[:, 128:] - new) * scale)
        sum_ref[...] = sum_ref[...] + (left + right)
        weights[side][:, at] = jnp.concatenate([left, right], axis=1).astype(jnp.bfloat16)

    def mix(t, side, c):
        at = pl.multiple_of(jnp.maximum(t, 0) * blk, blk)
        some = slice(c * piece, (c + 1) * piece)
        made = trans_dot(weights[side][...], cache[r, some, pl.ds(at, blk)])
        fade = fades[side][...]
        for k in range(piece // 128):
            here = slice(c * piece + k * 128, c * piece + (k + 1) * 128)
            acc_ref[:, here] = acc_ref[:, here] * fade + made[:, k * 128 : (k + 1) * 128]

    def turn(j, carry):
        for side in range(2):
            t = 2 * j + side
            settle(side)
            for c in range(blk // piece):
                if not (isinstance(t, int) and t + 1 == blocks):
                    score(t + 1, 1 - side, c)
                soften(side, c)
                mix(t - 1, 1 - side, c)
        return carry

    begin()
    for c in range(blk // piece):
        score(0, 0, c)
    lax.fori_loop(0, blocks // 2 - 1, turn, 0)
    turn(blocks // 2 - 1, 0)
    for c in range(lat // piece):
        mix(blocks - 1, 1, c)
    total = jnp.sum(sum_ref[...], axis=1, keepdims=True)
    done = (acc_ref[...] * (1.0 / total)).astype(lo.dtype)
    for p in range(ranks):
        lo[p, r] = done[p * block : (p + 1) * block]


def serve_kernel(
    lens_hbm, owner_hbm, ctx_hbm, new_hbm, shard_hbm, dq_hbm, kw_hbm, vw_hbm, q_hbm, cache_hbm,
    back, part_ref,
    spans_ref, got, tail, hot, tri, kw, vw, qs, dq, flat, wide, sent, keys, vals, buffers, cache,
    lo, tools, lens_ref, owner_ref, ctx_ref, new_ref,
    load_sems, cache_sems, small_sems, ring_send, ring_recv, swap_sems,
    give_sems, take_sems, back_send, back_recv,
    *, lat, ranks, heads, look, scale, pair, before, blk
):
    me = lax.axis_index("head")
    batch_rank = lax.axis_index("batch")
    place = place_of(me, ranks)
    right = rank_at((place + 1) % ranks, ranks)
    left = rank_at((place + ranks - 1) % ranks, ranks)
    owned = cache.shape[0]
    span_len = tail.shape[0]
    steps = sent.shape[2] // heads
    loads = [
        pltpu.make_async_copy(shard_hbm, spans_ref.at[me], load_sems.at[0]),
        pltpu.make_async_copy(dq_hbm, dq, load_sems.at[1]),
        pltpu.make_async_copy(kw_hbm, kw, load_sems.at[2]),
        pltpu.make_async_copy(vw_hbm, vw, load_sems.at[3]),
        pltpu.make_async_copy(q_hbm, qs, load_sems.at[4]),
    ] + [
        pltpu.make_async_copy(cache_hbm.at[r], cache.at[r], cache_sems.at[r])
        for r in range(owned)
    ]
    barrier = pltpu.get_barrier_semaphore()
    for k in range(1, ranks):
        pl.semaphore_signal(
            barrier, inc=1, device_id={"head": (me + k) % ranks}, device_id_type=MESH
        )
    pl.semaphore_signal(
        barrier, inc=1, device_id={"batch": 1 - batch_rank}, device_id_type=MESH
    )
    smalls = [
        pltpu.make_async_copy(lens_hbm, lens_ref, small_sems.at[0]),
        pltpu.make_async_copy(owner_hbm, owner_ref, small_sems.at[1]),
        pltpu.make_async_copy(ctx_hbm, ctx_ref, small_sems.at[2]),
        pltpu.make_async_copy(new_hbm, new_ref, small_sems.at[3]),
    ]
    for load in smalls + loads:
        load.start()
    pl.semaphore_wait(barrier, ranks)

    quarter = shard_hbm.shape[0] // 4
    most = ranks // 2

    def hop(way, part, t):
        back_by = t - 1 if way == 0 else ranks - t + 1
        origin = rank_at((place + ranks - back_by) % ranks, ranks)
        rows = pl.ds(part * quarter, quarter)
        begins = isinstance(t, int) and t == 1
        return pltpu.make_async_remote_copy(
            src_ref=shard_hbm.at[rows] if begins else spans_ref.at[origin, rows],
            dst_ref=spans_ref.at[origin, rows],
            send_sem=ring_send.at[way, part, t - 1],
            recv_sem=ring_recv.at[way, part, t - 1],
            device_id={"head": right if way == 0 else left},
            device_id_type=MESH,
        )

    def hops(way, part):
        return most if way == part // 2 else most - 1

    streams = [(0, 0), (1, 2), (0, 1), (1, 3), (0, 2), (1, 0), (0, 3), (1, 1)]
    for way, part in streams:
        hop(way, part, 1).start()
    for small in smalls:
        small.wait()
    start_marks(span_ends(lens_ref, batch_rank), tail, vals, hot, tri)
    loads[0].wait()
    loads[1].wait()
    loads[2].wait()
    absorb_into(dq, kw, sent, flat, wide, heads, lat)
    loads[3].wait()

    def exchange(source, target, r, send_sems, recv_sems):
        return [
            pltpu.make_async_remote_copy(
                src_ref=source.at[(me + k) % ranks, r],
                dst_ref=target.at[me, r],
                send_sem=send_sems.at[r, k - 1],
                recv_sem=recv_sems.at[r, k - 1],
                device_id={"head": (me + k) % ranks},
                device_id_type=MESH,
            )
            for k in range(1, ranks)
        ]

    gives = [exchange(sent, got, r, give_sems, take_sems) for r in range(owned)]
    backs = [exchange(lo, back, r, back_send, back_recv) for r in range(owned)]
    def project(origin):
        project_shard(origin, spans_ref, kw, vw, keys, vals, tail, lat, heads)

    def arrive(t, carry):
        for way, part in streams:
            if hops(way, part) == most:
                hop(way, part, t).wait_recv()
                pl.when(t < most)(lambda: hop(way, part, t + 1).start())
            else:

                @pl.when(t < most)
                def _():
                    hop(way, part, t).wait_recv()
                    pl.when(t < most - 1)(lambda: hop(way, part, t + 1).start())

        @pl.when(t == most - 1)
        def _():
            for copies in gives:
                for copy in copies:
                    copy.start()

        def one(side, carry):
            project(rank_at((place + side * t + (1 - side) * (ranks - t)) % ranks, ranks))
            return carry

        lax.fori_loop(0, 2 - t // most, one, 0)
        return carry

    project(me)
    lax.fori_loop(1, most + 1, arrive, 0)

    swap = pltpu.make_async_remote_copy(
        src_ref=spans_ref.at[:ranks],
        dst_ref=spans_ref.at[ranks:],
        send_sem=swap_sems.at[0],
        recv_sem=swap_sems.at[1],
        device_id={"batch": 1 - batch_rank},
        device_id_type=MESH,
    )
    swap.start()
    keep = pltpu.make_async_copy(sent.at[me], got.at[me], load_sems.at[5])
    keep.start()
    loads[4].wait()

    def attend(low, high):
        attend_groups(
            low, high, pair, qs, keys, tail, vals, hot, tri, part_ref, buffers, look, scale
        )

    groups = heads // pair
    attend(0, before)
    keep.wait()
    swap.wait()
    for r in range(owned):
        for copy in gives[r]:
            copy.wait()
        loads[5 + r].wait()
        row = batch_rank * (ranks * owned) + me * owned + r
        facts = request_facts(lens_ref, owner_ref, ctx_ref, r, row, batch_rank, span_len)
        decode_request(
            r, facts, got, new_ref, spans_ref, cache, lo, tools,
            lat=lat, heads=heads, steps=steps, scale=scale, blk=blk,
        )
        for copy in backs[r]:
            copy.start()
    stay = pltpu.make_async_copy(lo.at[me], back.at[me], load_sems.at[6])
    stay.start()
    attend(before, groups)
    for way, part in streams:
        for t in range(1, hops(way, part) + 1):
            hop(way, part, t).wait_send()
    for copies in backs:
        for copy in copies:
            copy.wait()
    stay.wait()


HBM_SPEC = pl.BlockSpec(memory_space=pltpu.HBM)
VMEM_SPEC = pl.BlockSpec(memory_space=pltpu.VMEM)
SMEM_SPEC = pl.BlockSpec(memory_space=pltpu.SMEM)


def serve_pallas(lens, owner, ctx, newest, shard, flat_queries, key_weight, value_weight, turned, cache, ranks, qb=256, pair=4, before=2, blk=512, ahead=4):
    heads, width, span_len = turned.shape
    kv, own = shard.shape
    lat = key_weight.shape[0]
    rows = flat_queries.shape[0]
    owned = cache.shape[0]
    block = rows // (ranks * owned)
    look = min(-(-(span_len // 2) // qb), span_len // qb - 1)
    marks = 128 - (kv - lat)
    deep = (look + 1) * qb
    asks = ranks * block
    bf16, f32 = jnp.bfloat16, jnp.float32
    vmem, dma = pltpu.VMEM, pltpu.SemaphoreType.DMA
    return pl.pallas_call(
        functools.partial(
            serve_kernel,
            lat=lat,
            ranks=ranks,
            heads=heads,
            look=look,
            scale=math.log2(math.e) / math.sqrt(width),
            pair=pair,
            before=before,
            blk=blk,
        ),
        out_shape=(
            jax.ShapeDtypeStruct((ranks, owned, block, lat), bf16),
            jax.ShapeDtypeStruct((span_len, heads * 128), bf16),
        ),
        in_specs=[HBM_SPEC] * 10,
        out_specs=(VMEM_SPEC,) * 2,
        scratch_shapes=[
            vmem((2 * ranks, kv, own), bf16),
            vmem((ranks, owned, block, kv), bf16),
            vmem((span_len, 128), bf16),
            vmem((marks, span_len), bf16),
            vmem((qb // 2, qb // 2), f32),
            vmem(key_weight.shape, bf16),
            vmem(value_weight.shape, bf16),
            vmem((heads, width, span_len), bf16),
            vmem((rows, width), bf16),
            vmem((rows, 128), f32),
            vmem((lat // 128, rows, 128), f32),
            vmem((ranks, owned, block, kv), bf16),
            vmem((heads, span_len, 128), bf16),
            vmem((heads, 144, span_len), bf16),
            [[vmem((deep, qb), f32)] * ahead, [vmem((deep, qb), bf16)] * ahead],
            vmem(cache.shape, bf16),
            vmem((ranks, owned, block, lat), bf16),
            [
                vmem((asks, 128), f32),
                vmem((asks, 128), f32),
                vmem((asks, lat), f32),
                vmem((asks, -(-(kv + 16) // 128) * 128), bf16),
                [vmem((asks, blk), f32)] * 2,
                [vmem((asks, 128), f32)] * 2,
                [vmem((asks, blk), bf16)] * 2,
                [vmem((asks, 128), f32)] * 2,
            ],
            pltpu.SMEM(lens.shape, lens.dtype),
            pltpu.SMEM(owner.shape, owner.dtype),
            pltpu.SMEM(ctx.shape, ctx.dtype),
            vmem(newest.shape, newest.dtype),
            dma((7,)),
            dma((owned,)),
            dma((4,)),
            dma((2, 4, ranks // 2)),
            dma((2, 4, ranks // 2)),
            dma((2,)),
            dma((owned, ranks - 1)),
            dma((owned, ranks - 1)),
            dma((owned, ranks - 1)),
            dma((owned, ranks - 1)),
        ],
        compiler_params=pltpu.CompilerParams(
            collective_id=0, has_side_effects=True, vmem_limit_bytes=46 << 20
        ),
        cost_estimate=pl.CostEstimate(
            flops=30 * 10**9, bytes_accessed=24 << 20, transcendentals=14 << 20
        ),
    )(lens, owner, ctx, newest, shard, flat_queries, key_weight, value_weight, turned, cache)


def project_kernel(back_ref, vw_ref, part_ref, out_ref, whole_ref, wide, sems, *, heads, lat):
    ranks, owned, block, _ = back_ref.shape
    steps = block // heads
    local = ranks * owned
    shown = pltpu.make_async_copy(part_ref, whole_ref, sems.at[0])
    shown.start()
    for p in range(ranks):
        for r in range(owned):
            at = (p * owned + r) * block
            for c in range(lat // 128):
                wide[c, at : at + block] = back_ref[p, r, :, c * 128 : (c + 1) * 128].astype(
                    jnp.float32
                )

    def some_heads(g, carry):
        for p in range(4):
            h = g * 4 + p
            mine = jnp.concatenate(
                [
                    jnp.concatenate(
                        [
                            wide[c, pl.ds(s * heads + h, local, stride=block), :]
                            for c in range(lat // 128)
                        ],
                        axis=1,
                    )
                    for s in range(steps)
                ],
                axis=0,
            ).astype(jnp.bfloat16)
            columns = pl.ds(pl.multiple_of(h * 128, 128), 128)
            out_ref[:, columns] = jnp.dot(
                mine, vw_ref[:, columns], preferred_element_type=jnp.float32
            ).astype(jnp.bfloat16)
        return carry

    lax.fori_loop(0, heads // 4, some_heads, 0)
    shown.wait()


def project_pallas(back, value_weight, part, heads):
    ranks, owned, block, lat = back.shape
    rows = ranks * owned * block
    return pl.pallas_call(
        functools.partial(project_kernel, heads=heads, lat=lat),
        out_shape=(
            jax.ShapeDtypeStruct((rows // heads, heads * 128), jnp.bfloat16),
            jax.ShapeDtypeStruct(part.shape, part.dtype),
        ),
        in_specs=[VMEM_SPEC, VMEM_SPEC, VMEM_SPEC],
        out_specs=(VMEM_SPEC, HBM_SPEC),
        scratch_shapes=[
            pltpu.VMEM((lat // 128, rows, 128), jnp.float32),
            pltpu.SemaphoreType.DMA((1,)),
        ],
        compiler_params=pltpu.CompilerParams(vmem_limit_bytes=8 << 20),
    )(back, value_weight, part)


def on_device(
    latent_rows,
    pre_queries,
    pre_lengths,
    owner_map,
    context_cache,
    context_lengths,
    new_latent,
    dec_queries,
    key_weight,
    value_weight,
):
    steps, rows_local, heads, width = dec_queries.shape
    ranks = lax.axis_size("head")
    if heads % 16 or latent_rows.shape[0] % 128 or ranks % 2:
        return plain_on_device(
            latent_rows,
            pre_queries,
            pre_lengths,
            owner_map,
            context_cache,
            context_lengths,
            new_latent,
            dec_queries,
            key_weight,
            value_weight,
        )
    stay = lambda x: pltpu.with_memory_space_constraint(x, pltpu.HBM)
    back, part = serve_pallas(
        stay(pre_lengths),
        stay(owner_map),
        stay(context_lengths),
        stay(new_latent),
        stay(jnp.transpose(latent_rows)),
        stay(dec_queries.reshape(-1, width)),
        stay(key_weight),
        stay(value_weight),
        stay(jnp.transpose(pre_queries, (1, 2, 0))),
        stay(jnp.transpose(context_cache, (0, 2, 1))),
        ranks,
    )
    decode_out, prefill_out = project_pallas(back, value_weight, part, heads)
    return (prefill_out, decode_out.reshape(steps, rows_local, heads * 128))


def solution(mesh):
    placed = (
        P(("groups", "batch", "head"), None),
        P(("groups", "batch"), "head", None),
        P("groups", None),
        P("groups", None),
        P(("groups", "batch", "head"), None, None),
        P(("groups", "batch", "head")),
        P("groups", ("batch", "head"), None),
        P("groups", "batch", "head", None),
        P(None, "head"),
        P(None, "head"),
    )
    return jax.shard_map(
        on_device,
        mesh=mesh,
        in_specs=placed,
        out_specs=(P(("groups", "batch"), "head"), P("groups", "batch", "head")),
        check_vma=False,
    )
```

```python
import functools
import math

import jax
import jax.numpy as jnp
from jax import lax
from jax.experimental import pallas as pl
from jax.experimental.pallas import tpu as pltpu
from jax.sharding import PartitionSpec as P

BLK = 512


NEGATIVE = -1e30


def from_partner(value, axis, distance):
    mask = 2**distance
    pairs = [(source, source ^ mask) for source in range(lax.axis_size(axis))]
    return lax.ppermute(value, axis, pairs)


def request_table(pre_lengths, owner_map, span_len):
    seg_ends = jnp.cumsum(pre_lengths, axis=1)
    span_base = jnp.arange(pre_lengths.shape[0], dtype=jnp.int32)[:, None] * span_len
    seg_starts = seg_ends - pre_lengths + span_base
    return (owner_map.reshape(-1), seg_starts.reshape(-1), pre_lengths.reshape(-1))


def prefill_heads(own_span, queries, span_lengths, key_weight, value_weight):
    span_len, head_count, query_width = queries.shape
    head_size = key_weight.shape[1] // head_count
    lat_width = key_weight.shape[0]
    score_scale = 1.0 / math.sqrt(query_width)
    latent = own_span[:, :lat_width]
    rope_keys = own_span[:, lat_width:]
    keys_nope = (
        jnp.dot(latent, key_weight, preferred_element_type=jnp.float32)
        .astype(jnp.bfloat16)
        .reshape(span_len, head_count, head_size)
    )
    values = (
        jnp.dot(latent, value_weight, preferred_element_type=jnp.float32)
        .astype(jnp.bfloat16)
        .reshape(span_len, head_count, head_size)
    )
    scores = jnp.einsum(
        "qhd,khd->hqk", queries[:, :, :head_size], keys_nope, preferred_element_type=jnp.float32
    )
    scores = scores + jnp.einsum(
        "qhr,kr->hqk", queries[:, :, head_size:], rope_keys, preferred_element_type=jnp.float32
    )
    scores = scores * score_scale
    seg_ends = jnp.cumsum(span_lengths)
    places = jnp.arange(span_len, dtype=jnp.int32)
    segment = jnp.sum((places[:, None] >= seg_ends[None, :]).astype(jnp.int32), axis=1)
    allowed = (segment[:, None] == segment[None, :]) & (places[None, :] <= places[:, None])
    masked = jnp.where(allowed[None], scores, NEGATIVE)
    peak_score = jnp.max(masked, axis=2, keepdims=True)
    weights = jnp.exp(masked - peak_score)
    weight_sum = jnp.sum(weights, axis=2)
    mixed_out = jnp.einsum(
        "hqk,khd->qhd", weights.astype(jnp.bfloat16), values, preferred_element_type=jnp.float32
    )
    mixed_out = mixed_out / jnp.transpose(weight_sum)[:, :, None]
    return mixed_out.astype(jnp.bfloat16).reshape(span_len, head_count * head_size)


def plain_on_device(
    latent_rows,
    pre_queries,
    pre_lengths,
    owner_map,
    context_cache,
    context_lengths,
    new_latent,
    dec_queries,
    key_weight,
    value_weight,
):
    head_rank = lax.axis_index("head")
    batch_rank = lax.axis_index("batch")
    span_len = pre_queries.shape[0]
    kv_width = latent_rows.shape[1]
    own_span = lax.all_gather(latent_rows, "head", axis=0, tiled=True)
    other_span = from_partner(own_span, "batch", 0)
    first_span = jnp.where(batch_rank == 0, own_span, other_span)
    second_span = jnp.where(batch_rank == 0, other_span, own_span)
    all_spans = jnp.concatenate([first_span, second_span], axis=0)
    span_lengths = lax.dynamic_index_in_dim(pre_lengths, batch_rank, 0, keepdims=False)
    prefill_out = prefill_heads(own_span, pre_queries, span_lengths, key_weight, value_weight)
    step_total, rows_local, head_count, query_width = dec_queries.shape
    lat_width = key_weight.shape[0]
    head_size = key_weight.shape[1] // head_count
    owned_rows = context_cache.shape[0]
    score_scale = 1.0 / math.sqrt(query_width)
    key_heads = key_weight.reshape(lat_width, head_count, head_size)
    value_heads = value_weight.reshape(lat_width, head_count, head_size)
    absorbed = jnp.einsum(
        "srhd,lhd->srhl",
        dec_queries[..., :head_size],
        key_heads,
        preferred_element_type=jnp.float32,
    ).astype(jnp.bfloat16)
    query_all = jnp.concatenate([absorbed, dec_queries[..., head_size:]], axis=3)
    flat_owner, flat_start, flat_length = request_table(pre_lengths, owner_map, span_len)
    row_ids = (
        batch_rank * rows_local + head_rank * owned_rows + jnp.arange(owned_rows, dtype=jnp.int32)
    )
    matches = (flat_owner[None, :] == row_ids[:, None]).astype(jnp.int32)
    is_target = jnp.sum(matches, axis=1) > 0
    first_row = jnp.sum(matches * flat_start[None, :], axis=1)
    prompt_len = jnp.sum(matches * flat_length[None, :], axis=1)
    effective = jnp.where(is_target, prompt_len, context_lengths)
    padded = jnp.concatenate([all_spans, jnp.zeros((span_len, kv_width), all_spans.dtype)], axis=0)
    replaced = jax.vmap(lambda offset: lax.dynamic_slice_in_dim(padded, offset, span_len, 0))(
        first_row
    )
    front_rows = jnp.where(is_target[:, None, None], replaced, context_cache[:, :span_len])
    front_blocks = span_len // BLK
    needed = (jnp.max(effective) + BLK - 1) // BLK
    fresh_latent = new_latent[..., :lat_width]
    owned_query = lax.all_to_all(query_all, "head", split_axis=1, concat_axis=2, tiled=True)
    fresh_scores = (
        jnp.einsum("srhk,jrk->srhj", owned_query, new_latent, preferred_element_type=jnp.float32)
        * score_scale
    )
    visible = (
        jnp.arange(new_latent.shape[0], dtype=jnp.int32)[None, :]
        <= jnp.arange(step_total, dtype=jnp.int32)[:, None]
    )
    fresh_scores = jnp.where(visible[:, None, None, :], fresh_scores, NEGATIVE)
    peak_score = jnp.max(fresh_scores, axis=3)
    weights = jnp.exp(fresh_scores - peak_score[..., None])
    weight_sum = jnp.sum(weights, axis=3)
    running = jnp.einsum(
        "srhj,jrl->srhl",
        weights.astype(jnp.bfloat16),
        fresh_latent,
        preferred_element_type=jnp.float32,
    )

    def advance(block_index, state_tuple, source):
        old_peak, old_sum, old_running = state_tuple
        key_block = lax.dynamic_slice_in_dim(source, block_index * BLK, BLK, 1)
        scores = (
            jnp.einsum("srhk,rtk->srht", owned_query, key_block, preferred_element_type=jnp.float32)
            * score_scale
        )
        places = block_index * BLK + jnp.arange(BLK, dtype=jnp.int32)
        in_context = places[None, :] < effective[:, None]
        scores = jnp.where(in_context[None, :, None, :], scores, NEGATIVE)
        new_peak = jnp.maximum(old_peak, jnp.max(scores, axis=3))
        factor = jnp.exp(old_peak - new_peak)
        block_weights = jnp.exp(scores - new_peak[..., None])
        new_sum = old_sum * factor + jnp.sum(block_weights, axis=3)
        new_running = old_running * factor[..., None] + jnp.einsum(
            "srht,rtl->srhl",
            block_weights.astype(jnp.bfloat16),
            key_block[..., :lat_width],
            preferred_element_type=jnp.float32,
        )
        return (new_peak, new_sum, new_running)

    state_tuple = lax.fori_loop(
        0,
        jnp.minimum(needed, front_blocks),
        lambda block_index, state_now: advance(block_index, state_now, front_rows),
        (peak_score, weight_sum, running),
    )
    state_tuple = lax.fori_loop(
        front_blocks,
        jnp.maximum(needed, front_blocks),
        lambda block_index, state_now: advance(block_index, state_now, context_cache),
        state_tuple,
    )
    latent_out = (state_tuple[2] / state_tuple[1][..., None]).astype(jnp.bfloat16)
    returned = lax.all_to_all(latent_out, "head", split_axis=2, concat_axis=1, tiled=True)
    projected = jnp.einsum(
        "srhl,lhd->srhd", returned, value_heads, preferred_element_type=jnp.float32
    ).astype(jnp.bfloat16)
    decode_out = projected.reshape(query_all.shape[0], rows_local, head_count * head_size)
    return (prefill_out, decode_out)


def trans_dot(left, right):
    return lax.dot_general(
        left, right, (((1,), (1,)), ((), ())), preferred_element_type=jnp.float32
    )


MESH = pl.DeviceIdType.MESH


def place_of(rank, ranks):
    odd = rank % 2
    return (1 - odd) * (rank // 2) + odd * (ranks - 1 - rank // 2)


def rank_at(place, ranks):
    late = place // (ranks // 2)
    return (1 - late) * (2 * place) + late * (2 * (ranks - 1 - place) + 1)


def start_marks(ends, tail, vals, hot, tri):
    span_len, full = tail.shape
    marks = hot.shape[0]
    segs = len(ends)
    where = lax.broadcasted_iota(jnp.int32, (span_len, marks), 0)
    lane = lax.broadcasted_iota(jnp.int32, (span_len, marks), 1)
    place = lax.broadcasted_iota(jnp.int32, (marks, span_len), 1)
    line = lax.broadcasted_iota(jnp.int32, (marks, span_len), 0)
    mine = jnp.zeros((span_len, marks), jnp.int32)
    seen = jnp.zeros((marks, span_len), jnp.int32)
    for k in range(segs - 1):
        mine = mine + (where >= ends[k]).astype(jnp.int32)
        seen = seen + (place >= ends[k]).astype(jnp.int32)
    mark = jnp.where((lane < segs) & (lane != mine), NEGATIVE, 0.0).astype(jnp.bfloat16)
    hot[...] = jnp.where(line == seen, 1.0, 0.0).astype(jnp.bfloat16)
    tail[:, full - marks :] = mark
    for h in range(vals.shape[0]):
        vals[h, 128:, :] = jnp.ones((vals.shape[1] - 128, span_len), jnp.bfloat16)
    size = tri.shape[0]
    key_at = lax.broadcasted_iota(jnp.int32, (size, size), 0)
    query_at = lax.broadcasted_iota(jnp.int32, (size, size), 1)
    tri[...] = jnp.where(key_at <= query_at, 0.0, NEGATIVE)


def project_shard(origin, spans_ref, kw, vw, keys, vals, tail, lat, heads):
    own = spans_ref.shape[2]
    rows = jnp.transpose(spans_ref[origin])
    at = pl.ds(pl.multiple_of(origin * own, own), own)
    tail[at, : rows.shape[1] - lat] = rows[:, lat:]
    latent = rows[:, :lat]
    pair = 2
    for g in range(heads // pair):
        columns = slice(g * pair * 128, (g + 1) * pair * 128)
        key = jnp.dot(latent, kw[:, columns], preferred_element_type=jnp.float32)
        value = jnp.dot(latent, vw[:, columns], preferred_element_type=jnp.float32)
        key = key.astype(jnp.bfloat16)
        value = jnp.transpose(value.astype(jnp.bfloat16))
        for p in range(pair):
            h = g * pair + p
            keys[h, at, :] = key[:, p * 128 : (p + 1) * 128]
            vals[h, :128, at] = value[p * 128 : (p + 1) * 128]


def attention(g, pair, qs, keys, tail, vals, hot, tri, part_ref, scores, weights, look, scale):
    span_len = tail.shape[0]
    qb = 2 * tri.shape[0]
    blocks = span_len // qb
    order = [(0, p) for p in range(pair // 2)]
    order += [(i, p) for i in range(1, blocks) for p in range(pair)]
    order += [(0, p) for p in range(pair // 2, pair)]
    count = len(order)
    lengths = [min(i, look) + 1 for i, _ in order]
    half = qb // 2
    skips = [half if length == look + 1 else 0 for length in lengths]
    peaks = [None] * count
    tops = [None] * count
    sums = [None] * count

    def score(n, c):
        i, p = order[n]
        if c > 0:
            return
        at = (i - lengths[n] + 1) * qb
        size = lengths[n] * qb
        query = jnp.concatenate(
            [qs[g * pair + p, :, i * qb : (i + 1) * qb], hot[:, i * qb : (i + 1) * qb]], axis=0
        )
        key = jnp.concatenate(
            [keys[g * pair + p, at : at + size, :], tail[at : at + size, :]], axis=1
        )
        s = jnp.dot(key, query, preferred_element_type=jnp.float32)
        left = [s[: size - qb, :half], s[size - qb : size - half, :half] + tri[...]]
        right = [s[skips[n] : size - half, half:], s[size - half :, half:] + tri[...]]
        row = 0
        for piece in left:
            if piece.shape[0]:
                scores[n % 4][row : row + piece.shape[0], :half] = piece
                row += piece.shape[0]
        row = skips[n]
        for piece in right:
            scores[n % 4][row : row + piece.shape[0], half:] = piece
            row += piece.shape[0]
        both = []
        for side in (left, right):
            best = None
            for piece in side:
                if piece.shape[0]:
                    top = jnp.max(piece.reshape(piece.shape[0] // 8, 8, half), axis=0)
                    best = top if best is None else jnp.maximum(best, top)
            both.append(best)
        peaks[n] = both

    def soften(n, c):
        if c == 0:
            tops[n] = [jnp.max(peak, axis=0, keepdims=True) for peak in peaks[n]]
        size = lengths[n] * qb
        for side in range(2):
            low, high = (0, size - half) if side == 0 else (skips[n], size)
            lanes = slice(side * half, (side + 1) * half)
            for k in range(c * qb, (c + 1) * qb, 64):
                at = slice(k, k + 64)
                if low <= k < high:
                    w = jnp.exp2((scores[n % 4][at, lanes] - tops[n][side]) * scale)
                    weights[n % 4][at, lanes] = w.astype(jnp.bfloat16)
                else:
                    weights[n % 4][at, lanes] = jnp.zeros((64, half), jnp.bfloat16)

    def mix(n, c):
        i, p = order[n]
        at = (i - lengths[n] + 1) * qb
        if c == 0:
            o = jnp.dot(
                vals[g * pair + p, :, at : at + lengths[n] * qb],
                weights[n % 4][: lengths[n] * qb, :],
                preferred_element_type=jnp.float32,
            )
            o = o[:128] * (1.0 / o[128:129])
            columns = pl.ds(pl.multiple_of((g * pair + p) * 128, 128), 128)
            part_ref[i * qb : (i + 1) * qb, columns] = jnp.transpose(o.astype(jnp.bfloat16))

    todo_score = [(n, c) for n in range(count) for c in range(lengths[n])]
    todo_soft = list(todo_score)
    todo_mix = list(todo_score)
    scored = [0] * count
    softened = [0] * count
    mixed = [0] * count
    while todo_mix:
        was = list(softened)
        if todo_score:
            n, c = todo_score[0]
            if n < 4 or softened[n - 4] == lengths[n - 4]:
                score(n, c)
                scored[n] += 1
                todo_score.pop(0)
        if todo_soft:
            n, c = todo_soft[0]
            free = n < 4 or mixed[n - 4] == lengths[n - 4]
            if scored[n] == lengths[n] and free and not (todo_score and todo_score[0][0] <= n + 2):
                soften(n, c)
                softened[n] += 1
                todo_soft.pop(0)
        n, c = todo_mix[0]
        if was[n] == lengths[n]:
            mix(n, c)
            mixed[n] += 1
            todo_mix.pop(0)


def attend_groups(low, high, pair, qs, keys, tail, vals, hot, tri, part_ref, buffers, look, scale):
    scores, weights = buffers

    def step(g, carry):
        attention(
            g, pair, qs, keys, tail, vals, hot, tri, part_ref, scores, weights, look, scale
        )
        return carry

    lax.fori_loop(low, high, step, 0)


def absorb_into(dq, kw, sent, flat, wide, heads, lat):
    rows = dq.shape[0]
    ranks, owned, block, _ = sent.shape
    steps = block // heads
    local = ranks * owned
    flat[...] = dq[:, :128].astype(jnp.float32)
    for h in range(heads):
        mine = flat[pl.ds(h, rows // heads, stride=heads), :].astype(jnp.bfloat16)
        res = trans_dot(mine, kw[:, h * 128 : (h + 1) * 128])
        for s in range(steps):
            for c in range(lat // 128):
                wide[c, pl.ds(s * heads + h, local, stride=block), :] = res[
                    s * local : (s + 1) * local, c * 128 : (c + 1) * 128
                ]
    for p in range(ranks):
        for r in range(owned):
            at = p * owned + r
            for c in range(lat // 128):
                sent[p, r, :, c * 128 : (c + 1) * 128] = wide[
                    c, at * block : (at + 1) * block
                ].astype(jnp.bfloat16)
            for s in range(steps):
                start = (s * local + at) * heads
                sent[p, r, s * heads : (s + 1) * heads, lat:] = dq[start : start + heads, 128:]


def span_ends(lens_ref, batch_rank):
    ends = []
    total = 0
    for k in range(lens_ref.shape[1]):
        total = total + lens_ref[batch_rank, k]
        ends.append(total)
    return ends


def request_facts(lens_ref, owner_ref, ctx_ref, r, row, batch_rank, span_len):
    target = jnp.int32(0)
    first = jnp.int32(0)
    length = jnp.int32(0)
    spans = lens_ref.shape[0]
    for c in range(spans):
        start = jnp.int32(((c + spans) % spans) * span_len)
        for k in range(lens_ref.shape[1]):
            hit = (owner_ref[c, k] == row).astype(jnp.int32)
            target = target + hit
            first = first + hit * start
            length = length + hit * lens_ref[c, k]
            start = start + lens_ref[c, k]
    first = ((first + batch_rank * span_len) % (2 * span_len)) * target
    return first, length, ctx_ref[r] * (1 - target)


def decode_request(r, facts, got, new_ref, spans_ref, cache, lo, tools, *, lat, heads, steps, scale, blk):
    peak_ref, sum_ref, acc_ref, asked, scores, tops, weights, fades = tools
    ranks, _, block, kv = got.shape
    rows = ranks * block
    first, length, held = facts
    own = spans_ref.shape[2]
    full = asked.shape[1]
    piece = 256
    blocks = cache.shape[2] // blk
    spread = (full - kv) // 16
    tail = lax.broadcasted_iota(jnp.int32, (rows, full - kv), 1)
    columns = lax.broadcasted_iota(jnp.int32, (16, piece), 1)

    line = lax.broadcasted_iota(jnp.int32, (16, piece), 0)

    def hidden(keep):
        mask = jnp.where((line == 0) & jnp.logical_not(keep), NEGATIVE, 0.0)
        return [mask.astype(jnp.bfloat16)] * spread

    def begin():
        asked[:, :kv] = got[:, r].reshape(rows, kv)
        row_step = (lax.broadcasted_iota(jnp.int32, tail.shape, 0) // heads) % steps
        asked[:, kv:] = jnp.where((tail == 0) | (tail == row_step + 1), 1.0, 0.0).astype(
            jnp.bfloat16
        )
        newest = new_ref[...].astype(jnp.float32)
        fresh = jnp.concatenate(
            [newest[s, r : r + 1] for s in range(steps)]
            + [jnp.zeros((own - steps, kv), jnp.float32)],
            axis=0,
        ).astype(jnp.bfloat16)
        fresh = jnp.transpose(fresh)
        span_len = spans_ref.shape[0] * own // 2
        shards = -(-(span_len // 2 + own - 1) // own)
        base = jnp.minimum(first // own, spans_ref.shape[0] - shards)
        each = piece // own
        most = (shards + 1) // each

        def block(c):
            parts = []
            for i in range(c * each, (c + 1) * each):
                parts.append(spans_ref[base + i] if i < shards else fresh)
            return jnp.concatenate(parts, axis=1)

        top = None
        for c in range(most):
            place = (base + c * each) * own + columns
            keep = (place >= first) & (place < first + length)
            mask = jnp.where((line == 0) & jnp.logical_not(keep), NEGATIVE, 0.0)
            if c == most - 1:
                new_at = columns - (piece - own)
                late = (line == 0) & (new_at >= steps)
                late = late | ((line > 0) & (new_at > line - 1))
                mask = jnp.where(new_at >= 0, jnp.where(late, NEGATIVE, 0.0), mask)
            keys = jnp.concatenate([block(c)] + [mask.astype(jnp.bfloat16)] * spread, axis=0)
            part = jnp.dot(asked[...], keys, preferred_element_type=jnp.float32)
            scores[c // 2][:, (c % 2) * piece : (c % 2 + 1) * piece] = part
            best = jnp.maximum(part[:, :128], part[:, 128:])
            top = best if top is None else jnp.maximum(top, best)
        m = jnp.max(top, axis=1, keepdims=True)
        peak_ref[...] = jnp.broadcast_to(m, peak_ref.shape)
        total, acc = None, None
        for c in range(most):
            w = jnp.exp2((scores[c // 2][:, (c % 2) * piece : (c % 2 + 1) * piece] - m) * scale)
            both = w[:, :128] + w[:, 128:]
            made = trans_dot(w.astype(jnp.bfloat16), block(c)[:lat])
            total = both if total is None else total + both
            acc = made if acc is None else acc + made
        sum_ref[...] = total
        acc_ref[...] = acc
        weights[1][...] = jnp.zeros(weights[1].shape, jnp.bfloat16)
        fades[1][...] = jnp.ones(fades[1].shape, jnp.float32)

    def score(t, side, c):
        at = pl.multiple_of(t * blk + c * piece, piece)
        keys = jnp.concatenate(
            [cache[r, :, pl.ds(at, piece)]] + hidden(at + columns < held), axis=0
        )
        s = jnp.dot(asked[...], keys, preferred_element_type=jnp.float32)
        scores[side][:, c * piece : (c + 1) * piece] = s
        top = jnp.maximum(s[:, :128], s[:, 128:])
        if c > 0:
            top = jnp.maximum(top, tops[side][...])
        tops[side][...] = top

    def settle(side):
        old = peak_ref[...]
        new = jnp.maximum(old, jnp.max(tops[side][...], axis=1, keepdims=True))
        fade = jnp.exp2((old - new) * scale)
        fades[side][...] = fade
        peak_ref[...] = new
        sum_ref[...] = sum_ref[...] * fade

    def soften(side, c):
        at = slice(c * piece, (c + 1) * piece)
        new = peak_ref[...]
        s = scores[side][:, at]
        left = jnp.exp2((s[:, :128] - new) * scale)
        right = jnp.exp2((s[:, 128:] - new) * scale)
        sum_ref[...] = sum_ref[...] + (left + right)
        weights[side][:, at] = jnp.concatenate([left, right], axis=1).astype(jnp.bfloat16)

    def mix(t, side, c):
        at = pl.multiple_of(jnp.maximum(t, 0) * blk, blk)
        some = slice(c * piece, (c + 1) * piece)
        made = trans_dot(weights[side][...], cache[r, some, pl.ds(at, blk)])
        fade = fades[side][...]
        for k in range(piece // 128):
            here = slice(c * piece + k * 128, c * piece + (k + 1) * 128)
            acc_ref[:, here] = acc_ref[:, here] * fade + made[:, k * 128 : (k + 1) * 128]

    def turn(j, carry):
        for side in range(2):
            t = 2 * j + side
            settle(side)
            for c in range(blk // piece):
                if not (isinstance(t, int) and t + 1 == blocks):
                    score(t + 1, 1 - side, c)
                soften(side, c)
                mix(t - 1, 1 - side, c)
        return carry

    begin()
    for c in range(blk // piece):
        score(0, 0, c)
    lax.fori_loop(0, blocks // 2 - 1, turn, 0)
    turn(blocks // 2 - 1, 0)
    for c in range(lat // piece):
        mix(blocks - 1, 1, c)
    total = jnp.sum(sum_ref[...], axis=1, keepdims=True)
    done = (acc_ref[...] * (1.0 / total)).astype(lo.dtype)
    for p in range(ranks):
        lo[p, r] = done[p * block : (p + 1) * block]


def serve_kernel(
    lens_hbm, owner_hbm, ctx_hbm, new_hbm, shard_hbm, dq_hbm, kw_hbm, vw_hbm, q_hbm, cache_hbm,
    back, part_ref,
    spans_ref, got, tail, hot, tri, kw, vw, qs, dq, flat, wide, sent, keys, vals, buffers, cache,
    lo, tools, lens_ref, owner_ref, ctx_ref, new_ref,
    load_sems, cache_sems, small_sems, ring_send, ring_recv, swap_sems,
    give_sems, take_sems, back_send, back_recv,
    *, lat, ranks, heads, look, scale, pair, before, blk
):
    me = lax.axis_index("head")
    batch_rank = lax.axis_index("batch")
    place = place_of(me, ranks)
    right = rank_at((place + 1) % ranks, ranks)
    left = rank_at((place + ranks - 1) % ranks, ranks)
    owned = cache.shape[0]
    span_len = tail.shape[0]
    steps = sent.shape[2] // heads
    loads = [
        pltpu.make_async_copy(shard_hbm, spans_ref.at[me], load_sems.at[0]),
        pltpu.make_async_copy(dq_hbm, dq, load_sems.at[1]),
        pltpu.make_async_copy(kw_hbm, kw, load_sems.at[2]),
        pltpu.make_async_copy(vw_hbm, vw, load_sems.at[3]),
        pltpu.make_async_copy(q_hbm, qs, load_sems.at[4]),
    ] + [
        pltpu.make_async_copy(cache_hbm.at[r], cache.at[r], cache_sems.at[r])
        for r in range(owned)
    ]
    barrier = pltpu.get_barrier_semaphore()
    for k in range(1, ranks):
        pl.semaphore_signal(
            barrier, inc=1, device_id={"head": (me + k) % ranks}, device_id_type=MESH
        )
    pl.semaphore_signal(
        barrier, inc=1, device_id={"batch": 1 - batch_rank}, device_id_type=MESH
    )
    smalls = [
        pltpu.make_async_copy(lens_hbm, lens_ref, small_sems.at[0]),
        pltpu.make_async_copy(owner_hbm, owner_ref, small_sems.at[1]),
        pltpu.make_async_copy(ctx_hbm, ctx_ref, small_sems.at[2]),
        pltpu.make_async_copy(new_hbm, new_ref, small_sems.at[3]),
    ]
    for load in smalls + loads:
        load.start()
    pl.semaphore_wait(barrier, ranks)

    quarter = shard_hbm.shape[0] // 4
    most = ranks // 2

    def hop(way, part, t):
        back_by = t - 1 if way == 0 else ranks - t + 1
        origin = rank_at((place + ranks - back_by) % ranks, ranks)
        rows = pl.ds(part * quarter, quarter)
        begins = isinstance(t, int) and t == 1
        return pltpu.make_async_remote_copy(
            src_ref=shard_hbm.at[rows] if begins else spans_ref.at[origin, rows],
            dst_ref=spans_ref.at[origin, rows],
            send_sem=ring_send.at[way, part, t - 1],
            recv_sem=ring_recv.at[way, part, t - 1],
            device_id={"head": right if way == 0 else left},
            device_id_type=MESH,
        )

    def hops(way, part):
        return most if way == part // 2 else most - 1

    streams = [(0, 0), (1, 2), (0, 1), (1, 3), (0, 2), (1, 0), (0, 3), (1, 1)]
    for way, part in streams:
        hop(way, part, 1).start()
    for small in smalls:
        small.wait()
    start_marks(span_ends(lens_ref, batch_rank), tail, vals, hot, tri)
    loads[0].wait()
    loads[1].wait()
    loads[2].wait()
    absorb_into(dq, kw, sent, flat, wide, heads, lat)
    loads[3].wait()

    def exchange(source, target, r, send_sems, recv_sems):
        return [
            pltpu.make_async_remote_copy(
                src_ref=source.at[(me + k) % ranks, r],
                dst_ref=target.at[me, r],
                send_sem=send_sems.at[r, k - 1],
                recv_sem=recv_sems.at[r, k - 1],
                device_id={"head": (me + k) % ranks},
                device_id_type=MESH,
            )
            for k in sorted(range(1, ranks), key=lambda k: abs(k - ranks // 2))
        ]

    gives = [exchange(sent, got, r, give_sems, take_sems) for r in range(owned)]
    backs = [exchange(lo, back, r, back_send, back_recv) for r in range(owned)]
    def project(origin):
        project_shard(origin, spans_ref, kw, vw, keys, vals, tail, lat, heads)

    def arrive(t, carry):
        for way, part in streams:
            if hops(way, part) == most:
                hop(way, part, t).wait_recv()
                pl.when(t < most)(lambda: hop(way, part, t + 1).start())
            else:

                @pl.when(t < most)
                def _():
                    hop(way, part, t).wait_recv()
                    pl.when(t < most - 1)(lambda: hop(way, part, t + 1).start())

        @pl.when(t == most - 1)
        def _():
            for copies in gives:
                for copy in copies:
                    copy.start()

        def one(side, carry):
            project(rank_at((place + side * t + (1 - side) * (ranks - t)) % ranks, ranks))
            return carry

        lax.fori_loop(0, 2 - t // most, one, 0)
        return carry

    project(me)
    lax.fori_loop(1, most + 1, arrive, 0)

    swap = pltpu.make_async_remote_copy(
        src_ref=spans_ref.at[:ranks],
        dst_ref=spans_ref.at[ranks:],
        send_sem=swap_sems.at[0],
        recv_sem=swap_sems.at[1],
        device_id={"batch": 1 - batch_rank},
        device_id_type=MESH,
    )
    swap.start()
    keep = pltpu.make_async_copy(sent.at[me], got.at[me], load_sems.at[5])
    keep.start()
    loads[4].wait()

    def attend(low, high):
        attend_groups(
            low, high, pair, qs, keys, tail, vals, hot, tri, part_ref, buffers, look, scale
        )

    groups = heads // pair
    attend(0, before)
    keep.wait()
    swap.wait()
    for r in range(owned):
        for copy in gives[r]:
            copy.wait()
        loads[5 + r].wait()
        row = batch_rank * (ranks * owned) + me * owned + r
        facts = request_facts(lens_ref, owner_ref, ctx_ref, r, row, batch_rank, span_len)
        decode_request(
            r, facts, got, new_ref, spans_ref, cache, lo, tools,
            lat=lat, heads=heads, steps=steps, scale=scale, blk=blk,
        )
        for copy in backs[r]:
            copy.start()
    stay = pltpu.make_async_copy(lo.at[me], back.at[me], load_sems.at[6])
    stay.start()
    attend(before, groups)
    for way, part in streams:
        for t in range(1, hops(way, part) + 1):
            hop(way, part, t).wait_send()
    for copies in backs:
        for copy in copies:
            copy.wait()
    stay.wait()


HBM_SPEC = pl.BlockSpec(memory_space=pltpu.HBM)
VMEM_SPEC = pl.BlockSpec(memory_space=pltpu.VMEM)
SMEM_SPEC = pl.BlockSpec(memory_space=pltpu.SMEM)


def serve_pallas(lens, owner, ctx, newest, shard, flat_queries, key_weight, value_weight, turned, cache, ranks, qb=256, pair=4, before=2, blk=512, ahead=4):
    heads, width, span_len = turned.shape
    kv, own = shard.shape
    lat = key_weight.shape[0]
    rows = flat_queries.shape[0]
    owned = cache.shape[0]
    block = rows // (ranks * owned)
    look = min(-(-(span_len // 2) // qb), span_len // qb - 1)
    marks = 128 - (kv - lat)
    deep = (look + 1) * qb
    asks = ranks * block
    bf16, f32 = jnp.bfloat16, jnp.float32
    vmem, dma = pltpu.VMEM, pltpu.SemaphoreType.DMA
    return pl.pallas_call(
        functools.partial(
            serve_kernel,
            lat=lat,
            ranks=ranks,
            heads=heads,
            look=look,
            scale=math.log2(math.e) / math.sqrt(width),
            pair=pair,
            before=before,
            blk=blk,
        ),
        out_shape=(
            jax.ShapeDtypeStruct((ranks, owned, block, lat), bf16),
            jax.ShapeDtypeStruct((span_len, heads * 128), bf16),
        ),
        in_specs=[HBM_SPEC] * 10,
        out_specs=(VMEM_SPEC,) * 2,
        scratch_shapes=[
            vmem((2 * ranks, kv, own), bf16),
            vmem((ranks, owned, block, kv), bf16),
            vmem((span_len, 128), bf16),
            vmem((marks, span_len), bf16),
            vmem((qb // 2, qb // 2), f32),
            vmem(key_weight.shape, bf16),
            vmem(value_weight.shape, bf16),
            vmem((heads, width, span_len), bf16),
            vmem((rows, width), bf16),
            vmem((rows, 128), f32),
            vmem((lat // 128, rows, 128), f32),
            vmem((ranks, owned, block, kv), bf16),
            vmem((heads, span_len, 128), bf16),
            vmem((heads, 144, span_len), bf16),
            [[vmem((deep, qb), f32)] * ahead, [vmem((deep, qb), bf16)] * ahead],
            vmem(cache.shape, bf16),
            vmem((ranks, owned, block, lat), bf16),
            [
                vmem((asks, 128), f32),
                vmem((asks, 128), f32),
                vmem((asks, lat), f32),
                vmem((asks, -(-(kv + 16) // 128) * 128), bf16),
                [vmem((asks, blk), f32)] * 2,
                [vmem((asks, 128), f32)] * 2,
                [vmem((asks, blk), bf16)] * 2,
                [vmem((asks, 128), f32)] * 2,
            ],
            pltpu.SMEM(lens.shape, lens.dtype),
            pltpu.SMEM(owner.shape, owner.dtype),
            pltpu.SMEM(ctx.shape, ctx.dtype),
            vmem(newest.shape, newest.dtype),
            dma((7,)),
            dma((owned,)),
            dma((4,)),
            dma((2, 4, ranks // 2)),
            dma((2, 4, ranks // 2)),
            dma((2,)),
            dma((owned, ranks - 1)),
            dma((owned, ranks - 1)),
            dma((owned, ranks - 1)),
            dma((owned, ranks - 1)),
        ],
        compiler_params=pltpu.CompilerParams(
            collective_id=0, has_side_effects=True, vmem_limit_bytes=46 << 20
        ),
        cost_estimate=pl.CostEstimate(
            flops=30 * 10**9, bytes_accessed=24 << 20, transcendentals=14 << 20
        ),
    )(lens, owner, ctx, newest, shard, flat_queries, key_weight, value_weight, turned, cache)


def project_kernel(back_ref, vw_ref, part_ref, out_ref, whole_ref, wide, sems, *, heads, lat):
    ranks, owned, block, _ = back_ref.shape
    steps = block // heads
    local = ranks * owned
    shown = pltpu.make_async_copy(part_ref, whole_ref, sems.at[0])
    shown.start()
    for p in range(ranks):
        for r in range(owned):
            at = (p * owned + r) * block
            for c in range(lat // 128):
                wide[c, at : at + block] = back_ref[p, r, :, c * 128 : (c + 1) * 128].astype(
                    jnp.float32
                )

    def some_heads(g, carry):
        for p in range(4):
            h = g * 4 + p
            mine = jnp.concatenate(
                [
                    jnp.concatenate(
                        [
                            wide[c, pl.ds(s * heads + h, local, stride=block), :]
                            for c in range(lat // 128)
                        ],
                        axis=1,
                    )
                    for s in range(steps)
                ],
                axis=0,
            ).astype(jnp.bfloat16)
            columns = pl.ds(pl.multiple_of(h * 128, 128), 128)
            out_ref[:, columns] = jnp.dot(
                mine, vw_ref[:, columns], preferred_element_type=jnp.float32
            ).astype(jnp.bfloat16)
        return carry

    lax.fori_loop(0, heads // 4, some_heads, 0)
    shown.wait()


def project_pallas(back, value_weight, part, heads):
    ranks, owned, block, lat = back.shape
    rows = ranks * owned * block
    return pl.pallas_call(
        functools.partial(project_kernel, heads=heads, lat=lat),
        out_shape=(
            jax.ShapeDtypeStruct((rows // heads, heads * 128), jnp.bfloat16),
            jax.ShapeDtypeStruct(part.shape, part.dtype),
        ),
        in_specs=[VMEM_SPEC, VMEM_SPEC, VMEM_SPEC],
        out_specs=(VMEM_SPEC, HBM_SPEC),
        scratch_shapes=[
            pltpu.VMEM((lat // 128, rows, 128), jnp.float32),
            pltpu.SemaphoreType.DMA((1,)),
        ],
        compiler_params=pltpu.CompilerParams(vmem_limit_bytes=8 << 20),
    )(back, value_weight, part)


def on_device(
    latent_rows,
    pre_queries,
    pre_lengths,
    owner_map,
    context_cache,
    context_lengths,
    new_latent,
    dec_queries,
    key_weight,
    value_weight,
):
    steps, rows_local, heads, width = dec_queries.shape
    ranks = lax.axis_size("head")
    if heads % 16 or latent_rows.shape[0] % 128 or ranks % 2:
        return plain_on_device(
            latent_rows,
            pre_queries,
            pre_lengths,
            owner_map,
            context_cache,
            context_lengths,
            new_latent,
            dec_queries,
            key_weight,
            value_weight,
        )
    stay = lambda x: pltpu.with_memory_space_constraint(x, pltpu.HBM)
    back, part = serve_pallas(
        stay(pre_lengths),
        stay(owner_map),
        stay(context_lengths),
        stay(new_latent),
        stay(jnp.transpose(latent_rows)),
        stay(dec_queries.reshape(-1, width)),
        stay(key_weight),
        stay(value_weight),
        stay(jnp.transpose(pre_queries, (1, 2, 0))),
        stay(jnp.transpose(context_cache, (0, 2, 1))),
        ranks,
    )
    decode_out, prefill_out = project_pallas(back, value_weight, part, heads)
    return (prefill_out, decode_out.reshape(steps, rows_local, heads * 128))


def solution(mesh):
    placed = (
        P(("groups", "batch", "head"), None),
        P(("groups", "batch"), "head", None),
        P("groups", None),
        P("groups", None),
        P(("groups", "batch", "head"), None, None),
        P(("groups", "batch", "head")),
        P("groups", ("batch", "head"), None),
        P("groups", "batch", "head", None),
        P(None, "head"),
        P(None, "head"),
    )
    return jax.shard_map(
        on_device,
        mesh=mesh,
        in_specs=placed,
        out_specs=(P(("groups", "batch"), "head"), P("groups", "batch", "head")),
        check_vma=False,
    )
```

```python
import functools
import math

import jax
import jax.numpy as jnp
from jax import lax
from jax.experimental import pallas as pl
from jax.experimental.pallas import tpu as pltpu
from jax.sharding import PartitionSpec as P

BLK = 512


NEGATIVE = -1e30


def from_partner(value, axis, distance):
    mask = 2**distance
    pairs = [(source, source ^ mask) for source in range(lax.axis_size(axis))]
    return lax.ppermute(value, axis, pairs)


def request_table(pre_lengths, owner_map, span_len):
    seg_ends = jnp.cumsum(pre_lengths, axis=1)
    span_base = jnp.arange(pre_lengths.shape[0], dtype=jnp.int32)[:, None] * span_len
    seg_starts = seg_ends - pre_lengths + span_base
    return (owner_map.reshape(-1), seg_starts.reshape(-1), pre_lengths.reshape(-1))


def prefill_heads(own_span, queries, span_lengths, key_weight, value_weight):
    span_len, head_count, query_width = queries.shape
    head_size = key_weight.shape[1] // head_count
    lat_width = key_weight.shape[0]
    score_scale = 1.0 / math.sqrt(query_width)
    latent = own_span[:, :lat_width]
    rope_keys = own_span[:, lat_width:]
    keys_nope = (
        jnp.dot(latent, key_weight, preferred_element_type=jnp.float32)
        .astype(jnp.bfloat16)
        .reshape(span_len, head_count, head_size)
    )
    values = (
        jnp.dot(latent, value_weight, preferred_element_type=jnp.float32)
        .astype(jnp.bfloat16)
        .reshape(span_len, head_count, head_size)
    )
    scores = jnp.einsum(
        "qhd,khd->hqk", queries[:, :, :head_size], keys_nope, preferred_element_type=jnp.float32
    )
    scores = scores + jnp.einsum(
        "qhr,kr->hqk", queries[:, :, head_size:], rope_keys, preferred_element_type=jnp.float32
    )
    scores = scores * score_scale
    seg_ends = jnp.cumsum(span_lengths)
    places = jnp.arange(span_len, dtype=jnp.int32)
    segment = jnp.sum((places[:, None] >= seg_ends[None, :]).astype(jnp.int32), axis=1)
    allowed = (segment[:, None] == segment[None, :]) & (places[None, :] <= places[:, None])
    masked = jnp.where(allowed[None], scores, NEGATIVE)
    peak_score = jnp.max(masked, axis=2, keepdims=True)
    weights = jnp.exp(masked - peak_score)
    weight_sum = jnp.sum(weights, axis=2)
    mixed_out = jnp.einsum(
        "hqk,khd->qhd", weights.astype(jnp.bfloat16), values, preferred_element_type=jnp.float32
    )
    mixed_out = mixed_out / jnp.transpose(weight_sum)[:, :, None]
    return mixed_out.astype(jnp.bfloat16).reshape(span_len, head_count * head_size)


def plain_on_device(
    latent_rows,
    pre_queries,
    pre_lengths,
    owner_map,
    context_cache,
    context_lengths,
    new_latent,
    dec_queries,
    key_weight,
    value_weight,
):
    head_rank = lax.axis_index("head")
    batch_rank = lax.axis_index("batch")
    span_len = pre_queries.shape[0]
    kv_width = latent_rows.shape[1]
    own_span = lax.all_gather(latent_rows, "head", axis=0, tiled=True)
    other_span = from_partner(own_span, "batch", 0)
    first_span = jnp.where(batch_rank == 0, own_span, other_span)
    second_span = jnp.where(batch_rank == 0, other_span, own_span)
    all_spans = jnp.concatenate([first_span, second_span], axis=0)
    span_lengths = lax.dynamic_index_in_dim(pre_lengths, batch_rank, 0, keepdims=False)
    prefill_out = prefill_heads(own_span, pre_queries, span_lengths, key_weight, value_weight)
    step_total, rows_local, head_count, query_width = dec_queries.shape
    lat_width = key_weight.shape[0]
    head_size = key_weight.shape[1] // head_count
    owned_rows = context_cache.shape[0]
    score_scale = 1.0 / math.sqrt(query_width)
    key_heads = key_weight.reshape(lat_width, head_count, head_size)
    value_heads = value_weight.reshape(lat_width, head_count, head_size)
    absorbed = jnp.einsum(
        "srhd,lhd->srhl",
        dec_queries[..., :head_size],
        key_heads,
        preferred_element_type=jnp.float32,
    ).astype(jnp.bfloat16)
    query_all = jnp.concatenate([absorbed, dec_queries[..., head_size:]], axis=3)
    flat_owner, flat_start, flat_length = request_table(pre_lengths, owner_map, span_len)
    row_ids = (
        batch_rank * rows_local + head_rank * owned_rows + jnp.arange(owned_rows, dtype=jnp.int32)
    )
    matches = (flat_owner[None, :] == row_ids[:, None]).astype(jnp.int32)
    is_target = jnp.sum(matches, axis=1) > 0
    first_row = jnp.sum(matches * flat_start[None, :], axis=1)
    prompt_len = jnp.sum(matches * flat_length[None, :], axis=1)
    effective = jnp.where(is_target, prompt_len, context_lengths)
    padded = jnp.concatenate([all_spans, jnp.zeros((span_len, kv_width), all_spans.dtype)], axis=0)
    replaced = jax.vmap(lambda offset: lax.dynamic_slice_in_dim(padded, offset, span_len, 0))(
        first_row
    )
    front_rows = jnp.where(is_target[:, None, None], replaced, context_cache[:, :span_len])
    front_blocks = span_len // BLK
    needed = (jnp.max(effective) + BLK - 1) // BLK
    fresh_latent = new_latent[..., :lat_width]
    owned_query = lax.all_to_all(query_all, "head", split_axis=1, concat_axis=2, tiled=True)
    fresh_scores = (
        jnp.einsum("srhk,jrk->srhj", owned_query, new_latent, preferred_element_type=jnp.float32)
        * score_scale
    )
    visible = (
        jnp.arange(new_latent.shape[0], dtype=jnp.int32)[None, :]
        <= jnp.arange(step_total, dtype=jnp.int32)[:, None]
    )
    fresh_scores = jnp.where(visible[:, None, None, :], fresh_scores, NEGATIVE)
    peak_score = jnp.max(fresh_scores, axis=3)
    weights = jnp.exp(fresh_scores - peak_score[..., None])
    weight_sum = jnp.sum(weights, axis=3)
    running = jnp.einsum(
        "srhj,jrl->srhl",
        weights.astype(jnp.bfloat16),
        fresh_latent,
        preferred_element_type=jnp.float32,
    )

    def advance(block_index, state_tuple, source):
        old_peak, old_sum, old_running = state_tuple
        key_block = lax.dynamic_slice_in_dim(source, block_index * BLK, BLK, 1)
        scores = (
            jnp.einsum("srhk,rtk->srht", owned_query, key_block, preferred_element_type=jnp.float32)
            * score_scale
        )
        places = block_index * BLK + jnp.arange(BLK, dtype=jnp.int32)
        in_context = places[None, :] < effective[:, None]
        scores = jnp.where(in_context[None, :, None, :], scores, NEGATIVE)
        new_peak = jnp.maximum(old_peak, jnp.max(scores, axis=3))
        factor = jnp.exp(old_peak - new_peak)
        block_weights = jnp.exp(scores - new_peak[..., None])
        new_sum = old_sum * factor + jnp.sum(block_weights, axis=3)
        new_running = old_running * factor[..., None] + jnp.einsum(
            "srht,rtl->srhl",
            block_weights.astype(jnp.bfloat16),
            key_block[..., :lat_width],
            preferred_element_type=jnp.float32,
        )
        return (new_peak, new_sum, new_running)

    state_tuple = lax.fori_loop(
        0,
        jnp.minimum(needed, front_blocks),
        lambda block_index, state_now: advance(block_index, state_now, front_rows),
        (peak_score, weight_sum, running),
    )
    state_tuple = lax.fori_loop(
        front_blocks,
        jnp.maximum(needed, front_blocks),
        lambda block_index, state_now: advance(block_index, state_now, context_cache),
        state_tuple,
    )
    latent_out = (state_tuple[2] / state_tuple[1][..., None]).astype(jnp.bfloat16)
    returned = lax.all_to_all(latent_out, "head", split_axis=2, concat_axis=1, tiled=True)
    projected = jnp.einsum(
        "srhl,lhd->srhd", returned, value_heads, preferred_element_type=jnp.float32
    ).astype(jnp.bfloat16)
    decode_out = projected.reshape(query_all.shape[0], rows_local, head_count * head_size)
    return (prefill_out, decode_out)


def trans_dot(left, right):
    return lax.dot_general(
        left, right, (((1,), (1,)), ((), ())), preferred_element_type=jnp.float32
    )


MESH = pl.DeviceIdType.MESH


def place_of(rank, ranks):
    odd = rank % 2
    return (1 - odd) * (rank // 2) + odd * (ranks - 1 - rank // 2)


def rank_at(place, ranks):
    late = place // (ranks // 2)
    return (1 - late) * (2 * place) + late * (2 * (ranks - 1 - place) + 1)


def start_marks(ends, tail, vals, hot, tri):
    span_len, full = tail.shape
    marks = hot.shape[0]
    segs = len(ends)
    where = lax.broadcasted_iota(jnp.int32, (span_len, marks), 0)
    lane = lax.broadcasted_iota(jnp.int32, (span_len, marks), 1)
    place = lax.broadcasted_iota(jnp.int32, (marks, span_len), 1)
    line = lax.broadcasted_iota(jnp.int32, (marks, span_len), 0)
    mine = jnp.zeros((span_len, marks), jnp.int32)
    seen = jnp.zeros((marks, span_len), jnp.int32)
    for k in range(segs - 1):
        mine = mine + (where >= ends[k]).astype(jnp.int32)
        seen = seen + (place >= ends[k]).astype(jnp.int32)
    mark = jnp.where((lane < segs) & (lane != mine), NEGATIVE, 0.0).astype(jnp.bfloat16)
    hot[...] = jnp.where(line == seen, 1.0, 0.0).astype(jnp.bfloat16)
    tail[:, full - marks :] = mark
    for h in range(vals.shape[0]):
        vals[h, 128:, :] = jnp.ones((vals.shape[1] - 128, span_len), jnp.bfloat16)
    size = tri.shape[0]
    key_at = lax.broadcasted_iota(jnp.int32, (size, size), 0)
    query_at = lax.broadcasted_iota(jnp.int32, (size, size), 1)
    tri[...] = jnp.where(key_at <= query_at, 0.0, NEGATIVE)


def project_shard(origin, spans_ref, kw, vw, keys, vals, tail, lat, heads):
    own = spans_ref.shape[2]
    rows = jnp.transpose(spans_ref[origin])
    at = pl.ds(pl.multiple_of(origin * own, own), own)
    tail[at, : rows.shape[1] - lat] = rows[:, lat:]
    latent = rows[:, :lat]
    pair = 2
    for g in range(heads // pair):
        columns = slice(g * pair * 128, (g + 1) * pair * 128)
        key = jnp.dot(latent, kw[:, columns], preferred_element_type=jnp.float32)
        value = jnp.dot(latent, vw[:, columns], preferred_element_type=jnp.float32)
        key = key.astype(jnp.bfloat16)
        value = jnp.transpose(value.astype(jnp.bfloat16))
        for p in range(pair):
            h = g * pair + p
            keys[h, at, :] = key[:, p * 128 : (p + 1) * 128]
            vals[h, :128, at] = value[p * 128 : (p + 1) * 128]


def attention(g, pair, qs, keys, tail, vals, hot, tri, part_ref, scores, weights, look, scale):
    span_len = tail.shape[0]
    qb = 2 * tri.shape[0]
    blocks = span_len // qb
    order = [(0, p) for p in range(pair // 2)]
    order += [(i, p) for i in range(1, blocks) for p in range(pair)]
    order += [(0, p) for p in range(pair // 2, pair)]
    count = len(order)
    lengths = [min(i, look) + 1 for i, _ in order]
    half = qb // 2
    skips = [half if length == look + 1 else 0 for length in lengths]
    peaks = [None] * count
    tops = [None] * count
    sums = [None] * count

    def score(n, c):
        i, p = order[n]
        if c > 0:
            return
        at = (i - lengths[n] + 1) * qb
        size = lengths[n] * qb
        query = jnp.concatenate(
            [qs[g * pair + p, :, i * qb : (i + 1) * qb], hot[:, i * qb : (i + 1) * qb]], axis=0
        )
        key = jnp.concatenate(
            [keys[g * pair + p, at : at + size, :], tail[at : at + size, :]], axis=1
        )
        s = jnp.dot(key, query, preferred_element_type=jnp.float32)
        left = [s[: size - qb, :half], s[size - qb : size - half, :half] + tri[...]]
        right = [s[skips[n] : size - half, half:], s[size - half :, half:] + tri[...]]
        row = 0
        for piece in left:
            if piece.shape[0]:
                scores[n % 4][row : row + piece.shape[0], :half] = piece
                row += piece.shape[0]
        row = skips[n]
        for piece in right:
            scores[n % 4][row : row + piece.shape[0], half:] = piece
            row += piece.shape[0]
        both = []
        for side in (left, right):
            best = None
            for piece in side:
                if piece.shape[0]:
                    top = jnp.max(piece.reshape(piece.shape[0] // 8, 8, half), axis=0)
                    best = top if best is None else jnp.maximum(best, top)
            both.append(best)
        peaks[n] = both

    def soften(n, c):
        if c == 0:
            tops[n] = [jnp.max(peak, axis=0, keepdims=True) for peak in peaks[n]]
        size = lengths[n] * qb
        for side in range(2):
            low, high = (0, size - half) if side == 0 else (skips[n], size)
            lanes = slice(side * half, (side + 1) * half)
            for k in range(c * qb, (c + 1) * qb, 64):
                at = slice(k, k + 64)
                if low <= k < high:
                    w = jnp.exp2((scores[n % 4][at, lanes] - tops[n][side]) * scale)
                    weights[n % 4][at, lanes] = w.astype(jnp.bfloat16)
                else:
                    weights[n % 4][at, lanes] = jnp.zeros((64, half), jnp.bfloat16)

    def mix(n, c):
        i, p = order[n]
        at = (i - lengths[n] + 1) * qb
        if c == 0:
            o = jnp.dot(
                vals[g * pair + p, :, at : at + lengths[n] * qb],
                weights[n % 4][: lengths[n] * qb, :],
                preferred_element_type=jnp.float32,
            )
            o = o[:128] * (1.0 / o[128:129])
            columns = pl.ds(pl.multiple_of((g * pair + p) * 128, 128), 128)
            part_ref[i * qb : (i + 1) * qb, columns] = jnp.transpose(o.astype(jnp.bfloat16))

    todo_score = [(n, c) for n in range(count) for c in range(lengths[n])]
    todo_soft = list(todo_score)
    todo_mix = list(todo_score)
    scored = [0] * count
    softened = [0] * count
    mixed = [0] * count
    while todo_mix:
        was = list(softened)
        if todo_score:
            n, c = todo_score[0]
            if n < 4 or softened[n - 4] == lengths[n - 4]:
                score(n, c)
                scored[n] += 1
                todo_score.pop(0)
        if todo_soft:
            n, c = todo_soft[0]
            free = n < 4 or mixed[n - 4] == lengths[n - 4]
            if scored[n] == lengths[n] and free and not (todo_score and todo_score[0][0] <= n + 2):
                soften(n, c)
                softened[n] += 1
                todo_soft.pop(0)
        n, c = todo_mix[0]
        if was[n] == lengths[n]:
            mix(n, c)
            mixed[n] += 1
            todo_mix.pop(0)


def attend_groups(low, high, pair, qs, keys, tail, vals, hot, tri, part_ref, buffers, look, scale):
    scores, weights = buffers

    def step(g, carry):
        attention(
            g, pair, qs, keys, tail, vals, hot, tri, part_ref, scores, weights, look, scale
        )
        return carry

    lax.fori_loop(low, high, step, 0)


def absorb_into(dq, kw, sent, flat, wide, heads, lat):
    rows = dq.shape[0]
    ranks, owned, block, _ = sent.shape
    steps = block // heads
    local = ranks * owned
    flat[...] = dq[:, :128].astype(jnp.float32)
    for h in range(heads):
        mine = flat[pl.ds(h, rows // heads, stride=heads), :].astype(jnp.bfloat16)
        res = trans_dot(mine, kw[:, h * 128 : (h + 1) * 128])
        for s in range(steps):
            for c in range(lat // 128):
                wide[c, pl.ds(s * heads + h, local, stride=block), :] = res[
                    s * local : (s + 1) * local, c * 128 : (c + 1) * 128
                ]
    for p in range(ranks):
        for r in range(owned):
            at = p * owned + r
            for c in range(lat // 128):
                sent[p, r, :, c * 128 : (c + 1) * 128] = wide[
                    c, at * block : (at + 1) * block
                ].astype(jnp.bfloat16)
            for s in range(steps):
                start = (s * local + at) * heads
                sent[p, r, s * heads : (s + 1) * heads, lat:] = dq[start : start + heads, 128:]


def span_ends(lens_ref, batch_rank):
    ends = []
    total = 0
    for k in range(lens_ref.shape[1]):
        total = total + lens_ref[batch_rank, k]
        ends.append(total)
    return ends


def request_facts(lens_ref, owner_ref, ctx_ref, r, row, batch_rank, span_len):
    target = jnp.int32(0)
    first = jnp.int32(0)
    length = jnp.int32(0)
    spans = lens_ref.shape[0]
    for c in range(spans):
        start = jnp.int32(((c + spans) % spans) * span_len)
        for k in range(lens_ref.shape[1]):
            hit = (owner_ref[c, k] == row).astype(jnp.int32)
            target = target + hit
            first = first + hit * start
            length = length + hit * lens_ref[c, k]
            start = start + lens_ref[c, k]
    first = ((first + batch_rank * span_len) % (2 * span_len)) * target
    return first, length, ctx_ref[r] * (1 - target)


def decode_request(r, facts, got, new_ref, spans_ref, cache, lo, tools, *, lat, heads, steps, scale, blk):
    peak_ref, sum_ref, acc_ref, asked, scores, tops, weights, fades = tools
    ranks, _, block, kv = got.shape
    rows = ranks * block
    first, length, held = facts
    own = spans_ref.shape[2]
    full = asked.shape[1]
    piece = 256
    blocks = cache.shape[2] // blk
    spread = (full - kv) // 16
    tail = lax.broadcasted_iota(jnp.int32, (rows, full - kv), 1)
    columns = lax.broadcasted_iota(jnp.int32, (16, piece), 1)

    line = lax.broadcasted_iota(jnp.int32, (16, piece), 0)

    def hidden(keep):
        mask = jnp.where((line == 0) & jnp.logical_not(keep), NEGATIVE, 0.0)
        return [mask.astype(jnp.bfloat16)] * spread

    def begin():
        asked[:, :kv] = got[:, r].reshape(rows, kv)
        row_step = (lax.broadcasted_iota(jnp.int32, tail.shape, 0) // heads) % steps
        asked[:, kv:] = jnp.where((tail == 0) | (tail == row_step + 1), 1.0, 0.0).astype(
            jnp.bfloat16
        )
        newest = new_ref[...].astype(jnp.float32)
        fresh = jnp.concatenate(
            [newest[s, r : r + 1] for s in range(steps)]
            + [jnp.zeros((own - steps, kv), jnp.float32)],
            axis=0,
        ).astype(jnp.bfloat16)
        fresh = jnp.transpose(fresh)
        span_len = spans_ref.shape[0] * own // 2
        shards = -(-(span_len // 2 + own - 1) // own)
        base = jnp.minimum(first // own, spans_ref.shape[0] - shards)
        each = piece // own
        most = (shards + 1) // each

        def block(c):
            parts = []
            for i in range(c * each, (c + 1) * each):
                parts.append(spans_ref[base + i] if i < shards else fresh)
            return jnp.concatenate(parts, axis=1)

        top = None
        for c in range(most):
            place = (base + c * each) * own + columns
            keep = (place >= first) & (place < first + length)
            mask = jnp.where((line == 0) & jnp.logical_not(keep), NEGATIVE, 0.0)
            if c == most - 1:
                new_at = columns - (piece - own)
                late = (line == 0) & (new_at >= steps)
                late = late | ((line > 0) & (new_at > line - 1))
                mask = jnp.where(new_at >= 0, jnp.where(late, NEGATIVE, 0.0), mask)
            keys = jnp.concatenate([block(c)] + [mask.astype(jnp.bfloat16)] * spread, axis=0)
            part = jnp.dot(asked[...], keys, preferred_element_type=jnp.float32)
            scores[c // 2][:, (c % 2) * piece : (c % 2 + 1) * piece] = part
            best = jnp.maximum(part[:, :128], part[:, 128:])
            top = best if top is None else jnp.maximum(top, best)
        m = jnp.max(top, axis=1, keepdims=True)
        peak_ref[...] = jnp.broadcast_to(m, peak_ref.shape)
        total, acc = None, None
        for c in range(most):
            w = jnp.exp2((scores[c // 2][:, (c % 2) * piece : (c % 2 + 1) * piece] - m) * scale)
            both = w[:, :128] + w[:, 128:]
            made = trans_dot(w.astype(jnp.bfloat16), block(c)[:lat])
            total = both if total is None else total + both
            acc = made if acc is None else acc + made
        sum_ref[...] = total
        acc_ref[...] = acc
        weights[1][...] = jnp.zeros(weights[1].shape, jnp.bfloat16)
        fades[1][...] = jnp.ones(fades[1].shape, jnp.float32)

    def score(t, side, c):
        at = pl.multiple_of(t * blk + c * piece, piece)
        keys = jnp.concatenate(
            [cache[r, :, pl.ds(at, piece)]] + hidden(at + columns < held), axis=0
        )
        s = jnp.dot(asked[...], keys, preferred_element_type=jnp.float32)
        scores[side][:, c * piece : (c + 1) * piece] = s
        top = jnp.maximum(s[:, :128], s[:, 128:])
        if c > 0:
            top = jnp.maximum(top, tops[side][...])
        tops[side][...] = top

    def settle(side):
        old = peak_ref[...]
        new = jnp.maximum(old, jnp.max(tops[side][...], axis=1, keepdims=True))
        fade = jnp.exp2((old - new) * scale)
        fades[side][...] = fade
        peak_ref[...] = new
        sum_ref[...] = sum_ref[...] * fade

    def soften(side, c):
        at = slice(c * piece, (c + 1) * piece)
        new = peak_ref[...]
        s = scores[side][:, at]
        left = jnp.exp2((s[:, :128] - new) * scale)
        right = jnp.exp2((s[:, 128:] - new) * scale)
        sum_ref[...] = sum_ref[...] + (left + right)
        weights[side][:, at] = jnp.concatenate([left, right], axis=1).astype(jnp.bfloat16)

    def mix(t, side, c):
        at = pl.multiple_of(jnp.maximum(t, 0) * blk, blk)
        some = slice(c * piece, (c + 1) * piece)
        made = trans_dot(weights[side][...], cache[r, some, pl.ds(at, blk)])
        fade = fades[side][...]
        for k in range(piece // 128):
            here = slice(c * piece + k * 128, c * piece + (k + 1) * 128)
            acc_ref[:, here] = acc_ref[:, here] * fade + made[:, k * 128 : (k + 1) * 128]

    def turn(j, carry):
        for side in range(2):
            t = 2 * j + side
            settle(side)
            for c in range(blk // piece):
                if not (isinstance(t, int) and t + 1 == blocks):
                    score(t + 1, 1 - side, c)
                soften(side, c)
                mix(t - 1, 1 - side, c)
        return carry

    begin()
    for c in range(blk // piece):
        score(0, 0, c)
    lax.fori_loop(0, blocks // 2 - 1, turn, 0)
    turn(blocks // 2 - 1, 0)
    for c in range(lat // piece):
        mix(blocks - 1, 1, c)
    total = jnp.sum(sum_ref[...], axis=1, keepdims=True)
    done = (acc_ref[...] * (1.0 / total)).astype(lo.dtype)
    for p in range(ranks):
        lo[p, r] = done[p * block : (p + 1) * block]


def serve_kernel(
    lens_hbm, owner_hbm, ctx_hbm, new_hbm, shard_hbm, dq_hbm, kw_hbm, vw_hbm, q_hbm, cache_hbm,
    back, part_ref,
    spans_ref, got, tail, hot, tri, kw, vw, qs, dq, flat, wide, sent, keys, vals, buffers, cache,
    lo, tools, lens_ref, owner_ref, ctx_ref, new_ref,
    load_sems, cache_sems, small_sems, ring_send, ring_recv, swap_sems,
    give_sems, take_sems, back_send, back_recv,
    *, lat, ranks, heads, look, scale, pair, before, blk
):
    me = lax.axis_index("head")
    batch_rank = lax.axis_index("batch")
    place = place_of(me, ranks)
    right = rank_at((place + 1) % ranks, ranks)
    left = rank_at((place + ranks - 1) % ranks, ranks)
    owned = cache.shape[0]
    span_len = tail.shape[0]
    steps = sent.shape[2] // heads
    loads = [
        pltpu.make_async_copy(shard_hbm, spans_ref.at[me], load_sems.at[0]),
        pltpu.make_async_copy(dq_hbm, dq, load_sems.at[1]),
        pltpu.make_async_copy(kw_hbm, kw, load_sems.at[2]),
        pltpu.make_async_copy(vw_hbm, vw, load_sems.at[3]),
        pltpu.make_async_copy(q_hbm, qs, load_sems.at[4]),
    ] + [
        pltpu.make_async_copy(cache_hbm.at[r], cache.at[r], cache_sems.at[r])
        for r in range(owned)
    ]
    barrier = pltpu.get_barrier_semaphore()
    for k in range(1, ranks):
        pl.semaphore_signal(
            barrier, inc=1, device_id={"head": (me + k) % ranks}, device_id_type=MESH
        )
    pl.semaphore_signal(
        barrier, inc=1, device_id={"batch": 1 - batch_rank}, device_id_type=MESH
    )
    smalls = [
        pltpu.make_async_copy(lens_hbm, lens_ref, small_sems.at[0]),
        pltpu.make_async_copy(owner_hbm, owner_ref, small_sems.at[1]),
        pltpu.make_async_copy(ctx_hbm, ctx_ref, small_sems.at[2]),
        pltpu.make_async_copy(new_hbm, new_ref, small_sems.at[3]),
    ]
    for load in smalls + loads:
        load.start()
    pl.semaphore_wait(barrier, ranks)

    quarter = shard_hbm.shape[0] // 4
    most = ranks // 2

    def hop(way, part, t):
        back_by = t - 1 if way == 0 else ranks - t + 1
        origin = rank_at((place + ranks - back_by) % ranks, ranks)
        rows = pl.ds(part * quarter, quarter)
        begins = isinstance(t, int) and t == 1
        return pltpu.make_async_remote_copy(
            src_ref=shard_hbm.at[rows] if begins else spans_ref.at[origin, rows],
            dst_ref=spans_ref.at[origin, rows],
            send_sem=ring_send.at[way, part, t - 1],
            recv_sem=ring_recv.at[way, part, t - 1],
            device_id={"head": right if way == 0 else left},
            device_id_type=MESH,
        )

    def hops(way, part):
        return most if way == part // 2 else most - 1

    streams = [(0, 0), (1, 2), (0, 1), (1, 3), (0, 2), (1, 0), (0, 3), (1, 1)]
    for way, part in streams:
        hop(way, part, 1).start()
    for small in smalls:
        small.wait()
    start_marks(span_ends(lens_ref, batch_rank), tail, vals, hot, tri)
    loads[0].wait()
    loads[1].wait()
    loads[2].wait()
    absorb_into(dq, kw, sent, flat, wide, heads, lat)
    loads[3].wait()

    def exchange(source, target, r, send_sems, recv_sems):
        return [
            pltpu.make_async_remote_copy(
                src_ref=source.at[(me + k) % ranks, r],
                dst_ref=target.at[me, r],
                send_sem=send_sems.at[r, k - 1],
                recv_sem=recv_sems.at[r, k - 1],
                device_id={"head": (me + k) % ranks},
                device_id_type=MESH,
            )
            for k in sorted(range(1, ranks), key=lambda k: abs(k - ranks // 2))
        ]

    gives = [exchange(sent, got, r, give_sems, take_sems) for r in range(owned)]
    backs = [exchange(lo, back, r, back_send, back_recv) for r in range(owned)]
    def project(origin):
        project_shard(origin, spans_ref, kw, vw, keys, vals, tail, lat, heads)

    def arrive(t, carry):
        for way, part in streams:
            if hops(way, part) == most:
                hop(way, part, t).wait_recv()
                pl.when(t < most)(lambda: hop(way, part, t + 1).start())
            else:

                @pl.when(t < most)
                def _():
                    hop(way, part, t).wait_recv()
                    pl.when(t < most - 1)(lambda: hop(way, part, t + 1).start())

        @pl.when(t == most - 1)
        def _():
            for copies in gives:
                for copy in copies:
                    copy.start()

        def one(side, carry):
            project(rank_at((place + side * t + (1 - side) * (ranks - t)) % ranks, ranks))
            return carry

        lax.fori_loop(0, 2 - t // most, one, 0)
        return carry

    project(me)
    lax.fori_loop(1, most + 1, arrive, 0)

    swap = pltpu.make_async_remote_copy(
        src_ref=spans_ref.at[:ranks],
        dst_ref=spans_ref.at[ranks:],
        send_sem=swap_sems.at[0],
        recv_sem=swap_sems.at[1],
        device_id={"batch": 1 - batch_rank},
        device_id_type=MESH,
    )
    swap.start()
    keep = pltpu.make_async_copy(sent.at[me], got.at[me], load_sems.at[5])
    keep.start()
    loads[4].wait()

    def attend(low, high):
        attend_groups(
            low, high, pair, qs, keys, tail, vals, hot, tri, part_ref, buffers, look, scale
        )

    groups = heads // pair
    attend(0, before)
    keep.wait()
    swap.wait()
    for r in range(owned):
        for copy in gives[r]:
            copy.wait()
        loads[5 + r].wait()
        row = batch_rank * (ranks * owned) + me * owned + r
        facts = request_facts(lens_ref, owner_ref, ctx_ref, r, row, batch_rank, span_len)
        decode_request(
            r, facts, got, new_ref, spans_ref, cache, lo, tools,
            lat=lat, heads=heads, steps=steps, scale=scale, blk=blk,
        )
        for copy in backs[r]:
            copy.start()
    stay = pltpu.make_async_copy(lo.at[me], back.at[me], load_sems.at[6])
    stay.start()
    attend(before, groups)
    for way, part in streams:
        for t in range(1, hops(way, part) + 1):
            hop(way, part, t).wait_send()
    for copies in backs:
        for copy in copies:
            copy.wait()
    stay.wait()


HBM_SPEC = pl.BlockSpec(memory_space=pltpu.HBM)
VMEM_SPEC = pl.BlockSpec(memory_space=pltpu.VMEM)
SMEM_SPEC = pl.BlockSpec(memory_space=pltpu.SMEM)


def serve_pallas(lens, owner, ctx, newest, shard, flat_queries, key_weight, value_weight, turned, cache, ranks, qb=256, pair=4, before=2, blk=512, ahead=4):
    heads, width, span_len = turned.shape
    kv, own = shard.shape
    lat = key_weight.shape[0]
    rows = flat_queries.shape[0]
    owned = cache.shape[0]
    block = rows // (ranks * owned)
    look = min(-(-(span_len // 2) // qb), span_len // qb - 1)
    marks = 128 - (kv - lat)
    deep = (look + 1) * qb
    asks = ranks * block
    bf16, f32 = jnp.bfloat16, jnp.float32
    vmem, dma = pltpu.VMEM, pltpu.SemaphoreType.DMA
    return pl.pallas_call(
        functools.partial(
            serve_kernel,
            lat=lat,
            ranks=ranks,
            heads=heads,
            look=look,
            scale=math.log2(math.e) / math.sqrt(width),
            pair=pair,
            before=before,
            blk=blk,
        ),
        out_shape=(
            jax.ShapeDtypeStruct((ranks, owned, block, lat), bf16),
            jax.ShapeDtypeStruct((span_len, heads * 128), bf16),
        ),
        in_specs=[HBM_SPEC] * 10,
        out_specs=(VMEM_SPEC,) * 2,
        scratch_shapes=[
            vmem((2 * ranks, kv, own), bf16),
            vmem((ranks, owned, block, kv), bf16),
            vmem((span_len, 128), bf16),
            vmem((marks, span_len), bf16),
            vmem((qb // 2, qb // 2), f32),
            vmem(key_weight.shape, bf16),
            vmem(value_weight.shape, bf16),
            vmem((heads, width, span_len), bf16),
            vmem((rows, width), bf16),
            vmem((rows, 128), f32),
            vmem((lat // 128, rows, 128), f32),
            vmem((ranks, owned, block, kv), bf16),
            vmem((heads, span_len, 128), bf16),
            vmem((heads, 144, span_len), bf16),
            [[vmem((deep, qb), f32)] * ahead, [vmem((deep, qb), bf16)] * ahead],
            vmem(cache.shape, bf16),
            vmem((ranks, owned, block, lat), bf16),
            [
                vmem((asks, 128), f32),
                vmem((asks, 128), f32),
                vmem((asks, lat), f32),
                vmem((asks, -(-(kv + 16) // 128) * 128), bf16),
                [vmem((asks, blk), f32)] * 2,
                [vmem((asks, 128), f32)] * 2,
                [vmem((asks, blk), bf16)] * 2,
                [vmem((asks, 128), f32)] * 2,
            ],
            pltpu.SMEM(lens.shape, lens.dtype),
            pltpu.SMEM(owner.shape, owner.dtype),
            pltpu.SMEM(ctx.shape, ctx.dtype),
            vmem(newest.shape, newest.dtype),
            dma((7,)),
            dma((owned,)),
            dma((4,)),
            dma((2, 4, ranks // 2)),
            dma((2, 4, ranks // 2)),
            dma((2,)),
            dma((owned, ranks - 1)),
            dma((owned, ranks - 1)),
            dma((owned, ranks - 1)),
            dma((owned, ranks - 1)),
        ],
        compiler_params=pltpu.CompilerParams(
            collective_id=0, has_side_effects=True, vmem_limit_bytes=46 << 20
        ),
        cost_estimate=pl.CostEstimate(
            flops=30 * 10**9, bytes_accessed=24 << 20, transcendentals=14 << 20
        ),
    )(lens, owner, ctx, newest, shard, flat_queries, key_weight, value_weight, turned, cache)


def project_kernel(back_ref, vw_ref, part_ref, out_ref, whole_ref, wide, sems, *, heads, lat):
    ranks, owned, block, _ = back_ref.shape
    steps = block // heads
    local = ranks * owned
    cut = part_ref.shape[0] // 4
    shown = [
        pltpu.make_async_copy(
            part_ref.at[pl.ds(k * cut, cut)], whole_ref.at[pl.ds(k * cut, cut)], sems.at[k]
        )
        for k in range(4)
    ]
    for copy in shown:
        copy.start()
    rows = local * block
    kept = steps * local

    def gather(g, carry):
        count = wide.shape[0] // 2
        out = g * count + lax.broadcasted_iota(jnp.int32, (count, 1), 0)
        head, rest = out // kept, out % kept
        wanted = (rest % local) * block + (rest // local) * heads + head
        source = lax.broadcasted_iota(jnp.int32, (count, rows), 1)
        pick = jnp.where(source == wanted, 1.0, 0.0).astype(jnp.bfloat16)
        wide[pl.ds(pl.multiple_of(g * count, count), count), :] = jnp.dot(
            pick, back_ref[...].reshape(rows, lat), preferred_element_type=jnp.float32
        ).astype(jnp.bfloat16)
        return carry

    lax.fori_loop(0, 2, gather, 0)
    for h in range(0, heads, 2):
        made = jnp.dot(
            wide[h * kept : (h + 2) * kept, :],
            vw_ref[:, h * 128 : (h + 2) * 128],
            preferred_element_type=jnp.float32,
        ).astype(jnp.bfloat16)
        out_ref[:, h * 128 : (h + 1) * 128] = made[:kept, :128]
        out_ref[:, (h + 1) * 128 : (h + 2) * 128] = made[kept:, 128:]
    for copy in shown:
        copy.wait()


def project_pallas(back, value_weight, part, heads):
    ranks, owned, block, lat = back.shape
    rows = ranks * owned * block
    return pl.pallas_call(
        functools.partial(project_kernel, heads=heads, lat=lat),
        out_shape=(
            jax.ShapeDtypeStruct((rows // heads, heads * 128), jnp.bfloat16),
            jax.ShapeDtypeStruct(part.shape, part.dtype),
        ),
        in_specs=[VMEM_SPEC, VMEM_SPEC, VMEM_SPEC],
        out_specs=(VMEM_SPEC, HBM_SPEC),
        scratch_shapes=[
            pltpu.VMEM((rows, lat), jnp.bfloat16),
            pltpu.SemaphoreType.DMA((4,)),
        ],
        compiler_params=pltpu.CompilerParams(vmem_limit_bytes=8 << 20),
    )(back, value_weight, part)


def on_device(
    latent_rows,
    pre_queries,
    pre_lengths,
    owner_map,
    context_cache,
    context_lengths,
    new_latent,
    dec_queries,
    key_weight,
    value_weight,
):
    steps, rows_local, heads, width = dec_queries.shape
    ranks = lax.axis_size("head")
    if heads % 16 or latent_rows.shape[0] % 128 or ranks % 2:
        return plain_on_device(
            latent_rows,
            pre_queries,
            pre_lengths,
            owner_map,
            context_cache,
            context_lengths,
            new_latent,
            dec_queries,
            key_weight,
            value_weight,
        )
    stay = lambda x: pltpu.with_memory_space_constraint(x, pltpu.HBM)
    back, part = serve_pallas(
        stay(pre_lengths),
        stay(owner_map),
        stay(context_lengths),
        stay(new_latent),
        stay(jnp.transpose(latent_rows)),
        stay(dec_queries.reshape(-1, width)),
        stay(key_weight),
        stay(value_weight),
        stay(jnp.transpose(pre_queries, (1, 2, 0))),
        stay(jnp.transpose(context_cache, (0, 2, 1))),
        ranks,
    )
    decode_out, prefill_out = project_pallas(back, value_weight, part, heads)
    return (prefill_out, decode_out.reshape(steps, rows_local, heads * 128))


def solution(mesh):
    placed = (
        P(("groups", "batch", "head"), None),
        P(("groups", "batch"), "head", None),
        P("groups", None),
        P("groups", None),
        P(("groups", "batch", "head"), None, None),
        P(("groups", "batch", "head")),
        P("groups", ("batch", "head"), None),
        P("groups", "batch", "head", None),
        P(None, "head"),
        P(None, "head"),
    )
    return jax.shard_map(
        on_device,
        mesh=mesh,
        in_specs=placed,
        out_specs=(P(("groups", "batch"), "head"), P("groups", "batch", "head")),
        check_vma=False,
    )
```
